16 devices in a mesh: tp: 2 (over z), cp: 8 (over y, x, core).
Axes of the slice: x: 2, y: 2, z: 2, core: 2. Of those that a mesh axis runs over, the one named last changes fastest.
Arguments:
- query: bfloat16 [16, 1024, 64, 128], P(None, 'cp', 'tp'), parts along dimension 2
- keys: bfloat16 [16, 1024, 8, 128], P(None, 'cp', 'tp'), parts along dimension 2
- values: bfloat16 [16, 1024, 8, 128], P(None, 'cp', 'tp'), parts along dimension 2
- positions: int32 [16, 1024], P(None, 'cp')
- grad_out: bfloat16 [16, 1024, 64, 128], P(None, 'cp', 'tp'), parts along dimension 2
Outputs:
- output 1: bfloat16 [16, 1024, 64, 128], P(None, 'cp', 'tp'), parts along dimension 2
- output 2: bfloat16 [16, 1024, 64, 128], P(None, 'cp', 'tp'), parts along dimension 2
- output 3: bfloat16 [16, 1024, 8, 128], P(None, 'cp', 'tp'), parts along dimension 2
- output 4: bfloat16 [16, 1024, 8, 128], P(None, 'cp', 'tp'), parts along dimension 2
There are 2 independent parts. The reference program is written for one: setup_inputs(seed, part) draws one part's arguments, and reference() takes and returns one part's arrays. A program takes and returns all parts, laid end to end along the dimension named above; an argument that names none is the same for every part.
All inputs are finite; a program needn't handle non-finite values.
Results may differ from the reference program's by a relative error of at most 0.00828705.
Values are sent between devices in bfloat16 or wider.
A program may use at most 1 GiB of HBM per device.

```python
import jax
import jax.numpy as jnp
from jax import lax

BATCH = 16
SEQ_LEN = 1024
CP_SIZE = 8
PART_HEADS = 32
PART_KV_HEADS = 4
HEAD_DIM = 128
ROPE_THETA = 1000000
QUERY_BLOCK = 128

GROUP_SIZE = PART_HEADS // PART_KV_HEADS
LOCAL_LEN = SEQ_LEN // CP_SIZE
HALF_LEN = LOCAL_LEN // 2
NUM_BLOCKS = SEQ_LEN // QUERY_BLOCK


def layout_index():
    stored = jnp.arange(SEQ_LEN, dtype=jnp.int32)
    device = stored // LOCAL_LEN
    within = stored % LOCAL_LEN
    piece_id = jnp.where(within < HALF_LEN, device, 2 * CP_SIZE - 1 - device)
    return piece_id * HALF_LEN + within % HALF_LEN


def draw_positions(pos_key):
    offset_key, gap_key = jax.random.split(pos_key)
    offsets = jax.random.randint(offset_key, (BATCH, 1), 0, SEQ_LEN, dtype=jnp.int32)
    gaps = jax.random.randint(gap_key, (BATCH, SEQ_LEN), 1, 3, dtype=jnp.int32)
    seq_pos = offsets + jnp.cumsum(gaps, axis=1) - gaps[:, :1]
    return jnp.take(seq_pos, layout_index(), axis=1)


def setup_inputs(seed: int = 0, part: int = 0) -> dict:
    base_key = jax.random.key(seed)
    shared_key, part_root = jax.random.split(base_key)
    part_key = jax.random.fold_in(part_root, part)
    key_query, key_keys, key_values, key_grad = jax.random.split(part_key, 4)
    q_shape = (BATCH, SEQ_LEN, PART_HEADS, HEAD_DIM)
    kv_shape = (BATCH, SEQ_LEN, PART_KV_HEADS, HEAD_DIM)
    return {
        'query': jax.random.normal(key_query, q_shape, jnp.float32).astype(jnp.bfloat16),
        'keys': jax.random.normal(key_keys, kv_shape, jnp.float32).astype(jnp.bfloat16),
        'values': jax.random.normal(key_values, kv_shape, jnp.float32).astype(jnp.bfloat16),
        'positions': draw_positions(shared_key),
        'grad_out': jax.random.normal(key_grad, q_shape, jnp.float32).astype(jnp.bfloat16),
    }


def rotary(tensor, positions, angle_sign):
    half_dim = HEAD_DIM // 2
    freq_expo = jnp.arange(half_dim, dtype=jnp.float32) * (2.0 / HEAD_DIM)
    inv_freq = 1.0 / (ROPE_THETA ** freq_expo)
    angles = positions.astype(jnp.float32)[:, :, None] * inv_freq
    cosine = jnp.cos(angles)[:, :, None, :]
    sine_val = angle_sign * jnp.sin(angles)[:, :, None, :]
    pairs = tensor.astype(jnp.float32).reshape(tensor.shape[:-1] + (half_dim, 2))
    even_part = pairs[..., 0]
    odd_part = pairs[..., 1]
    new_even = even_part * cosine - odd_part * sine_val
    new_odd = even_part * sine_val + odd_part * cosine
    return jnp.stack([new_even, new_odd], axis=-1).reshape(tensor.shape)


def reference(query, keys, values, positions, grad_out):
    score_scale = HEAD_DIM ** -0.5
    q_rot = rotary(query, positions, 1.0).astype(jnp.bfloat16)
    k_rot = rotary(keys, positions, 1.0).astype(jnp.bfloat16)

    def by_group(tensor):
        grouped = tensor.reshape(BATCH, NUM_BLOCKS, QUERY_BLOCK, PART_KV_HEADS, GROUP_SIZE, HEAD_DIM)
        grouped = grouped.transpose(0, 3, 1, 2, 4, 5)
        return grouped.reshape(BATCH * PART_KV_HEADS, NUM_BLOCKS, QUERY_BLOCK, GROUP_SIZE, HEAD_DIM)

    def by_kv(tensor):
        return tensor.transpose(0, 2, 1, 3).reshape(BATCH * PART_KV_HEADS, SEQ_LEN, HEAD_DIM)

    pos_rows = jnp.repeat(positions, PART_KV_HEADS, axis=0)

    def one_group(operands):
        q_blocks, k_group, v_group, g_blocks, pos_group = operands
        k_wide = k_group.astype(jnp.float32)
        v_wide = v_group.astype(jnp.float32)
        qpos_blocks = pos_group.reshape(NUM_BLOCKS, QUERY_BLOCK)

        def block_step(acc_pair, blk_inputs):
            dk_acc, dv_acc = acc_pair
            q_blk, g_blk, q_pos = blk_inputs
            q_wide = q_blk.astype(jnp.float32)
            g_wide = g_blk.astype(jnp.float32)
            scores = jnp.einsum('qgd,kd->gqk', q_wide, k_wide) * score_scale
            visible = pos_group[None, :] <= q_pos[:, None]
            scores = jnp.where(visible[None], scores, -jnp.inf)
            weights = jax.nn.softmax(scores, axis=-1)
            out_blk = jnp.einsum('gqk,kd->qgd', weights, v_wide)
            grad_weights = jnp.einsum('qgd,kd->gqk', g_wide, v_wide)
            row_delta = jnp.sum(weights * grad_weights, axis=-1, keepdims=True)
            grad_scores = weights * (grad_weights - row_delta) * score_scale
            dq_blk = jnp.einsum('gqk,kd->qgd', grad_scores, k_wide)
            dk_acc = dk_acc + jnp.einsum('gqk,qgd->kd', grad_scores, q_wide)
            dv_acc = dv_acc + jnp.einsum('gqk,qgd->kd', weights, g_wide)
            return (dk_acc, dv_acc), (out_blk, dq_blk)

        zero_kv = jnp.zeros((SEQ_LEN, HEAD_DIM), jnp.float32)
        sums, per_block = lax.scan(block_step, (zero_kv, zero_kv), (q_blocks, g_blocks, qpos_blocks))
        return per_block[0], per_block[1], sums[0], sums[1]

    out_all, dq_all, dk_all, dv_all = lax.map(
        one_group, (by_group(q_rot), by_kv(k_rot), by_kv(values), by_group(grad_out), pos_rows))

    def from_group(tensor):
        grouped = tensor.reshape(BATCH, PART_KV_HEADS, NUM_BLOCKS, QUERY_BLOCK, GROUP_SIZE, HEAD_DIM)
        return grouped.transpose(0, 2, 3, 1, 4, 5).reshape(BATCH, SEQ_LEN, PART_HEADS, HEAD_DIM)

    def from_kv(tensor):
        return tensor.reshape(BATCH, PART_KV_HEADS, SEQ_LEN, HEAD_DIM).transpose(0, 2, 1, 3)

    attn_out = from_group(out_all).astype(jnp.bfloat16)
    grad_query = rotary(from_group(dq_all), positions, -1.0).astype(jnp.bfloat16)
    grad_keys = rotary(from_kv(dk_all), positions, -1.0).astype(jnp.bfloat16)
    grad_values = from_kv(dv_all).astype(jnp.bfloat16)
    return (attn_out, grad_query, grad_keys, grad_values)
```

```python
import functools

import jax
import jax.numpy as jnp
from jax import lax
from jax.experimental import pallas as pl
from jax.experimental.pallas import tpu as pltpu
from jax.sharding import PartitionSpec as P

ROPE_THETA = 1000000.0
LOG2E = 1.4426950408889634
PIECE = 64
KEY_BLOCK = 256
N_CHUNKS = 4


def rope_tables(positions, head_dim):
    half_dim = head_dim // 2
    freq_expo = jnp.arange(half_dim, dtype=jnp.float32) * (2.0 / head_dim)
    inv_freq = 1.0 / (ROPE_THETA ** freq_expo)
    angles = positions.astype(jnp.float32)[:, :, None] * inv_freq
    return jnp.cos(angles), jnp.sin(angles)


def rotary(tensor, cosine, sine_val):
    cosine = cosine[:, :, None, :]
    sine_val = sine_val[:, :, None, :]
    pairs = tensor.astype(jnp.float32).reshape(tensor.shape[:-1] + (tensor.shape[-1] // 2, 2))
    even_part = pairs[..., 0]
    odd_part = pairs[..., 1]
    new_even = even_part * cosine - odd_part * sine_val
    new_odd = even_part * sine_val + odd_part * cosine
    return jnp.stack([new_even, new_odd], axis=-1).reshape(tensor.shape)


def dot_nn(a, b):
    return jnp.dot(a, b, preferred_element_type=jnp.float32)


def dot_nt(a, b):
    return lax.dot_general(a, b, (((1,), (1,)), ((), ())), preferred_element_type=jnp.float32)


def swap_pairs(x):
    lane = lax.broadcasted_iota(jnp.int32, x.shape, 1)
    return jnp.where(lane % 2 == 0, pltpu.roll(x, x.shape[1] - 1, axis=1), pltpu.roll(x, 1, axis=1))


def unit_kernel(n_dev, rows, idx_ref, q_ref, g_ref, cos_ref, sin_ref, kv_ref, o_in, dq_in,
                o_ref, dq_ref, dkv_ref,
                cosb, sinb, qr, gs, ks, vs, kt, vt, dk, dv, s_ref, o_t, dq_t):
    del o_in, dq_in
    tokens, group, dim = q_ref.shape[1:]
    total = tokens * group
    half = dim // 2
    scale = dim ** -0.5
    c1 = scale * LOG2E
    me = idx_ref[0]
    n_pieces = 2 * n_dev
    per_block = KEY_BLOCK // PIECE

    @pl.when(pl.program_id(1) == 0)
    def _():
        cosb[...] = jnp.broadcast_to(cos_ref[0][:, None, :], cosb.shape)
        sinb[...] = jnp.broadcast_to(sin_ref[0][:, None, :], sinb.shape)

    cos_rows = cosb[...].reshape(total, dim)
    sin_rows = sinb[...].reshape(total, dim)
    x = q_ref[0].astype(jnp.float32).reshape(total, dim)
    qr[...] = (x * cos_rows + swap_pairs(x) * sin_rows).astype(jnp.bfloat16)
    gs[...] = g_ref[0].astype(jnp.float32).reshape(total, dim).astype(jnp.bfloat16)

    for p in range(n_pieces):
        d, hf = min(p, n_pieces - 1 - p), int(p >= n_dev)
        ks[p * PIECE:(p + 1) * PIECE, :] = kv_ref[d, hf, 0, 0, 0]
        vs[p * PIECE:(p + 1) * PIECE, :] = kv_ref[d, hf, 0, 0, 1]
    eye = (lax.broadcasted_iota(jnp.int32, (dim, dim), 0) ==
           lax.broadcasted_iota(jnp.int32, (dim, dim), 1)).astype(jnp.float32).astype(jnp.bfloat16)
    n_blocks = n_pieces // per_block
    for j in range(n_blocks):
        kt[j] = dot_nt(eye, ks[j * KEY_BLOCK:(j + 1) * KEY_BLOCK, :]).astype(jnp.bfloat16)
        vt[j] = dot_nt(eye, vs[j * KEY_BLOCK:(j + 1) * KEY_BLOCK, :]).astype(jnp.bfloat16)
    dk[...] = jnp.zeros_like(dk)
    dv[...] = jnp.zeros_like(dv)

    for part in range(2):
        piece = me if part == 0 else n_pieces - 1 - me
        n_full = piece // per_block
        base = part * rows
        q_blk = qr[base:base + rows, :]
        g_blk = gs[base:base + rows, :]

        def block_ds(j):
            return pl.ds(pl.multiple_of(j * KEY_BLOCK, KEY_BLOCK), KEY_BLOCK)

        def fold_max(s):
            return jnp.max(s.reshape(KEY_BLOCK // 8, 8, rows), axis=0)

        def score_step(j, m8):
            s = dot_nt(ks[block_ds(j), :], qr[base:base + rows, :])
            s_ref[j] = s
            return jnp.maximum(m8, fold_max(s))

        m8 = lax.fori_loop(0, n_full, score_step, jnp.full((8, rows), -jnp.inf, jnp.float32))
        s = dot_nt(ks[block_ds(n_full), :], q_blk)
        key_tok = lax.broadcasted_iota(jnp.int32, s.shape, 0) + (n_full * KEY_BLOCK - piece * PIECE)
        q_tok = lax.broadcasted_iota(jnp.int32, s.shape, 1) // group
        s = jnp.where(key_tok <= q_tok, s, -jnp.inf)
        s_ref[n_full] = s
        m8 = jnp.maximum(m8, fold_max(s))
        row_max = jnp.max(m8, axis=0, keepdims=True) * c1

        o_t[...] = jnp.zeros_like(o_t)

        def out_step(j, l8):
            p = jnp.exp2(s_ref[j] * c1 - row_max)
            o_t[...] += dot_nn(vt[j], p.astype(jnp.bfloat16))
            return l8 + jnp.sum(p.reshape(KEY_BLOCK // 8, 8, rows), axis=0)

        l8 = lax.fori_loop(0, n_full + 1, out_step, jnp.zeros((8, rows), jnp.float32))
        row_sum = jnp.sum(l8, axis=0, keepdims=True)
        out_t = o_t[...] / row_sum
        g_t = dot_nt(eye, g_blk)
        delta = jnp.sum(g_t * out_t, axis=0, keepdims=True)
        o_ref[0, part * PIECE:(part + 1) * PIECE] = jnp.transpose(out_t).reshape(PIECE, group, dim).astype(jnp.bfloat16)
        log_norm = row_max + jnp.log2(row_sum)

        dq_t[...] = jnp.zeros_like(dq_t)

        def grad_step(j, carry):
            ds_j = block_ds(j)
            p = jnp.exp2(s_ref[j] * c1 - log_norm)
            dp = dot_nt(vs[ds_j, :], gs[base:base + rows, :])
            ds = (p * (dp - delta)).astype(jnp.bfloat16)
            dv[ds_j, :] += dot_nn(p.astype(jnp.bfloat16), gs[base:base + rows, :])
            dk[ds_j, :] += dot_nn(ds, qr[base:base + rows, :])
            dq_t[...] += dot_nn(kt[j], ds)
            return carry

        lax.fori_loop(0, n_full + 1, grad_step, 0)
        dq = jnp.transpose(dq_t[...]) * scale
        cs = cosb[part * PIECE:(part + 1) * PIECE].reshape(rows, dim)
        sn = sinb[part * PIECE:(part + 1) * PIECE].reshape(rows, dim)
        dq = dq * cs - swap_pairs(dq) * sn
        dq_ref[0, part * PIECE:(part + 1) * PIECE] = dq.reshape(PIECE, group, dim).astype(jnp.bfloat16)

    for p in range(n_pieces):
        d, hf = min(p, n_pieces - 1 - p), int(p >= n_dev)
        dkv_ref[d, hf, 0, 0, 0] = dk[p * PIECE:(p + 1) * PIECE, :] * scale
        dkv_ref[d, hf, 0, 0, 1] = dv[p * PIECE:(p + 1) * PIECE, :]


def attend(idx, query, grad_out, cos_l, sin_l, kv, o_buf, dq_buf, first_batch, n_batch, n_dev):
    batch, length, n_heads, dim = query.shape
    n_kv = kv.shape[3]
    group = n_heads // n_kv
    rows = PIECE * group
    n_keys = n_dev * length
    n_blocks = n_keys // KEY_BLOCK
    head_block = pl.BlockSpec((1, length, group, dim), lambda b, h, idx: (first_batch + b, 0, h, 0))
    table_block = pl.BlockSpec((1, length, dim), lambda b, h, idx: (first_batch + b, 0, 0))
    kv_block = pl.BlockSpec((n_dev, 2, 1, 1, 2, PIECE, dim), lambda b, h, idx: (0, 0, b, h, 0, 0, 0))
    any_block = pl.BlockSpec(memory_space=pl.ANY)
    aliased = o_buf is not None
    if not aliased:
        o_buf = dq_buf = jnp.zeros((8, 128), jnp.bfloat16)
    n_elems = n_batch * n_kv * 5 * KEY_BLOCK * rows
    return pl.pallas_call(
        functools.partial(unit_kernel, n_dev, rows),
        name=f'attend_{first_batch}',
        grid_spec=pltpu.PrefetchScalarGridSpec(
            num_scalar_prefetch=1,
            grid=(n_batch, n_kv),
            in_specs=[head_block, head_block, table_block, table_block, kv_block, any_block, any_block],
            out_specs=[head_block, head_block, kv_block],
            scratch_shapes=[
                pltpu.VMEM((length, group, dim), jnp.float32),
                pltpu.VMEM((length, group, dim), jnp.float32),
                pltpu.VMEM((2 * rows, dim), jnp.bfloat16),
                pltpu.VMEM((2 * rows, dim), jnp.bfloat16),
                pltpu.VMEM((n_keys, dim), jnp.bfloat16),
                pltpu.VMEM((n_keys, dim), jnp.bfloat16),
                pltpu.VMEM((n_blocks, dim, KEY_BLOCK), jnp.bfloat16),
                pltpu.VMEM((n_blocks, dim, KEY_BLOCK), jnp.bfloat16),
                pltpu.VMEM((n_keys, dim), jnp.float32),
                pltpu.VMEM((n_keys, dim), jnp.float32),
                pltpu.VMEM((n_blocks, KEY_BLOCK, rows), jnp.float32),
                pltpu.VMEM((dim, rows), jnp.float32),
                pltpu.VMEM((dim, rows), jnp.float32),
            ]),
        out_shape=[
            jax.ShapeDtypeStruct(query.shape, jnp.bfloat16),
            jax.ShapeDtypeStruct(query.shape, jnp.bfloat16),
            jax.ShapeDtypeStruct(kv.shape, jnp.float32),
        ],
        input_output_aliases={6: 0, 7: 1} if aliased else {},
        cost_estimate=pl.CostEstimate(
            flops=12 * n_elems * dim, transcendentals=2 * n_elems,
            bytes_accessed=n_batch * (query.size // batch) * 8 + kv.size * 6),
        compiler_params=pltpu.CompilerParams(
            dimension_semantics=('arbitrary', 'arbitrary'), vmem_limit_bytes=48 * 1024 * 1024),
    )(idx, query, grad_out, cos_l, sin_l, kv, o_buf, dq_buf)


def solution(mesh):
    n_dev = mesh.shape['cp']
    head_spec = P(None, 'cp', 'tp', None)
    pos_spec = P(None, 'cp')

    def local_step(query, keys, values, positions, grad_out):
        batch, length, n_heads, dim = query.shape
        n_kv = keys.shape[2]
        cosine, sine_val = rope_tables(positions, dim)
        k_rot = rotary(keys, cosine, sine_val).astype(jnp.bfloat16)

        def by_piece(tensor):
            return tensor.reshape(batch, 2, PIECE, n_kv, dim).transpose(1, 0, 3, 2, 4)

        kv_own = jnp.stack([by_piece(k_rot), by_piece(values)], axis=3)
        cos_l = jnp.repeat(cosine, 2, axis=-1)
        sin_l = jnp.stack([-sine_val, sine_val], axis=-1).reshape(batch, length, dim)
        idx = lax.axis_index('cp').astype(jnp.int32).reshape(1)

        n_batch = batch // N_CHUNKS
        gathered = [lax.all_gather(kv_own[:, c * n_batch:(c + 1) * n_batch], 'cp') for c in range(N_CHUNKS)]
        o_buf = dq_buf = None
        sums = []
        for c in range(N_CHUNKS):
            o_buf, dq_buf, dkv = attend(idx, query, grad_out, cos_l, sin_l, gathered[c], o_buf, dq_buf,
                                        c * n_batch, n_batch, n_dev)
            sums.append(lax.psum_scatter(dkv, 'cp', scatter_dimension=0, tiled=False))
        dkv_sum = jnp.concatenate(sums, axis=1)

        def from_piece(tensor):
            return tensor.transpose(1, 0, 3, 2, 4).reshape(batch, length, n_kv, dim)

        grad_keys = rotary(from_piece(dkv_sum[:, :, :, 0]), cosine, -sine_val).astype(jnp.bfloat16)
        grad_values = from_piece(dkv_sum[:, :, :, 1]).astype(jnp.bfloat16)
        return o_buf, dq_buf, grad_keys, grad_values

    return jax.shard_map(local_step, mesh=mesh,
                         in_specs=(head_spec, head_spec, head_spec, pos_spec, head_spec),
                         out_specs=(head_spec, head_spec, head_spec, head_spec), check_vma=False)
```

```python
import functools

import jax
import jax.numpy as jnp
from jax import lax
from jax.experimental import pallas as pl
from jax.experimental.pallas import tpu as pltpu
from jax.sharding import PartitionSpec as P

ROPE_THETA = 1000000.0
LOG2E = 1.4426950408889634
DIM = 128
GROUP = 8
HEADS = 4
PIECE = 64
PAIR = 128
N_PAIRS = 8
BATCHES = 8
UNITS = BATCHES * HEADS
KEY_BLOCK = 512
MESH_ID = pl.DeviceIdType.MESH

X_STEP, Y_STEP = 1, 2
FIRST_HOP = [(0, 0, X_STEP), (0, 0, Y_STEP), (1, 1, X_STEP), (1, 1, Y_STEP), (2, 2, X_STEP), (2, 2, Y_STEP),
             (3, 3, X_STEP), (3, 3, Y_STEP), (4, 3, X_STEP), (4, 3, Y_STEP), (5, 2, Y_STEP), (5, 2, X_STEP),
             (6, 1, X_STEP)]
RELAY_HOP = [(0, 2, X_STEP), (1, 3, X_STEP), (2, 3, Y_STEP), (3, 2, Y_STEP), (4, 1, X_STEP), (5, 3, Y_STEP)]
SUM_LEAF = [(0, 3, X_STEP), (0, 1, X_STEP), (1, 2, Y_STEP), (1, 3, Y_STEP), (2, 1, Y_STEP), (2, 0, Y_STEP),
            (3, 0, Y_STEP), (3, 1, Y_STEP), (4, 0, X_STEP), (4, 2, X_STEP), (5, 1, X_STEP), (6, 0, X_STEP)]
SUM_RELAY = [(0, 2, Y_STEP), (1, 0, X_STEP), (2, 3, X_STEP), (3, 2, X_STEP), (4, 1, Y_STEP), (5, 0, Y_STEP)]

AG_LEAD = 8
RELAY_LEAD = 4
AG_RING = 4
SUM_LAG = 3
OWN_LAG = 6
PART_RING = OWN_LAG + 2


def owner(pair):
    return pair if pair < 4 else 7 - pair


def inbox(chip):
    found = []
    for pair, src, step in SUM_LEAF + SUM_RELAY:
        if src ^ step == chip:
            found.append((pair, src))
    return found


N_INBOX = max(len(inbox(c)) for c in range(4))


def rope_tables(positions, head_dim):
    half_dim = head_dim // 2
    freq_expo = jnp.arange(half_dim, dtype=jnp.float32) * (2.0 / head_dim)
    inv_freq = 1.0 / (ROPE_THETA ** freq_expo)
    angles = positions.astype(jnp.float32)[:, :, None] * inv_freq
    cosine, sine_val = jnp.cos(angles), jnp.sin(angles)
    cos_l = jnp.repeat(cosine, 2, axis=-1)
    sin_l = jnp.stack([-sine_val, sine_val], axis=-1).reshape(cos_l.shape)
    return jnp.stack([cos_l, sin_l], axis=1)


def dot_nn(a, b):
    return jnp.dot(a, b, preferred_element_type=jnp.float32)


def dot_nt(a, b):
    return lax.dot_general(a, b, (((1,), (1,)), ((), ())), preferred_element_type=jnp.float32)


def iota(shape, axis):
    return lax.broadcasted_iota(jnp.int32, shape, axis)


def identity():
    return (iota((DIM, DIM), 0) == iota((DIM, DIM), 1)).astype(jnp.float32).astype(jnp.bfloat16)


def swap_pairs(x):
    return jnp.where(iota(x.shape, 1) % 2 == 0, pltpu.roll(x, DIM - 1, axis=1), pltpu.roll(x, 1, axis=1))


def prep_kernel(info_ref, k_mine, k_sib, v_mine, v_sib, tab_mine, tab_sib, kv_out, send_out):
    del info_ref

    def put(k_ref, v_ref, tab, write):
        for h in range(HEADS):
            x = k_ref[0, h].astype(jnp.float32)
            write(h, (x * tab[0, 0] + swap_pairs(x) * tab[0, 1]).astype(jnp.bfloat16), v_ref[0, h])

    def write_mine(h, k_rot, val):
        kv_out[0, h, 0] = k_rot
        kv_out[0, h, 1] = val

    def write_sib(h, k_rot, val):
        send_out[0, 0, h, 0] = k_rot
        send_out[0, 0, h, 1] = val

    put(k_mine, v_mine, tab_mine, write_mine)
    put(k_sib, v_sib, tab_sib, write_sib)


def prepare(info, k_t, v_t, tab):
    mine = lambda b, half, info: BATCHES * info[0] + b
    sib = lambda b, half, info: BATCHES * (1 - info[0]) + b
    kv_spec = lambda row: pl.BlockSpec((1, HEADS, PIECE, DIM), lambda b, half, info: (row(b, half, info), 0, half, 0))
    tab_spec = lambda row: pl.BlockSpec((1, 2, PIECE, DIM), lambda b, half, info: (row(b, half, info), 0, half, 0))
    return pl.pallas_call(
        prep_kernel, name='prepare',
        grid_spec=pltpu.PrefetchScalarGridSpec(
            num_scalar_prefetch=1, grid=(BATCHES, 2),
            in_specs=[kv_spec(mine), kv_spec(sib), kv_spec(mine), kv_spec(sib), tab_spec(mine), tab_spec(sib)],
            out_specs=[
                pl.BlockSpec((1, HEADS, 2, PIECE, DIM), lambda b, half, info: (b, 0, 0, info[1 + half], 0)),
                pl.BlockSpec((1, 1, HEADS, 2, PIECE, DIM), lambda b, half, info: (b, half, 0, 0, 0, 0))]),
        out_shape=[jax.ShapeDtypeStruct((BATCHES, HEADS, 2, N_PAIRS * PAIR, DIM), jnp.bfloat16),
                   jax.ShapeDtypeStruct((BATCHES, 2, HEADS, 2, PIECE, DIM), jnp.bfloat16)],
    )(info, k_t, k_t, v_t, v_t, tab, tab)


def rows_steps(n_keys, tok, seg, q_v, g_v, tab, kv, kt, vt, part, o_v, dq_v, s_ref):
    core, start, place = seg
    rows = tok * GROUP
    scale = DIM ** -0.5
    c1 = scale * LOG2E
    toks = pl.ds(start, tok)

    def table(k):
        return jnp.broadcast_to(tab[k, core, toks, :][:, None, :], (tok, GROUP, DIM)).reshape(rows, DIM)

    x = q_v[core, toks].astype(jnp.float32).reshape(rows, DIM)
    qr = (x * table(0) + swap_pairs(x) * table(1)).astype(jnp.bfloat16)
    g = g_v[core, toks].astype(jnp.float32).reshape(rows, DIM).astype(jnp.bfloat16)
    blocks = [(a, min(KEY_BLOCK, n_keys - a)) for a in range(0, n_keys, KEY_BLOCK)]
    m8 = None
    for a, n in blocks:
        s = dot_nt(kv[0, a:a + n, :], qr) * c1
        if a + n == n_keys:
            last = s[n - PAIR:, :]
            q_tok = iota(last.shape, 1) // GROUP + place
            last = jnp.where(iota(last.shape, 0) <= q_tok, last, -jnp.inf)
            s = last if n == PAIR else jnp.concatenate([s[:n - PAIR, :], last], axis=0)
        s_ref[a:a + n, :] = s
        f = jnp.max(s.reshape(n // 8, 8, rows), axis=0)
        m8 = f if m8 is None else jnp.maximum(m8, f)
        yield
    row_max = jnp.max(m8, axis=0, keepdims=True)
    l8 = None
    o_t = None
    for a, n in blocks:
        p = jnp.exp2(s_ref[a:a + n, :] - row_max)
        s_ref[a:a + n, :] = p
        f = jnp.sum(p.reshape(n // 8, 8, rows), axis=0)
        l8 = f if l8 is None else l8 + f
        d = dot_nn(vt[:, a:a + n], p.astype(jnp.bfloat16))
        o_t = d if o_t is None else o_t + d
        yield
    inv = 1.0 / jnp.sum(l8, axis=0, keepdims=True)
    out_t = o_t * inv
    o_v[core, toks] = jnp.transpose(out_t).reshape(tok, GROUP, DIM).astype(jnp.bfloat16)
    delta = jnp.sum(dot_nt(identity(), g) * out_t, axis=0, keepdims=True)
    yield
    dq_t = None
    for a, n in blocks:
        p = s_ref[a:a + n, :] * inv
        ds = (p * (dot_nt(kv[1, a:a + n, :], g) - delta)).astype(jnp.bfloat16)
        part[1, a:a + n, :] += dot_nn(p.astype(jnp.bfloat16), g)
        part[0, a:a + n, :] += dot_nn(ds, qr)
        d = dot_nn(kt[:, a:a + n], ds)
        dq_t = d if dq_t is None else dq_t + d
        yield
    dq = jnp.transpose(dq_t) * scale
    dq = dq * table(0) - swap_pairs(dq) * table(1)
    dq_v[core, toks] = dq.reshape(tok, GROUP, DIM).astype(jnp.bfloat16)


def interleave(gens, lag):
    live, waiting, count = [], list(gens), 0
    while live or waiting:
        if waiting and (not live or count >= lag):
            live.append(waiting.pop(0))
            count = 0
        for gen in list(live):
            if next(gen, 'end') == 'end':
                live.remove(gen)
        count += 1


def unit_compute(c, q_v, g_v, tab, kv, o_v, dq_v, part, kt, vt, s_a, s_b, s_e):
    n_late, n_early = (N_PAIRS - c) * PAIR, (c + 1) * PAIR
    eye = identity()
    for a in range(0, n_late, 256):
        n = min(256, n_late - a)
        kt[:, a:a + n] = dot_nt(eye, kv[0, a:a + n, :]).astype(jnp.bfloat16)
        vt[:, a:a + n] = dot_nt(eye, kv[1, a:a + n, :]).astype(jnp.bfloat16)
    part[:, :n_late, :] = jnp.zeros((2, n_late, DIM), jnp.float32)
    refs = (q_v, g_v, tab, kv, kt, vt, part, o_v, dq_v)

    def step(i, carry):
        late = [rows_steps(n_late, 32, (1 - i, PIECE + 32 * k, i * PIECE + 32 * k), *refs, s)
                for k, s in ((0, s_a), (1, s_b))]
        early = rows_steps(n_early, PIECE, (i, 0, i * PIECE), *refs, s_e)
        interleave(late + [early], 2 * pl.cdiv(n_late, KEY_BLOCK) + 1)
        return carry

    lax.fori_loop(0, 2, step, 0)


def remote(src, dst, send_sem, recv_sem, device):
    return pltpu.make_async_remote_copy(src_ref=src, dst_ref=dst, send_sem=send_sem, recv_sem=recv_sem,
                                        device_id={'cp': device}, device_id_type=MESH_ID)


def chip_program(c, core, q_hbm, g_hbm, kv_send, tab_hbm, o_hbm, dq_hbm, gkv_hbm, kv_hbm, qs_hbm, gs_hbm,
                 q_v, g_v, o_v, dq_v, kv_v, tab_v, part, recv, fin_v, kt, vt, s_a, s_b, s_e,
                 kvx_s, kvx_r, tab_s, tab_r, qx_s, qx_r, gx_s, gx_r, ag_s, ag_r, sum_s, sum_r,
                 load_s, out_s, out_r, fin_s, fin_r):
    n_late = (N_PAIRS - c) * PAIR
    sib = 2 * c + 1 - core
    nbr = {step: 2 * (c ^ step) + core for step in (X_STEP, Y_STEP)}
    mine, other = BATCHES * core, BATCHES * (1 - core)
    first_hops = [(p, step) for p, src, step in FIRST_HOP if src == c]
    relay_hops = [(p, step) for p, src, step in RELAY_HOP if src == c]
    leaves = [(p, step) for p, src, step in SUM_LEAF if src == c]
    relays = [(p, step) for p, src, step in SUM_RELAY if src == c]
    needed = [p for p in range(N_PAIRS - c) if owner(p) != c]
    sib_pieces = (2 * c + 1 - core, 15 - 2 * c - (1 - core))

    def split(u):
        return u // HEADS, u % HEADS

    def pair_rows(p):
        return pl.ds(p * PAIR, PAIR)

    def kvx(b, half):
        rows = pl.ds(pl.multiple_of((2 * c + core if half == 0 else 15 - 2 * c - core) * PIECE, PIECE), PIECE)
        return remote(kv_send.at[b, half], kv_hbm.at[b, :, :, rows, :], kvx_s.at[b, half], kvx_r.at[b, half], sib)

    def kvx_in(b, half):
        rows = pl.ds(pl.multiple_of(sib_pieces[half] * PIECE, PIECE), PIECE)
        dst = kv_hbm.at[b, :, :, rows, :]
        return remote(kv_send.at[b, half], dst, kvx_s.at[b, half], kvx_r.at[b, half], sib)

    def qx(b):
        return remote(q_hbm.at[other + b], qs_hbm.at[b], qx_s.at[b], qx_r.at[b], sib)

    def gx(b):
        return remote(g_hbm.at[other + b], gs_hbm.at[b], gx_s.at[b], gx_r.at[b], sib)

    def tab_in():
        return pltpu.make_async_copy(tab_hbm.at[pl.ds(mine, BATCHES)], tab_v.at[:, :, core], load_s.at[5, 0])

    def tab_out():
        return remote(tab_hbm.at[pl.ds(other, BATCHES)], tab_v.at[:, :, core], tab_s, tab_r, sib)

    def tab_arrive():
        return remote(tab_hbm.at[pl.ds(other, BATCHES)], tab_v.at[:, :, 1 - core], tab_s, tab_r, sib)

    def kv_copy(u, p, slot, step):
        b, h = split(u)
        ref = kv_hbm.at[b, h, :, pair_rows(p), :]
        return remote(ref, ref, ag_s.at[slot, u % AG_RING], ag_r.at[u, p], nbr[step])

    def send_kv(u, hops, base):
        @pl.when(u >= AG_RING)
        def _():
            for i, (p, step) in enumerate(hops):
                kv_copy(u - AG_RING, p, base + i, step).wait_send()

        for i, (p, step) in enumerate(hops):
            kv_copy(u, p, base + i, step).start()

    def first_hop(u):
        @pl.when(u % HEADS == 0)
        def _():
            for half in range(2):
                kvx_in(u // HEADS, half).wait_recv()

        send_kv(u, first_hops, 0)

    def relay_hop(u):
        for p, _ in relay_hops:
            kv_copy(u, p, 0, X_STEP).wait_recv()
        send_kv(u, relay_hops, len(first_hops))

    def loads(u):
        b, h = split(u)
        slot = u % 2
        late = pl.ds(0, n_late)
        return [
            pltpu.make_async_copy(q_hbm.at[mine + b, :, h], q_v.at[slot, core], load_s.at[0, slot]),
            pltpu.make_async_copy(g_hbm.at[mine + b, :, h], g_v.at[slot, core], load_s.at[1, slot]),
            pltpu.make_async_copy(qs_hbm.at[b, :, h], q_v.at[slot, 1 - core], load_s.at[2, slot]),
            pltpu.make_async_copy(gs_hbm.at[b, :, h], g_v.at[slot, 1 - core], load_s.at[3, slot]),
            pltpu.make_async_copy(kv_hbm.at[b, h, :, late, :], kv_v.at[slot, :, late, :], load_s.at[4, slot]),
        ]

    def start_loads(u):
        @pl.when(u % HEADS == 0)
        def _():
            qx(u // HEADS).wait_recv()
            gx(u // HEADS).wait_recv()

        for p in needed:
            if p not in [r for r, _ in relay_hops]:
                kv_copy(u, p, 0, X_STEP).wait_recv()
        for copy in loads(u):
            copy.start()

    def out_local(u):
        b, h = split(u)
        slot = u % 2
        return [pltpu.make_async_copy(o_v.at[slot, core], o_hbm.at[mine + b, :, h], out_s.at[0, slot]),
                pltpu.make_async_copy(dq_v.at[slot, core], dq_hbm.at[mine + b, :, h], out_s.at[1, slot])]

    def out_remote(u):
        b, h = split(u)
        slot = u % 2
        return [remote(o_v.at[slot, 1 - core], o_hbm.at[mine + b, :, h], out_s.at[2, slot], out_r.at[0, b], sib),
                remote(dq_v.at[slot, 1 - core], dq_hbm.at[mine + b, :, h], out_s.at[3, slot], out_r.at[1, b], sib)]

    def out_arrive(b):
        return [remote(q_hbm.at[other + b], o_hbm.at[other + b], out_s.at[2, 0], out_r.at[0, b], sib),
                remote(q_hbm.at[other + b], dq_hbm.at[other + b], out_s.at[3, 0], out_r.at[1, b], sib)]

    def wait_outs(u):
        for copy in out_local(u):
            copy.wait()
        for copy in out_remote(u):
            copy.wait_send()

    def sum_copy(u, p, i, step):
        dst = inbox(c ^ step).index((p, c))
        return remote(part.at[u % PART_RING, :, pair_rows(p), :], recv.at[u, dst],
                      sum_s.at[i, u % PART_RING], sum_r.at[u, dst], nbr[step])

    def sum_arrive(u, k):
        dst = recv.at[u, k]
        return remote(dst, dst, sum_s.at[0, 0], sum_r.at[u, k], nbr[X_STEP])

    def messages(p):
        return [k for k, (pair, _) in enumerate(inbox(c)) if pair == p]

    def wait_sums(u):
        for i, (p, step) in enumerate(leaves + relays):
            sum_copy(u, p, i, step).wait_send()

    def send_leaves(u):
        for i, (p, step) in enumerate(leaves):
            sum_copy(u, p, i, step).start()

    def add_relays(u):
        for p, _ in relays:
            for k in messages(p):
                sum_arrive(u, k).wait_recv()
                part[u % PART_RING, :, pair_rows(p), :] += recv[u, k]

    def send_relays(u):
        for i, (p, step) in enumerate(relays):
            sum_copy(u, p, len(leaves) + i, step).start()

    def fin_local(u):
        b, h = split(u)
        return pltpu.make_async_copy(fin_v.at[u % 2, core], gkv_hbm.at[mine + b, h], fin_s.at[0, u % 2])

    def fin_remote(u):
        b, h = split(u)
        return remote(fin_v.at[u % 2, 1 - core], gkv_hbm.at[mine + b, h], fin_s.at[1, u % 2], fin_r.at[b], sib)

    def fin_arrive(b):
        return remote(gkv_hbm.at[other + b], gkv_hbm.at[other + b], fin_s.at[1, 0], fin_r.at[b], sib)

    def wait_fin(u):
        fin_local(u).wait()
        fin_remote(u).wait_send()

    def finish(u):
        @pl.when(u >= 2)
        def _():
            wait_fin(u - 2)

        b, slot = u // HEADS, u % 2
        for late, p in ((0, c), (1, N_PAIRS - 1 - c)):
            total = part[u % PART_RING, :, pair_rows(p), :]
            for k in messages(p):
                sum_arrive(u, k).wait_recv()
                total = total + recv[u, k]
            for i in range(2):
                who = 1 - i if late else i
                toks = slice(late * PIECE, (late + 1) * PIECE)
                dk = total[0, i * PIECE:(i + 1) * PIECE] * (DIM ** -0.5)
                dk = dk * tab_v[b, 0, who, toks] - swap_pairs(dk) * tab_v[b, 1, who, toks]
                fin_v[slot, who, 0, toks] = dk.astype(jnp.bfloat16)
                fin_v[slot, who, 1, toks] = total[1, i * PIECE:(i + 1) * PIECE].astype(jnp.bfloat16)

    def send_fin(u):
        fin_local(u).start()
        fin_remote(u).start()

    for b in range(BATCHES):
        for half in range(2):
            kvx(b, half).start()
    tab_in().start()
    tab_out().start()

    def start_exchange(b, carry):
        qx(b).start()
        gx(b).start()
        return carry

    lax.fori_loop(0, BATCHES, start_exchange, 0)
    for u in range(AG_LEAD):
        first_hop(jnp.int32(u))
        if 1 <= u <= RELAY_LEAD:
            relay_hop(jnp.int32(u - 1))
    tab_in().wait()
    tab_arrive().wait_recv()
    start_loads(jnp.int32(0))

    def tick(t, carry):
        @pl.when(t + AG_LEAD < UNITS)
        def _():
            first_hop(t + AG_LEAD)

        @pl.when(t + RELAY_LEAD < UNITS)
        def _():
            relay_hop(t + RELAY_LEAD)

        @pl.when((t >= 1) & (t - 1 < UNITS))
        def _():
            send_leaves(t - 1)

        @pl.when((t >= 1 + SUM_LAG) & (t - 1 - SUM_LAG < UNITS))
        def _():
            add_relays(t - 1 - SUM_LAG)

        @pl.when((t >= 1 + OWN_LAG) & (t - 1 - OWN_LAG < UNITS))
        def _():
            finish(t - 1 - OWN_LAG)

        @pl.when((t >= 1 + SUM_LAG) & (t - 1 - SUM_LAG < UNITS))
        def _():
            send_relays(t - 1 - SUM_LAG)

        @pl.when((t >= 1 + OWN_LAG) & (t - 1 - OWN_LAG < UNITS))
        def _():
            send_fin(t - 1 - OWN_LAG)

        @pl.when(t < UNITS)
        def _():
            for copy in loads(t):
                copy.wait()

            @pl.when(t + 1 < UNITS)
            def _():
                start_loads(t + 1)

            @pl.when(t >= 2)
            def _():
                wait_outs(t - 2)

            @pl.when(t >= PART_RING)
            def _():
                wait_sums(t - PART_RING)

            slot = t % 2
            unit_compute(c, q_v.at[slot], g_v.at[slot], tab_v.at[t // HEADS], kv_v.at[slot], o_v.at[slot],
                         dq_v.at[slot], part.at[t % PART_RING], kt, vt, s_a, s_b, s_e)
            for copy in out_local(t) + out_remote(t):
                copy.start()

        return carry

    lax.fori_loop(0, UNITS + 1 + OWN_LAG, tick, 0)

    tab_out().wait_send()
    for u in range(UNITS - 2, UNITS):
        wait_outs(jnp.int32(u))
        wait_fin(jnp.int32(u))

    def drain_batch(b, carry):
        for half in range(2):
            kvx(b, half).wait_send()
        qx(b).wait_send()
        gx(b).wait_send()
        for copy in out_arrive(b):
            copy.wait_recv()
        fin_arrive(b).wait_recv()
        return carry

    lax.fori_loop(0, BATCHES, drain_batch, 0)

    def drain_sums(u, carry):
        wait_sums(u)
        return carry

    lax.fori_loop(UNITS - PART_RING, UNITS, drain_sums, 0)

    def drain_kv(u, carry):
        for i, (p, step) in enumerate(first_hops + relay_hops):
            kv_copy(u, p, i, step).wait_send()
        return carry

    lax.fori_loop(UNITS - AG_RING, UNITS, drain_kv, 0)


def attend_kernel(q_hbm, g_hbm, kv_in, kv_send, tab_hbm, o_hbm, dq_hbm, gkv_hbm, kv_hbm, qs_hbm, gs_hbm, *scratch):
    del kv_in
    me = lax.axis_index('cp')
    chip, core = me // 2, me % 2
    barrier = pltpu.get_barrier_semaphore()
    for c in range(4):
        @pl.when(chip == c)
        def _(c=c):
            for device in (2 * c + 1 - core, 2 * (c ^ X_STEP) + core, 2 * (c ^ Y_STEP) + core):
                pl.semaphore_signal(barrier, inc=1, device_id={'cp': device}, device_id_type=MESH_ID)
    pl.semaphore_wait(barrier, 3)
    for c in range(4):
        @pl.when(chip == c)
        def _(c=c):
            chip_program(c, core, q_hbm, g_hbm, kv_send, tab_hbm, o_hbm, dq_hbm, gkv_hbm, kv_hbm, qs_hbm, gs_hbm,
                         *scratch)


def attend(q5, g5, kv_buf, kv_send, tab):
    any_spec = pl.BlockSpec(memory_space=pl.ANY)
    head_shape = jax.ShapeDtypeStruct(q5.shape, jnp.bfloat16)
    half_shape = jax.ShapeDtypeStruct((BATCHES,) + q5.shape[1:], jnp.bfloat16)
    head_buf = pltpu.VMEM((2, 2, PAIR, GROUP, DIM), jnp.bfloat16)
    dma = pltpu.SemaphoreType.DMA
    return pl.pallas_call(
        attend_kernel, name='attend',
        in_specs=[any_spec] * 5,
        out_specs=[any_spec] * 6,
        out_shape=[head_shape, head_shape,
                   jax.ShapeDtypeStruct((2 * BATCHES, HEADS, 2, PAIR, DIM), jnp.bfloat16),
                   jax.ShapeDtypeStruct(kv_buf.shape, jnp.bfloat16), half_shape, half_shape],
        input_output_aliases={2: 3},
        scratch_shapes=[
            head_buf, head_buf, head_buf, head_buf,
            pltpu.VMEM((2, 2, N_PAIRS * PAIR, DIM), jnp.bfloat16),
            pltpu.VMEM((BATCHES, 2, 2, PAIR, DIM), jnp.float32),
            pltpu.VMEM((PART_RING, 2, N_PAIRS * PAIR, DIM), jnp.float32),
            pltpu.VMEM((UNITS, N_INBOX, 2, PAIR, DIM), jnp.float32),
            pltpu.VMEM((2, 2, 2, PAIR, DIM), jnp.bfloat16),
            pltpu.VMEM((DIM, N_PAIRS * PAIR), jnp.bfloat16),
            pltpu.VMEM((DIM, N_PAIRS * PAIR), jnp.bfloat16),
            pltpu.VMEM((N_PAIRS * PAIR, 32 * GROUP), jnp.float32),
            pltpu.VMEM((N_PAIRS * PAIR, 32 * GROUP), jnp.float32),
            pltpu.VMEM((4 * PAIR, PIECE * GROUP), jnp.float32),
            dma((BATCHES, 2)), dma((BATCHES, 2)), dma, dma,
            dma((BATCHES,)), dma((BATCHES,)), dma((BATCHES,)), dma((BATCHES,)),
            dma((7, AG_RING)), dma((UNITS, 7)), dma((6, PART_RING)), dma((UNITS, N_INBOX)),
            dma((6, 2)), dma((4, 2)), dma((2, BATCHES)), dma((2, 2)), dma((BATCHES,)),
        ],
        compiler_params=pltpu.CompilerParams(
            collective_id=0, has_side_effects=True, vmem_limit_bytes=60 * 1024 * 1024),
    )(q5, g5, kv_buf, kv_send, tab)


def solution(mesh):
    head_spec = P(None, 'cp', 'tp', None)
    pos_spec = P(None, 'cp')

    def local_step(query, keys, values, positions, grad_out):
        batch, length, n_heads, dim = query.shape
        me = lax.axis_index('cp').astype(jnp.int32)
        info = jnp.stack([me % 2, me, 15 - me])
        tab = rope_tables(positions, dim)
        kv_buf, kv_send = prepare(info, keys.transpose(0, 2, 1, 3), values.transpose(0, 2, 1, 3), tab)
        split_shape = (batch, length, HEADS, GROUP, dim)
        o5, dq5, gkv, _, _, _ = attend(query.reshape(split_shape), grad_out.reshape(split_shape), kv_buf, kv_send, tab)
        grads = gkv.transpose(2, 0, 3, 1, 4)
        return o5.reshape(query.shape), dq5.reshape(query.shape), grads[0], grads[1]

    return jax.shard_map(local_step, mesh=mesh,
                         in_specs=(head_spec, head_spec, head_spec, pos_spec, head_spec),
                         out_specs=(head_spec, head_spec, head_spec, head_spec), check_vma=False)
```

```python
import functools

import jax
import jax.numpy as jnp
from jax import lax
from jax.experimental import pallas as pl
from jax.experimental.pallas import tpu as pltpu
from jax.sharding import PartitionSpec as P

ROPE_THETA = 1000000.0
LOG2E = 1.4426950408889634
DIM = 128
GROUP = 8
HEADS = 4
PIECE = 64
PAIR = 128
N_PAIRS = 8
BATCHES = 8
UNITS = BATCHES * HEADS
KEY_BLOCK = 512
MESH_ID = pl.DeviceIdType.MESH

X_STEP, Y_STEP = 1, 2
FIRST_HOP = [(0, 0, X_STEP), (0, 0, Y_STEP), (1, 1, X_STEP), (1, 1, Y_STEP), (2, 2, X_STEP), (2, 2, Y_STEP),
             (3, 3, X_STEP), (3, 3, Y_STEP), (4, 3, X_STEP), (4, 3, Y_STEP), (5, 2, Y_STEP), (5, 2, X_STEP),
             (6, 1, X_STEP)]
RELAY_HOP = [(0, 2, X_STEP), (1, 3, X_STEP), (2, 3, Y_STEP), (3, 2, Y_STEP), (4, 1, X_STEP), (5, 3, Y_STEP)]
SUM_LEAF = [(0, 3, X_STEP), (0, 1, X_STEP), (1, 2, Y_STEP), (1, 3, Y_STEP), (2, 1, Y_STEP), (2, 0, Y_STEP),
            (3, 0, Y_STEP), (3, 1, Y_STEP), (4, 0, X_STEP), (4, 2, X_STEP), (5, 1, X_STEP), (6, 0, X_STEP)]
SUM_RELAY = [(0, 2, Y_STEP), (1, 0, X_STEP), (2, 3, X_STEP), (3, 2, X_STEP), (4, 1, Y_STEP), (5, 0, Y_STEP)]

EARLY_LEAD = 20
AG_LEAD = 8
RELAY_LEAD = 4
EARLY_HOP = [(0, 0, X_STEP), (0, 0, Y_STEP), (1, 1, Y_STEP)]
SUM_LAG = 3
OWN_LAG = 6
PART_RING = OWN_LAG + 2


def owner(pair):
    return pair if pair < 4 else 7 - pair


def inbox(chip):
    found = []
    for pair, src, step in SUM_LEAF + SUM_RELAY:
        if src ^ step == chip:
            found.append((pair, src))
    return found


N_INBOX = max(len(inbox(c)) for c in range(4))


def rope_tables(positions, head_dim):
    half_dim = head_dim // 2
    freq_expo = jnp.arange(half_dim, dtype=jnp.float32) * (2.0 / head_dim)
    inv_freq = 1.0 / (ROPE_THETA ** freq_expo)
    angles = positions.astype(jnp.float32)[:, :, None] * inv_freq
    cosine, sine_val = jnp.cos(angles), jnp.sin(angles)
    cos_l = jnp.repeat(cosine, 2, axis=-1)
    sin_l = jnp.stack([-sine_val, sine_val], axis=-1).reshape(cos_l.shape)
    return jnp.stack([cos_l, sin_l], axis=1)


def dot_nn(a, b):
    return jnp.dot(a, b, preferred_element_type=jnp.float32)


def dot_nt(a, b):
    return lax.dot_general(a, b, (((1,), (1,)), ((), ())), preferred_element_type=jnp.float32)


def iota(shape, axis):
    return lax.broadcasted_iota(jnp.int32, shape, axis)


def identity():
    return (iota((DIM, DIM), 0) == iota((DIM, DIM), 1)).astype(jnp.float32).astype(jnp.bfloat16)


def swap_pairs(x):
    return jnp.where(iota(x.shape, 1) % 2 == 0, pltpu.roll(x, DIM - 1, axis=1), pltpu.roll(x, 1, axis=1))


def rows_steps(n_keys, tok, seg, q_v, g_v, tab, kv, kt, vt, part, o_v, dq_v, s_ref):
    core, start, place = seg
    rows = tok * GROUP
    scale = DIM ** -0.5
    c1 = scale * LOG2E
    toks = pl.ds(start, tok)

    def table(k):
        return jnp.broadcast_to(tab[k, core, toks, :][:, None, :], (tok, GROUP, DIM)).reshape(rows, DIM)

    x = q_v[core, toks].astype(jnp.float32).reshape(rows, DIM)
    qr = (x * table(0) + swap_pairs(x) * table(1)).astype(jnp.bfloat16)
    g = g_v[core, toks].astype(jnp.float32).reshape(rows, DIM).astype(jnp.bfloat16)
    blocks = [(a, min(KEY_BLOCK, n_keys - a)) for a in range(0, n_keys, KEY_BLOCK)]
    m8 = None
    for a, n in blocks:
        s = dot_nt(kv[0, a:a + n, :], qr) * c1
        if a + n == n_keys:
            last = s[n - PAIR:, :]
            q_tok = iota(last.shape, 1) // GROUP + place
            last = jnp.where(iota(last.shape, 0) <= q_tok, last, -jnp.inf)
            s = last if n == PAIR else jnp.concatenate([s[:n - PAIR, :], last], axis=0)
        s_ref[a:a + n, :] = s
        f = jnp.max(s.reshape(n // 8, 8, rows), axis=0)
        m8 = f if m8 is None else jnp.maximum(m8, f)
        yield
    row_max = jnp.max(m8, axis=0, keepdims=True)
    l8 = None
    o_t = None
    for a, n in blocks:
        p = jnp.exp2(s_ref[a:a + n, :] - row_max)
        s_ref[a:a + n, :] = p
        f = jnp.sum(p.reshape(n // 8, 8, rows), axis=0)
        l8 = f if l8 is None else l8 + f
        d = dot_nn(vt[:, a:a + n], p.astype(jnp.bfloat16))
        o_t = d if o_t is None else o_t + d
        yield
    inv = 1.0 / jnp.sum(l8, axis=0, keepdims=True)
    out_t = o_t * inv
    o_v[core, toks] = jnp.transpose(out_t).reshape(tok, GROUP, DIM).astype(jnp.bfloat16)
    delta = jnp.sum(dot_nt(identity(), g) * out_t, axis=0, keepdims=True)
    yield
    dq_t = None
    for a, n in blocks:
        p = s_ref[a:a + n, :] * inv
        ds = (p * (dot_nt(kv[1, a:a + n, :], g) - delta)).astype(jnp.bfloat16)
        part[1, a:a + n, :] += dot_nn(p.astype(jnp.bfloat16), g)
        part[0, a:a + n, :] += dot_nn(ds, qr)
        d = dot_nn(kt[:, a:a + n], ds)
        dq_t = d if dq_t is None else dq_t + d
        yield
    dq = jnp.transpose(dq_t) * scale
    dq = dq * table(0) - swap_pairs(dq) * table(1)
    dq_v[core, toks] = dq.reshape(tok, GROUP, DIM).astype(jnp.bfloat16)


def interleave(gens, lag):
    live, waiting, count = [], list(gens), 0
    while live or waiting:
        if waiting and (not live or count >= lag):
            live.append(waiting.pop(0))
            count = 0
        for gen in list(live):
            if next(gen, 'end') == 'end':
                live.remove(gen)
        count += 1


def unit_compute(c, q_v, g_v, tab, kv, o_v, dq_v, part, kt, vt, s_a, s_b, s_e):
    n_late, n_early = (N_PAIRS - c) * PAIR, (c + 1) * PAIR
    eye = identity()
    for a in range(0, n_late, 256):
        n = min(256, n_late - a)
        kt[:, a:a + n] = dot_nt(eye, kv[0, a:a + n, :]).astype(jnp.bfloat16)
        vt[:, a:a + n] = dot_nt(eye, kv[1, a:a + n, :]).astype(jnp.bfloat16)
    part[:, :n_late, :] = jnp.zeros((2, n_late, DIM), jnp.float32)
    refs = (q_v, g_v, tab, kv, kt, vt, part, o_v, dq_v)

    def step(i, carry):
        late = [rows_steps(n_late, 32, (1 - i, PIECE + 32 * k, i * PIECE + 32 * k), *refs, s)
                for k, s in ((0, s_a), (1, s_b))]
        early = rows_steps(n_early, PIECE, (i, 0, i * PIECE), *refs, s_e)
        interleave(late + [early], 2 * pl.cdiv(n_late, KEY_BLOCK) + 1)
        return carry

    lax.fori_loop(0, 2, step, 0)


def remote(src, dst, send_sem, recv_sem, device):
    return pltpu.make_async_remote_copy(src_ref=src, dst_ref=dst, send_sem=send_sem, recv_sem=recv_sem,
                                        device_id={'cp': device}, device_id_type=MESH_ID)


def chip_program(c, core, q_hbm, g_hbm, k_hbm, v_hbm, tab_hbm, o_hbm, dq_hbm, gk_hbm, gv_hbm, kv_hbm, qs_hbm, gs_hbm,
                 q_v, g_v, o_v, dq_v, kv_v, tab_v, tab_x, raw_v, ready_v, part, recv, fin_st, fin_v,
                 kt, vt, s_a, s_b, s_e,
                 raw_s, kvl_s, kvx_s, kvx_r, tab_s, tab_r, qx_s, qx_r, gx_s, gx_r, ag_s, ag_r, sum_s, sum_r,
                 load_s, out_s, out_r, fin_s, fin_r):
    n_late = (N_PAIRS - c) * PAIR
    sib = 2 * c + 1 - core
    nbr = {step: 2 * (c ^ step) + core for step in (X_STEP, Y_STEP)}
    mine, other = BATCHES * core, BATCHES * (1 - core)
    early_hops = [(p, step) for p, src, step in EARLY_HOP if src == c]
    first_hops = [(p, step) for p, src, step in FIRST_HOP if src == c and (p, src, step) not in EARLY_HOP]
    relay_hops = [(p, step) for p, src, step in RELAY_HOP if src == c]
    leaves = [(p, step) for p, src, step in SUM_LEAF if src == c]
    relays = [(p, step) for p, src, step in SUM_RELAY if src == c]
    needed = [p for p in range(N_PAIRS - c) if owner(p) != c]
    sib_pieces = (2 * c + 1 - core, 15 - 2 * c - (1 - core))

    def split(u):
        return u // HEADS, u % HEADS

    def pair_rows(p):
        return pl.ds(p * PAIR, PAIR)

    own_pieces = (2 * c + core, 15 - 2 * c - core)

    def raw_in(b, side):
        src = (mine, other)[side] + b
        return [pltpu.make_async_copy(k_hbm.at[src], raw_v.at[b, side, 0], raw_s.at[b, side, 0]),
                pltpu.make_async_copy(v_hbm.at[src], raw_v.at[b, side, 1], raw_s.at[b, side, 1])]

    def piece_rows(piece):
        return pl.ds(pl.multiple_of(piece * PIECE, PIECE), PIECE)

    def own_out(b, half):
        return pltpu.make_async_copy(ready_v.at[b, 0, :, :, pl.ds(half * PIECE, PIECE), :],
                                     kv_hbm.at[b, :, :, piece_rows(own_pieces[half]), :], kvl_s.at[b, half])

    def kvx(b, half):
        return remote(ready_v.at[b, 1, :, :, pl.ds(half * PIECE, PIECE), :],
                      kv_hbm.at[b, :, :, piece_rows(own_pieces[half]), :], kvx_s.at[b, half], kvx_r.at[b, half], sib)

    def kvx_in(b, half):
        dst = kv_hbm.at[b, :, :, piece_rows(sib_pieces[half]), :]
        return remote(dst, dst, kvx_s.at[b, half], kvx_r.at[b, half], sib)

    def make_ready(b):
        for side in (1, 0):
            for copy in raw_in(b, side):
                copy.wait()
            tab = tab_x.at[b] if side else tab_v.at[b, :, core]
            k_raw = raw_v[b, side, 0].astype(jnp.float32)
            v_raw = raw_v[b, side, 1].astype(jnp.float32)
            for h in range(HEADS):
                x = k_raw[:, h, :]
                ready_v[b, side, h, 0] = (x * tab[0] + swap_pairs(x) * tab[1]).astype(jnp.bfloat16)
                ready_v[b, side, h, 1] = v_raw[:, h, :].astype(jnp.bfloat16)
            for half in range(2):
                (kvx if side else own_out)(b, half).start()

    def qx(b):
        return remote(q_hbm.at[other + b], qs_hbm.at[b], qx_s.at[b], qx_r.at[b], sib)

    def gx(b):
        return remote(g_hbm.at[other + b], gs_hbm.at[b], gx_s.at[b], gx_r.at[b], sib)

    def tab_in():
        return pltpu.make_async_copy(tab_hbm.at[pl.ds(mine, BATCHES)], tab_v.at[:, :, core], load_s.at[5, 0])

    def tab_other():
        return pltpu.make_async_copy(tab_hbm.at[pl.ds(other, BATCHES)], tab_x, load_s.at[5, 1])

    def tab_out():
        return remote(tab_hbm.at[pl.ds(other, BATCHES)], tab_v.at[:, :, core], tab_s, tab_r, sib)

    def tab_arrive():
        return remote(tab_hbm.at[pl.ds(other, BATCHES)], tab_v.at[:, :, 1 - core], tab_s, tab_r, sib)

    def kv_copy(u, p, slot, step):
        b, h = split(u)
        ref = kv_hbm.at[b, h, :, pair_rows(p), :]
        return remote(ref, ref, ag_s.at[u, slot], ag_r.at[u, p], nbr[step])

    def send_kv(u, hops, base):
        for i, (p, step) in enumerate(hops):
            kv_copy(u, p, base + i, step).start()

    def have_own(b):
        for half in range(2):
            own_out(b, half).wait()
            kvx_in(b, half).wait_recv()

    def early_hop(u):
        send_kv(u, early_hops, 0)

    def first_hop(u):
        send_kv(u, first_hops, len(early_hops))

    def relay_hop(u):
        for p, _ in relay_hops:
            kv_copy(u, p, 0, X_STEP).wait_recv()
        send_kv(u, relay_hops, len(early_hops) + len(first_hops))

    def loads(u):
        b, h = split(u)
        slot = u % 2
        late = pl.ds(0, n_late)
        return [
            pltpu.make_async_copy(q_hbm.at[mine + b, :, h], q_v.at[slot, core], load_s.at[0, slot]),
            pltpu.make_async_copy(g_hbm.at[mine + b, :, h], g_v.at[slot, core], load_s.at[1, slot]),
            pltpu.make_async_copy(qs_hbm.at[b, :, h], q_v.at[slot, 1 - core], load_s.at[2, slot]),
            pltpu.make_async_copy(gs_hbm.at[b, :, h], g_v.at[slot, 1 - core], load_s.at[3, slot]),
            pltpu.make_async_copy(kv_hbm.at[b, h, :, late, :], kv_v.at[slot, :, late, :], load_s.at[4, slot]),
        ]

    def start_loads(u):
        @pl.when(u % HEADS == 0)
        def _():
            qx(u // HEADS).wait_recv()
            gx(u // HEADS).wait_recv()

        for p in needed:
            if p not in [r for r, _ in relay_hops]:
                kv_copy(u, p, 0, X_STEP).wait_recv()
        for copy in loads(u):
            copy.start()

    def out_local(u):
        b, h = split(u)
        slot = u % 2
        return [pltpu.make_async_copy(o_v.at[slot, core], o_hbm.at[mine + b, :, h], out_s.at[0, slot]),
                pltpu.make_async_copy(dq_v.at[slot, core], dq_hbm.at[mine + b, :, h], out_s.at[1, slot])]

    def out_remote(u):
        b, h = split(u)
        slot = u % 2
        return [remote(o_v.at[slot, 1 - core], o_hbm.at[mine + b, :, h], out_s.at[2, slot], out_r.at[0, b], sib),
                remote(dq_v.at[slot, 1 - core], dq_hbm.at[mine + b, :, h], out_s.at[3, slot], out_r.at[1, b], sib)]

    def out_arrive(b):
        return [remote(q_hbm.at[other + b], o_hbm.at[other + b], out_s.at[2, 0], out_r.at[0, b], sib),
                remote(q_hbm.at[other + b], dq_hbm.at[other + b], out_s.at[3, 0], out_r.at[1, b], sib)]

    def wait_outs(u):
        for copy in out_local(u):
            copy.wait()
        for copy in out_remote(u):
            copy.wait_send()

    def sum_copy(u, p, i, step):
        dst = inbox(c ^ step).index((p, c))
        return remote(part.at[u % PART_RING, :, pair_rows(p), :], recv.at[u, dst],
                      sum_s.at[i, u % PART_RING], sum_r.at[u, dst], nbr[step])

    def sum_arrive(u, k):
        dst = recv.at[u, k]
        return remote(dst, dst, sum_s.at[0, 0], sum_r.at[u, k], nbr[X_STEP])

    def messages(p):
        return [k for k, (pair, _) in enumerate(inbox(c)) if pair == p]

    def wait_sums(u):
        for i, (p, step) in enumerate(leaves + relays):
            sum_copy(u, p, i, step).wait_send()

    def send_leaves(u):
        for i, (p, step) in enumerate(leaves):
            sum_copy(u, p, i, step).start()

    def add_relays(u):
        for p, _ in relays:
            for k in messages(p):
                sum_arrive(u, k).wait_recv()
                part[u % PART_RING, :, pair_rows(p), :] += recv[u, k]

    def send_relays(u):
        for i, (p, step) in enumerate(relays):
            sum_copy(u, p, len(leaves) + i, step).start()

    def fin_local(b):
        return [pltpu.make_async_copy(fin_v.at[b % 2, core, i], (gk_hbm, gv_hbm)[i].at[mine + b], fin_s.at[i, b % 2])
                for i in range(2)]

    def fin_remote(b):
        return [remote(fin_v.at[b % 2, 1 - core, i], (gk_hbm, gv_hbm)[i].at[mine + b], fin_s.at[2 + i, b % 2],
                       fin_r.at[i, b], sib) for i in range(2)]

    def fin_arrive(b):
        return [remote(dst.at[other + b], dst.at[other + b], fin_s.at[2 + i, 0], fin_r.at[i, b], sib)
                for i, dst in enumerate((gk_hbm, gv_hbm))]

    def wait_fin(b):
        for copy in fin_local(b):
            copy.wait()
        for copy in fin_remote(b):
            copy.wait_send()

    def finish(u):
        b, h = split(u)
        for late, p in ((0, c), (1, N_PAIRS - 1 - c)):
            total = part[u % PART_RING, :, pair_rows(p), :]
            for k in messages(p):
                sum_arrive(u, k).wait_recv()
                total = total + recv[u, k]
            for i in range(2):
                who = 1 - i if late else i
                toks = slice(late * PIECE, (late + 1) * PIECE)
                dk = total[0, i * PIECE:(i + 1) * PIECE] * (DIM ** -0.5)
                dk = dk * tab_v[b, 0, who, toks] - swap_pairs(dk) * tab_v[b, 1, who, toks]
                fin_st[who, 0, h, toks] = dk.astype(jnp.bfloat16)
                fin_st[who, 1, h, toks] = total[1, i * PIECE:(i + 1) * PIECE].astype(jnp.bfloat16)

        @pl.when(h == HEADS - 1)
        def _():
            @pl.when(b >= 2)
            def _():
                wait_fin(b - 2)

            for who in range(2):
                for i in range(2):
                    rows = jnp.transpose(fin_st[who, i].astype(jnp.float32), (1, 0, 2))
                    fin_v[b % 2, who, i] = rows.astype(jnp.bfloat16)

    def send_fin(u):
        @pl.when(u % HEADS == HEADS - 1)
        def _():
            for copy in fin_local(u // HEADS) + fin_remote(u // HEADS):
                copy.start()

    tab_other().start()
    tab_in().start()

    def start_raw(b, carry):
        for side in (1, 0):
            for copy in raw_in(b, side):
                copy.start()
        return carry

    lax.fori_loop(0, BATCHES, start_raw, 0)
    tab_other().wait()
    tab_in().wait()
    make_ready(jnp.int32(0))
    tab_out().start()

    def start_exchange(b, carry):
        qx(b).start()
        gx(b).start()
        return carry

    lax.fori_loop(0, BATCHES, start_exchange, 0)

    def prologue(u, carry):
        @pl.when(u % HEADS == 0)
        def _():
            have_own(u // HEADS)

        first_hop(u)
        early_hop(u)

        @pl.when(u + 1 < BATCHES)
        def _():
            make_ready(u + 1)

        @pl.when((u >= 1) & (u <= RELAY_LEAD))
        def _():
            relay_hop(u - 1)

        return carry

    lax.fori_loop(0, AG_LEAD, prologue, 0)

    def own_ready(b, carry):
        have_own(b)
        return carry

    lax.fori_loop(AG_LEAD // HEADS, BATCHES, own_ready, 0)

    def more_early(u, carry):
        early_hop(u)
        return carry

    lax.fori_loop(AG_LEAD, min(EARLY_LEAD, UNITS), more_early, 0)
    tab_arrive().wait_recv()
    start_loads(jnp.int32(0))

    def tick(t, carry):
        @pl.when(t + AG_LEAD < UNITS)
        def _():
            first_hop(t + AG_LEAD)

        @pl.when(t + EARLY_LEAD < UNITS)
        def _():
            early_hop(t + EARLY_LEAD)

        @pl.when(t + RELAY_LEAD < UNITS)
        def _():
            relay_hop(t + RELAY_LEAD)

        @pl.when((t >= 1) & (t - 1 < UNITS))
        def _():
            send_leaves(t - 1)

        @pl.when((t >= 1 + SUM_LAG) & (t - 1 - SUM_LAG < UNITS))
        def _():
            add_relays(t - 1 - SUM_LAG)

        @pl.when((t >= 1 + OWN_LAG) & (t - 1 - OWN_LAG < UNITS))
        def _():
            finish(t - 1 - OWN_LAG)

        @pl.when((t >= 1 + SUM_LAG) & (t - 1 - SUM_LAG < UNITS))
        def _():
            send_relays(t - 1 - SUM_LAG)

        @pl.when((t >= 1 + OWN_LAG) & (t - 1 - OWN_LAG < UNITS))
        def _():
            send_fin(t - 1 - OWN_LAG)

        @pl.when(t < UNITS)
        def _():
            for copy in loads(t):
                copy.wait()

            @pl.when(t + 1 < UNITS)
            def _():
                start_loads(t + 1)

            @pl.when(t >= 2)
            def _():
                wait_outs(t - 2)

            @pl.when(t >= PART_RING)
            def _():
                wait_sums(t - PART_RING)

            slot = t % 2
            unit_compute(c, q_v.at[slot], g_v.at[slot], tab_v.at[t // HEADS], kv_v.at[slot], o_v.at[slot],
                         dq_v.at[slot], part.at[t % PART_RING], kt, vt, s_a, s_b, s_e)
            for copy in out_local(t) + out_remote(t):
                copy.start()

        return carry

    lax.fori_loop(0, UNITS + 1 + OWN_LAG, tick, 0)

    tab_out().wait_send()
    for u in range(UNITS - 2, UNITS):
        wait_outs(jnp.int32(u))
    for b in range(BATCHES - 2, BATCHES):
        wait_fin(jnp.int32(b))

    def drain_batch(b, carry):
        for half in range(2):
            kvx(b, half).wait_send()
        qx(b).wait_send()
        gx(b).wait_send()
        for copy in out_arrive(b):
            copy.wait_recv()
        for copy in fin_arrive(b):
            copy.wait_recv()
        return carry

    lax.fori_loop(0, BATCHES, drain_batch, 0)

    def drain_sums(u, carry):
        wait_sums(u)
        return carry

    lax.fori_loop(UNITS - PART_RING, UNITS, drain_sums, 0)

    def drain_kv(u, carry):
        for i, (p, step) in enumerate(early_hops + first_hops + relay_hops):
            kv_copy(u, p, i, step).wait_send()
        return carry

    lax.fori_loop(0, UNITS, drain_kv, 0)


def attend_kernel(*refs):
    me = lax.axis_index('cp')
    chip, core = me // 2, me % 2
    barrier = pltpu.get_barrier_semaphore()
    for c in range(4):
        @pl.when(chip == c)
        def _(c=c):
            for device in (2 * c + 1 - core, 2 * (c ^ X_STEP) + core, 2 * (c ^ Y_STEP) + core):
                pl.semaphore_signal(barrier, inc=1, device_id={'cp': device}, device_id_type=MESH_ID)
    pl.semaphore_wait(barrier, 3)
    for c in range(4):
        @pl.when(chip == c)
        def _(c=c):
            chip_program(c, core, *refs)


def attend(q5, g5, keys, values, tab):
    any_spec = pl.BlockSpec(memory_space=pl.ANY)
    head_shape = jax.ShapeDtypeStruct(q5.shape, jnp.bfloat16)
    half_shape = jax.ShapeDtypeStruct((BATCHES,) + q5.shape[1:], jnp.bfloat16)
    head_buf = pltpu.VMEM((2, 2, PAIR, GROUP, DIM), jnp.bfloat16)
    dma = pltpu.SemaphoreType.DMA
    return pl.pallas_call(
        attend_kernel, name='attend',
        in_specs=[any_spec] * 5,
        out_specs=[any_spec] * 7,
        out_shape=[head_shape, head_shape,
                   jax.ShapeDtypeStruct(keys.shape, jnp.bfloat16), jax.ShapeDtypeStruct(keys.shape, jnp.bfloat16),
                   jax.ShapeDtypeStruct((BATCHES, HEADS, 2, N_PAIRS * PAIR, DIM), jnp.bfloat16),
                   half_shape, half_shape],
        scratch_shapes=[
            head_buf, head_buf, head_buf, head_buf,
            pltpu.VMEM((2, 2, N_PAIRS * PAIR, DIM), jnp.bfloat16),
            pltpu.VMEM((BATCHES, 2, 2, PAIR, DIM), jnp.float32),
            pltpu.VMEM((BATCHES, 2, PAIR, DIM), jnp.float32),
            pltpu.VMEM((BATCHES, 2, 2, PAIR, HEADS, DIM), jnp.bfloat16),
            pltpu.VMEM((BATCHES, 2, HEADS, 2, PAIR, DIM), jnp.bfloat16),
            pltpu.VMEM((PART_RING, 2, N_PAIRS * PAIR, DIM), jnp.float32),
            pltpu.VMEM((UNITS, N_INBOX, 2, PAIR, DIM), jnp.float32),
            pltpu.VMEM((2, 2, HEADS, PAIR, DIM), jnp.bfloat16),
            pltpu.VMEM((2, 2, 2, PAIR, HEADS, DIM), jnp.bfloat16),
            pltpu.VMEM((DIM, N_PAIRS * PAIR), jnp.bfloat16),
            pltpu.VMEM((DIM, N_PAIRS * PAIR), jnp.bfloat16),
            pltpu.VMEM((N_PAIRS * PAIR, 32 * GROUP), jnp.float32),
            pltpu.VMEM((N_PAIRS * PAIR, 32 * GROUP), jnp.float32),
            pltpu.VMEM((4 * PAIR, PIECE * GROUP), jnp.float32),
            dma((BATCHES, 2, 2)), dma((BATCHES, 2)), dma((BATCHES, 2)), dma((BATCHES, 2)), dma, dma,
            dma((BATCHES,)), dma((BATCHES,)), dma((BATCHES,)), dma((BATCHES,)),
            dma((UNITS, 7)), dma((UNITS, 7)), dma((6, PART_RING)), dma((UNITS, N_INBOX)),
            dma((6, 2)), dma((4, 2)), dma((2, BATCHES)), dma((4, 2)), dma((2, BATCHES)),
        ],
        compiler_params=pltpu.CompilerParams(
            collective_id=0, has_side_effects=True, vmem_limit_bytes=60 * 1024 * 1024),
    )(q5, g5, keys, values, tab)


def solution(mesh):
    head_spec = P(None, 'cp', 'tp', None)
    pos_spec = P(None, 'cp')

    def local_step(query, keys, values, positions, grad_out):
        batch, length, n_heads, dim = query.shape
        tab = rope_tables(positions, dim)
        split_shape = (batch, length, HEADS, GROUP, dim)
        outs = attend(query.reshape(split_shape), grad_out.reshape(split_shape), keys, values, tab)
        return outs[0].reshape(query.shape), outs[1].reshape(query.shape), outs[2], outs[3]

    return jax.shard_map(local_step, mesh=mesh,
                         in_specs=(head_spec, head_spec, head_spec, pos_spec, head_spec),
                         out_specs=(head_spec, head_spec, head_spec, head_spec), check_vma=False)
```

```python
import functools

import jax
import jax.numpy as jnp
from jax import lax
from jax.experimental import pallas as pl
from jax.experimental.pallas import tpu as pltpu
from jax.sharding import PartitionSpec as P

ROPE_THETA = 1000000.0
LOG2E = 1.4426950408889634
DIM = 128
GROUP = 8
HEADS = 4
PIECE = 64
PAIR = 128
N_PAIRS = 8
BATCHES = 8
UNITS = BATCHES * HEADS
KEY_BLOCK = 512
MESH_ID = pl.DeviceIdType.MESH

X_STEP, Y_STEP = 1, 2
FIRST_HOP = [(0, 0, X_STEP), (0, 0, Y_STEP), (1, 1, X_STEP), (1, 1, Y_STEP), (2, 2, X_STEP), (2, 2, Y_STEP),
             (3, 3, X_STEP), (3, 3, Y_STEP), (4, 3, X_STEP), (4, 3, Y_STEP), (5, 2, Y_STEP), (5, 2, X_STEP),
             (6, 1, X_STEP)]
RELAY_HOP = [(0, 2, X_STEP), (1, 3, X_STEP), (2, 3, Y_STEP), (3, 2, Y_STEP), (4, 1, X_STEP), (5, 3, Y_STEP)]
SUM_LEAF = [(0, 3, X_STEP), (0, 1, X_STEP), (1, 2, Y_STEP), (1, 3, Y_STEP), (2, 1, Y_STEP), (2, 0, Y_STEP),
            (3, 0, Y_STEP), (3, 1, Y_STEP), (4, 0, X_STEP), (4, 2, X_STEP), (5, 1, X_STEP), (6, 0, X_STEP)]
SUM_RELAY = [(0, 2, Y_STEP), (1, 0, X_STEP), (2, 3, X_STEP), (3, 2, X_STEP), (4, 1, Y_STEP), (5, 0, Y_STEP)]

START_UNITS = 2 * HEADS
RELAY_LEAD = 4
EARLY_HOP = [(0, 0, X_STEP), (0, 0, Y_STEP), (1, 1, Y_STEP)]
SUM_LAG = 2
OWN_LAG = 5
PART_RING = OWN_LAG + 2
INBOX_RING = 8


def owner(pair):
    return pair if pair < 4 else 7 - pair


def inbox(chip):
    found = []
    for pair, src, step in SUM_LEAF + SUM_RELAY:
        if src ^ step == chip:
            found.append((pair, src))
    return found


def outbox(chip):
    return [(pair, step) for pair, src, step in SUM_LEAF + SUM_RELAY if src == chip]


N_INBOX = max(len(inbox(c)) for c in range(4))
N_OUTBOX = max(len(outbox(c)) for c in range(4))


def rope_tables(positions, head_dim):
    half_dim = head_dim // 2
    freq_expo = jnp.arange(half_dim, dtype=jnp.float32) * (2.0 / head_dim)
    inv_freq = 1.0 / (ROPE_THETA ** freq_expo)
    angles = positions.astype(jnp.float32)[:, :, None] * inv_freq
    cosine, sine_val = jnp.cos(angles), jnp.sin(angles)
    cos_l = jnp.repeat(cosine, 2, axis=-1)
    sin_l = jnp.stack([-sine_val, sine_val], axis=-1).reshape(cos_l.shape)
    return jnp.stack([cos_l, sin_l], axis=1)


def dot_nn(a, b):
    return jnp.dot(a, b, preferred_element_type=jnp.float32)


def dot_nt(a, b):
    return lax.dot_general(a, b, (((1,), (1,)), ((), ())), preferred_element_type=jnp.float32)


def iota(shape, axis):
    return lax.broadcasted_iota(jnp.int32, shape, axis)


def identity():
    return (iota((DIM, DIM), 0) == iota((DIM, DIM), 1)).astype(jnp.float32).astype(jnp.bfloat16)


def swap_pairs(x):
    return jnp.where(iota(x.shape, 1) % 2 == 0, pltpu.roll(x, DIM - 1, axis=1), pltpu.roll(x, 1, axis=1))


def rows_steps(n_keys, tok, seg, q_v, g_v, tab, kv, kt, vt, part, o_v, dq_v, s_ref):
    core, start, place = seg
    rows = tok * GROUP
    scale = DIM ** -0.5
    c1 = scale * LOG2E
    toks = pl.ds(start, tok)

    def table(k):
        return jnp.broadcast_to(tab[k, core, toks, :][:, None, :], (tok, GROUP, DIM)).reshape(rows, DIM)

    x = q_v[core, toks].astype(jnp.float32).reshape(rows, DIM)
    qr = (x * table(0) + swap_pairs(x) * table(1)).astype(jnp.bfloat16)
    g = g_v[core, toks].astype(jnp.float32).reshape(rows, DIM).astype(jnp.bfloat16)
    blocks = [(a, min(KEY_BLOCK, n_keys - a)) for a in range(0, n_keys, KEY_BLOCK)]
    m8 = None
    for a, n in blocks:
        s = dot_nt(kv[0, a:a + n, :], qr) * c1
        if a + n == n_keys:
            last = s[n - PAIR:, :]
            q_tok = iota(last.shape, 1) // GROUP + place
            last = jnp.where(iota(last.shape, 0) <= q_tok, last, -jnp.inf)
            s = last if n == PAIR else jnp.concatenate([s[:n - PAIR, :], last], axis=0)
        s_ref[a:a + n, :] = s
        f = jnp.max(s.reshape(n // 8, 8, rows), axis=0)
        m8 = f if m8 is None else jnp.maximum(m8, f)
        yield
    row_max = jnp.max(m8, axis=0, keepdims=True)
    l8 = None
    o_t = None
    for a, n in blocks:
        p = jnp.exp2(s_ref[a:a + n, :] - row_max)
        s_ref[a:a + n, :] = p
        f = jnp.sum(p.reshape(n // 8, 8, rows), axis=0)
        l8 = f if l8 is None else l8 + f
        d = dot_nn(vt[:, a:a + n], p.astype(jnp.bfloat16))
        o_t = d if o_t is None else o_t + d
        yield
    inv = 1.0 / jnp.sum(l8, axis=0, keepdims=True)
    out_t = o_t * inv
    o_v[core, toks] = jnp.transpose(out_t).reshape(tok, GROUP, DIM).astype(jnp.bfloat16)
    delta = jnp.sum(dot_nt(identity(), g) * out_t, axis=0, keepdims=True)
    yield
    dq_t = None
    for a, n in blocks:
        p = s_ref[a:a + n, :] * inv
        ds = (p * (dot_nt(kv[1, a:a + n, :], g) - delta)).astype(jnp.bfloat16)
        part[1, a:a + n, :] += dot_nn(p.astype(jnp.bfloat16), g)
        part[0, a:a + n, :] += dot_nn(ds, qr)
        d = dot_nn(kt[:, a:a + n], ds)
        dq_t = d if dq_t is None else dq_t + d
        yield
    dq = jnp.transpose(dq_t) * scale
    dq = dq * table(0) - swap_pairs(dq) * table(1)
    dq_v[core, toks] = dq.reshape(tok, GROUP, DIM).astype(jnp.bfloat16)


def interleave(gens, lag):
    live, waiting, count = [], list(gens), 0
    while live or waiting:
        if waiting and (not live or count >= lag):
            live.append(waiting.pop(0))
            count = 0
        for gen in list(live):
            if next(gen, 'end') == 'end':
                live.remove(gen)
        count += 1


def unit_compute(c, q_v, g_v, tab, kv, o_v, dq_v, part, kt, vt, s_a, s_b, s_e):
    n_late, n_early = (N_PAIRS - c) * PAIR, (c + 1) * PAIR
    eye = identity()
    for a in range(0, n_late, 256):
        n = min(256, n_late - a)
        kt[:, a:a + n] = dot_nt(eye, kv[0, a:a + n, :]).astype(jnp.bfloat16)
        vt[:, a:a + n] = dot_nt(eye, kv[1, a:a + n, :]).astype(jnp.bfloat16)
    part[:, :n_late, :] = jnp.zeros((2, n_late, DIM), jnp.float32)
    refs = (q_v, g_v, tab, kv, kt, vt, part, o_v, dq_v)

    def step(i, carry):
        late = [rows_steps(n_late, 32, (1 - i, PIECE + 32 * k, i * PIECE + 32 * k), *refs, s)
                for k, s in ((0, s_a), (1, s_b))]
        early = rows_steps(n_early, PIECE, (i, 0, i * PIECE), *refs, s_e)
        interleave(late + [early], 2 * pl.cdiv(n_late, KEY_BLOCK) + 1)
        return carry

    lax.fori_loop(0, 2, step, 0)


def remote(src, dst, send_sem, recv_sem, device):
    return pltpu.make_async_remote_copy(src_ref=src, dst_ref=dst, send_sem=send_sem, recv_sem=recv_sem,
                                        device_id={'cp': device}, device_id_type=MESH_ID)


def chip_program(c, core, q_hbm, g_hbm, k_hbm, v_hbm, tab_hbm, o_hbm, dq_hbm, gk_hbm, gv_hbm, kv_hbm, qs_hbm, gs_hbm,
                 q_v, g_v, o_v, dq_v, kv_v, tab_v, tab_x, raw_v, ready_v, part, recv, fin_st, fin_v,
                 perm_in, perm_out, kt, vt, s_a, s_b, s_e,
                 raw_s, kvl_s, kvx_s, kvx_r, tab_s, tab_r, qx_s, qx_r, gx_s, gx_r, ag_s, ag_r, sum_s, sum_r,
                 load_s, out_s, out_r, fin_s, fin_r, credit):
    n_late = (N_PAIRS - c) * PAIR
    sib = 2 * c + 1 - core
    nbr = {step: 2 * (c ^ step) + core for step in (X_STEP, Y_STEP)}
    mine, other = BATCHES * core, BATCHES * (1 - core)
    early_hops = [(p, step) for p, src, step in EARLY_HOP if src == c]
    first_hops = [(p, step) for p, src, step in FIRST_HOP if src == c and (p, src, step) not in EARLY_HOP]
    relay_hops = [(p, step) for p, src, step in RELAY_HOP if src == c]
    leaves = [(p, step) for p, src, step in SUM_LEAF if src == c]
    relays = [(p, step) for p, src, step in SUM_RELAY if src == c]
    needed = [p for p in range(N_PAIRS - c) if owner(p) != c]
    sib_pieces = (2 * c + 1 - core, 15 - 2 * c - (1 - core))

    def split(u):
        return u // HEADS, u % HEADS

    def pair_rows(p):
        return pl.ds(p * PAIR, PAIR)

    own_pieces = (2 * c + core, 15 - 2 * c - core)

    def raw_in(b, side):
        src, slot = (mine, other)[side] + b, b % 2
        copies = [pltpu.make_async_copy(k_hbm.at[src], raw_v.at[slot, side, 0], raw_s.at[slot, side, 0]),
                  pltpu.make_async_copy(v_hbm.at[src], raw_v.at[slot, side, 1], raw_s.at[slot, side, 1])]
        if side:
            copies.append(pltpu.make_async_copy(tab_hbm.at[src], tab_x.at[slot], raw_s.at[slot, side, 2]))
        return copies

    def start_raw(b):
        for side in (1, 0):
            for copy in raw_in(b, side):
                copy.start()

    def piece_rows(piece):
        return pl.ds(pl.multiple_of(piece * PIECE, PIECE), PIECE)

    def own_out(b, half):
        return pltpu.make_async_copy(ready_v.at[b % 2, 0, :, :, pl.ds(half * PIECE, PIECE), :],
                                     kv_hbm.at[b, :, :, piece_rows(own_pieces[half]), :], kvl_s.at[b, half])

    def kvx(b, half):
        return remote(ready_v.at[b % 2, 1, :, :, pl.ds(half * PIECE, PIECE), :],
                      kv_hbm.at[b, :, :, piece_rows(own_pieces[half]), :], kvx_s.at[b, half], kvx_r.at[b, half], sib)

    def kvx_in(b, half):
        dst = kv_hbm.at[b, :, :, piece_rows(sib_pieces[half]), :]
        return remote(dst, dst, kvx_s.at[b, half], kvx_r.at[b, half], sib)

    def make_ready(b):
        slot = b % 2

        @pl.when(b >= 2)
        def _():
            for half in range(2):
                kvx(b - 2, half).wait_send()

        for side in (1, 0):
            for copy in raw_in(b, side):
                copy.wait()
            tab = tab_x.at[slot] if side else tab_v.at[b, :, core]
            k_rows = dot_nn(perm_in[...], raw_v[slot, side, 0])
            v_rows = dot_nn(perm_in[...], raw_v[slot, side, 1])
            for h in range(HEADS):
                x = k_rows[h * PAIR:(h + 1) * PAIR]
                ready_v[slot, side, h, 0] = (x * tab[0] + swap_pairs(x) * tab[1]).astype(jnp.bfloat16)
                ready_v[slot, side, h, 1] = v_rows[h * PAIR:(h + 1) * PAIR].astype(jnp.bfloat16)
            for half in range(2):
                (kvx if side else own_out)(b, half).start()

        @pl.when(b + 2 < BATCHES)
        def _():
            start_raw(b + 2)

    def qx(b):
        return remote(q_hbm.at[other + b], qs_hbm.at[b], qx_s.at[b], qx_r.at[b], sib)

    def gx(b):
        return remote(g_hbm.at[other + b], gs_hbm.at[b], gx_s.at[b], gx_r.at[b], sib)

    def tab_in():
        return pltpu.make_async_copy(tab_hbm.at[pl.ds(mine, BATCHES)], tab_v.at[:, :, core], load_s.at[5, 0])

    def tab_out():
        return remote(tab_hbm.at[pl.ds(other, BATCHES)], tab_v.at[:, :, core], tab_s, tab_r, sib)

    def tab_arrive():
        return remote(tab_hbm.at[pl.ds(other, BATCHES)], tab_v.at[:, :, 1 - core], tab_s, tab_r, sib)

    def kv_copy(u, p, slot, step):
        b, h = split(u)
        ref = kv_hbm.at[b, h, :, pair_rows(p), :]
        return remote(ref, ref, ag_s.at[u, slot], ag_r.at[u, p], nbr[step])

    def send_kv(u, hops, base):
        for i, (p, step) in enumerate(hops):
            kv_copy(u, p, base + i, step).start()

    def have_own(b):
        for half in range(2):
            own_out(b, half).wait()
            kvx_in(b, half).wait_recv()

    def early_hop(u):
        send_kv(u, early_hops, 0)

    def first_hop(u):
        send_kv(u, first_hops, len(early_hops))

    def relay_hop(u):
        for p, _ in relay_hops:
            kv_copy(u, p, 0, X_STEP).wait_recv()
        send_kv(u, relay_hops, len(early_hops) + len(first_hops))

    def loads(u):
        b, h = split(u)
        slot = u % 2
        late = pl.ds(0, n_late)
        return [
            pltpu.make_async_copy(q_hbm.at[mine + b, :, h], q_v.at[slot, core], load_s.at[0, slot]),
            pltpu.make_async_copy(g_hbm.at[mine + b, :, h], g_v.at[slot, core], load_s.at[1, slot]),
            pltpu.make_async_copy(qs_hbm.at[b, :, h], q_v.at[slot, 1 - core], load_s.at[2, slot]),
            pltpu.make_async_copy(gs_hbm.at[b, :, h], g_v.at[slot, 1 - core], load_s.at[3, slot]),
            pltpu.make_async_copy(kv_hbm.at[b, h, :, late, :], kv_v.at[slot, :, late, :], load_s.at[4, slot]),
        ]

    def start_loads(u):
        @pl.when(u % HEADS == 0)
        def _():
            qx(u // HEADS).wait_recv()
            gx(u // HEADS).wait_recv()

        for p in needed:
            if p not in [r for r, _ in relay_hops]:
                kv_copy(u, p, 0, X_STEP).wait_recv()
        for copy in loads(u):
            copy.start()

    def out_local(u):
        b, h = split(u)
        slot = u % 2
        return [pltpu.make_async_copy(o_v.at[slot, core], o_hbm.at[mine + b, :, h], out_s.at[0, slot]),
                pltpu.make_async_copy(dq_v.at[slot, core], dq_hbm.at[mine + b, :, h], out_s.at[1, slot])]

    def out_remote(u):
        b, h = split(u)
        slot = u % 2
        return [remote(o_v.at[slot, 1 - core], o_hbm.at[mine + b, :, h], out_s.at[2, slot], out_r.at[0, b], sib),
                remote(dq_v.at[slot, 1 - core], dq_hbm.at[mine + b, :, h], out_s.at[3, slot], out_r.at[1, b], sib)]

    def out_arrive(b):
        return [remote(q_hbm.at[other + b], o_hbm.at[other + b], out_s.at[2, 0], out_r.at[0, b], sib),
                remote(q_hbm.at[other + b], dq_hbm.at[other + b], out_s.at[3, 0], out_r.at[1, b], sib)]

    def wait_outs(u):
        for copy in out_local(u):
            copy.wait()
        for copy in out_remote(u):
            copy.wait_send()

    def sum_copy(u, p, i, step):
        k, slot = inbox(c ^ step).index((p, c)), u % INBOX_RING
        return remote(part.at[u % PART_RING, :, pair_rows(p), :], recv.at[slot, k],
                      sum_s.at[i, u % PART_RING], sum_r.at[slot, k], nbr[step])

    def sum_arrive(u, k):
        dst = recv.at[u % INBOX_RING, k]
        return remote(dst, dst, sum_s.at[0, 0], sum_r.at[u % INBOX_RING, k], nbr[X_STEP])

    def give_credits(u, pairs):
        @pl.when(u + INBOX_RING < UNITS)
        def _():
            for k, (pair, src) in enumerate(inbox(c)):
                if pair in pairs:
                    pl.semaphore_signal(credit.at[outbox(src).index((pair, src ^ c))], inc=1,
                                        device_id={'cp': 2 * src + core}, device_id_type=MESH_ID)

    def take_credits(u, which):
        @pl.when(u >= INBOX_RING)
        def _():
            for i in which:
                pl.semaphore_wait(credit.at[i], 1)

    def messages(p):
        return [k for k, (pair, _) in enumerate(inbox(c)) if pair == p]

    def wait_sums(u):
        for i, (p, step) in enumerate(leaves + relays):
            sum_copy(u, p, i, step).wait_send()

    def send_leaves(u):
        take_credits(u, range(len(leaves)))
        for i, (p, step) in enumerate(leaves):
            sum_copy(u, p, i, step).start()

    def add_relays(u):
        for p, _ in relays:
            for k in messages(p):
                sum_arrive(u, k).wait_recv()
                part[u % PART_RING, :, pair_rows(p), :] += recv[u % INBOX_RING, k]
        give_credits(u, [p for p, _ in relays])

    def send_relays(u):
        take_credits(u, range(len(leaves), len(leaves) + len(relays)))
        for i, (p, step) in enumerate(relays):
            sum_copy(u, p, len(leaves) + i, step).start()

    def fin_local(b):
        return [pltpu.make_async_copy(fin_v.at[b % 2, core, i], (gk_hbm, gv_hbm)[i].at[mine + b], fin_s.at[i, b % 2])
                for i in range(2)]

    def fin_remote(b):
        return [remote(fin_v.at[b % 2, 1 - core, i], (gk_hbm, gv_hbm)[i].at[mine + b], fin_s.at[2 + i, b % 2],
                       fin_r.at[i, b], sib) for i in range(2)]

    def fin_arrive(b):
        return [remote(dst.at[other + b], dst.at[other + b], fin_s.at[2 + i, 0], fin_r.at[i, b], sib)
                for i, dst in enumerate((gk_hbm, gv_hbm))]

    def wait_fin(b):
        for copy in fin_local(b):
            copy.wait()
        for copy in fin_remote(b):
            copy.wait_send()

    def finish(u):
        b, h = split(u)
        for late, p in ((0, c), (1, N_PAIRS - 1 - c)):
            total = part[u % PART_RING, :, pair_rows(p), :]
            for k in messages(p):
                sum_arrive(u, k).wait_recv()
                total = total + recv[u % INBOX_RING, k]
            for i in range(2):
                who = 1 - i if late else i
                toks = slice(late * PIECE, (late + 1) * PIECE)
                dk = total[0, i * PIECE:(i + 1) * PIECE] * (DIM ** -0.5)
                dk = dk * tab_v[b, 0, who, toks] - swap_pairs(dk) * tab_v[b, 1, who, toks]
                fin_st[who, 0, h, toks] = dk.astype(jnp.bfloat16)
                fin_st[who, 1, h, toks] = total[1, i * PIECE:(i + 1) * PIECE].astype(jnp.bfloat16)
        give_credits(u, [c, N_PAIRS - 1 - c])

        @pl.when(h == HEADS - 1)
        def _():
            @pl.when(b >= 2)
            def _():
                wait_fin(b - 2)

            for who in range(2):
                for i in range(2):
                    rows = fin_st[who, i].reshape(HEADS * PAIR, DIM)
                    fin_v[b % 2, who, i] = dot_nn(perm_out[...], rows).astype(jnp.bfloat16)

    def send_fin(u):
        @pl.when(u % HEADS == HEADS - 1)
        def _():
            for copy in fin_local(u // HEADS) + fin_remote(u // HEADS):
                copy.start()

    def exchange_queries(b):
        qx(b).start()
        gx(b).start()

    start_raw(jnp.int32(0))
    tab_in().start()
    start_raw(jnp.int32(1))
    row, col = iota((HEADS * PAIR, HEADS * PAIR), 0), iota((HEADS * PAIR, HEADS * PAIR), 1)
    perm_in[...] = (col == (row % PAIR) * HEADS + row // PAIR).astype(jnp.float32).astype(jnp.bfloat16)
    perm_out[...] = (row == (col % PAIR) * HEADS + col // PAIR).astype(jnp.float32).astype(jnp.bfloat16)
    tab_in().wait()
    make_ready(jnp.int32(0))
    tab_out().start()
    have_own(jnp.int32(0))

    def hops(u, carry):
        first_hop(u)
        early_hop(u)
        return carry

    def relay_step(u, carry):
        relay_hop(u)
        return carry

    lax.fori_loop(0, HEADS, hops, 0)
    exchange_queries(jnp.int32(0))
    make_ready(jnp.int32(1))
    lax.fori_loop(0, RELAY_LEAD, relay_step, 0)
    have_own(jnp.int32(1))
    lax.fori_loop(HEADS, START_UNITS, hops, 0)
    exchange_queries(jnp.int32(1))
    tab_arrive().wait_recv()
    start_loads(jnp.int32(0))

    def tick(t, carry):
        @pl.when((t >= 1) & (t + 1 < BATCHES))
        def _():
            have_own(t + 1)

        @pl.when(t + 2 < BATCHES)
        def _():
            make_ready(t + 2)

        @pl.when((t % HEADS == 0) & (t // HEADS + 2 < BATCHES))
        def _():
            exchange_queries(t // HEADS + 2)

        @pl.when((t >= 1) & (t - 1 + START_UNITS < UNITS))
        def _():
            first_hop(t - 1 + START_UNITS)

        @pl.when((t >= 1) & (2 * t - 2 + START_UNITS < UNITS))
        def _():
            early_hop(2 * t - 2 + START_UNITS)
            early_hop(2 * t - 1 + START_UNITS)

        @pl.when(t + RELAY_LEAD < UNITS)
        def _():
            relay_hop(t + RELAY_LEAD)

        @pl.when((t >= 1) & (t - 1 < UNITS))
        def _():
            send_leaves(t - 1)

        @pl.when((t >= 1 + SUM_LAG) & (t - 1 - SUM_LAG < UNITS))
        def _():
            add_relays(t - 1 - SUM_LAG)

        @pl.when((t >= 1 + OWN_LAG) & (t - 1 - OWN_LAG < UNITS))
        def _():
            finish(t - 1 - OWN_LAG)

        @pl.when((t >= 1 + SUM_LAG) & (t - 1 - SUM_LAG < UNITS))
        def _():
            send_relays(t - 1 - SUM_LAG)

        @pl.when((t >= 1 + OWN_LAG) & (t - 1 - OWN_LAG < UNITS))
        def _():
            send_fin(t - 1 - OWN_LAG)

        @pl.when(t < UNITS)
        def _():
            for copy in loads(t):
                copy.wait()

            @pl.when(t + 1 < UNITS)
            def _():
                start_loads(t + 1)

            @pl.when(t >= 2)
            def _():
                wait_outs(t - 2)

            @pl.when(t >= PART_RING)
            def _():
                wait_sums(t - PART_RING)

            slot = t % 2
            unit_compute(c, q_v.at[slot], g_v.at[slot], tab_v.at[t // HEADS], kv_v.at[slot], o_v.at[slot],
                         dq_v.at[slot], part.at[t % PART_RING], kt, vt, s_a, s_b, s_e)
            for copy in out_local(t) + out_remote(t):
                copy.start()

        return carry

    lax.fori_loop(0, UNITS + 1 + OWN_LAG, tick, 0)

    tab_out().wait_send()
    for u in range(UNITS - 2, UNITS):
        wait_outs(jnp.int32(u))
    for b in range(BATCHES - 2, BATCHES):
        wait_fin(jnp.int32(b))

    def drain_batch(b, carry):
        @pl.when(b >= BATCHES - 2)
        def _():
            for half in range(2):
                kvx(b, half).wait_send()

        qx(b).wait_send()
        gx(b).wait_send()
        for copy in out_arrive(b):
            copy.wait_recv()
        for copy in fin_arrive(b):
            copy.wait_recv()
        return carry

    lax.fori_loop(0, BATCHES, drain_batch, 0)

    def drain_sums(u, carry):
        wait_sums(u)
        return carry

    lax.fori_loop(UNITS - PART_RING, UNITS, drain_sums, 0)

    def drain_kv(u, carry):
        for i, (p, step) in enumerate(early_hops + first_hops + relay_hops):
            kv_copy(u, p, i, step).wait_send()
        return carry

    lax.fori_loop(0, UNITS, drain_kv, 0)


def attend_kernel(*refs):
    me = lax.axis_index('cp')
    chip, core = me // 2, me % 2
    barrier = pltpu.get_barrier_semaphore()
    for c in range(4):
        @pl.when(chip == c)
        def _(c=c):
            for device in (2 * c + 1 - core, 2 * (c ^ X_STEP) + core, 2 * (c ^ Y_STEP) + core):
                pl.semaphore_signal(barrier, inc=1, device_id={'cp': device}, device_id_type=MESH_ID)
    pl.semaphore_wait(barrier, 3)
    for c in range(4):
        @pl.when(chip == c)
        def _(c=c):
            chip_program(c, core, *refs)


def attend(q5, g5, keys, values, tab):
    any_spec = pl.BlockSpec(memory_space=pl.ANY)
    hbm_spec = pl.BlockSpec(memory_space=pltpu.HBM)
    head_shape = pltpu.VMEM(q5.shape, jnp.bfloat16)
    half_shape = pltpu.HBM((BATCHES,) + q5.shape[1:], jnp.bfloat16)
    row_shape = pltpu.HBM((2 * BATCHES, HEADS * PAIR, DIM), jnp.bfloat16)
    head_buf = pltpu.VMEM((2, 2, PAIR, GROUP, DIM), jnp.bfloat16)
    dma = pltpu.SemaphoreType.DMA
    return pl.pallas_call(
        attend_kernel, name='attend',
        in_specs=[any_spec] * 5,
        out_specs=[any_spec] * 2 + [hbm_spec] * 5,
        out_shape=[head_shape, head_shape,
                   row_shape, row_shape,
                   pltpu.HBM((BATCHES, HEADS, 2, N_PAIRS * PAIR, DIM), jnp.bfloat16),
                   half_shape, half_shape],
        scratch_shapes=[
            head_buf, head_buf, head_buf, head_buf,
            pltpu.VMEM((2, 2, N_PAIRS * PAIR, DIM), jnp.bfloat16),
            pltpu.VMEM((BATCHES, 2, 2, PAIR, DIM), jnp.float32),
            pltpu.VMEM((2, 2, PAIR, DIM), jnp.float32),
            pltpu.VMEM((2, 2, 2, HEADS * PAIR, DIM), jnp.bfloat16),
            pltpu.VMEM((2, 2, HEADS, 2, PAIR, DIM), jnp.bfloat16),
            pltpu.VMEM((PART_RING, 2, N_PAIRS * PAIR, DIM), jnp.float32),
            pltpu.VMEM((INBOX_RING, N_INBOX, 2, PAIR, DIM), jnp.float32),
            pltpu.VMEM((2, 2, HEADS, PAIR, DIM), jnp.bfloat16),
            pltpu.VMEM((2, 2, 2, HEADS * PAIR, DIM), jnp.bfloat16),
            pltpu.VMEM((HEADS * PAIR, HEADS * PAIR), jnp.bfloat16),
            pltpu.VMEM((HEADS * PAIR, HEADS * PAIR), jnp.bfloat16),
            pltpu.VMEM((DIM, N_PAIRS * PAIR), jnp.bfloat16),
            pltpu.VMEM((DIM, N_PAIRS * PAIR), jnp.bfloat16),
            pltpu.VMEM((N_PAIRS * PAIR, 32 * GROUP), jnp.float32),
            pltpu.VMEM((N_PAIRS * PAIR, 32 * GROUP), jnp.float32),
            pltpu.VMEM((4 * PAIR, PIECE * GROUP), jnp.float32),
            dma((2, 2, 3)), dma((BATCHES, 2)), dma((BATCHES, 2)), dma((BATCHES, 2)), dma, dma,
            dma((BATCHES,)), dma((BATCHES,)), dma((BATCHES,)), dma((BATCHES,)),
            dma((UNITS, 7)), dma((UNITS, 7)), dma((N_OUTBOX, PART_RING)), dma((INBOX_RING, N_INBOX)),
            dma((6, 2)), dma((4, 2)), dma((2, BATCHES)), dma((4, 2)), dma((2, BATCHES)),
            pltpu.SemaphoreType.REGULAR((N_OUTBOX,)),
        ],
        compiler_params=pltpu.CompilerParams(
            collective_id=0, has_side_effects=True, vmem_limit_bytes=31 * 1024 * 1024),
    )(*(pltpu.with_memory_space_constraint(x, pltpu.HBM) for x in (q5, g5, keys, values, tab)))


def solution(mesh):
    head_spec = P(None, 'cp', 'tp', None)
    pos_spec = P(None, 'cp')

    def local_step(query, keys, values, positions, grad_out):
        batch, length, n_heads, dim = query.shape
        tab = rope_tables(positions, dim)
        split_shape = (batch, length, HEADS, GROUP, dim)
        row_shape = (batch, length * HEADS, dim)
        outs = attend(query.reshape(split_shape), grad_out.reshape(split_shape), keys.reshape(row_shape),
                      values.reshape(row_shape), tab)
        return tuple(out.reshape(like.shape) for out, like in zip(outs[:4], (query, query, keys, values)))

    return jax.shard_map(local_step, mesh=mesh,
                         in_specs=(head_spec, head_spec, head_spec, pos_spec, head_spec),
                         out_specs=(head_spec, head_spec, head_spec, head_spec), check_vma=False)
```

```python
import functools

import jax
import jax.numpy as jnp
from jax import lax
from jax.experimental import pallas as pl
from jax.experimental.pallas import tpu as pltpu
from jax.sharding import PartitionSpec as P

ROPE_THETA = 1000000.0
LOG2E = 1.4426950408889634
DIM = 128
GROUP = 8
HEADS = 4
PIECE = 64
PAIR = 128
N_PAIRS = 8
BATCHES = 8
UNITS = BATCHES * HEADS
KEY_BLOCK = 512
MESH_ID = pl.DeviceIdType.MESH

X_STEP, Y_STEP = 1, 2
FIRST_HOP = [(0, 0, X_STEP), (0, 0, Y_STEP), (1, 1, X_STEP), (1, 1, Y_STEP), (2, 2, X_STEP), (2, 2, Y_STEP),
             (3, 3, X_STEP), (3, 3, Y_STEP), (4, 3, X_STEP), (4, 3, Y_STEP), (5, 2, Y_STEP), (5, 2, X_STEP),
             (6, 1, X_STEP)]
RELAY_HOP = [(0, 2, X_STEP), (1, 3, X_STEP), (2, 3, Y_STEP), (3, 2, Y_STEP), (4, 1, X_STEP), (5, 3, Y_STEP)]
SUM_LEAF = [(3, 0, Y_STEP), (4, 0, X_STEP), (2, 0, Y_STEP), (6, 0, X_STEP), (2, 1, Y_STEP), (5, 1, X_STEP),
            (0, 1, X_STEP), (3, 1, Y_STEP), (1, 2, Y_STEP), (4, 2, X_STEP), (0, 3, X_STEP), (1, 3, Y_STEP)]
SUM_RELAY = [(0, 2, Y_STEP), (1, 0, X_STEP), (2, 3, X_STEP), (3, 2, X_STEP), (4, 1, Y_STEP), (5, 0, Y_STEP)]

START_BATCHES = 4
START_UNITS = 2 * START_BATCHES
HOP_LEAD = START_UNITS - 2
RELAY_LEAD = START_BATCHES
START_EARLY = 4 * START_BATCHES
EARLY_HOP = [(0, 0, X_STEP), (0, 0, Y_STEP), (1, 1, Y_STEP)]
SUM_LAG = 3
OWN_LAG = 6
PART_RING = OWN_LAG + 2
INBOX_RING = 8


def owner(pair):
    return pair if pair < 4 else 7 - pair


def inbox(chip):
    found = []
    for pair, src, step in SUM_LEAF + SUM_RELAY:
        if src ^ step == chip:
            found.append((pair, src))
    return found


def outbox(chip):
    return [(pair, step) for pair, src, step in SUM_LEAF + SUM_RELAY if src == chip]


N_INBOX = max(len(inbox(c)) for c in range(4))
N_OUTBOX = max(len(outbox(c)) for c in range(4))


def rope_tables(positions, head_dim):
    half_dim = head_dim // 2
    freq_expo = jnp.arange(half_dim, dtype=jnp.float32) * (2.0 / head_dim)
    inv_freq = 1.0 / (ROPE_THETA ** freq_expo)
    angles = positions.astype(jnp.float32)[:, :, None] * inv_freq
    cosine, sine_val = jnp.cos(angles), jnp.sin(angles)
    cos_l = jnp.repeat(cosine, 2, axis=-1)
    sin_l = jnp.stack([-sine_val, sine_val], axis=-1).reshape(cos_l.shape)
    return jnp.stack([cos_l, sin_l], axis=1)


def dot_nn(a, b):
    return jnp.dot(a, b, preferred_element_type=jnp.float32)


def dot_nt(a, b):
    return lax.dot_general(a, b, (((1,), (1,)), ((), ())), preferred_element_type=jnp.float32)


def iota(shape, axis):
    return lax.broadcasted_iota(jnp.int32, shape, axis)


def identity():
    return (iota((DIM, DIM), 0) == iota((DIM, DIM), 1)).astype(jnp.float32).astype(jnp.bfloat16)


def swap_pairs(x):
    return jnp.where(iota(x.shape, 1) % 2 == 0, pltpu.roll(x, DIM - 1, axis=1), pltpu.roll(x, 1, axis=1))


def rows_steps(n_keys, tok, seg, q_v, g_v, tab, kv, kt, vt, part, o_v, dq_v, s_ref):
    core, start, place = seg
    rows = tok * GROUP
    scale = DIM ** -0.5
    c1 = scale * LOG2E
    toks = pl.ds(start, tok)

    def table(k):
        return jnp.broadcast_to(tab[k, core, toks, :][:, None, :], (tok, GROUP, DIM)).reshape(rows, DIM)

    x = q_v[core, toks].astype(jnp.float32).reshape(rows, DIM)
    qr = (x * table(0) + swap_pairs(x) * table(1)).astype(jnp.bfloat16)
    g = g_v[core, toks].astype(jnp.float32).reshape(rows, DIM).astype(jnp.bfloat16)
    blocks = [(a, min(KEY_BLOCK, n_keys - a)) for a in range(0, n_keys, KEY_BLOCK)]
    m8 = None
    for a, n in blocks:
        s = dot_nt(kv[0, a:a + n, :], qr) * c1
        if a + n == n_keys:
            last = s[n - PAIR:, :]
            q_tok = iota(last.shape, 1) // GROUP + place
            last = jnp.where(iota(last.shape, 0) <= q_tok, last, -jnp.inf)
            s = last if n == PAIR else jnp.concatenate([s[:n - PAIR, :], last], axis=0)
        s_ref[a:a + n, :] = s
        f = jnp.max(s.reshape(n // 8, 8, rows), axis=0)
        m8 = f if m8 is None else jnp.maximum(m8, f)
        yield
    row_max = jnp.max(m8, axis=0, keepdims=True)
    l8 = None
    o_t = None
    for a, n in blocks:
        p = jnp.exp2(s_ref[a:a + n, :] - row_max)
        s_ref[a:a + n, :] = p
        f = jnp.sum(p.reshape(n // 8, 8, rows), axis=0)
        l8 = f if l8 is None else l8 + f
        d = dot_nn(vt[:, a:a + n], p.astype(jnp.bfloat16))
        o_t = d if o_t is None else o_t + d
        yield
    inv = 1.0 / jnp.sum(l8, axis=0, keepdims=True)
    out_t = o_t * inv
    o_v[core, toks] = jnp.transpose(out_t).reshape(tok, GROUP, DIM).astype(jnp.bfloat16)
    delta = jnp.sum(dot_nt(identity(), g) * out_t, axis=0, keepdims=True)
    yield
    dq_t = None
    for a, n in blocks:
        p = s_ref[a:a + n, :] * inv
        ds = (p * (dot_nt(kv[1, a:a + n, :], g) - delta)).astype(jnp.bfloat16)
        part[1, a:a + n, :] += dot_nn(p.astype(jnp.bfloat16), g)
        part[0, a:a + n, :] += dot_nn(ds, qr)
        d = dot_nn(kt[:, a:a + n], ds)
        dq_t = d if dq_t is None else dq_t + d
        yield
    dq = jnp.transpose(dq_t) * scale
    dq = dq * table(0) - swap_pairs(dq) * table(1)
    dq_v[core, toks] = dq.reshape(tok, GROUP, DIM).astype(jnp.bfloat16)


def interleave(gens, lag):
    live, waiting, count = [], list(gens), 0
    while live or waiting:
        if waiting and (not live or count >= lag):
            live.append(waiting.pop(0))
            count = 0
        for gen in list(live):
            if next(gen, 'end') == 'end':
                live.remove(gen)
        count += 1


def unit_compute(c, q_v, g_v, tab, kv, o_v, dq_v, part, kt, vt, s_a, s_b, s_e):
    n_late, n_early = (N_PAIRS - c) * PAIR, (c + 1) * PAIR
    eye = identity()
    for a in range(0, n_late, 256):
        n = min(256, n_late - a)
        kt[:, a:a + n] = dot_nt(eye, kv[0, a:a + n, :]).astype(jnp.bfloat16)
        vt[:, a:a + n] = dot_nt(eye, kv[1, a:a + n, :]).astype(jnp.bfloat16)
    part[:, :n_late, :] = jnp.zeros((2, n_late, DIM), jnp.float32)
    refs = (q_v, g_v, tab, kv, kt, vt, part, o_v, dq_v)

    def step(i, carry):
        late = [rows_steps(n_late, 32, (1 - i, PIECE + 32 * k, i * PIECE + 32 * k), *refs, s)
                for k, s in ((0, s_a), (1, s_b))]
        early = rows_steps(n_early, PIECE, (i, 0, i * PIECE), *refs, s_e)
        interleave(late + [early], 2 * pl.cdiv(n_late, KEY_BLOCK) + 1)
        return carry

    lax.fori_loop(0, 2, step, 0)


def remote(src, dst, send_sem, recv_sem, device):
    return pltpu.make_async_remote_copy(src_ref=src, dst_ref=dst, send_sem=send_sem, recv_sem=recv_sem,
                                        device_id={'cp': device}, device_id_type=MESH_ID)


def chip_program(c, core, barrier, q_hbm, g_hbm, k_hbm, v_hbm, tab_hbm, o_hbm, dq_hbm, gk_hbm, gv_hbm, kv_hbm, qs_hbm, gs_hbm,
                 q_v, g_v, o_v, dq_v, kv_v, tab_v, tab_x, raw_v, ready_v, part, recv, fin_st, fin_v,
                 perm_in, perm_out, kt, vt, s_a, s_b, s_e,
                 raw_s, kvl_s, kvx_s, kvx_r, tab_s, tab_r, qx_s, qx_r, gx_s, gx_r, ag_s, ag_r, sum_s, sum_r,
                 load_s, out_s, out_r, fin_s, fin_r, credit):
    n_late = (N_PAIRS - c) * PAIR
    sib = 2 * c + 1 - core
    nbr = {step: 2 * (c ^ step) + core for step in (X_STEP, Y_STEP)}
    mine, other = BATCHES * core, BATCHES * (1 - core)
    early_hops = [(p, step) for p, src, step in EARLY_HOP if src == c]
    first_hops = [(p, step) for p, src, step in FIRST_HOP if src == c and (p, src, step) not in EARLY_HOP]
    relay_hops = [(p, step) for p, src, step in RELAY_HOP if src == c]
    leaves = [(p, step) for p, src, step in SUM_LEAF if src == c]
    relays = [(p, step) for p, src, step in SUM_RELAY if src == c]
    needed = [p for p in range(N_PAIRS - c) if owner(p) != c]
    sib_pieces = (2 * c + 1 - core, 15 - 2 * c - (1 - core))

    def split(u):
        return u // HEADS, u % HEADS

    def pair_rows(p):
        return pl.ds(p * PAIR, PAIR)

    own_pieces = (2 * c + core, 15 - 2 * c - core)

    def raw_in(b, side):
        src, slot = (mine, other)[side] + b, b % 2
        copies = [pltpu.make_async_copy(k_hbm.at[src], raw_v.at[slot, side, 0], raw_s.at[slot, side, 0]),
                  pltpu.make_async_copy(v_hbm.at[src], raw_v.at[slot, side, 1], raw_s.at[slot, side, 1])]
        if side:
            copies.append(pltpu.make_async_copy(tab_hbm.at[src], tab_x.at[slot], raw_s.at[slot, side, 2]))
        return copies

    def start_raw(b):
        for side in (1, 0):
            for copy in raw_in(b, side):
                copy.start()

    def piece_rows(piece):
        return pl.ds(pl.multiple_of(piece * PIECE, PIECE), PIECE)

    def own_out(b, half):
        return pltpu.make_async_copy(ready_v.at[b % 2, 0, :, :, pl.ds(half * PIECE, PIECE), :],
                                     kv_hbm.at[b, :, :, piece_rows(own_pieces[half]), :], kvl_s.at[b, half])

    def kvx(b, half):
        return remote(ready_v.at[b % 2, 1, :, :, pl.ds(half * PIECE, PIECE), :],
                      kv_hbm.at[b, :, :, piece_rows(own_pieces[half]), :], kvx_s.at[b, half], kvx_r.at[b, half], sib)

    def kvx_in(b, half):
        dst = kv_hbm.at[b, :, :, piece_rows(sib_pieces[half]), :]
        return remote(dst, dst, kvx_s.at[b, half], kvx_r.at[b, half], sib)

    def make_ready(b):
        slot = b % 2

        @pl.when(b >= 2)
        def _():
            for half in range(2):
                kvx(b - 2, half).wait_send()

        for side in (1, 0):
            for copy in raw_in(b, side):
                copy.wait()
            tab = tab_x.at[slot] if side else tab_v.at[b, :, core]
            k_rows = dot_nn(perm_in[...], raw_v[slot, side, 0])
            v_rows = dot_nn(perm_in[...], raw_v[slot, side, 1])
            for h in range(HEADS):
                x = k_rows[h * PAIR:(h + 1) * PAIR]
                ready_v[slot, side, h, 0] = (x * tab[0] + swap_pairs(x) * tab[1]).astype(jnp.bfloat16)
                ready_v[slot, side, h, 1] = v_rows[h * PAIR:(h + 1) * PAIR].astype(jnp.bfloat16)
        for half in range(2):
            own_out(b, half).start()

        @pl.when(b + 2 < BATCHES)
        def _():
            start_raw(b + 2)

    def send_ready(b):
        for half in range(2):
            kvx(b, half).start()

    def qx(b):
        return remote(q_hbm.at[other + b], qs_hbm.at[b], qx_s.at[b], qx_r.at[b], sib)

    def gx(b):
        return remote(g_hbm.at[other + b], gs_hbm.at[b], gx_s.at[b], gx_r.at[b], sib)

    def tab_in():
        return pltpu.make_async_copy(tab_hbm.at[pl.ds(mine, BATCHES)], tab_v.at[:, :, core], load_s.at[5, 0])

    def tab_out():
        return remote(tab_hbm.at[pl.ds(other, BATCHES)], tab_v.at[:, :, core], tab_s, tab_r, sib)

    def tab_arrive():
        return remote(tab_hbm.at[pl.ds(other, BATCHES)], tab_v.at[:, :, 1 - core], tab_s, tab_r, sib)

    def kv_copy(u, p, slot, step):
        b, h = split(u)
        ref = kv_hbm.at[b, h, :, pair_rows(p), :]
        return remote(ref, ref, ag_s.at[u, slot], ag_r.at[u, p], nbr[step])

    def send_kv(u, hops, base):
        for i, (p, step) in enumerate(hops):
            kv_copy(u, p, base + i, step).start()

    def have_own(b):
        for half in range(2):
            own_out(b, half).wait()
            kvx_in(b, half).wait_recv()

    def early_hop(u):
        send_kv(u, early_hops, 0)

    def first_hop(u):
        send_kv(u, first_hops, len(early_hops))

    def relay_hop(u):
        for p, _ in relay_hops:
            kv_copy(u, p, 0, X_STEP).wait_recv()
        send_kv(u, relay_hops, len(early_hops) + len(first_hops))

    def loads(u):
        b, h = split(u)
        slot = u % 2
        late = pl.ds(0, n_late)
        return [
            pltpu.make_async_copy(q_hbm.at[mine + b, :, h], q_v.at[slot, core], load_s.at[0, slot]),
            pltpu.make_async_copy(g_hbm.at[mine + b, :, h], g_v.at[slot, core], load_s.at[1, slot]),
            pltpu.make_async_copy(qs_hbm.at[b, :, h], q_v.at[slot, 1 - core], load_s.at[2, slot]),
            pltpu.make_async_copy(gs_hbm.at[b, :, h], g_v.at[slot, 1 - core], load_s.at[3, slot]),
            pltpu.make_async_copy(kv_hbm.at[b, h, :, late, :], kv_v.at[slot, :, late, :], load_s.at[4, slot]),
        ]

    def start_loads(u):
        @pl.when(u % HEADS == 0)
        def _():
            qx(u // HEADS).wait_recv()
            gx(u // HEADS).wait_recv()

        for p in needed:
            if p not in [r for r, _ in relay_hops]:
                kv_copy(u, p, 0, X_STEP).wait_recv()
        for copy in loads(u):
            copy.start()

    def out_local(u):
        b, h = split(u)
        slot = u % 2
        return [pltpu.make_async_copy(o_v.at[slot, core], o_hbm.at[mine + b, :, h], out_s.at[0, slot]),
                pltpu.make_async_copy(dq_v.at[slot, core], dq_hbm.at[mine + b, :, h], out_s.at[1, slot])]

    def out_remote(u):
        b, h = split(u)
        slot = u % 2
        return [remote(o_v.at[slot, 1 - core], o_hbm.at[mine + b, :, h], out_s.at[2, slot], out_r.at[0, b], sib),
                remote(dq_v.at[slot, 1 - core], dq_hbm.at[mine + b, :, h], out_s.at[3, slot], out_r.at[1, b], sib)]

    def out_arrive(b):
        return [remote(q_hbm.at[other + b], o_hbm.at[other + b], out_s.at[2, 0], out_r.at[0, b], sib),
                remote(q_hbm.at[other + b], dq_hbm.at[other + b], out_s.at[3, 0], out_r.at[1, b], sib)]

    def wait_outs(u):
        for copy in out_local(u):
            copy.wait()
        for copy in out_remote(u):
            copy.wait_send()

    def sum_copy(u, p, i, step):
        k, slot = inbox(c ^ step).index((p, c)), u % INBOX_RING
        return remote(part.at[u % PART_RING, :, pair_rows(p), :], recv.at[slot, k],
                      sum_s.at[i, u % PART_RING], sum_r.at[slot, k], nbr[step])

    def sum_arrive(u, k):
        dst = recv.at[u % INBOX_RING, k]
        return remote(dst, dst, sum_s.at[0, 0], sum_r.at[u % INBOX_RING, k], nbr[X_STEP])

    def give_credits(u, pairs):
        @pl.when(u + INBOX_RING < UNITS)
        def _():
            for k, (pair, src) in enumerate(inbox(c)):
                if pair in pairs:
                    pl.semaphore_signal(credit.at[outbox(src).index((pair, src ^ c))], inc=1,
                                        device_id={'cp': 2 * src + core}, device_id_type=MESH_ID)

    def take_credits(u, which):
        @pl.when(u >= INBOX_RING)
        def _():
            for i in which:
                pl.semaphore_wait(credit.at[i], 1)

    def messages(p):
        return [k for k, (pair, _) in enumerate(inbox(c)) if pair == p]

    def wait_sums(u):
        for i, (p, step) in enumerate(leaves + relays):
            sum_copy(u, p, i, step).wait_send()

    def send_leaves(u):
        take_credits(u, range(len(leaves)))
        for i, (p, step) in enumerate(leaves):
            sum_copy(u, p, i, step).start()

    def add_relays(u):
        for p, _ in relays:
            for k in messages(p):
                sum_arrive(u, k).wait_recv()
                part[u % PART_RING, :, pair_rows(p), :] += recv[u % INBOX_RING, k]
        give_credits(u, [p for p, _ in relays])

    def send_relays(u):
        take_credits(u, range(len(leaves), len(leaves) + len(relays)))
        for i, (p, step) in enumerate(relays):
            sum_copy(u, p, len(leaves) + i, step).start()

    def fin_local(b):
        return [pltpu.make_async_copy(fin_v.at[b % 2, core, i], (gk_hbm, gv_hbm)[i].at[mine + b], fin_s.at[i, b % 2])
                for i in range(2)]

    def fin_remote(b):
        return [remote(fin_v.at[b % 2, 1 - core, i], (gk_hbm, gv_hbm)[i].at[mine + b], fin_s.at[2 + i, b % 2],
                       fin_r.at[i, b], sib) for i in range(2)]

    def fin_arrive(b):
        return [remote(dst.at[other + b], dst.at[other + b], fin_s.at[2 + i, 0], fin_r.at[i, b], sib)
                for i, dst in enumerate((gk_hbm, gv_hbm))]

    def wait_fin(b):
        for copy in fin_local(b):
            copy.wait()
        for copy in fin_remote(b):
            copy.wait_send()

    def finish(u):
        b, h = split(u)
        for late, p in ((0, c), (1, N_PAIRS - 1 - c)):
            total = part[u % PART_RING, :, pair_rows(p), :]
            for k in messages(p):
                sum_arrive(u, k).wait_recv()
                total = total + recv[u % INBOX_RING, k]
            for i in range(2):
                who = 1 - i if late else i
                toks = slice(late * PIECE, (late + 1) * PIECE)
                dk = total[0, i * PIECE:(i + 1) * PIECE] * (DIM ** -0.5)
                dk = dk * tab_v[b, 0, who, toks] - swap_pairs(dk) * tab_v[b, 1, who, toks]
                fin_st[who, 0, h, toks] = dk.astype(jnp.bfloat16)
                fin_st[who, 1, h, toks] = total[1, i * PIECE:(i + 1) * PIECE].astype(jnp.bfloat16)
        give_credits(u, [c, N_PAIRS - 1 - c])

        @pl.when(h == HEADS - 1)
        def _():
            @pl.when(b >= 2)
            def _():
                wait_fin(b - 2)

            for who in range(2):
                for i in range(2):
                    rows = fin_st[who, i].reshape(HEADS * PAIR, DIM)
                    fin_v[b % 2, who, i] = dot_nn(perm_out[...], rows).astype(jnp.bfloat16)

    def send_fin(u):
        @pl.when(u % HEADS == HEADS - 1)
        def _():
            for copy in fin_local(u // HEADS) + fin_remote(u // HEADS):
                copy.start()

    def exchange_queries(b):
        qx(b).start()
        gx(b).start()

    for device in (sib, nbr[X_STEP], nbr[Y_STEP]):
        pl.semaphore_signal(barrier, inc=1, device_id={'cp': device}, device_id_type=MESH_ID)
    start_raw(jnp.int32(0))
    tab_in().start()
    start_raw(jnp.int32(1))
    row, col = iota((HEADS * PAIR, HEADS * PAIR), 0), iota((HEADS * PAIR, HEADS * PAIR), 1)
    perm_in[...] = (col == (row % PAIR) * HEADS + row // PAIR).astype(jnp.float32).astype(jnp.bfloat16)
    tab_in().wait()

    def up_to(op, first, last):
        def one(u, carry):
            op(u)
            return carry

        lax.fori_loop(first, last, one, 0)

    def start_step(j, carry):
        make_ready(j)

        @pl.when(j == 0)
        def _():
            pl.semaphore_wait(barrier, 3)

        send_ready(j)

        @pl.when(j == 0)
        def _():
            tab_out().start()
            have_own(j)
            exchange_queries(j)

        up_to(relay_hop, jnp.maximum(j - 1, 0), j + j // 3)
        up_to(first_hop, 2 * j, 2 * j + 2)

        @pl.when(j >= 1)
        def _():
            have_own(j)

        up_to(early_hop, 4 * j, 4 * j + 4)
        return carry

    lax.fori_loop(0, START_BATCHES, start_step, 0)
    row, col = iota((HEADS * PAIR, HEADS * PAIR), 0), iota((HEADS * PAIR, HEADS * PAIR), 1)
    perm_out[...] = (row == (col % PAIR) * HEADS + col // PAIR).astype(jnp.float32).astype(jnp.bfloat16)
    tab_arrive().wait_recv()
    start_loads(jnp.int32(0))

    def tick(t, carry):
        @pl.when((t % 2 == 0) & (t // 2 + 4 < BATCHES))
        def _():
            make_ready(t // 2 + 4)
            send_ready(t // 2 + 4)

        @pl.when((t % 2 == 1) & (t // 2 + 4 < BATCHES))
        def _():
            have_own(t // 2 + 4)

        @pl.when((t % HEADS == 0) & (t // HEADS + 1 < BATCHES))
        def _():
            exchange_queries(t // HEADS + 1)

        @pl.when((t == 0) & (START_UNITS < UNITS))
        def _():
            first_hop(t + START_UNITS)

        @pl.when((t + HOP_LEAD > START_UNITS) & (t + HOP_LEAD < UNITS))
        def _():
            first_hop(t + HOP_LEAD)

        @pl.when((t >= 1) & (2 * t - 2 + START_EARLY < UNITS))
        def _():
            early_hop(2 * t - 2 + START_EARLY)
            early_hop(2 * t - 1 + START_EARLY)

        @pl.when(t + RELAY_LEAD < UNITS)
        def _():
            relay_hop(t + RELAY_LEAD)

        @pl.when((t >= 1) & (t - 1 < UNITS))
        def _():
            send_leaves(t - 1)

        @pl.when((t >= 1 + SUM_LAG) & (t - 1 - SUM_LAG < UNITS))
        def _():
            add_relays(t - 1 - SUM_LAG)

        @pl.when((t >= 1 + OWN_LAG) & (t - 1 - OWN_LAG < UNITS))
        def _():
            finish(t - 1 - OWN_LAG)

        @pl.when((t >= 1 + SUM_LAG) & (t - 1 - SUM_LAG < UNITS))
        def _():
            send_relays(t - 1 - SUM_LAG)

        @pl.when((t >= 1 + OWN_LAG) & (t - 1 - OWN_LAG < UNITS))
        def _():
            send_fin(t - 1 - OWN_LAG)

        @pl.when(t < UNITS)
        def _():
            for copy in loads(t):
                copy.wait()

            @pl.when(t + 1 < UNITS)
            def _():
                start_loads(t + 1)

            @pl.when(t >= 2)
            def _():
                wait_outs(t - 2)

            @pl.when(t >= PART_RING)
            def _():
                wait_sums(t - PART_RING)

            slot = t % 2
            unit_compute(c, q_v.at[slot], g_v.at[slot], tab_v.at[t // HEADS], kv_v.at[slot], o_v.at[slot],
                         dq_v.at[slot], part.at[t % PART_RING], kt, vt, s_a, s_b, s_e)
            for copy in out_local(t) + out_remote(t):
                copy.start()

        return carry

    lax.fori_loop(0, UNITS + 1 + OWN_LAG, tick, 0)

    tab_out().wait_send()
    for u in range(UNITS - 2, UNITS):
        wait_outs(jnp.int32(u))
    for b in range(BATCHES - 2, BATCHES):
        wait_fin(jnp.int32(b))

    def drain_batch(b, carry):
        @pl.when(b >= BATCHES - 2)
        def _():
            for half in range(2):
                kvx(b, half).wait_send()

        qx(b).wait_send()
        gx(b).wait_send()
        for copy in out_arrive(b):
            copy.wait_recv()
        for copy in fin_arrive(b):
            copy.wait_recv()
        return carry

    lax.fori_loop(0, BATCHES, drain_batch, 0)

    def drain_sums(u, carry):
        wait_sums(u)
        return carry

    lax.fori_loop(UNITS - PART_RING, UNITS, drain_sums, 0)

    def drain_kv(u, carry):
        for i, (p, step) in enumerate(early_hops + first_hops + relay_hops):
            kv_copy(u, p, i, step).wait_send()
        return carry

    lax.fori_loop(0, UNITS, drain_kv, 0)


def attend_kernel(*refs):
    me = lax.axis_index('cp')
    chip, core = me // 2, me % 2
    barrier = pltpu.get_barrier_semaphore()
    for c in range(4):
        @pl.when(chip == c)
        def _(c=c):
            chip_program(c, core, barrier, *refs)


def attend(q5, g5, keys, values, tab):
    any_spec = pl.BlockSpec(memory_space=pl.ANY)
    hbm_spec = pl.BlockSpec(memory_space=pltpu.HBM)
    head_shape = pltpu.VMEM(q5.shape, jnp.bfloat16)
    half_shape = pltpu.HBM((BATCHES,) + q5.shape[1:], jnp.bfloat16)
    row_shape = pltpu.HBM((2 * BATCHES, HEADS * PAIR, DIM), jnp.bfloat16)
    head_buf = pltpu.VMEM((2, 2, PAIR, GROUP, DIM), jnp.bfloat16)
    dma = pltpu.SemaphoreType.DMA
    return pl.pallas_call(
        attend_kernel, name='attend',
        in_specs=[any_spec] * 5,
        out_specs=[any_spec] * 2 + [hbm_spec] * 5,
        out_shape=[head_shape, head_shape,
                   row_shape, row_shape,
                   pltpu.HBM((BATCHES, HEADS, 2, N_PAIRS * PAIR, DIM), jnp.bfloat16),
                   half_shape, half_shape],
        scratch_shapes=[
            head_buf, head_buf, head_buf, head_buf,
            pltpu.VMEM((2, 2, N_PAIRS * PAIR, DIM), jnp.bfloat16),
            pltpu.VMEM((BATCHES, 2, 2, PAIR, DIM), jnp.float32),
            pltpu.VMEM((2, 2, PAIR, DIM), jnp.float32),
            pltpu.VMEM((2, 2, 2, HEADS * PAIR, DIM), jnp.bfloat16),
            pltpu.VMEM((2, 2, HEADS, 2, PAIR, DIM), jnp.bfloat16),
            pltpu.VMEM((PART_RING, 2, N_PAIRS * PAIR, DIM), jnp.float32),
            pltpu.VMEM((INBOX_RING, N_INBOX, 2, PAIR, DIM), jnp.float32),
            pltpu.VMEM((2, 2, HEADS, PAIR, DIM), jnp.bfloat16),
            pltpu.VMEM((2, 2, 2, HEADS * PAIR, DIM), jnp.bfloat16),
            pltpu.VMEM((HEADS * PAIR, HEADS * PAIR), jnp.bfloat16),
            pltpu.VMEM((HEADS * PAIR, HEADS * PAIR), jnp.bfloat16),
            pltpu.VMEM((DIM, N_PAIRS * PAIR), jnp.bfloat16),
            pltpu.VMEM((DIM, N_PAIRS * PAIR), jnp.bfloat16),
            pltpu.VMEM((N_PAIRS * PAIR, 32 * GROUP), jnp.float32),
            pltpu.VMEM((N_PAIRS * PAIR, 32 * GROUP), jnp.float32),
            pltpu.VMEM((4 * PAIR, PIECE * GROUP), jnp.float32),
            dma((2, 2, 3)), dma((BATCHES, 2)), dma((BATCHES, 2)), dma((BATCHES, 2)), dma, dma,
            dma((BATCHES,)), dma((BATCHES,)), dma((BATCHES,)), dma((BATCHES,)),
            dma((UNITS, 7)), dma((UNITS, 7)), dma((N_OUTBOX, PART_RING)), dma((INBOX_RING, N_INBOX)),
            dma((6, 2)), dma((4, 2)), dma((2, BATCHES)), dma((4, 2)), dma((2, BATCHES)),
            pltpu.SemaphoreType.REGULAR((N_OUTBOX,)),
        ],
        compiler_params=pltpu.CompilerParams(
            collective_id=0, has_side_effects=True, vmem_limit_bytes=32512 * 1024),
    )(*(pltpu.with_memory_space_constraint(x, pltpu.HBM) for x in (q5, g5, keys, values, tab)))


def solution(mesh):
    head_spec = P(None, 'cp', 'tp', None)
    pos_spec = P(None, 'cp')

    def local_step(query, keys, values, positions, grad_out):
        batch, length, n_heads, dim = query.shape
        tab = rope_tables(positions, dim)
        split_shape = (batch, length, HEADS, GROUP, dim)
        row_shape = (batch, length * HEADS, dim)
        outs = attend(query.reshape(split_shape), grad_out.reshape(split_shape), keys.reshape(row_shape),
                      values.reshape(row_shape), tab)
        return tuple(out.reshape(like.shape) for out, like in zip(outs[:4], (query, query, keys, values)))

    return jax.shard_map(local_step, mesh=mesh,
                         in_specs=(head_spec, head_spec, head_spec, pos_spec, head_spec),
                         out_specs=(head_spec, head_spec, head_spec, head_spec), check_vma=False)
```

```python
import functools

import jax
import jax.numpy as jnp
from jax import lax
from jax.experimental import pallas as pl
from jax.experimental.pallas import tpu as pltpu
from jax.sharding import PartitionSpec as P

ROPE_THETA = 1000000.0
LOG2E = 1.4426950408889634
DIM = 128
GROUP = 8
HEADS = 4
PIECE = 64
PAIR = 128
N_PAIRS = 8
BATCHES = 8
UNITS = BATCHES * HEADS
KEY_BLOCK = 512
MESH_ID = pl.DeviceIdType.MESH

X_STEP, Y_STEP = 1, 2
FIRST_HOP = [(0, 0, X_STEP), (0, 0, Y_STEP), (1, 1, X_STEP), (1, 1, Y_STEP), (2, 2, X_STEP), (2, 2, Y_STEP),
             (3, 3, X_STEP), (3, 3, Y_STEP), (4, 3, X_STEP), (4, 3, Y_STEP), (5, 2, Y_STEP), (5, 2, X_STEP),
             (6, 1, X_STEP)]
RELAY_HOP = [(0, 2, X_STEP), (1, 3, X_STEP), (2, 3, Y_STEP), (3, 2, Y_STEP), (4, 1, X_STEP), (5, 3, Y_STEP)]
SUM_LEAF = [(3, 0, Y_STEP), (4, 0, X_STEP), (2, 0, Y_STEP), (6, 0, X_STEP), (2, 1, Y_STEP), (5, 1, X_STEP),
            (0, 1, X_STEP), (3, 1, Y_STEP), (1, 2, Y_STEP), (4, 2, X_STEP), (0, 3, X_STEP), (1, 3, Y_STEP)]
SUM_RELAY = [(0, 2, Y_STEP), (1, 0, X_STEP), (2, 3, X_STEP), (3, 2, X_STEP), (4, 1, Y_STEP), (5, 0, Y_STEP)]

START_BATCHES = 4
START_UNITS = 2 * START_BATCHES
HOP_LEAD = START_UNITS - 2
RELAY_LEAD = START_BATCHES
START_EARLY = 4 * START_BATCHES
EARLY_HOP = [(0, 0, X_STEP), (0, 0, Y_STEP), (1, 1, Y_STEP)]
SUM_LAG = 3
OWN_LAG = 6
PART_RING = OWN_LAG + 2
INBOX_RING = 8


def owner(pair):
    return pair if pair < 4 else 7 - pair


def inbox(chip):
    found = []
    for pair, src, step in SUM_LEAF + SUM_RELAY:
        if src ^ step == chip:
            found.append((pair, src))
    return found


def outbox(chip):
    return [(pair, step) for pair, src, step in SUM_LEAF + SUM_RELAY if src == chip]


N_INBOX = max(len(inbox(c)) for c in range(4))
N_OUTBOX = max(len(outbox(c)) for c in range(4))


def lane_freq(head_dim):
    half_dim = head_dim // 2
    freq_expo = jnp.arange(half_dim, dtype=jnp.float32) * (2.0 / head_dim)
    return jnp.repeat(1.0 / (ROPE_THETA ** freq_expo), 2)[None, :]


def dot_nn(a, b):
    return jnp.dot(a, b, preferred_element_type=jnp.float32)


def dot_nt(a, b):
    return lax.dot_general(a, b, (((1,), (1,)), ((), ())), preferred_element_type=jnp.float32)


def iota(shape, axis):
    return lax.broadcasted_iota(jnp.int32, shape, axis)


def identity():
    return (iota((DIM, DIM), 0) == iota((DIM, DIM), 1)).astype(jnp.float32).astype(jnp.bfloat16)


def swap_pairs(x):
    return jnp.where(iota(x.shape, 1) % 2 == 0, pltpu.roll(x, DIM - 1, axis=1), pltpu.roll(x, 1, axis=1))


def rows_steps(n_keys, tok, seg, q_v, g_v, tab, kv, kt, vt, part, o_v, dq_v, s_ref):
    core, start, place = seg
    rows = tok * GROUP
    scale = DIM ** -0.5
    c1 = scale * LOG2E
    toks = pl.ds(start, tok)

    def table(k):
        return jnp.broadcast_to(tab[k, core, toks, :][:, None, :], (tok, GROUP, DIM)).reshape(rows, DIM)

    x = q_v[core, toks].astype(jnp.float32).reshape(rows, DIM)
    qr = (x * table(0) + swap_pairs(x) * table(1)).astype(jnp.bfloat16)
    g = g_v[core, toks].astype(jnp.float32).reshape(rows, DIM).astype(jnp.bfloat16)
    blocks = [(a, min(KEY_BLOCK, n_keys - a)) for a in range(0, n_keys, KEY_BLOCK)]
    m8 = None
    for a, n in blocks:
        s = dot_nt(kv[0, a:a + n, :], qr) * c1
        if a + n == n_keys:
            last = s[n - PAIR:, :]
            q_tok = iota(last.shape, 1) // GROUP + place
            last = jnp.where(iota(last.shape, 0) <= q_tok, last, -jnp.inf)
            s = last if n == PAIR else jnp.concatenate([s[:n - PAIR, :], last], axis=0)
        s_ref[a:a + n, :] = s
        f = jnp.max(s.reshape(n // 8, 8, rows), axis=0)
        m8 = f if m8 is None else jnp.maximum(m8, f)
        yield
    row_max = jnp.max(m8, axis=0, keepdims=True)
    l8 = None
    o_t = None
    for a, n in blocks:
        p = jnp.exp2(s_ref[a:a + n, :] - row_max)
        s_ref[a:a + n, :] = p
        f = jnp.sum(p.reshape(n // 8, 8, rows), axis=0)
        l8 = f if l8 is None else l8 + f
        d = dot_nn(vt[:, a:a + n], p.astype(jnp.bfloat16))
        o_t = d if o_t is None else o_t + d
        yield
    inv = 1.0 / jnp.sum(l8, axis=0, keepdims=True)
    out_t = o_t * inv
    o_v[core, toks] = jnp.transpose(out_t).reshape(tok, GROUP, DIM).astype(jnp.bfloat16)
    delta = jnp.sum(dot_nt(identity(), g) * out_t, axis=0, keepdims=True)
    yield
    dq_t = None
    for a, n in blocks:
        p = s_ref[a:a + n, :] * inv
        ds = (p * (dot_nt(kv[1, a:a + n, :], g) - delta)).astype(jnp.bfloat16)
        part[1, a:a + n, :] += dot_nn(p.astype(jnp.bfloat16), g)
        part[0, a:a + n, :] += dot_nn(ds, qr)
        d = dot_nn(kt[:, a:a + n], ds)
        dq_t = d if dq_t is None else dq_t + d
        yield
    dq = jnp.transpose(dq_t) * scale
    dq = dq * table(0) - swap_pairs(dq) * table(1)
    dq_v[core, toks] = dq.reshape(tok, GROUP, DIM).astype(jnp.bfloat16)


def interleave(gens, lag):
    live, waiting, count = [], list(gens), 0
    while live or waiting:
        if waiting and (not live or count >= lag):
            live.append(waiting.pop(0))
            count = 0
        for gen in list(live):
            if next(gen, 'end') == 'end':
                live.remove(gen)
        count += 1


def unit_compute(c, q_v, g_v, tab, kv, o_v, dq_v, part, kt, vt, s_a, s_b, s_e):
    n_late, n_early = (N_PAIRS - c) * PAIR, (c + 1) * PAIR
    eye = identity()
    for a in range(0, n_late, 256):
        n = min(256, n_late - a)
        kt[:, a:a + n] = dot_nt(eye, kv[0, a:a + n, :]).astype(jnp.bfloat16)
        vt[:, a:a + n] = dot_nt(eye, kv[1, a:a + n, :]).astype(jnp.bfloat16)
    part[:, :n_late, :] = jnp.zeros((2, n_late, DIM), jnp.float32)
    refs = (q_v, g_v, tab, kv, kt, vt, part, o_v, dq_v)

    def step(i, carry):
        late = [rows_steps(n_late, 32, (1 - i, PIECE + 32 * k, i * PIECE + 32 * k), *refs, s)
                for k, s in ((0, s_a), (1, s_b))]
        early = rows_steps(n_early, PIECE, (i, 0, i * PIECE), *refs, s_e)
        interleave(late + [early], 2 * pl.cdiv(n_late, KEY_BLOCK) + 1)
        return carry

    lax.fori_loop(0, 2, step, 0)


def remote(src, dst, send_sem, recv_sem, device):
    return pltpu.make_async_remote_copy(src_ref=src, dst_ref=dst, send_sem=send_sem, recv_sem=recv_sem,
                                        device_id={'cp': device}, device_id_type=MESH_ID)


def chip_program(c, core, barrier, q_hbm, g_hbm, k_hbm, v_hbm, pos_hbm, freq_hbm, o_hbm, dq_hbm, gk_hbm, gv_hbm, kv_hbm, qs_hbm, gs_hbm,
                 q_v, g_v, o_v, dq_v, kv_v, tab_v, tab_x, pos_v, freq_v, raw_v, ready_v, part, recv, fin_st, fin_v,
                 perm_in, perm_out, kt, vt, s_a, s_b, s_e,
                 raw_s, kvl_s, kvx_s, kvx_r, tab_s, tab_r, qx_s, qx_r, gx_s, gx_r, ag_s, ag_r, sum_s, sum_r,
                 load_s, out_s, out_r, fin_s, fin_r, credit):
    n_late = (N_PAIRS - c) * PAIR
    sib = 2 * c + 1 - core
    nbr = {step: 2 * (c ^ step) + core for step in (X_STEP, Y_STEP)}
    mine, other = BATCHES * core, BATCHES * (1 - core)
    early_hops = [(p, step) for p, src, step in EARLY_HOP if src == c]
    first_hops = [(p, step) for p, src, step in FIRST_HOP if src == c and (p, src, step) not in EARLY_HOP]
    relay_hops = [(p, step) for p, src, step in RELAY_HOP if src == c]
    leaves = [(p, step) for p, src, step in SUM_LEAF if src == c]
    relays = [(p, step) for p, src, step in SUM_RELAY if src == c]
    needed = [p for p in range(N_PAIRS - c) if owner(p) != c]
    sib_pieces = (2 * c + 1 - core, 15 - 2 * c - (1 - core))

    def split(u):
        return u // HEADS, u % HEADS

    def pair_rows(p):
        return pl.ds(p * PAIR, PAIR)

    own_pieces = (2 * c + core, 15 - 2 * c - core)

    def raw_in(b, side):
        src, slot = (mine, other)[side] + b, b % 2
        return [pltpu.make_async_copy(k_hbm.at[src], raw_v.at[slot, side, 0], raw_s.at[slot, side, 0]),
                pltpu.make_async_copy(v_hbm.at[src], raw_v.at[slot, side, 1], raw_s.at[slot, side, 1])]

    def start_raw(b):
        for side in (1, 0):
            for copy in raw_in(b, side):
                copy.start()

    def piece_rows(piece):
        return pl.ds(pl.multiple_of(piece * PIECE, PIECE), PIECE)

    def own_out(b, half):
        return pltpu.make_async_copy(ready_v.at[b % 2, 0, :, :, pl.ds(half * PIECE, PIECE), :],
                                     kv_hbm.at[b, :, :, piece_rows(own_pieces[half]), :], kvl_s.at[b, half])

    def kvx(b, half):
        return remote(ready_v.at[b % 2, 1, :, :, pl.ds(half * PIECE, PIECE), :],
                      kv_hbm.at[b, :, :, piece_rows(own_pieces[half]), :], kvx_s.at[b, half], kvx_r.at[b, half], sib)

    def kvx_in(b, half):
        dst = kv_hbm.at[b, :, :, piece_rows(sib_pieces[half]), :]
        return remote(dst, dst, kvx_s.at[b, half], kvx_r.at[b, half], sib)

    def make_table(tab, row):
        pos = pos_v[pl.ds(row, 1), :].astype(jnp.float32)
        angles = jnp.transpose(jnp.broadcast_to(pos, (PAIR, PAIR))) * freq_v[...]
        tab[0] = jnp.cos(angles)
        sine_val = jnp.sin(angles)
        tab[1] = jnp.where(iota(sine_val.shape, 1) % 2 == 0, -sine_val, sine_val)

    def make_ready(b):
        slot = b % 2

        @pl.when(b >= 2)
        def _():
            for half in range(2):
                kvx(b - 2, half).wait_send()
            tab_out(b - 2).wait_send()

        make_table(tab_x.at[slot], other + b)
        make_table(tab_v.at[b, :, core], mine + b)
        for side in (1, 0):
            for copy in raw_in(b, side):
                copy.wait()
            tab = tab_x.at[slot] if side else tab_v.at[b, :, core]
            k_rows = dot_nn(perm_in[...], raw_v[slot, side, 0])
            v_rows = dot_nn(perm_in[...], raw_v[slot, side, 1])
            for h in range(HEADS):
                x = k_rows[h * PAIR:(h + 1) * PAIR]
                ready_v[slot, side, h, 0] = (x * tab[0] + swap_pairs(x) * tab[1]).astype(jnp.bfloat16)
                ready_v[slot, side, h, 1] = v_rows[h * PAIR:(h + 1) * PAIR].astype(jnp.bfloat16)
        for half in range(2):
            own_out(b, half).start()

        @pl.when(b + 2 < BATCHES)
        def _():
            start_raw(b + 2)

    def send_ready(b):
        for half in range(2):
            kvx(b, half).start()
        tab_out(b).start()

    def qx(b):
        return remote(q_hbm.at[other + b], qs_hbm.at[b], qx_s.at[b], qx_r.at[b], sib)

    def gx(b):
        return remote(g_hbm.at[other + b], gs_hbm.at[b], gx_s.at[b], gx_r.at[b], sib)

    def tab_out(b):
        return remote(tab_x.at[b % 2], tab_v.at[b, :, core], tab_s.at[b % 2], tab_r.at[b], sib)

    def tab_arrive(b):
        dst = tab_v.at[b, :, 1 - core]
        return remote(dst, dst, tab_s.at[0], tab_r.at[b], sib)

    def small_in():
        return [pltpu.make_async_copy(pos_hbm, pos_v, load_s.at[5, 0]),
                pltpu.make_async_copy(freq_hbm, freq_v, load_s.at[5, 1])]

    def kv_copy(u, p, slot, step):
        b, h = split(u)
        ref = kv_hbm.at[b, h, :, pair_rows(p), :]
        return remote(ref, ref, ag_s.at[u, slot], ag_r.at[u, p], nbr[step])

    def send_kv(u, hops, base):
        for i, (p, step) in enumerate(hops):
            kv_copy(u, p, base + i, step).start()

    def have_own(b):
        for half in range(2):
            own_out(b, half).wait()
            kvx_in(b, half).wait_recv()

    def early_hop(u):
        send_kv(u, early_hops, 0)

    def first_hop(u):
        send_kv(u, first_hops, len(early_hops))

    def relay_hop(u):
        for p, _ in relay_hops:
            kv_copy(u, p, 0, X_STEP).wait_recv()
        send_kv(u, relay_hops, len(early_hops) + len(first_hops))

    def loads(u):
        b, h = split(u)
        slot = u % 2
        late = pl.ds(0, n_late)
        return [
            pltpu.make_async_copy(q_hbm.at[mine + b, :, h], q_v.at[slot, core], load_s.at[0, slot]),
            pltpu.make_async_copy(g_hbm.at[mine + b, :, h], g_v.at[slot, core], load_s.at[1, slot]),
            pltpu.make_async_copy(qs_hbm.at[b, :, h], q_v.at[slot, 1 - core], load_s.at[2, slot]),
            pltpu.make_async_copy(gs_hbm.at[b, :, h], g_v.at[slot, 1 - core], load_s.at[3, slot]),
            pltpu.make_async_copy(kv_hbm.at[b, h, :, late, :], kv_v.at[slot, :, late, :], load_s.at[4, slot]),
        ]

    def start_loads(u):
        @pl.when(u % HEADS == 0)
        def _():
            qx(u // HEADS).wait_recv()
            gx(u // HEADS).wait_recv()
            tab_arrive(u // HEADS).wait_recv()

        for p in needed:
            if p not in [r for r, _ in relay_hops]:
                kv_copy(u, p, 0, X_STEP).wait_recv()
        for copy in loads(u):
            copy.start()

    def out_local(u):
        b, h = split(u)
        slot = u % 2
        return [pltpu.make_async_copy(o_v.at[slot, core], o_hbm.at[mine + b, :, h], out_s.at[0, slot]),
                pltpu.make_async_copy(dq_v.at[slot, core], dq_hbm.at[mine + b, :, h], out_s.at[1, slot])]

    def out_remote(u):
        b, h = split(u)
        slot = u % 2
        return [remote(o_v.at[slot, 1 - core], o_hbm.at[mine + b, :, h], out_s.at[2, slot], out_r.at[0, b], sib),
                remote(dq_v.at[slot, 1 - core], dq_hbm.at[mine + b, :, h], out_s.at[3, slot], out_r.at[1, b], sib)]

    def out_arrive(b):
        return [remote(q_hbm.at[other + b], o_hbm.at[other + b], out_s.at[2, 0], out_r.at[0, b], sib),
                remote(q_hbm.at[other + b], dq_hbm.at[other + b], out_s.at[3, 0], out_r.at[1, b], sib)]

    def wait_outs(u):
        for copy in out_local(u):
            copy.wait()
        for copy in out_remote(u):
            copy.wait_send()

    def sum_copy(u, p, i, step):
        k, slot = inbox(c ^ step).index((p, c)), u % INBOX_RING
        return remote(part.at[u % PART_RING, :, pair_rows(p), :], recv.at[slot, k],
                      sum_s.at[i, u % PART_RING], sum_r.at[slot, k], nbr[step])

    def sum_arrive(u, k):
        dst = recv.at[u % INBOX_RING, k]
        return remote(dst, dst, sum_s.at[0, 0], sum_r.at[u % INBOX_RING, k], nbr[X_STEP])

    def give_credits(u, pairs):
        @pl.when(u + INBOX_RING < UNITS)
        def _():
            for k, (pair, src) in enumerate(inbox(c)):
                if pair in pairs:
                    pl.semaphore_signal(credit.at[outbox(src).index((pair, src ^ c))], inc=1,
                                        device_id={'cp': 2 * src + core}, device_id_type=MESH_ID)

    def take_credits(u, which):
        @pl.when(u >= INBOX_RING)
        def _():
            for i in which:
                pl.semaphore_wait(credit.at[i], 1)

    def messages(p):
        return [k for k, (pair, _) in enumerate(inbox(c)) if pair == p]

    def wait_sums(u):
        for i, (p, step) in enumerate(leaves + relays):
            sum_copy(u, p, i, step).wait_send()

    def send_leaves(u):
        take_credits(u, range(len(leaves)))
        for i, (p, step) in enumerate(leaves):
            sum_copy(u, p, i, step).start()

    def add_relays(u):
        for p, _ in relays:
            for k in messages(p):
                sum_arrive(u, k).wait_recv()
                part[u % PART_RING, :, pair_rows(p), :] += recv[u % INBOX_RING, k]
        give_credits(u, [p for p, _ in relays])

    def send_relays(u):
        take_credits(u, range(len(leaves), len(leaves) + len(relays)))
        for i, (p, step) in enumerate(relays):
            sum_copy(u, p, len(leaves) + i, step).start()

    def fin_local(b):
        return [pltpu.make_async_copy(fin_v.at[b % 2, core, i], (gk_hbm, gv_hbm)[i].at[mine + b], fin_s.at[i, b % 2])
                for i in range(2)]

    def fin_remote(b):
        return [remote(fin_v.at[b % 2, 1 - core, i], (gk_hbm, gv_hbm)[i].at[mine + b], fin_s.at[2 + i, b % 2],
                       fin_r.at[i, b], sib) for i in range(2)]

    def fin_arrive(b):
        return [remote(dst.at[other + b], dst.at[other + b], fin_s.at[2 + i, 0], fin_r.at[i, b], sib)
                for i, dst in enumerate((gk_hbm, gv_hbm))]

    def wait_fin(b):
        for copy in fin_local(b):
            copy.wait()
        for copy in fin_remote(b):
            copy.wait_send()

    def finish(u):
        b, h = split(u)
        for late, p in ((0, c), (1, N_PAIRS - 1 - c)):
            total = part[u % PART_RING, :, pair_rows(p), :]
            for k in messages(p):
                sum_arrive(u, k).wait_recv()
                total = total + recv[u % INBOX_RING, k]
            for i in range(2):
                who = 1 - i if late else i
                toks = slice(late * PIECE, (late + 1) * PIECE)
                dk = total[0, i * PIECE:(i + 1) * PIECE] * (DIM ** -0.5)
                dk = dk * tab_v[b, 0, who, toks] - swap_pairs(dk) * tab_v[b, 1, who, toks]
                fin_st[who, 0, h, toks] = dk.astype(jnp.bfloat16)
                fin_st[who, 1, h, toks] = total[1, i * PIECE:(i + 1) * PIECE].astype(jnp.bfloat16)
        give_credits(u, [c, N_PAIRS - 1 - c])

        @pl.when(h == HEADS - 1)
        def _():
            @pl.when(b >= 2)
            def _():
                wait_fin(b - 2)

            for who in range(2):
                for i in range(2):
                    rows = fin_st[who, i].reshape(HEADS * PAIR, DIM)
                    fin_v[b % 2, who, i] = dot_nn(perm_out[...], rows).astype(jnp.bfloat16)

    def send_fin(u):
        @pl.when(u % HEADS == HEADS - 1)
        def _():
            for copy in fin_local(u // HEADS) + fin_remote(u // HEADS):
                copy.start()

    def exchange_queries(b):
        qx(b).start()
        gx(b).start()

    for device in (sib, nbr[X_STEP], nbr[Y_STEP]):
        pl.semaphore_signal(barrier, inc=1, device_id={'cp': device}, device_id_type=MESH_ID)
    for copy in small_in():
        copy.start()
    start_raw(jnp.int32(0))
    start_raw(jnp.int32(1))
    row, col = iota((HEADS * PAIR, HEADS * PAIR), 0), iota((HEADS * PAIR, HEADS * PAIR), 1)
    perm_in[...] = (col == (row % PAIR) * HEADS + row // PAIR).astype(jnp.float32).astype(jnp.bfloat16)
    for copy in small_in():
        copy.wait()

    def up_to(op, first, last):
        def one(u, carry):
            op(u)
            return carry

        lax.fori_loop(first, last, one, 0)

    def start_step(j, carry):
        make_ready(j)

        @pl.when(j == 0)
        def _():
            pl.semaphore_wait(barrier, 3)

        send_ready(j)

        @pl.when(j == 0)
        def _():
            have_own(j)
            exchange_queries(j)

        up_to(relay_hop, jnp.maximum(j - 1, 0), j + j // 3)
        up_to(first_hop, 2 * j, 2 * j + 2)

        @pl.when(j >= 1)
        def _():
            have_own(j)

        up_to(early_hop, 4 * j, 4 * j + 4)
        return carry

    lax.fori_loop(0, START_BATCHES, start_step, 0)
    row, col = iota((HEADS * PAIR, HEADS * PAIR), 0), iota((HEADS * PAIR, HEADS * PAIR), 1)
    perm_out[...] = (row == (col % PAIR) * HEADS + col // PAIR).astype(jnp.float32).astype(jnp.bfloat16)
    start_loads(jnp.int32(0))

    def tick(t, carry):
        @pl.when((t % 2 == 0) & (t // 2 + 4 < BATCHES))
        def _():
            make_ready(t // 2 + 4)
            send_ready(t // 2 + 4)

        @pl.when((t % 2 == 1) & (t // 2 + 4 < BATCHES))
        def _():
            have_own(t // 2 + 4)

        @pl.when((t % HEADS == 0) & (t // HEADS + 1 < BATCHES))
        def _():
            exchange_queries(t // HEADS + 1)

        @pl.when((t == 0) & (START_UNITS < UNITS))
        def _():
            first_hop(t + START_UNITS)

        @pl.when((t + HOP_LEAD > START_UNITS) & (t + HOP_LEAD < UNITS))
        def _():
            first_hop(t + HOP_LEAD)

        @pl.when((t >= 1) & (2 * t - 2 + START_EARLY < UNITS))
        def _():
            early_hop(2 * t - 2 + START_EARLY)
            early_hop(2 * t - 1 + START_EARLY)

        @pl.when(t + RELAY_LEAD < UNITS)
        def _():
            relay_hop(t + RELAY_LEAD)

        @pl.when((t >= 1) & (t - 1 < UNITS))
        def _():
            send_leaves(t - 1)

        @pl.when((t >= 1 + SUM_LAG) & (t - 1 - SUM_LAG < UNITS))
        def _():
            add_relays(t - 1 - SUM_LAG)

        @pl.when((t >= 1 + OWN_LAG) & (t - 1 - OWN_LAG < UNITS))
        def _():
            finish(t - 1 - OWN_LAG)

        @pl.when((t >= 1 + SUM_LAG) & (t - 1 - SUM_LAG < UNITS))
        def _():
            send_relays(t - 1 - SUM_LAG)

        @pl.when((t >= 1 + OWN_LAG) & (t - 1 - OWN_LAG < UNITS))
        def _():
            send_fin(t - 1 - OWN_LAG)

        @pl.when(t < UNITS)
        def _():
            for copy in loads(t):
                copy.wait()

            @pl.when(t + 1 < UNITS)
            def _():
                start_loads(t + 1)

            @pl.when(t >= 2)
            def _():
                wait_outs(t - 2)

            @pl.when(t >= PART_RING)
            def _():
                wait_sums(t - PART_RING)

            slot = t % 2
            unit_compute(c, q_v.at[slot], g_v.at[slot], tab_v.at[t // HEADS], kv_v.at[slot], o_v.at[slot],
                         dq_v.at[slot], part.at[t % PART_RING], kt, vt, s_a, s_b, s_e)
            for copy in out_local(t) + out_remote(t):
                copy.start()

        return carry

    lax.fori_loop(0, UNITS + 1 + OWN_LAG, tick, 0)

    for u in range(UNITS - 2, UNITS):
        wait_outs(jnp.int32(u))
    for b in range(BATCHES - 2, BATCHES):
        wait_fin(jnp.int32(b))

    def drain_batch(b, carry):
        @pl.when(b >= BATCHES - 2)
        def _():
            for half in range(2):
                kvx(b, half).wait_send()
            tab_out(b).wait_send()

        qx(b).wait_send()
        gx(b).wait_send()
        for copy in out_arrive(b):
            copy.wait_recv()
        for copy in fin_arrive(b):
            copy.wait_recv()
        return carry

    lax.fori_loop(0, BATCHES, drain_batch, 0)

    def drain_sums(u, carry):
        wait_sums(u)
        return carry

    lax.fori_loop(UNITS - PART_RING, UNITS, drain_sums, 0)

    def drain_kv(u, carry):
        for i, (p, step) in enumerate(early_hops + first_hops + relay_hops):
            kv_copy(u, p, i, step).wait_send()
        return carry

    lax.fori_loop(0, UNITS, drain_kv, 0)


def attend_kernel(*refs):
    me = lax.axis_index('cp')
    chip, core = me // 2, me % 2
    barrier = pltpu.get_barrier_semaphore()
    for c in range(4):
        @pl.when(chip == c)
        def _(c=c):
            chip_program(c, core, barrier, *refs)


def attend(q5, g5, keys, values, positions, freq):
    any_spec = pl.BlockSpec(memory_space=pl.ANY)
    hbm_spec = pl.BlockSpec(memory_space=pltpu.HBM)
    head_shape = pltpu.VMEM(q5.shape, jnp.bfloat16)
    half_shape = pltpu.HBM((BATCHES,) + q5.shape[1:], jnp.bfloat16)
    row_shape = pltpu.HBM((2 * BATCHES, HEADS * PAIR, DIM), jnp.bfloat16)
    head_buf = pltpu.VMEM((2, 2, PAIR, GROUP, DIM), jnp.bfloat16)
    dma = pltpu.SemaphoreType.DMA
    return pl.pallas_call(
        attend_kernel, name='attend',
        in_specs=[any_spec] * 6,
        out_specs=[any_spec] * 2 + [hbm_spec] * 5,
        out_shape=[head_shape, head_shape,
                   row_shape, row_shape,
                   pltpu.HBM((BATCHES, HEADS, 2, N_PAIRS * PAIR, DIM), jnp.bfloat16),
                   half_shape, half_shape],
        scratch_shapes=[
            head_buf, head_buf, head_buf, head_buf,
            pltpu.VMEM((2, 2, N_PAIRS * PAIR, DIM), jnp.bfloat16),
            pltpu.VMEM((BATCHES, 2, 2, PAIR, DIM), jnp.float32),
            pltpu.VMEM((2, 2, PAIR, DIM), jnp.float32),
            pltpu.VMEM((2 * BATCHES, PAIR), jnp.int32),
            pltpu.VMEM((1, DIM), jnp.float32),
            pltpu.VMEM((2, 2, 2, HEADS * PAIR, DIM), jnp.bfloat16),
            pltpu.VMEM((2, 2, HEADS, 2, PAIR, DIM), jnp.bfloat16),
            pltpu.VMEM((PART_RING, 2, N_PAIRS * PAIR, DIM), jnp.float32),
            pltpu.VMEM((INBOX_RING, N_INBOX, 2, PAIR, DIM), jnp.float32),
            pltpu.VMEM((2, 2, HEADS, PAIR, DIM), jnp.bfloat16),
            pltpu.VMEM((2, 2, 2, HEADS * PAIR, DIM), jnp.bfloat16),
            pltpu.VMEM((HEADS * PAIR, HEADS * PAIR), jnp.bfloat16),
            pltpu.VMEM((HEADS * PAIR, HEADS * PAIR), jnp.bfloat16),
            pltpu.VMEM((DIM, N_PAIRS * PAIR), jnp.bfloat16),
            pltpu.VMEM((DIM, N_PAIRS * PAIR), jnp.bfloat16),
            pltpu.VMEM((N_PAIRS * PAIR, 32 * GROUP), jnp.float32),
            pltpu.VMEM((N_PAIRS * PAIR, 32 * GROUP), jnp.float32),
            pltpu.VMEM((4 * PAIR, PIECE * GROUP), jnp.float32),
            dma((2, 2, 2)), dma((BATCHES, 2)), dma((BATCHES, 2)), dma((BATCHES, 2)), dma((2,)), dma((BATCHES,)),
            dma((BATCHES,)), dma((BATCHES,)), dma((BATCHES,)), dma((BATCHES,)),
            dma((UNITS, 7)), dma((UNITS, 7)), dma((N_OUTBOX, PART_RING)), dma((INBOX_RING, N_INBOX)),
            dma((6, 2)), dma((4, 2)), dma((2, BATCHES)), dma((4, 2)), dma((2, BATCHES)),
            pltpu.SemaphoreType.REGULAR((N_OUTBOX,)),
        ],
        compiler_params=pltpu.CompilerParams(
            collective_id=0, has_side_effects=True, vmem_limit_bytes=32512 * 1024),
    )(*(pltpu.with_memory_space_constraint(x, pltpu.HBM) for x in (q5, g5, keys, values, positions, freq)))


def solution(mesh):
    head_spec = P(None, 'cp', 'tp', None)
    pos_spec = P(None, 'cp')

    def local_step(query, keys, values, positions, grad_out):
        batch, length, n_heads, dim = query.shape
        split_shape = (batch, length, HEADS, GROUP, dim)
        row_shape = (batch, length * HEADS, dim)
        outs = attend(query.reshape(split_shape), grad_out.reshape(split_shape), keys.reshape(row_shape),
                      values.reshape(row_shape), positions, lane_freq(dim))
        return tuple(out.reshape(like.shape) for out, like in zip(outs[:4], (query, query, keys, values)))

    return jax.shard_map(local_step, mesh=mesh,
                         in_specs=(head_spec, head_spec, head_spec, pos_spec, head_spec),
                         out_specs=(head_spec, head_spec, head_spec, head_spec), check_vma=False)
```

```python
import functools

import jax
import jax.numpy as jnp
from jax import lax
from jax.experimental import pallas as pl
from jax.experimental.pallas import tpu as pltpu
from jax.sharding import PartitionSpec as P

ROPE_THETA = 1000000.0
LOG2E = 1.4426950408889634
DIM = 128
GROUP = 8
HEADS = 4
PIECE = 64
PAIR = 128
N_PAIRS = 8
BATCHES = 8
UNITS = BATCHES * HEADS
KEY_BLOCK = 512
STEP_LAG = 2
MESH_ID = pl.DeviceIdType.MESH

X_STEP, Y_STEP = 1, 2
FIRST_HOP = [(0, 0, X_STEP), (0, 0, Y_STEP), (1, 1, X_STEP), (1, 1, Y_STEP), (2, 2, X_STEP), (2, 2, Y_STEP),
             (3, 3, X_STEP), (3, 3, Y_STEP), (4, 3, X_STEP), (4, 3, Y_STEP), (5, 2, Y_STEP), (5, 2, X_STEP),
             (6, 1, X_STEP)]
RELAY_HOP = [(0, 2, X_STEP), (1, 3, X_STEP), (2, 3, Y_STEP), (3, 2, Y_STEP), (4, 1, X_STEP), (5, 3, Y_STEP)]
SUM_LEAF = [(3, 0, Y_STEP), (4, 0, X_STEP), (2, 0, Y_STEP), (6, 0, X_STEP), (2, 1, Y_STEP), (5, 1, X_STEP),
            (0, 1, X_STEP), (3, 1, Y_STEP), (1, 2, Y_STEP), (4, 2, X_STEP), (0, 3, X_STEP), (1, 3, Y_STEP)]
SUM_RELAY = [(0, 2, Y_STEP), (1, 0, X_STEP), (2, 3, X_STEP), (3, 2, X_STEP), (4, 1, Y_STEP), (5, 0, Y_STEP)]

START_BATCHES = 4
START_UNITS = 2 * START_BATCHES
HOP_LEAD = START_UNITS - 2
RELAY_LEAD = START_BATCHES
START_EARLY = 4 * START_BATCHES
EARLY_HOP = [(0, 0, X_STEP), (0, 0, Y_STEP), (1, 1, Y_STEP)]
SUM_LAG = 3
OWN_LAG = 6
PART_RING = OWN_LAG + 2
INBOX_RING = 8


def owner(pair):
    return pair if pair < 4 else 7 - pair


def inbox(chip):
    found = []
    for pair, src, step in SUM_LEAF + SUM_RELAY:
        if src ^ step == chip:
            found.append((pair, src))
    return found


def outbox(chip):
    return [(pair, step) for pair, src, step in SUM_LEAF + SUM_RELAY if src == chip]


N_INBOX = max(len(inbox(c)) for c in range(4))
N_OUTBOX = max(len(outbox(c)) for c in range(4))


def lane_freq(head_dim):
    half_dim = head_dim // 2
    freq_expo = jnp.arange(half_dim, dtype=jnp.float32) * (2.0 / head_dim)
    return jnp.repeat(1.0 / (ROPE_THETA ** freq_expo), 2)[None, :]


def dot_nn(a, b):
    return jnp.dot(a, b, preferred_element_type=jnp.float32)


def dot_nt(a, b):
    return lax.dot_general(a, b, (((1,), (1,)), ((), ())), preferred_element_type=jnp.float32)


def iota(shape, axis):
    return lax.broadcasted_iota(jnp.int32, shape, axis)


def identity():
    return (iota((DIM, DIM), 0) == iota((DIM, DIM), 1)).astype(jnp.float32).astype(jnp.bfloat16)


def swap_pairs(x):
    return jnp.where(iota(x.shape, 1) % 2 == 0, pltpu.roll(x, DIM - 1, axis=1), pltpu.roll(x, 1, axis=1))


def rows_steps(n_keys, tok, seg, q_v, g_v, tab, kv, kt, vt, part, o_v, dq_v, s_ref):
    core, start, place = seg
    rows = tok * GROUP
    scale = DIM ** -0.5
    c1 = scale * LOG2E
    toks = pl.ds(start, tok)

    def table(k):
        return jnp.broadcast_to(tab[k, core, toks, :][:, None, :], (tok, GROUP, DIM)).reshape(rows, DIM)

    x = q_v[core, toks].astype(jnp.float32).reshape(rows, DIM)
    qr = (x * table(0) + swap_pairs(x) * table(1)).astype(jnp.bfloat16)
    g = g_v[core, toks].astype(jnp.float32).reshape(rows, DIM).astype(jnp.bfloat16)
    blocks = [(a, min(KEY_BLOCK, n_keys - a)) for a in range(0, n_keys, KEY_BLOCK)]
    m8 = None
    for a, n in blocks:
        s = dot_nt(kv[0, a:a + n, :], qr) * c1
        if a + n == n_keys:
            last = s[n - PAIR:, :]
            q_tok = iota(last.shape, 1) // GROUP + place
            last = jnp.where(iota(last.shape, 0) <= q_tok, last, -jnp.inf)
            s = last if n == PAIR else jnp.concatenate([s[:n - PAIR, :], last], axis=0)
        s_ref[a:a + n, :] = s
        f = jnp.max(s.reshape(n // 8, 8, rows), axis=0)
        m8 = f if m8 is None else jnp.maximum(m8, f)
        yield
    row_max = jnp.max(m8, axis=0, keepdims=True)
    l8 = None
    o_t = None
    for a, n in blocks:
        p = jnp.exp2(s_ref[a:a + n, :] - row_max)
        s_ref[a:a + n, :] = p
        f = jnp.sum(p.reshape(n // 8, 8, rows), axis=0)
        l8 = f if l8 is None else l8 + f
        d = dot_nn(vt[:, a:a + n], p.astype(jnp.bfloat16))
        o_t = d if o_t is None else o_t + d
        yield
    inv = 1.0 / jnp.sum(l8, axis=0, keepdims=True)
    out_t = o_t * inv
    o_v[core, toks] = jnp.transpose(out_t).reshape(tok, GROUP, DIM).astype(jnp.bfloat16)
    delta = jnp.sum(dot_nt(identity(), g) * out_t, axis=0, keepdims=True)
    yield
    dq_t = None
    for a, n in blocks:
        p = s_ref[a:a + n, :] * inv
        ds = (p * (dot_nt(kv[1, a:a + n, :], g) - delta)).astype(jnp.bfloat16)
        part[1, a:a + n, :] += dot_nn(p.astype(jnp.bfloat16), g)
        part[0, a:a + n, :] += dot_nn(ds, qr)
        d = dot_nn(kt[:, a:a + n], ds)
        dq_t = d if dq_t is None else dq_t + d
        yield
    dq = jnp.transpose(dq_t) * scale
    dq = dq * table(0) - swap_pairs(dq) * table(1)
    dq_v[core, toks] = dq.reshape(tok, GROUP, DIM).astype(jnp.bfloat16)


def interleave(gens, lag):
    live, waiting, count = [], list(gens), 0
    while live or waiting:
        if waiting and (not live or count >= lag):
            live.append(waiting.pop(0))
            count = 0
        for gen in list(live):
            if next(gen, 'end') == 'end':
                live.remove(gen)
        count += 1


def unit_compute(c, q_v, g_v, tab, kv, o_v, dq_v, part, kt, vt, s_a, s_b, s_e):
    n_late, n_early = (N_PAIRS - c) * PAIR, (c + 1) * PAIR
    eye = identity()
    for a in range(0, n_late, 256):
        n = min(256, n_late - a)
        kt[:, a:a + n] = dot_nt(eye, kv[0, a:a + n, :]).astype(jnp.bfloat16)
        vt[:, a:a + n] = dot_nt(eye, kv[1, a:a + n, :]).astype(jnp.bfloat16)
    part[:, :n_late, :] = jnp.zeros((2, n_late, DIM), jnp.float32)
    refs = (q_v, g_v, tab, kv, kt, vt, part, o_v, dq_v)

    def step(i, carry):
        late = [rows_steps(n_late, 32, (1 - i, PIECE + 32 * k, i * PIECE + 32 * k), *refs, s)
                for k, s in ((0, s_a), (1, s_b))]
        early = rows_steps(n_early, PIECE, (i, 0, i * PIECE), *refs, s_e)
        interleave(late + [early], STEP_LAG)
        return carry

    lax.fori_loop(0, 2, step, 0)


def remote(src, dst, send_sem, recv_sem, device):
    return pltpu.make_async_remote_copy(src_ref=src, dst_ref=dst, send_sem=send_sem, recv_sem=recv_sem,
                                        device_id={'cp': device}, device_id_type=MESH_ID)


def chip_program(c, core, barrier, q_hbm, g_hbm, k_hbm, v_hbm, pos_hbm, freq_hbm, odq_hbm, gk_hbm, gv_hbm, kv_hbm, qs_hbm, gs_hbm,
                 q_v, g_v, o_v, dq_v, kv_v, tab_v, tab_x, pos_v, freq_v, raw_v, ready_v, part, recv, fin_st, fin_v,
                 perm_in, perm_out, kt, vt, s_a, s_b, s_e,
                 raw_s, kvl_s, kvx_s, kvx_r, tab_s, tab_r, qx_s, qx_r, gx_s, gx_r, ag_s, ag_r, sum_s, sum_r,
                 load_s, out_s, out_r, fin_s, fin_r, credit):
    o_hbm, dq_hbm = odq_hbm.at[0], odq_hbm.at[1]
    n_late = (N_PAIRS - c) * PAIR
    sib = 2 * c + 1 - core
    nbr = {step: 2 * (c ^ step) + core for step in (X_STEP, Y_STEP)}
    mine, other = BATCHES * core, BATCHES * (1 - core)
    early_hops = [(p, step) for p, src, step in EARLY_HOP if src == c]
    first_hops = [(p, step) for p, src, step in FIRST_HOP if src == c and (p, src, step) not in EARLY_HOP]
    relay_hops = [(p, step) for p, src, step in RELAY_HOP if src == c]
    leaves = [(p, step) for p, src, step in SUM_LEAF if src == c]
    relays = [(p, step) for p, src, step in SUM_RELAY if src == c]
    needed = [p for p in range(N_PAIRS - c) if owner(p) != c]
    sib_pieces = (2 * c + 1 - core, 15 - 2 * c - (1 - core))

    def split(u):
        return u // HEADS, u % HEADS

    def pair_rows(p):
        return pl.ds(p * PAIR, PAIR)

    own_pieces = (2 * c + core, 15 - 2 * c - core)

    def raw_in(b, side):
        src, slot = (mine, other)[side] + b, b % 2
        return [pltpu.make_async_copy(k_hbm.at[src], raw_v.at[slot, side, 0], raw_s.at[slot, side, 0]),
                pltpu.make_async_copy(v_hbm.at[src], raw_v.at[slot, side, 1], raw_s.at[slot, side, 1])]

    def start_raw(b):
        for side in (1, 0):
            for copy in raw_in(b, side):
                copy.start()

    def piece_rows(piece):
        return pl.ds(pl.multiple_of(piece * PIECE, PIECE), PIECE)

    def own_out(b, half):
        return pltpu.make_async_copy(ready_v.at[b % 2, 0, :, :, pl.ds(half * PIECE, PIECE), :],
                                     kv_hbm.at[b, :, :, piece_rows(own_pieces[half]), :], kvl_s.at[b, half])

    def kvx(b, half):
        return remote(ready_v.at[b % 2, 1, :, :, pl.ds(half * PIECE, PIECE), :],
                      kv_hbm.at[b, :, :, piece_rows(own_pieces[half]), :], kvx_s.at[b, half], kvx_r.at[b, half], sib)

    def kvx_in(b, half):
        dst = kv_hbm.at[b, :, :, piece_rows(sib_pieces[half]), :]
        return remote(dst, dst, kvx_s.at[b, half], kvx_r.at[b, half], sib)

    def make_table(tab, row):
        pos = pos_v[pl.ds(row, 1), :].astype(jnp.float32)
        angles = jnp.transpose(jnp.broadcast_to(pos, (PAIR, PAIR))) * freq_v[...]
        tab[0] = jnp.cos(angles)
        sine_val = jnp.sin(angles)
        tab[1] = jnp.where(iota(sine_val.shape, 1) % 2 == 0, -sine_val, sine_val)

    def make_ready(b):
        slot = b % 2

        @pl.when(b >= 2)
        def _():
            for half in range(2):
                kvx(b - 2, half).wait_send()
            tab_out(b - 2).wait_send()

        make_table(tab_x.at[slot], other + b)
        make_table(tab_v.at[b, :, core], mine + b)
        for side in (1, 0):
            for copy in raw_in(b, side):
                copy.wait()
            tab = tab_x.at[slot] if side else tab_v.at[b, :, core]
            k_rows = dot_nn(perm_in[...], raw_v[slot, side, 0])
            v_rows = dot_nn(perm_in[...], raw_v[slot, side, 1])
            for h in range(HEADS):
                x = k_rows[h * PAIR:(h + 1) * PAIR]
                ready_v[slot, side, h, 0] = (x * tab[0] + swap_pairs(x) * tab[1]).astype(jnp.bfloat16)
                ready_v[slot, side, h, 1] = v_rows[h * PAIR:(h + 1) * PAIR].astype(jnp.bfloat16)
        for half in range(2):
            own_out(b, half).start()

        @pl.when(b + 2 < BATCHES)
        def _():
            start_raw(b + 2)

    def send_ready(b):
        for half in range(2):
            kvx(b, half).start()
        tab_out(b).start()

    def qx(b):
        return remote(q_hbm.at[other + b], qs_hbm.at[b], qx_s.at[b], qx_r.at[b], sib)

    def gx(b):
        return remote(g_hbm.at[other + b], gs_hbm.at[b], gx_s.at[b], gx_r.at[b], sib)

    def tab_out(b):
        return remote(tab_x.at[b % 2], tab_v.at[b, :, core], tab_s.at[b % 2], tab_r.at[b], sib)

    def tab_arrive(b):
        dst = tab_v.at[b, :, 1 - core]
        return remote(dst, dst, tab_s.at[0], tab_r.at[b], sib)

    def small_in():
        return [pltpu.make_async_copy(pos_hbm, pos_v, load_s.at[5, 0]),
                pltpu.make_async_copy(freq_hbm, freq_v, load_s.at[5, 1])]

    def kv_copy(u, p, slot, step):
        b, h = split(u)
        ref = kv_hbm.at[b, h, :, pair_rows(p), :]
        return remote(ref, ref, ag_s.at[u, slot], ag_r.at[u, p], nbr[step])

    def send_kv(u, hops, base):
        for i, (p, step) in enumerate(hops):
            kv_copy(u, p, base + i, step).start()

    def have_own(b):
        for half in range(2):
            own_out(b, half).wait()
            kvx_in(b, half).wait_recv()

    def early_hop(u):
        send_kv(u, early_hops, 0)

    def first_hop(u):
        send_kv(u, first_hops, len(early_hops))

    def relay_hop(u):
        for p, _ in relay_hops:
            kv_copy(u, p, 0, X_STEP).wait_recv()
        send_kv(u, relay_hops, len(early_hops) + len(first_hops))

    def loads(u):
        b, h = split(u)
        slot = u % 2
        late = pl.ds(0, n_late)
        return [
            pltpu.make_async_copy(q_hbm.at[mine + b, :, h], q_v.at[slot, core], load_s.at[0, slot]),
            pltpu.make_async_copy(g_hbm.at[mine + b, :, h], g_v.at[slot, core], load_s.at[1, slot]),
            pltpu.make_async_copy(qs_hbm.at[b, :, h], q_v.at[slot, 1 - core], load_s.at[2, slot]),
            pltpu.make_async_copy(gs_hbm.at[b, :, h], g_v.at[slot, 1 - core], load_s.at[3, slot]),
            pltpu.make_async_copy(kv_hbm.at[b, h, :, late, :], kv_v.at[slot, :, late, :], load_s.at[4, slot]),
        ]

    def start_loads(u):
        @pl.when(u % HEADS == 0)
        def _():
            qx(u // HEADS).wait_recv()
            gx(u // HEADS).wait_recv()
            tab_arrive(u // HEADS).wait_recv()

        for p in needed:
            if p not in [r for r, _ in relay_hops]:
                kv_copy(u, p, 0, X_STEP).wait_recv()
        for copy in loads(u):
            copy.start()

    def out_local(u):
        b, h = split(u)
        slot = u % 2
        return [pltpu.make_async_copy(o_v.at[slot, core], o_hbm.at[mine + b, :, h], out_s.at[0, slot]),
                pltpu.make_async_copy(dq_v.at[slot, core], dq_hbm.at[mine + b, :, h], out_s.at[1, slot])]

    def out_remote(u):
        b, h = split(u)
        slot = u % 2
        return [remote(o_v.at[slot, 1 - core], o_hbm.at[mine + b, :, h], out_s.at[2, slot], out_r.at[0, b], sib),
                remote(dq_v.at[slot, 1 - core], dq_hbm.at[mine + b, :, h], out_s.at[3, slot], out_r.at[1, b], sib)]

    def out_arrive(b):
        return [remote(q_hbm.at[other + b], o_hbm.at[other + b], out_s.at[2, 0], out_r.at[0, b], sib),
                remote(q_hbm.at[other + b], dq_hbm.at[other + b], out_s.at[3, 0], out_r.at[1, b], sib)]

    def wait_outs(u):
        for copy in out_local(u):
            copy.wait()
        for copy in out_remote(u):
            copy.wait_send()

    def sum_copy(u, p, i, step):
        k, slot = inbox(c ^ step).index((p, c)), u % INBOX_RING
        return remote(part.at[u % PART_RING, :, pair_rows(p), :], recv.at[slot, k],
                      sum_s.at[i, u % PART_RING], sum_r.at[slot, k], nbr[step])

    def sum_arrive(u, k):
        dst = recv.at[u % INBOX_RING, k]
        return remote(dst, dst, sum_s.at[0, 0], sum_r.at[u % INBOX_RING, k], nbr[X_STEP])

    def give_credits(u, pairs):
        @pl.when(u + INBOX_RING < UNITS)
        def _():
            for k, (pair, src) in enumerate(inbox(c)):
                if pair in pairs:
                    pl.semaphore_signal(credit.at[outbox(src).index((pair, src ^ c))], inc=1,
                                        device_id={'cp': 2 * src + core}, device_id_type=MESH_ID)

    def take_credits(u, which):
        @pl.when(u >= INBOX_RING)
        def _():
            for i in which:
                pl.semaphore_wait(credit.at[i], 1)

    def messages(p):
        return [k for k, (pair, _) in enumerate(inbox(c)) if pair == p]

    def wait_sums(u):
        for i, (p, step) in enumerate(leaves + relays):
            sum_copy(u, p, i, step).wait_send()

    def send_leaves(u):
        take_credits(u, range(len(leaves)))
        for i, (p, step) in enumerate(leaves):
            sum_copy(u, p, i, step).start()

    def add_relays(u):
        for p, _ in relays:
            for k in messages(p):
                sum_arrive(u, k).wait_recv()
                part[u % PART_RING, :, pair_rows(p), :] += recv[u % INBOX_RING, k]
        give_credits(u, [p for p, _ in relays])

    def send_relays(u):
        take_credits(u, range(len(leaves), len(leaves) + len(relays)))
        for i, (p, step) in enumerate(relays):
            sum_copy(u, p, len(leaves) + i, step).start()

    def fin_local(b):
        return [pltpu.make_async_copy(fin_v.at[b % 2, core, i], (gk_hbm, gv_hbm)[i].at[mine + b], fin_s.at[i, b % 2])
                for i in range(2)]

    def fin_remote(b):
        return [remote(fin_v.at[b % 2, 1 - core, i], (gk_hbm, gv_hbm)[i].at[mine + b], fin_s.at[2 + i, b % 2],
                       fin_r.at[i, b], sib) for i in range(2)]

    def fin_arrive(b):
        return [remote(dst.at[other + b], dst.at[other + b], fin_s.at[2 + i, 0], fin_r.at[i, b], sib)
                for i, dst in enumerate((gk_hbm, gv_hbm))]

    def wait_fin(b):
        for copy in fin_local(b):
            copy.wait()
        for copy in fin_remote(b):
            copy.wait_send()

    def finish(u):
        b, h = split(u)
        for late, p in ((0, c), (1, N_PAIRS - 1 - c)):
            total = part[u % PART_RING, :, pair_rows(p), :]
            for k in messages(p):
                sum_arrive(u, k).wait_recv()
                total = total + recv[u % INBOX_RING, k]
            for i in range(2):
                who = 1 - i if late else i
                toks = slice(late * PIECE, (late + 1) * PIECE)
                dk = total[0, i * PIECE:(i + 1) * PIECE] * (DIM ** -0.5)
                dk = dk * tab_v[b, 0, who, toks] - swap_pairs(dk) * tab_v[b, 1, who, toks]
                fin_st[who, 0, h, toks] = dk.astype(jnp.bfloat16)
                fin_st[who, 1, h, toks] = total[1, i * PIECE:(i + 1) * PIECE].astype(jnp.bfloat16)
        give_credits(u, [c, N_PAIRS - 1 - c])

        @pl.when(h == HEADS - 1)
        def _():
            @pl.when(b >= 2)
            def _():
                wait_fin(b - 2)

            for who in range(2):
                for i in range(2):
                    rows = fin_st[who, i].reshape(HEADS * PAIR, DIM)
                    fin_v[b % 2, who, i] = dot_nn(perm_out[...], rows).astype(jnp.bfloat16)

    def send_fin(u):
        @pl.when(u % HEADS == HEADS - 1)
        def _():
            for copy in fin_local(u // HEADS) + fin_remote(u // HEADS):
                copy.start()

    def exchange_queries(b):
        qx(b).start()
        gx(b).start()

    for device in (sib, nbr[X_STEP], nbr[Y_STEP]):
        pl.semaphore_signal(barrier, inc=1, device_id={'cp': device}, device_id_type=MESH_ID)
    for copy in small_in():
        copy.start()
    start_raw(jnp.int32(0))
    start_raw(jnp.int32(1))
    row, col = iota((HEADS * PAIR, HEADS * PAIR), 0), iota((HEADS * PAIR, HEADS * PAIR), 1)
    perm_in[...] = (col == (row % PAIR) * HEADS + row // PAIR).astype(jnp.float32).astype(jnp.bfloat16)
    for copy in small_in():
        copy.wait()

    def up_to(op, first, last):
        def one(u, carry):
            op(u)
            return carry

        lax.fori_loop(first, last, one, 0)

    def start_step(j, carry):
        make_ready(j)

        @pl.when(j == 0)
        def _():
            pl.semaphore_wait(barrier, 3)

        send_ready(j)

        @pl.when(j == 0)
        def _():
            have_own(j)
            exchange_queries(j)

        up_to(relay_hop, jnp.maximum(j - 1, 0), j + j // 3)
        up_to(first_hop, 2 * j, 2 * j + 2)

        @pl.when(j >= 1)
        def _():
            have_own(j)

        up_to(early_hop, 4 * j, 4 * j + 4)
        return carry

    lax.fori_loop(0, START_BATCHES, start_step, 0)
    row, col = iota((HEADS * PAIR, HEADS * PAIR), 0), iota((HEADS * PAIR, HEADS * PAIR), 1)
    perm_out[...] = (row == (col % PAIR) * HEADS + col // PAIR).astype(jnp.float32).astype(jnp.bfloat16)
    start_loads(jnp.int32(0))

    def tick(t, carry):
        @pl.when((t % 2 == 0) & (t // 2 + 4 < BATCHES))
        def _():
            make_ready(t // 2 + 4)
            send_ready(t // 2 + 4)

        @pl.when((t % 2 == 1) & (t // 2 + 4 < BATCHES))
        def _():
            have_own(t // 2 + 4)

        @pl.when((t % HEADS == 0) & (t // HEADS + 1 < BATCHES))
        def _():
            exchange_queries(t // HEADS + 1)

        @pl.when((t == 0) & (START_UNITS < UNITS))
        def _():
            first_hop(t + START_UNITS)

        @pl.when((t + HOP_LEAD > START_UNITS) & (t + HOP_LEAD < UNITS))
        def _():
            first_hop(t + HOP_LEAD)

        @pl.when((t >= 1) & (2 * t - 2 + START_EARLY < UNITS))
        def _():
            early_hop(2 * t - 2 + START_EARLY)
            early_hop(2 * t - 1 + START_EARLY)

        @pl.when(t + RELAY_LEAD < UNITS)
        def _():
            relay_hop(t + RELAY_LEAD)

        @pl.when((t >= 1) & (t - 1 < UNITS))
        def _():
            send_leaves(t - 1)

        @pl.when((t >= 1 + SUM_LAG) & (t - 1 - SUM_LAG < UNITS))
        def _():
            add_relays(t - 1 - SUM_LAG)

        @pl.when((t >= 1 + OWN_LAG) & (t - 1 - OWN_LAG < UNITS))
        def _():
            finish(t - 1 - OWN_LAG)

        @pl.when((t >= 1 + SUM_LAG) & (t - 1 - SUM_LAG < UNITS))
        def _():
            send_relays(t - 1 - SUM_LAG)

        @pl.when((t >= 1 + OWN_LAG) & (t - 1 - OWN_LAG < UNITS))
        def _():
            send_fin(t - 1 - OWN_LAG)

        @pl.when(t < UNITS)
        def _():
            for copy in loads(t):
                copy.wait()

            @pl.when(t + 1 < UNITS)
            def _():
                start_loads(t + 1)

            @pl.when(t >= 2)
            def _():
                wait_outs(t - 2)

            @pl.when(t >= PART_RING)
            def _():
                wait_sums(t - PART_RING)

            slot = t % 2
            unit_compute(c, q_v.at[slot], g_v.at[slot], tab_v.at[t // HEADS], kv_v.at[slot], o_v.at[slot],
                         dq_v.at[slot], part.at[t % PART_RING], kt, vt, s_a, s_b, s_e)
            for copy in out_local(t) + out_remote(t):
                copy.start()

        return carry

    lax.fori_loop(0, UNITS + 1 + OWN_LAG, tick, 0)

    for u in range(UNITS - 2, UNITS):
        wait_outs(jnp.int32(u))
    for b in range(BATCHES - 2, BATCHES):
        wait_fin(jnp.int32(b))

    def drain_batch(b, carry):
        @pl.when(b >= BATCHES - 2)
        def _():
            for half in range(2):
                kvx(b, half).wait_send()
            tab_out(b).wait_send()

        qx(b).wait_send()
        gx(b).wait_send()
        for copy in out_arrive(b):
            copy.wait_recv()
        for copy in fin_arrive(b):
            copy.wait_recv()
        return carry

    lax.fori_loop(0, BATCHES, drain_batch, 0)

    def drain_sums(u, carry):
        wait_sums(u)
        return carry

    lax.fori_loop(UNITS - PART_RING, UNITS, drain_sums, 0)

    def drain_kv(u, carry):
        for i, (p, step) in enumerate(early_hops + first_hops + relay_hops):
            kv_copy(u, p, i, step).wait_send()
        return carry

    lax.fori_loop(0, UNITS, drain_kv, 0)


def attend_kernel(*refs):
    me = lax.axis_index('cp')
    chip, core = me // 2, me % 2
    barrier = pltpu.get_barrier_semaphore()
    for c in range(4):
        @pl.when(chip == c)
        def _(c=c):
            chip_program(c, core, barrier, *refs)


def attend(q5, g5, keys, values, positions, freq):
    any_spec = pl.BlockSpec(memory_space=pl.ANY)
    hbm_spec = pl.BlockSpec(memory_space=pltpu.HBM)
    head_shape = pltpu.VMEM((2,) + q5.shape, jnp.bfloat16)
    half_shape = pltpu.HBM((BATCHES,) + q5.shape[1:], jnp.bfloat16)
    row_shape = pltpu.HBM((2 * BATCHES, HEADS * PAIR, DIM), jnp.bfloat16)
    head_buf = pltpu.VMEM((2, 2, PAIR, GROUP, DIM), jnp.bfloat16)
    dma = pltpu.SemaphoreType.DMA
    return pl.pallas_call(
        attend_kernel, name='attend',
        in_specs=[any_spec] * 6,
        out_specs=[any_spec] + [hbm_spec] * 5,
        out_shape=[head_shape,
                   row_shape, row_shape,
                   pltpu.HBM((BATCHES, HEADS, 2, N_PAIRS * PAIR, DIM), jnp.bfloat16),
                   half_shape, half_shape],
        scratch_shapes=[
            head_buf, head_buf, head_buf, head_buf,
            pltpu.VMEM((2, 2, N_PAIRS * PAIR, DIM), jnp.bfloat16),
            pltpu.VMEM((BATCHES, 2, 2, PAIR, DIM), jnp.float32),
            pltpu.VMEM((2, 2, PAIR, DIM), jnp.float32),
            pltpu.VMEM((2 * BATCHES, PAIR), jnp.int32),
            pltpu.VMEM((1, DIM), jnp.float32),
            pltpu.VMEM((2, 2, 2, HEADS * PAIR, DIM), jnp.bfloat16),
            pltpu.VMEM((2, 2, HEADS, 2, PAIR, DIM), jnp.bfloat16),
            pltpu.VMEM((PART_RING, 2, N_PAIRS * PAIR, DIM), jnp.float32),
            pltpu.VMEM((INBOX_RING, N_INBOX, 2, PAIR, DIM), jnp.float32),
            pltpu.VMEM((2, 2, HEADS, PAIR, DIM), jnp.bfloat16),
            pltpu.VMEM((2, 2, 2, HEADS * PAIR, DIM), jnp.bfloat16),
            pltpu.VMEM((HEADS * PAIR, HEADS * PAIR), jnp.bfloat16),
            pltpu.VMEM((HEADS * PAIR, HEADS * PAIR), jnp.bfloat16),
            pltpu.VMEM((DIM, N_PAIRS * PAIR), jnp.bfloat16),
            pltpu.VMEM((DIM, N_PAIRS * PAIR), jnp.bfloat16),
            pltpu.VMEM((N_PAIRS * PAIR, 32 * GROUP), jnp.float32),
            pltpu.VMEM((N_PAIRS * PAIR, 32 * GROUP), jnp.float32),
            pltpu.VMEM((4 * PAIR, PIECE * GROUP), jnp.float32),
            dma((2, 2, 2)), dma((BATCHES, 2)), dma((BATCHES, 2)), dma((BATCHES, 2)), dma((2,)), dma((BATCHES,)),
            dma((BATCHES,)), dma((BATCHES,)), dma((BATCHES,)), dma((BATCHES,)),
            dma((UNITS, 7)), dma((UNITS, 7)), dma((N_OUTBOX, PART_RING)), dma((INBOX_RING, N_INBOX)),
            dma((6, 2)), dma((4, 2)), dma((2, BATCHES)), dma((4, 2)), dma((2, BATCHES)),
            pltpu.SemaphoreType.REGULAR((N_OUTBOX,)),
        ],
        compiler_params=pltpu.CompilerParams(
            collective_id=0, has_side_effects=True, vmem_limit_bytes=32512 * 1024),
    )(*(pltpu.with_memory_space_constraint(x, pltpu.HBM) for x in (q5, g5, keys, values, positions, freq)))


def place_kernel(odq, gk_in, gv_in, o_out, dq_out, gk_out, gv_out, small_v, sems):
    small = [pltpu.make_async_copy(src, small_v.at[i], sems.at[0, i]) for i, src in enumerate((gk_in, gv_in))]
    for copy in small:
        copy.start()
    part = odq.shape[1] // 4
    large = [pltpu.make_async_copy(odq.at[k, pl.ds(i * part, part)], dst.at[pl.ds(i * part, part)], sems.at[1 + k, i])
             for i in range(4) for k, dst in enumerate((o_out, dq_out))]
    for copy in large:
        copy.start()
    for copy in small:
        copy.wait()
    last = [pltpu.make_async_copy(small_v.at[i], dst, sems.at[0, 2 + i]) for i, dst in enumerate((gk_out, gv_out))]
    for copy in last:
        copy.start()
    for copy in large + last:
        copy.wait()


def place(odq, gk, gv):
    any_spec = pl.BlockSpec(memory_space=pl.ANY)
    head_shape = pltpu.HBM(odq.shape[1:], jnp.bfloat16)
    row_shape = pltpu.HBM(gk.shape, jnp.bfloat16)
    return pl.pallas_call(
        place_kernel, name='place', in_specs=[any_spec] * 3, out_specs=[any_spec] * 4,
        out_shape=[head_shape, head_shape, row_shape, row_shape],
        scratch_shapes=[pltpu.VMEM((2,) + gk.shape, jnp.bfloat16), pltpu.SemaphoreType.DMA((3, 4))],
        compiler_params=pltpu.CompilerParams(vmem_limit_bytes=6 * 1024 * 1024),
    )(odq, pltpu.with_memory_space_constraint(gk, pltpu.HBM), pltpu.with_memory_space_constraint(gv, pltpu.HBM))


def solution(mesh):
    head_spec = P(None, 'cp', 'tp', None)
    pos_spec = P(None, 'cp')

    def local_step(query, keys, values, positions, grad_out):
        batch, length, n_heads, dim = query.shape
        split_shape = (batch, length, HEADS, GROUP, dim)
        row_shape = (batch, length * HEADS, dim)
        outs = attend(query.reshape(split_shape), grad_out.reshape(split_shape), keys.reshape(row_shape),
                      values.reshape(row_shape), positions, lane_freq(dim))
        return tuple(out.reshape(like.shape) for out, like in zip(place(*outs[:3]), (query, query, keys, values)))

    return jax.shard_map(local_step, mesh=mesh,
                         in_specs=(head_spec, head_spec, head_spec, pos_spec, head_spec),
                         out_specs=(head_spec, head_spec, head_spec, head_spec), check_vma=False)
```

```python
import functools

import jax
import jax.numpy as jnp
import numpy as np
from jax import lax
from jax.experimental import pallas as pl
from jax.experimental.pallas import tpu as pltpu
from jax.sharding import PartitionSpec as P

ROPE_THETA = 1000000.0
LOG2E = 1.4426950408889634
DIM = 128
GROUP = 8
HEADS = 4
PIECE = 64
PAIR = 128
N_PAIRS = 8
BATCHES = 8
UNITS = BATCHES * HEADS
KEY_BLOCK = 512
STEP_LAG = 2
MESH_ID = pl.DeviceIdType.MESH

X_STEP, Y_STEP = 1, 2
FIRST_HOP = [(0, 0, X_STEP), (0, 0, Y_STEP), (1, 1, X_STEP), (1, 1, Y_STEP), (2, 2, X_STEP), (2, 2, Y_STEP),
             (3, 3, X_STEP), (3, 3, Y_STEP), (4, 3, X_STEP), (4, 3, Y_STEP), (5, 2, Y_STEP), (5, 2, X_STEP),
             (6, 1, X_STEP)]
RELAY_HOP = [(0, 2, X_STEP), (1, 3, X_STEP), (2, 3, Y_STEP), (3, 2, Y_STEP), (4, 1, X_STEP), (5, 3, Y_STEP)]
SUM_LEAF = [(3, 0, Y_STEP), (4, 0, X_STEP), (2, 0, Y_STEP), (6, 0, X_STEP), (2, 1, Y_STEP), (5, 1, X_STEP),
            (0, 1, X_STEP), (3, 1, Y_STEP), (1, 2, Y_STEP), (4, 2, X_STEP), (0, 3, X_STEP), (1, 3, Y_STEP)]
SUM_RELAY = [(0, 2, Y_STEP), (1, 0, X_STEP), (2, 3, X_STEP), (3, 2, X_STEP), (4, 1, Y_STEP), (5, 0, Y_STEP)]

START_BATCHES = 5
START_UNITS = 8
HOP_LEAD = START_UNITS - 2
RELAY_LEAD = 4
START_EARLY = HEADS * START_BATCHES
FAST_UNITS = 2
EARLY_HOP = [(0, 0, X_STEP), (0, 0, Y_STEP), (1, 1, Y_STEP)]
SUM_LAG = 3
OWN_LAG = 6
PART_RING = OWN_LAG + 2
INBOX_RING = 8


def owner(pair):
    return pair if pair < 4 else 7 - pair


def inbox(chip):
    found = []
    for pair, src, step in SUM_LEAF + SUM_RELAY:
        if src ^ step == chip:
            found.append((pair, src))
    return found


def outbox(chip):
    return [(pair, step) for pair, src, step in SUM_LEAF + SUM_RELAY if src == chip]


N_INBOX = max(len(inbox(c)) for c in range(4))
N_OUTBOX = max(len(outbox(c)) for c in range(4))


def lane_freq(head_dim):
    exponent = np.arange(head_dim // 2, dtype=np.float64) * (2.0 / head_dim)
    return np.repeat(ROPE_THETA ** -exponent, 2).astype(np.float32)[None, :]


def dot_nn(a, b):
    return jnp.dot(a, b, preferred_element_type=jnp.float32)


def dot_nt(a, b):
    return lax.dot_general(a, b, (((1,), (1,)), ((), ())), preferred_element_type=jnp.float32)


def iota(shape, axis):
    return lax.broadcasted_iota(jnp.int32, shape, axis)


def identity():
    return (iota((DIM, DIM), 0) == iota((DIM, DIM), 1)).astype(jnp.float32).astype(jnp.bfloat16)


def swap_pairs(x):
    return jnp.where(iota(x.shape, 1) % 2 == 0, pltpu.roll(x, DIM - 1, axis=1), pltpu.roll(x, 1, axis=1))


def rows_steps(n_keys, tok, seg, q_v, g_v, tab, kv, kt, vt, part, o_v, dq_v, s_ref):
    core, start, place = seg
    rows = tok * GROUP
    scale = DIM ** -0.5
    c1 = scale * LOG2E
    toks = pl.ds(start, tok)

    def table(k):
        return jnp.broadcast_to(tab[k, core, toks, :][:, None, :], (tok, GROUP, DIM)).reshape(rows, DIM)

    x = q_v[core, toks].astype(jnp.float32).reshape(rows, DIM)
    qr = (x * table(0) + swap_pairs(x) * table(1)).astype(jnp.bfloat16)
    g = g_v[core, toks].astype(jnp.float32).reshape(rows, DIM).astype(jnp.bfloat16)
    blocks = [(a, min(KEY_BLOCK, n_keys - a)) for a in range(0, n_keys, KEY_BLOCK)]
    m8 = None
    for a, n in blocks:
        s = dot_nt(kv[0, a:a + n, :], qr) * c1
        if a + n == n_keys:
            last = s[n - PAIR:, :]
            q_tok = iota(last.shape, 1) // GROUP + place
            last = jnp.where(iota(last.shape, 0) <= q_tok, last, -jnp.inf)
            s = last if n == PAIR else jnp.concatenate([s[:n - PAIR, :], last], axis=0)
        s_ref[a:a + n, :] = s
        f = jnp.max(s.reshape(n // 8, 8, rows), axis=0)
        m8 = f if m8 is None else jnp.maximum(m8, f)
        yield
    row_max = jnp.max(m8, axis=0, keepdims=True)
    l8 = None
    o_t = None
    for a, n in blocks:
        p = jnp.exp2(s_ref[a:a + n, :] - row_max)
        s_ref[a:a + n, :] = p
        f = jnp.sum(p.reshape(n // 8, 8, rows), axis=0)
        l8 = f if l8 is None else l8 + f
        d = dot_nn(vt[:, a:a + n], p.astype(jnp.bfloat16))
        o_t = d if o_t is None else o_t + d
        yield
    inv = 1.0 / jnp.sum(l8, axis=0, keepdims=True)
    out_t = o_t * inv
    o_v[core, toks] = jnp.transpose(out_t).reshape(tok, GROUP, DIM).astype(jnp.bfloat16)
    delta = jnp.sum(dot_nt(identity(), g) * out_t, axis=0, keepdims=True)
    yield
    dq_t = None
    for a, n in blocks:
        p = s_ref[a:a + n, :] * inv
        ds = (p * (dot_nt(kv[1, a:a + n, :], g) - delta)).astype(jnp.bfloat16)
        part[1, a:a + n, :] += dot_nn(p.astype(jnp.bfloat16), g)
        part[0, a:a + n, :] += dot_nn(ds, qr)
        d = dot_nn(kt[:, a:a + n], ds)
        dq_t = d if dq_t is None else dq_t + d
        yield
    dq = jnp.transpose(dq_t) * scale
    dq = dq * table(0) - swap_pairs(dq) * table(1)
    dq_v[core, toks] = dq.reshape(tok, GROUP, DIM).astype(jnp.bfloat16)


def interleave(gens, lag):
    live, waiting, count = [], list(gens), 0
    while live or waiting:
        if waiting and (not live or count >= lag):
            live.append(waiting.pop(0))
            count = 0
        for gen in list(live):
            if next(gen, 'end') == 'end':
                live.remove(gen)
        count += 1


def unit_compute(c, q_v, g_v, tab, kv, o_v, dq_v, part, kt, vt, s_a, s_b, s_e):
    n_late, n_early = (N_PAIRS - c) * PAIR, (c + 1) * PAIR
    eye = identity()
    for a in range(0, n_late, 256):
        n = min(256, n_late - a)
        kt[:, a:a + n] = dot_nt(eye, kv[0, a:a + n, :]).astype(jnp.bfloat16)
        vt[:, a:a + n] = dot_nt(eye, kv[1, a:a + n, :]).astype(jnp.bfloat16)
    part[:, :n_late, :] = jnp.zeros((2, n_late, DIM), jnp.float32)
    refs = (q_v, g_v, tab, kv, kt, vt, part, o_v, dq_v)

    def step(i, carry):
        late = [rows_steps(n_late, 32, (1 - i, PIECE + 32 * k, i * PIECE + 32 * k), *refs, s)
                for k, s in ((0, s_a), (1, s_b))]
        early = rows_steps(n_early, PIECE, (i, 0, i * PIECE), *refs, s_e)
        interleave(late + [early], STEP_LAG)
        return carry

    lax.fori_loop(0, 2, step, 0)


def remote(src, dst, send_sem, recv_sem, device):
    return pltpu.make_async_remote_copy(src_ref=src, dst_ref=dst, send_sem=send_sem, recv_sem=recv_sem,
                                        device_id={'cp': device}, device_id_type=MESH_ID)


def chip_program(c, core, barrier, q_hbm, g_hbm, k_hbm, v_hbm, pos_hbm, freq_hbm, odq_hbm, gkv_hbm, kv_hbm, qs_hbm, gs_hbm,
                 q_v, g_v, o_v, dq_v, kv_v, tab_v, tab_x, pos_v, freq_v, raw_v, ready_v, part, recv, fin_v,
                 perm_in, kt, vt, s_a, s_b, s_e,
                 raw_s, kvl_s, kvx_s, kvx_r, tab_s, tab_r, qx_s, qx_r, gx_s, gx_r, ag_s, ag_r, sum_s, sum_r,
                 load_s, out_s, out_r, fin_s, fin_r, credit):
    o_hbm, dq_hbm = odq_hbm.at[0], odq_hbm.at[1]
    n_late = (N_PAIRS - c) * PAIR
    sib = 2 * c + 1 - core
    nbr = {step: 2 * (c ^ step) + core for step in (X_STEP, Y_STEP)}
    mine, other = BATCHES * core, BATCHES * (1 - core)
    early_hops = [(p, step) for p, src, step in EARLY_HOP if src == c]
    first_hops = [(p, step) for p, src, step in FIRST_HOP if src == c and (p, src, step) not in EARLY_HOP]
    relay_hops = [(p, step) for p, src, step in RELAY_HOP if src == c]
    leaves = [(p, step) for p, src, step in SUM_LEAF if src == c]
    relays = [(p, step) for p, src, step in SUM_RELAY if src == c]
    needed = [p for p in range(N_PAIRS - c) if owner(p) != c]
    sib_pieces = (2 * c + 1 - core, 15 - 2 * c - (1 - core))

    def split(u):
        return u // HEADS, u % HEADS

    def pair_rows(p):
        return pl.ds(p * PAIR, PAIR)

    own_pieces = (2 * c + core, 15 - 2 * c - core)

    def raw_in(b, side):
        src, slot = (mine, other)[side] + b, b % 2
        return [pltpu.make_async_copy(k_hbm.at[src], raw_v.at[slot, side, 0], raw_s.at[slot, side, 0]),
                pltpu.make_async_copy(v_hbm.at[src], raw_v.at[slot, side, 1], raw_s.at[slot, side, 1])]

    def start_raw(b):
        for side in (1, 0):
            for copy in raw_in(b, side):
                copy.start()

    def piece_rows(piece):
        return pl.ds(pl.multiple_of(piece * PIECE, PIECE), PIECE)

    def own_out(b, half):
        return pltpu.make_async_copy(ready_v.at[b % 2, 0, :, :, pl.ds(half * PIECE, PIECE), :],
                                     kv_hbm.at[b, :, :, piece_rows(own_pieces[half]), :], kvl_s.at[b, half])

    def kvx(b, half):
        return remote(ready_v.at[b % 2, 1, :, :, pl.ds(half * PIECE, PIECE), :],
                      kv_hbm.at[b, :, :, piece_rows(own_pieces[half]), :], kvx_s.at[b, half], kvx_r.at[b, half], sib)

    def kvx_in(b, half):
        dst = kv_hbm.at[b, :, :, piece_rows(sib_pieces[half]), :]
        return remote(dst, dst, kvx_s.at[b, half], kvx_r.at[b, half], sib)

    def make_table(tab, row):
        pos = pos_v[pl.ds(row, 1), :].astype(jnp.float32)
        angles = jnp.transpose(jnp.broadcast_to(pos, (PAIR, PAIR))) * freq_v[...]
        tab[0] = jnp.cos(angles)
        sine_val = jnp.sin(angles)
        tab[1] = jnp.where(iota(sine_val.shape, 1) % 2 == 0, -sine_val, sine_val)

    def make_ready(b):
        slot = b % 2

        @pl.when(b >= 2)
        def _():
            for half in range(2):
                kvx(b - 2, half).wait_send()
            tab_out(b - 2).wait_send()

        @pl.when(b == 2)
        def _():
            for u in range(FAST_UNITS):
                for i, (p, step) in enumerate(early_hops + first_hops):
                    kv_copy(jnp.int32(u), p, i, step).wait_send()

        make_table(tab_x.at[slot], other + b)
        make_table(tab_v.at[b, :, core], mine + b)
        for side in (1, 0):
            for copy in raw_in(b, side):
                copy.wait()
            tab = tab_x.at[slot] if side else tab_v.at[b, :, core]
            k_rows = dot_nn(perm_in[...], raw_v[slot, side, 0])
            v_rows = dot_nn(perm_in[...], raw_v[slot, side, 1])
            for h in range(HEADS):
                x = k_rows[h * PAIR:(h + 1) * PAIR]
                ready_v[slot, side, h, 0] = (x * tab[0] + swap_pairs(x) * tab[1]).astype(jnp.bfloat16)
                ready_v[slot, side, h, 1] = v_rows[h * PAIR:(h + 1) * PAIR].astype(jnp.bfloat16)
        for half in range(2):
            own_out(b, half).start()

        @pl.when(b + 2 < BATCHES)
        def _():
            start_raw(b + 2)

    def send_ready(b):
        for half in range(2):
            kvx(b, half).start()
        tab_out(b).start()

    def qx(b):
        return remote(q_hbm.at[other + b], qs_hbm.at[b], qx_s.at[b], qx_r.at[b], sib)

    def gx(b):
        return remote(g_hbm.at[other + b], gs_hbm.at[b], gx_s.at[b], gx_r.at[b], sib)

    def tab_out(b):
        return remote(tab_x.at[b % 2], tab_v.at[b, :, core], tab_s.at[b % 2], tab_r.at[b], sib)

    def tab_arrive(b):
        dst = tab_v.at[b, :, 1 - core]
        return remote(dst, dst, tab_s.at[0], tab_r.at[b], sib)

    def small_in():
        return [pltpu.make_async_copy(pos_hbm, pos_v, load_s.at[5, 0]),
                pltpu.make_async_copy(freq_hbm, freq_v, load_s.at[5, 1])]

    def kv_copy(u, p, slot, step):
        b, h = split(u)
        ref = kv_hbm.at[b, h, :, pair_rows(p), :]
        return remote(ref, ref, ag_s.at[u, slot], ag_r.at[u, p], nbr[step])

    def send_kv(u, hops, base):
        for i, (p, step) in enumerate(hops):
            kv_copy(u, p, base + i, step).start()

    def have_own(b):
        for half in range(2):
            own_out(b, half).wait()
            kvx_in(b, half).wait_recv()

    def half_copy(u, p, slot, step, own):
        b, h = split(u)
        half = 0 if p == c else 1
        dst = kv_hbm.at[b, h, :, piece_rows((own_pieces if own else sib_pieces)[half]), :]
        src = ready_v.at[b % 2, 0, h, :, pl.ds(half * PIECE, PIECE), :] if own else dst
        return remote(src, dst, ag_s.at[u, slot], ag_r.at[u, p], nbr[step])

    def fast_hop(u, own):
        for i, (p, step) in enumerate(early_hops + first_hops):
            half_copy(u, p, i, step, own).start()

    def early_hop(u):
        send_kv(u, early_hops, 0)

    def first_hop(u):
        send_kv(u, first_hops, len(early_hops))

    def relay_hop(u):
        for p, _ in relay_hops:
            kv_copy(u, p, 0, X_STEP).wait_recv()
        send_kv(u, relay_hops, len(early_hops) + len(first_hops))

    def loads(u):
        b, h = split(u)
        slot = u % 2
        late = pl.ds(0, n_late)
        return [
            pltpu.make_async_copy(q_hbm.at[mine + b, :, h], q_v.at[slot, core], load_s.at[0, slot]),
            pltpu.make_async_copy(g_hbm.at[mine + b, :, h], g_v.at[slot, core], load_s.at[1, slot]),
            pltpu.make_async_copy(qs_hbm.at[b, :, h], q_v.at[slot, 1 - core], load_s.at[2, slot]),
            pltpu.make_async_copy(gs_hbm.at[b, :, h], g_v.at[slot, 1 - core], load_s.at[3, slot]),
            pltpu.make_async_copy(kv_hbm.at[b, h, :, late, :], kv_v.at[slot, :, late, :], load_s.at[4, slot]),
        ]

    def start_loads(u):
        @pl.when(u % HEADS == 0)
        def _():
            qx(u // HEADS).wait_recv()
            gx(u // HEADS).wait_recv()
            tab_arrive(u // HEADS).wait_recv()

        for p in needed:
            if p not in [r for r, _ in relay_hops]:
                kv_copy(u, p, 0, X_STEP).wait_recv()
        for copy in loads(u):
            copy.start()

    def out_local(u):
        b, h = split(u)
        slot = u % 2
        return [pltpu.make_async_copy(o_v.at[slot, core], o_hbm.at[mine + b, :, h], out_s.at[0, slot]),
                pltpu.make_async_copy(dq_v.at[slot, core], dq_hbm.at[mine + b, :, h], out_s.at[1, slot])]

    def out_remote(u):
        b, h = split(u)
        slot = u % 2
        return [remote(o_v.at[slot, 1 - core], o_hbm.at[mine + b, :, h], out_s.at[2, slot], out_r.at[0, b], sib),
                remote(dq_v.at[slot, 1 - core], dq_hbm.at[mine + b, :, h], out_s.at[3, slot], out_r.at[1, b], sib)]

    def out_arrive(b):
        return [remote(q_hbm.at[other + b], o_hbm.at[other + b], out_s.at[2, 0], out_r.at[0, b], sib),
                remote(q_hbm.at[other + b], dq_hbm.at[other + b], out_s.at[3, 0], out_r.at[1, b], sib)]

    def wait_outs(u):
        for copy in out_local(u):
            copy.wait()
        for copy in out_remote(u):
            copy.wait_send()

    def sum_copy(u, p, i, step):
        k, slot = inbox(c ^ step).index((p, c)), u % INBOX_RING
        return remote(part.at[u % PART_RING, :, pair_rows(p), :], recv.at[slot, k],
                      sum_s.at[i, u % PART_RING], sum_r.at[slot, k], nbr[step])

    def sum_arrive(u, k):
        dst = recv.at[u % INBOX_RING, k]
        return remote(dst, dst, sum_s.at[0, 0], sum_r.at[u % INBOX_RING, k], nbr[X_STEP])

    def give_credits(u, pairs):
        @pl.when(u + INBOX_RING < UNITS)
        def _():
            for k, (pair, src) in enumerate(inbox(c)):
                if pair in pairs:
                    pl.semaphore_signal(credit.at[outbox(src).index((pair, src ^ c))], inc=1,
                                        device_id={'cp': 2 * src + core}, device_id_type=MESH_ID)

    def take_credits(u, which):
        @pl.when(u >= INBOX_RING)
        def _():
            for i in which:
                pl.semaphore_wait(credit.at[i], 1)

    def messages(p):
        return [k for k, (pair, _) in enumerate(inbox(c)) if pair == p]

    def wait_sums(u):
        for i, (p, step) in enumerate(leaves + relays):
            sum_copy(u, p, i, step).wait_send()

    def send_leaves(u):
        take_credits(u, range(len(leaves)))
        for i, (p, step) in enumerate(leaves):
            sum_copy(u, p, i, step).start()

    def add_relays(u):
        for p, _ in relays:
            for k in messages(p):
                sum_arrive(u, k).wait_recv()
                part[u % PART_RING, :, pair_rows(p), :] += recv[u % INBOX_RING, k]
        give_credits(u, [p for p, _ in relays])

    def send_relays(u):
        take_credits(u, range(len(leaves), len(leaves) + len(relays)))
        for i, (p, step) in enumerate(relays):
            sum_copy(u, p, len(leaves) + i, step).start()

    def fin_local(u):
        b, h = split(u)
        return pltpu.make_async_copy(fin_v.at[u % 2, core], gkv_hbm.at[mine + b, h], fin_s.at[0, u % 2])

    def fin_remote(u):
        b, h = split(u)
        return remote(fin_v.at[u % 2, 1 - core], gkv_hbm.at[mine + b, h], fin_s.at[1, u % 2], fin_r.at[b], sib)

    def fin_arrive(b):
        dst = gkv_hbm.at[other + b]
        return remote(dst, dst, fin_s.at[1, 0], fin_r.at[b], sib)

    def wait_fin(u):
        fin_local(u).wait()
        fin_remote(u).wait_send()

    def finish(u):
        @pl.when(u >= 2)
        def _():
            wait_fin(u - 2)

        b, slot = u // HEADS, u % 2
        for late, p in ((0, c), (1, N_PAIRS - 1 - c)):
            total = part[u % PART_RING, :, pair_rows(p), :]
            for k in messages(p):
                sum_arrive(u, k).wait_recv()
                total = total + recv[u % INBOX_RING, k]
            for i in range(2):
                who = 1 - i if late else i
                toks = slice(late * PIECE, (late + 1) * PIECE)
                dk = total[0, i * PIECE:(i + 1) * PIECE] * (DIM ** -0.5)
                dk = dk * tab_v[b, 0, who, toks] - swap_pairs(dk) * tab_v[b, 1, who, toks]
                fin_v[slot, who, 0, toks] = dk.astype(jnp.bfloat16)
                fin_v[slot, who, 1, toks] = total[1, i * PIECE:(i + 1) * PIECE].astype(jnp.bfloat16)
        give_credits(u, [c, N_PAIRS - 1 - c])

    def send_fin(u):
        fin_local(u).start()
        fin_remote(u).start()

    def exchange_queries(b):
        qx(b).start()
        gx(b).start()

    for device in (sib, nbr[X_STEP], nbr[Y_STEP]):
        pl.semaphore_signal(barrier, inc=1, device_id={'cp': device}, device_id_type=MESH_ID)
    for copy in small_in():
        copy.start()
    start_raw(jnp.int32(0))
    start_raw(jnp.int32(1))
    row, col = iota((HEADS * PAIR, HEADS * PAIR), 0), iota((HEADS * PAIR, HEADS * PAIR), 1)
    perm_in[...] = (col == (row % PAIR) * HEADS + row // PAIR).astype(jnp.float32).astype(jnp.bfloat16)
    for copy in small_in():
        copy.wait()

    def up_to(op, first, last):
        def one(u, carry):
            op(u)
            return carry

        lax.fori_loop(first, last, one, 0)

    def start_step(j, carry):
        make_ready(j)

        @pl.when(j == 0)
        def _():
            pl.semaphore_wait(barrier, 3)

        send_ready(j)

        @pl.when(j == 0)
        def _():
            for u in range(FAST_UNITS):
                fast_hop(jnp.int32(u), True)
            have_own(j)
            for u in range(FAST_UNITS):
                fast_hop(jnp.int32(u), False)
            exchange_queries(j)

        up_to(relay_hop, jnp.where(j < RELAY_LEAD, jnp.maximum(j - 1, 0), RELAY_LEAD), jnp.minimum(j + j // 3, RELAY_LEAD))
        up_to(first_hop, jnp.clip(2 * j, FAST_UNITS, START_UNITS), jnp.clip(2 * j + 2, FAST_UNITS, START_UNITS))

        @pl.when(j >= 1)
        def _():
            have_own(j)

        up_to(early_hop, jnp.maximum(HEADS * j, FAST_UNITS), HEADS * j + HEADS)
        return carry

    lax.fori_loop(0, START_BATCHES, start_step, 0)
    start_loads(jnp.int32(0))

    def tick(t, carry):
        @pl.when((t % 2 == 0) & (t // 2 + START_BATCHES < BATCHES))
        def _():
            make_ready(t // 2 + START_BATCHES)
            send_ready(t // 2 + START_BATCHES)

        @pl.when((t % 2 == 1) & (t // 2 + START_BATCHES < BATCHES))
        def _():
            have_own(t // 2 + START_BATCHES)

        @pl.when((t % HEADS == 0) & (t // HEADS + 1 < BATCHES))
        def _():
            exchange_queries(t // HEADS + 1)

        @pl.when((t == 0) & (START_UNITS < UNITS))
        def _():
            first_hop(t + START_UNITS)

        @pl.when((t + HOP_LEAD > START_UNITS) & (t + HOP_LEAD < UNITS))
        def _():
            first_hop(t + HOP_LEAD)

        @pl.when((t >= 1) & (2 * t - 2 + START_EARLY < UNITS))
        def _():
            early_hop(2 * t - 2 + START_EARLY)
            early_hop(2 * t - 1 + START_EARLY)

        @pl.when(t + RELAY_LEAD < UNITS)
        def _():
            relay_hop(t + RELAY_LEAD)

        @pl.when((t >= 1) & (t - 1 < UNITS))
        def _():
            send_leaves(t - 1)

        @pl.when((t >= 1 + SUM_LAG) & (t - 1 - SUM_LAG < UNITS))
        def _():
            add_relays(t - 1 - SUM_LAG)

        @pl.when((t >= 1 + OWN_LAG) & (t - 1 - OWN_LAG < UNITS))
        def _():
            finish(t - 1 - OWN_LAG)

        @pl.when((t >= 1 + SUM_LAG) & (t - 1 - SUM_LAG < UNITS))
        def _():
            send_relays(t - 1 - SUM_LAG)

        @pl.when((t >= 1 + OWN_LAG) & (t - 1 - OWN_LAG < UNITS))
        def _():
            send_fin(t - 1 - OWN_LAG)

        @pl.when(t < UNITS)
        def _():
            for copy in loads(t):
                copy.wait()

            @pl.when(t + 1 < UNITS)
            def _():
                start_loads(t + 1)

            @pl.when(t >= 2)
            def _():
                wait_outs(t - 2)

            @pl.when(t >= PART_RING)
            def _():
                wait_sums(t - PART_RING)

            slot = t % 2
            unit_compute(c, q_v.at[slot], g_v.at[slot], tab_v.at[t // HEADS], kv_v.at[slot], o_v.at[slot],
                         dq_v.at[slot], part.at[t % PART_RING], kt, vt, s_a, s_b, s_e)
            for copy in out_local(t) + out_remote(t):
                copy.start()

        return carry

    lax.fori_loop(0, UNITS + 1 + OWN_LAG, tick, 0)

    for u in range(UNITS - 2, UNITS):
        wait_outs(jnp.int32(u))
        wait_fin(jnp.int32(u))

    def drain_batch(b, carry):
        @pl.when(b >= BATCHES - 2)
        def _():
            for half in range(2):
                kvx(b, half).wait_send()
            tab_out(b).wait_send()

        qx(b).wait_send()
        gx(b).wait_send()
        for copy in out_arrive(b):
            copy.wait_recv()
        fin_arrive(b).wait_recv()
        return carry

    lax.fori_loop(0, BATCHES, drain_batch, 0)

    def drain_sums(u, carry):
        wait_sums(u)
        return carry

    lax.fori_loop(UNITS - PART_RING, UNITS, drain_sums, 0)

    def drain_kv(u, carry):
        @pl.when(u >= FAST_UNITS)
        def _():
            for i, (p, step) in enumerate(early_hops + first_hops):
                kv_copy(u, p, i, step).wait_send()

        for i, (p, step) in enumerate(relay_hops):
            kv_copy(u, p, len(early_hops + first_hops) + i, step).wait_send()
        return carry

    lax.fori_loop(0, UNITS, drain_kv, 0)


def attend_kernel(*refs):
    me = lax.axis_index('cp')
    chip, core = me // 2, me % 2
    barrier = pltpu.get_barrier_semaphore()
    for c in range(4):
        @pl.when(chip == c)
        def _(c=c):
            chip_program(c, core, barrier, *refs)


def attend(q5, g5, keys, values, positions, freq):
    any_spec = pl.BlockSpec(memory_space=pl.ANY)
    hbm_spec = pl.BlockSpec(memory_space=pltpu.HBM)
    head_shape = pltpu.VMEM((2,) + q5.shape, jnp.bfloat16)
    half_shape = pltpu.HBM((BATCHES,) + q5.shape[1:], jnp.bfloat16)
    head_buf = pltpu.VMEM((2, 2, PAIR, GROUP, DIM), jnp.bfloat16)
    dma = pltpu.SemaphoreType.DMA
    return pl.pallas_call(
        attend_kernel, name='attend',
        in_specs=[any_spec] * 6,
        out_specs=[any_spec] + [hbm_spec] * 4,
        out_shape=[head_shape,
                   pltpu.HBM((2 * BATCHES, HEADS, 2, PAIR, DIM), jnp.bfloat16),
                   pltpu.HBM((BATCHES, HEADS, 2, N_PAIRS * PAIR, DIM), jnp.bfloat16),
                   half_shape, half_shape],
        scratch_shapes=[
            head_buf, head_buf, head_buf, head_buf,
            pltpu.VMEM((2, 2, N_PAIRS * PAIR, DIM), jnp.bfloat16),
            pltpu.VMEM((BATCHES, 2, 2, PAIR, DIM), jnp.float32),
            pltpu.VMEM((2, 2, PAIR, DIM), jnp.float32),
            pltpu.VMEM((2 * BATCHES, PAIR), jnp.int32),
            pltpu.VMEM((1, DIM), jnp.float32),
            pltpu.VMEM((2, 2, 2, HEADS * PAIR, DIM), jnp.bfloat16),
            pltpu.VMEM((2, 2, HEADS, 2, PAIR, DIM), jnp.bfloat16),
            pltpu.VMEM((PART_RING, 2, N_PAIRS * PAIR, DIM), jnp.float32),
            pltpu.VMEM((INBOX_RING, N_INBOX, 2, PAIR, DIM), jnp.float32),
            pltpu.VMEM((2, 2, 2, PAIR, DIM), jnp.bfloat16),
            pltpu.VMEM((HEADS * PAIR, HEADS * PAIR), jnp.bfloat16),
            pltpu.VMEM((DIM, N_PAIRS * PAIR), jnp.bfloat16),
            pltpu.VMEM((DIM, N_PAIRS * PAIR), jnp.bfloat16),
            pltpu.VMEM((N_PAIRS * PAIR, 32 * GROUP), jnp.float32),
            pltpu.VMEM((N_PAIRS * PAIR, 32 * GROUP), jnp.float32),
            pltpu.VMEM((4 * PAIR, PIECE * GROUP), jnp.float32),
            dma((2, 2, 2)), dma((BATCHES, 2)), dma((BATCHES, 2)), dma((BATCHES, 2)), dma((2,)), dma((BATCHES,)),
            dma((BATCHES,)), dma((BATCHES,)), dma((BATCHES,)), dma((BATCHES,)),
            dma((UNITS, 7)), dma((UNITS, 7)), dma((N_OUTBOX, PART_RING)), dma((INBOX_RING, N_INBOX)),
            dma((6, 2)), dma((4, 2)), dma((2, BATCHES)), dma((2, 2)), dma((BATCHES,)),
            pltpu.SemaphoreType.REGULAR((N_OUTBOX,)),
        ],
        compiler_params=pltpu.CompilerParams(
            collective_id=0, has_side_effects=True, vmem_limit_bytes=32512 * 1024),
    )(*(pltpu.with_memory_space_constraint(x, pltpu.HBM) for x in (q5, g5, keys, values, positions, freq)))


def place_kernel(odq, gkv, o_out, dq_out, gk_out, gv_out, in_v, out_v, perm, sems, in_s, out_s):
    n_batch = gkv.shape[0]

    def batch_in(b):
        return pltpu.make_async_copy(gkv.at[b], in_v.at[b], in_s.at[b])

    def batch_out(b):
        return [pltpu.make_async_copy(out_v.at[b, i], dst.at[b], out_s.at[b, i]) for i, dst in enumerate((gk_out, gv_out))]

    def start_in(b, carry):
        batch_in(b).start()
        return carry

    lax.fori_loop(0, n_batch, start_in, 0)
    part = n_batch // 4
    large = [pltpu.make_async_copy(odq.at[k, pl.ds(i * part, part)], dst.at[pl.ds(i * part, part)], sems.at[k, i])
             for i in range(4) for k, dst in enumerate((o_out, dq_out))]
    for copy in large:
        copy.start()
    row, col = iota(perm.shape, 0), iota(perm.shape, 1)
    perm[...] = (row == (col % PAIR) * HEADS + col // PAIR).astype(jnp.float32).astype(jnp.bfloat16)

    def regroup(b, carry):
        batch_in(b).wait()
        for i in range(2):
            rows = in_v[b, :, i].reshape(HEADS * PAIR, DIM)
            out_v[b, i] = dot_nn(perm[...], rows).astype(jnp.bfloat16)
        for copy in batch_out(b):
            copy.start()
        return carry

    lax.fori_loop(0, n_batch, regroup, 0)

    def finish_out(b, carry):
        for copy in batch_out(b):
            copy.wait()
        return carry

    lax.fori_loop(0, n_batch, finish_out, 0)
    for copy in large:
        copy.wait()


def place(odq, gkv):
    any_spec = pl.BlockSpec(memory_space=pl.ANY)
    n_batch = gkv.shape[0]
    head_shape = pltpu.HBM(odq.shape[1:], jnp.bfloat16)
    row_shape = pltpu.HBM((n_batch, HEADS * PAIR, DIM), jnp.bfloat16)
    dma = pltpu.SemaphoreType.DMA
    return pl.pallas_call(
        place_kernel, name='place', in_specs=[any_spec] * 2, out_specs=[any_spec] * 4,
        out_shape=[head_shape, head_shape, row_shape, row_shape],
        scratch_shapes=[pltpu.VMEM(gkv.shape, jnp.bfloat16), pltpu.VMEM((n_batch, 2, HEADS * PAIR, DIM), jnp.bfloat16),
                        pltpu.VMEM((HEADS * PAIR, HEADS * PAIR), jnp.bfloat16),
                        dma((2, 4)), dma((n_batch,)), dma((n_batch, 2))],
        compiler_params=pltpu.CompilerParams(vmem_limit_bytes=12 * 1024 * 1024),
    )(odq, pltpu.with_memory_space_constraint(gkv, pltpu.HBM))


def solution(mesh):
    head_spec = P(None, 'cp', 'tp', None)
    pos_spec = P(None, 'cp')

    def local_step(query, keys, values, positions, grad_out):
        batch, length, n_heads, dim = query.shape
        split_shape = (batch, length, HEADS, GROUP, dim)
        row_shape = (batch, length * HEADS, dim)
        outs = attend(query.reshape(split_shape), grad_out.reshape(split_shape), keys.reshape(row_shape),
                      values.reshape(row_shape), positions, jnp.asarray(lane_freq(dim)))
        return tuple(out.reshape(like.shape) for out, like in zip(place(*outs[:2]), (query, query, keys, values)))

    return jax.shard_map(local_step, mesh=mesh,
                         in_specs=(head_spec, head_spec, head_spec, pos_spec, head_spec),
                         out_specs=(head_spec, head_spec, head_spec, head_spec), check_vma=False)
```

```python
import functools

import jax
import jax.numpy as jnp
import numpy as np
from jax import lax
from jax.experimental import pallas as pl
from jax.experimental.pallas import tpu as pltpu
from jax.sharding import PartitionSpec as P

ROPE_THETA = 1000000.0
LOG2E = 1.4426950408889634
DIM = 128
GROUP = 8
HEADS = 4
PIECE = 64
PAIR = 128
N_PAIRS = 8
BATCHES = 8
UNITS = BATCHES * HEADS
KEY_BLOCK = 512
STEP_LAG = 2
MESH_ID = pl.DeviceIdType.MESH

X_STEP, Y_STEP = 1, 2
FIRST_HOP = [(0, 0, X_STEP), (0, 0, Y_STEP), (1, 1, X_STEP), (1, 1, Y_STEP), (2, 2, X_STEP), (2, 2, Y_STEP),
             (3, 3, X_STEP), (3, 3, Y_STEP), (4, 3, X_STEP), (4, 3, Y_STEP), (5, 2, Y_STEP), (5, 2, X_STEP),
             (6, 1, X_STEP)]
RELAY_HOP = [(0, 2, X_STEP), (1, 3, X_STEP), (2, 3, Y_STEP), (3, 2, Y_STEP), (4, 1, X_STEP), (5, 3, Y_STEP)]
SUM_LEAF = [(3, 0, Y_STEP), (4, 0, X_STEP), (2, 0, Y_STEP), (6, 0, X_STEP), (2, 1, Y_STEP), (5, 1, X_STEP),
            (0, 1, X_STEP), (3, 1, Y_STEP), (1, 2, Y_STEP), (4, 2, X_STEP), (0, 3, X_STEP), (1, 3, Y_STEP)]
SUM_RELAY = [(0, 2, Y_STEP), (1, 0, X_STEP), (2, 3, X_STEP), (3, 2, X_STEP), (4, 1, Y_STEP), (5, 0, Y_STEP)]

START_BATCHES = 6
START_UNITS = 8
START_RELAYS = 4
RELAY_LEAD = 6
START_EARLY = HEADS * START_BATCHES
FAST_UNITS = 2
EARLY_HOP = [(0, 0, X_STEP), (0, 0, Y_STEP), (1, 1, Y_STEP)]
SUM_LAG = 4
OWN_LAG = 8
PART_RING = OWN_LAG + 2
INBOX_RING = 9


def owner(pair):
    return pair if pair < 4 else 7 - pair


def inbox(chip):
    found = []
    for pair, src, step in SUM_LEAF + SUM_RELAY:
        if src ^ step == chip:
            found.append((pair, src))
    return found


def outbox(chip):
    return [(pair, step) for pair, src, step in SUM_LEAF + SUM_RELAY if src == chip]


N_INBOX = max(len(inbox(c)) for c in range(4))
N_OUTBOX = max(len(outbox(c)) for c in range(4))


def lane_freq(head_dim):
    exponent = np.arange(head_dim // 2, dtype=np.float64) * (2.0 / head_dim)
    return np.repeat(ROPE_THETA ** -exponent, 2).astype(np.float32)[None, :]


def dot_nn(a, b):
    return jnp.dot(a, b, preferred_element_type=jnp.float32)


def dot_nt(a, b):
    return lax.dot_general(a, b, (((1,), (1,)), ((), ())), preferred_element_type=jnp.float32)


def iota(shape, axis):
    return lax.broadcasted_iota(jnp.int32, shape, axis)


def identity():
    return (iota((DIM, DIM), 0) == iota((DIM, DIM), 1)).astype(jnp.float32).astype(jnp.bfloat16)


def swap_pairs(x):
    return jnp.where(iota(x.shape, 1) % 2 == 0, pltpu.roll(x, DIM - 1, axis=1), pltpu.roll(x, 1, axis=1))


def rows_steps(n_keys, tok, seg, q_v, g_v, tab, kv, kt, vt, part, o_v, dq_v, s_ref):
    core, start, place = seg
    rows = tok * GROUP
    scale = DIM ** -0.5
    c1 = scale * LOG2E
    toks = pl.ds(start, tok)

    def table(k):
        return jnp.broadcast_to(tab[k, core, toks, :][:, None, :], (tok, GROUP, DIM)).reshape(rows, DIM)

    x = q_v[core, toks].astype(jnp.float32).reshape(rows, DIM)
    qr = (x * table(0) + swap_pairs(x) * table(1)).astype(jnp.bfloat16)
    g = g_v[core, toks].astype(jnp.float32).reshape(rows, DIM).astype(jnp.bfloat16)
    blocks = [(a, min(KEY_BLOCK, n_keys - a)) for a in range(0, n_keys, KEY_BLOCK)]
    m8 = None
    for a, n in blocks:
        s = dot_nt(kv[0, a:a + n, :], qr) * c1
        if a + n == n_keys:
            last = s[n - PAIR:, :]
            q_tok = iota(last.shape, 1) // GROUP + place
            last = jnp.where(iota(last.shape, 0) <= q_tok, last, -jnp.inf)
            s = last if n == PAIR else jnp.concatenate([s[:n - PAIR, :], last], axis=0)
        s_ref[a:a + n, :] = s
        f = jnp.max(s.reshape(n // 8, 8, rows), axis=0)
        m8 = f if m8 is None else jnp.maximum(m8, f)
        yield
    row_max = jnp.max(m8, axis=0, keepdims=True)
    l8 = None
    o_t = None
    for a, n in blocks:
        p = jnp.exp2(s_ref[a:a + n, :] - row_max)
        s_ref[a:a + n, :] = p
        f = jnp.sum(p.reshape(n // 8, 8, rows), axis=0)
        l8 = f if l8 is None else l8 + f
        d = dot_nn(vt[:, a:a + n], p.astype(jnp.bfloat16))
        o_t = d if o_t is None else o_t + d
        yield
    inv = 1.0 / jnp.sum(l8, axis=0, keepdims=True)
    out_t = o_t * inv
    o_v[core, toks] = jnp.transpose(out_t).reshape(tok, GROUP, DIM).astype(jnp.bfloat16)
    delta = jnp.sum(dot_nt(identity(), g) * out_t, axis=0, keepdims=True)
    yield
    dq_t = None
    for a, n in blocks:
        p = s_ref[a:a + n, :] * inv
        ds = (p * (dot_nt(kv[1, a:a + n, :], g) - delta)).astype(jnp.bfloat16)
        part[1, a:a + n, :] += dot_nn(p.astype(jnp.bfloat16), g)
        part[0, a:a + n, :] += dot_nn(ds, qr)
        d = dot_nn(kt[:, a:a + n], ds)
        dq_t = d if dq_t is None else dq_t + d
        yield
    dq = jnp.transpose(dq_t) * scale
    dq = dq * table(0) - swap_pairs(dq) * table(1)
    dq_v[core, toks] = dq.reshape(tok, GROUP, DIM).astype(jnp.bfloat16)


def interleave(gens, lag):
    live, waiting, count = [], list(gens), 0
    while live or waiting:
        if waiting and (not live or count >= lag):
            live.append(waiting.pop(0))
            count = 0
        for gen in list(live):
            if next(gen, 'end') == 'end':
                live.remove(gen)
        count += 1


def unit_compute(c, q_v, g_v, tab, kv, o_v, dq_v, part, kt, vt, s_a, s_b, s_e):
    n_late, n_early = (N_PAIRS - c) * PAIR, (c + 1) * PAIR
    eye = identity()
    for a in range(0, n_late, 256):
        n = min(256, n_late - a)
        kt[:, a:a + n] = dot_nt(eye, kv[0, a:a + n, :]).astype(jnp.bfloat16)
        vt[:, a:a + n] = dot_nt(eye, kv[1, a:a + n, :]).astype(jnp.bfloat16)
    part[:, :n_late, :] = jnp.zeros((2, n_late, DIM), jnp.float32)
    refs = (q_v, g_v, tab, kv, kt, vt, part, o_v, dq_v)

    def step(i, carry):
        late = [rows_steps(n_late, 32, (1 - i, PIECE + 32 * k, i * PIECE + 32 * k), *refs, s)
                for k, s in ((0, s_a), (1, s_b))]
        early = rows_steps(n_early, PIECE, (i, 0, i * PIECE), *refs, s_e)
        interleave(late + [early], STEP_LAG)
        return carry

    lax.fori_loop(0, 2, step, 0)


def remote(src, dst, send_sem, recv_sem, device):
    return pltpu.make_async_remote_copy(src_ref=src, dst_ref=dst, send_sem=send_sem, recv_sem=recv_sem,
                                        device_id={'cp': device}, device_id_type=MESH_ID)


def chip_program(c, core, barrier, q_hbm, g_hbm, k_hbm, v_hbm, pos_hbm, freq_hbm, odq_hbm, gkv_hbm, kv_hbm, qs_hbm, gs_hbm,
                 q_v, g_v, o_v, dq_v, kv_v, tab_v, tab_x, pos_v, freq_v, raw_v, ready_v, part, recv, fin_v,
                 perm_in, kt, vt, s_a, s_b, s_e,
                 raw_s, kvl_s, kvx_s, kvx_r, tab_s, tab_r, qx_s, qx_r, gx_s, gx_r, ag_s, ag_r, sum_s, sum_r,
                 load_s, out_s, out_r, fin_s, fin_r, credit):
    o_hbm, dq_hbm = odq_hbm.at[0], odq_hbm.at[1]
    n_late = (N_PAIRS - c) * PAIR
    sib = 2 * c + 1 - core
    nbr = {step: 2 * (c ^ step) + core for step in (X_STEP, Y_STEP)}
    mine, other = BATCHES * core, BATCHES * (1 - core)
    early_hops = [(p, step) for p, src, step in EARLY_HOP if src == c]
    first_hops = [(p, step) for p, src, step in FIRST_HOP if src == c and (p, src, step) not in EARLY_HOP]
    relay_hops = [(p, step) for p, src, step in RELAY_HOP if src == c]
    leaves = [(p, step) for p, src, step in SUM_LEAF if src == c]
    relays = [(p, step) for p, src, step in SUM_RELAY if src == c]
    needed = [p for p in range(N_PAIRS - c) if owner(p) != c]
    sib_pieces = (2 * c + 1 - core, 15 - 2 * c - (1 - core))

    def split(u):
        return u // HEADS, u % HEADS

    def pair_rows(p):
        return pl.ds(p * PAIR, PAIR)

    own_pieces = (2 * c + core, 15 - 2 * c - core)

    def raw_in(b, side):
        src, slot = (mine, other)[side] + b, b % 2
        return [pltpu.make_async_copy(k_hbm.at[src], raw_v.at[slot, side, 0], raw_s.at[slot, side, 0]),
                pltpu.make_async_copy(v_hbm.at[src], raw_v.at[slot, side, 1], raw_s.at[slot, side, 1])]

    def start_raw(b):
        for side in (1, 0):
            for copy in raw_in(b, side):
                copy.start()

    def piece_rows(piece):
        return pl.ds(pl.multiple_of(piece * PIECE, PIECE), PIECE)

    def own_out(b, half):
        return pltpu.make_async_copy(ready_v.at[b % 2, 0, :, :, pl.ds(half * PIECE, PIECE), :],
                                     kv_hbm.at[b, :, :, piece_rows(own_pieces[half]), :], kvl_s.at[b, half])

    def kvx(b, half):
        return remote(ready_v.at[b % 2, 1, :, :, pl.ds(half * PIECE, PIECE), :],
                      kv_hbm.at[b, :, :, piece_rows(own_pieces[half]), :], kvx_s.at[b, half], kvx_r.at[b, half], sib)

    def kvx_in(b, half):
        dst = kv_hbm.at[b, :, :, piece_rows(sib_pieces[half]), :]
        return remote(dst, dst, kvx_s.at[b, half], kvx_r.at[b, half], sib)

    def make_table(tab, row):
        pos = pos_v[pl.ds(row, 1), :].astype(jnp.float32)
        angles = jnp.transpose(jnp.broadcast_to(pos, (PAIR, PAIR))) * freq_v[...]
        tab[0] = jnp.cos(angles)
        sine_val = jnp.sin(angles)
        tab[1] = jnp.where(iota(sine_val.shape, 1) % 2 == 0, -sine_val, sine_val)

    def make_ready(b):
        slot, part_rows = b % 2, PAIR // HEADS

        @pl.when(b >= 2)
        def _():
            for half in range(2):
                kvx(b - 2, half).wait_send()
            tab_out(b - 2).wait_send()

        @pl.when(b == 2)
        def _():
            for u in range(FAST_UNITS):
                for i, (p, step) in enumerate(early_hops + first_hops):
                    kv_copy(jnp.int32(u), p, i, step).wait_send()

        make_table(tab_x.at[slot], other + b)
        make_table(tab_v.at[b, :, core], mine + b)
        for side in (1, 0):
            for copy in raw_in(b, side):
                copy.wait()
            tab = tab_x.at[slot] if side else tab_v.at[b, :, core]
            for i in range(2):
                blocks = [dot_nn(perm_in[...], raw_v[slot, side, i, j * PAIR:(j + 1) * PAIR]) for j in range(HEADS)]
                for h in range(HEADS):
                    x = jnp.concatenate([block[h * part_rows:(h + 1) * part_rows] for block in blocks], axis=0)
                    if i == 0:
                        x = x * tab[0] + swap_pairs(x) * tab[1]
                    ready_v[slot, side, h, i] = x.astype(jnp.bfloat16)
        for half in range(2):
            own_out(b, half).start()

        @pl.when(b + 2 < BATCHES)
        def _():
            start_raw(b + 2)

    def send_ready(b):
        for half in range(2):
            kvx(b, half).start()
        tab_out(b).start()

    def qx(b):
        return remote(q_hbm.at[other + b], qs_hbm.at[b], qx_s.at[b], qx_r.at[b], sib)

    def gx(b):
        return remote(g_hbm.at[other + b], gs_hbm.at[b], gx_s.at[b], gx_r.at[b], sib)

    def tab_out(b):
        return remote(tab_x.at[b % 2], tab_v.at[b, :, core], tab_s.at[b % 2], tab_r.at[b], sib)

    def tab_arrive(b):
        dst = tab_v.at[b, :, 1 - core]
        return remote(dst, dst, tab_s.at[0], tab_r.at[b], sib)

    def small_in():
        return [pltpu.make_async_copy(pos_hbm, pos_v, load_s.at[5, 0]),
                pltpu.make_async_copy(freq_hbm, freq_v, load_s.at[5, 1])]

    def kv_copy(u, p, slot, step):
        b, h = split(u)
        ref = kv_hbm.at[b, h, :, pair_rows(p), :]
        return remote(ref, ref, ag_s.at[u, slot], ag_r.at[u, p], nbr[step])

    def send_kv(u, hops, base):
        for i, (p, step) in enumerate(hops):
            kv_copy(u, p, base + i, step).start()

    def have_own(b):
        for half in range(2):
            own_out(b, half).wait()
            kvx_in(b, half).wait_recv()

    def half_copy(u, p, slot, step, own):
        b, h = split(u)
        half = 0 if p == c else 1
        dst = kv_hbm.at[b, h, :, piece_rows((own_pieces if own else sib_pieces)[half]), :]
        src = ready_v.at[b % 2, 0, h, :, pl.ds(half * PIECE, PIECE), :] if own else dst
        return remote(src, dst, ag_s.at[u, slot], ag_r.at[u, p], nbr[step])

    def fast_hop(u, own):
        for i, (p, step) in enumerate(early_hops + first_hops):
            half_copy(u, p, i, step, own).start()

    def early_hop(u):
        send_kv(u, early_hops, 0)

    def first_hop(u):
        send_kv(u, first_hops, len(early_hops))

    def relay_hop(u):
        for p, _ in relay_hops:
            kv_copy(u, p, 0, X_STEP).wait_recv()
        send_kv(u, relay_hops, len(early_hops) + len(first_hops))

    def loads(u):
        b, h = split(u)
        slot = u % 2
        late = pl.ds(0, n_late)
        return [
            pltpu.make_async_copy(q_hbm.at[mine + b, :, h], q_v.at[slot, core], load_s.at[0, slot]),
            pltpu.make_async_copy(g_hbm.at[mine + b, :, h], g_v.at[slot, core], load_s.at[1, slot]),
            pltpu.make_async_copy(qs_hbm.at[b, :, h], q_v.at[slot, 1 - core], load_s.at[2, slot]),
            pltpu.make_async_copy(gs_hbm.at[b, :, h], g_v.at[slot, 1 - core], load_s.at[3, slot]),
            pltpu.make_async_copy(kv_hbm.at[b, h, :, late, :], kv_v.at[slot, :, late, :], load_s.at[4, slot]),
        ]

    def start_loads(u):
        @pl.when(u % HEADS == 0)
        def _():
            qx(u // HEADS).wait_recv()
            gx(u // HEADS).wait_recv()
            tab_arrive(u // HEADS).wait_recv()

        for p in needed:
            if p not in [r for r, _ in relay_hops]:
                kv_copy(u, p, 0, X_STEP).wait_recv()
        for copy in loads(u):
            copy.start()

    def out_local(u):
        b, h = split(u)
        slot = u % 2
        return [pltpu.make_async_copy(o_v.at[slot, core], o_hbm.at[mine + b, :, h], out_s.at[0, slot]),
                pltpu.make_async_copy(dq_v.at[slot, core], dq_hbm.at[mine + b, :, h], out_s.at[1, slot])]

    def out_remote(u):
        b, h = split(u)
        slot = u % 2
        return [remote(o_v.at[slot, 1 - core], o_hbm.at[mine + b, :, h], out_s.at[2, slot], out_r.at[0, b], sib),
                remote(dq_v.at[slot, 1 - core], dq_hbm.at[mine + b, :, h], out_s.at[3, slot], out_r.at[1, b], sib)]

    def out_arrive(b):
        return [remote(q_hbm.at[other + b], o_hbm.at[other + b], out_s.at[2, 0], out_r.at[0, b], sib),
                remote(q_hbm.at[other + b], dq_hbm.at[other + b], out_s.at[3, 0], out_r.at[1, b], sib)]

    def wait_outs(u):
        for copy in out_local(u):
            copy.wait()
        for copy in out_remote(u):
            copy.wait_send()

    def sum_copy(u, p, i, step):
        k, slot = inbox(c ^ step).index((p, c)), u % INBOX_RING
        return remote(part.at[u % PART_RING, :, pair_rows(p), :], recv.at[slot, k],
                      sum_s.at[i, u % PART_RING], sum_r.at[slot, k], nbr[step])

    def sum_arrive(u, k):
        dst = recv.at[u % INBOX_RING, k]
        return remote(dst, dst, sum_s.at[0, 0], sum_r.at[u % INBOX_RING, k], nbr[X_STEP])

    def give_credits(u, pairs):
        @pl.when(u + INBOX_RING < UNITS)
        def _():
            for k, (pair, src) in enumerate(inbox(c)):
                if pair in pairs:
                    pl.semaphore_signal(credit.at[outbox(src).index((pair, src ^ c))], inc=1,
                                        device_id={'cp': 2 * src + core}, device_id_type=MESH_ID)

    def take_credits(u, which):
        @pl.when(u >= INBOX_RING)
        def _():
            for i in which:
                pl.semaphore_wait(credit.at[i], 1)

    def messages(p):
        return [k for k, (pair, _) in enumerate(inbox(c)) if pair == p]

    def wait_sums(u):
        for i, (p, step) in enumerate(leaves + relays):
            sum_copy(u, p, i, step).wait_send()

    def send_leaves(u):
        take_credits(u, range(len(leaves)))
        for i, (p, step) in enumerate(leaves):
            sum_copy(u, p, i, step).start()

    def add_relays(u):
        for p, _ in relays:
            for k in messages(p):
                sum_arrive(u, k).wait_recv()
                part[u % PART_RING, :, pair_rows(p), :] += recv[u % INBOX_RING, k]
        give_credits(u, [p for p, _ in relays])

    def send_relays(u):
        take_credits(u, range(len(leaves), len(leaves) + len(relays)))
        for i, (p, step) in enumerate(relays):
            sum_copy(u, p, len(leaves) + i, step).start()

    def fin_local(u):
        b, h = split(u)
        return pltpu.make_async_copy(fin_v.at[u % 2, core], gkv_hbm.at[mine + b, h], fin_s.at[0, u % 2])

    def fin_remote(u):
        b, h = split(u)
        return remote(fin_v.at[u % 2, 1 - core], gkv_hbm.at[mine + b, h], fin_s.at[1, u % 2], fin_r.at[b], sib)

    def fin_arrive(b):
        dst = gkv_hbm.at[other + b]
        return remote(dst, dst, fin_s.at[1, 0], fin_r.at[b], sib)

    def wait_fin(u):
        fin_local(u).wait()
        fin_remote(u).wait_send()

    def finish(u):
        @pl.when(u >= 2)
        def _():
            wait_fin(u - 2)

        b, slot = u // HEADS, u % 2
        for late, p in ((0, c), (1, N_PAIRS - 1 - c)):
            total = part[u % PART_RING, :, pair_rows(p), :]
            for k in messages(p):
                sum_arrive(u, k).wait_recv()
                total = total + recv[u % INBOX_RING, k]
            for i in range(2):
                who = 1 - i if late else i
                toks = slice(late * PIECE, (late + 1) * PIECE)
                dk = total[0, i * PIECE:(i + 1) * PIECE] * (DIM ** -0.5)
                dk = dk * tab_v[b, 0, who, toks] - swap_pairs(dk) * tab_v[b, 1, who, toks]
                fin_v[slot, who, 0, toks] = dk.astype(jnp.bfloat16)
                fin_v[slot, who, 1, toks] = total[1, i * PIECE:(i + 1) * PIECE].astype(jnp.bfloat16)
        give_credits(u, [c, N_PAIRS - 1 - c])

    def send_fin(u):
        fin_local(u).start()
        fin_remote(u).start()

    def exchange_queries(b):
        qx(b).start()
        gx(b).start()

    for device in (sib, nbr[X_STEP], nbr[Y_STEP]):
        pl.semaphore_signal(barrier, inc=1, device_id={'cp': device}, device_id_type=MESH_ID)
    for copy in small_in():
        copy.start()
    start_raw(jnp.int32(0))
    start_raw(jnp.int32(1))
    row, col = iota(perm_in.shape, 0), iota(perm_in.shape, 1)
    part_rows = PAIR // HEADS
    perm_in[...] = (col == (row % part_rows) * HEADS + row // part_rows).astype(jnp.float32).astype(jnp.bfloat16)
    for copy in small_in():
        copy.wait()

    def up_to(op, first, last):
        def one(u, carry):
            op(u)
            return carry

        lax.fori_loop(first, last, one, 0)

    def start_step(j, carry):
        make_ready(j)

        @pl.when(j == 0)
        def _():
            pl.semaphore_wait(barrier, 3)

        send_ready(j)

        @pl.when(j == 0)
        def _():
            for u in range(FAST_UNITS):
                fast_hop(jnp.int32(u), True)
            have_own(j)
            for u in range(FAST_UNITS):
                fast_hop(jnp.int32(u), False)
            exchange_queries(j)

        up_to(relay_hop, jnp.where(j < START_RELAYS, jnp.maximum(j - 1, 0), START_RELAYS),
              jnp.minimum(j + j // 3, START_RELAYS))
        up_to(first_hop, jnp.clip(2 * j, FAST_UNITS, START_UNITS), jnp.clip(2 * j + 2, FAST_UNITS, START_UNITS))

        @pl.when(j >= 1)
        def _():
            have_own(j)

        up_to(early_hop, jnp.maximum(HEADS * j, FAST_UNITS), HEADS * j + HEADS)
        return carry

    lax.fori_loop(0, START_BATCHES, start_step, 0)
    start_loads(jnp.int32(0))

    def tick(t, carry):
        @pl.when((t % 2 == 0) & (t // 2 + START_BATCHES < BATCHES))
        def _():
            make_ready(t // 2 + START_BATCHES)
            send_ready(t // 2 + START_BATCHES)

        @pl.when((t % 2 == 1) & (t // 2 + START_BATCHES < BATCHES))
        def _():
            have_own(t // 2 + START_BATCHES)

        @pl.when((t % HEADS == 0) & (t // HEADS + 1 < BATCHES))
        def _():
            exchange_queries(t // HEADS + 1)

        @pl.when((t >= 1) & (2 * t - 2 + START_EARLY < UNITS))
        def _():
            early_hop(2 * t - 2 + START_EARLY)
            early_hop(2 * t - 1 + START_EARLY)

        @pl.when(t == 0)
        def _():
            for u in range(START_RELAYS, RELAY_LEAD - 1):
                relay_hop(jnp.int32(u))

        @pl.when(t + RELAY_LEAD - 1 < UNITS)
        def _():
            relay_hop(t + RELAY_LEAD - 1)

        @pl.when((t >= 1) & (t - 1 < UNITS))
        def _():
            send_leaves(t - 1)

        @pl.when((t >= 1 + SUM_LAG) & (t - 1 - SUM_LAG < UNITS))
        def _():
            add_relays(t - 1 - SUM_LAG)

        @pl.when((t >= 1 + OWN_LAG) & (t - 1 - OWN_LAG < UNITS))
        def _():
            finish(t - 1 - OWN_LAG)

        @pl.when((t >= 1 + SUM_LAG) & (t - 1 - SUM_LAG < UNITS))
        def _():
            send_relays(t - 1 - SUM_LAG)

        @pl.when((t >= 1 + OWN_LAG) & (t - 1 - OWN_LAG < UNITS))
        def _():
            send_fin(t - 1 - OWN_LAG)

        @pl.when(t + START_UNITS < UNITS)
        def _():
            first_hop(t + START_UNITS)

        @pl.when(t < UNITS)
        def _():
            for copy in loads(t):
                copy.wait()

            @pl.when(t + 1 < UNITS)
            def _():
                start_loads(t + 1)

            @pl.when(t >= 2)
            def _():
                wait_outs(t - 2)

            @pl.when(t >= PART_RING)
            def _():
                wait_sums(t - PART_RING)

            slot = t % 2
            unit_compute(c, q_v.at[slot], g_v.at[slot], tab_v.at[t // HEADS], kv_v.at[slot], o_v.at[slot],
                         dq_v.at[slot], part.at[t % PART_RING], kt, vt, s_a, s_b, s_e)
            for copy in out_local(t) + out_remote(t):
                copy.start()

        return carry

    lax.fori_loop(0, UNITS + 1 + OWN_LAG, tick, 0)

    for u in range(UNITS - 2, UNITS):
        wait_outs(jnp.int32(u))
        wait_fin(jnp.int32(u))

    def drain_batch(b, carry):
        @pl.when(b >= BATCHES - 2)
        def _():
            for half in range(2):
                kvx(b, half).wait_send()
            tab_out(b).wait_send()

        qx(b).wait_send()
        gx(b).wait_send()
        for copy in out_arrive(b):
            copy.wait_recv()
        fin_arrive(b).wait_recv()
        return carry

    lax.fori_loop(0, BATCHES, drain_batch, 0)

    def drain_sums(u, carry):
        wait_sums(u)
        return carry

    lax.fori_loop(UNITS - PART_RING, UNITS, drain_sums, 0)

    def drain_kv(u, carry):
        @pl.when(u >= FAST_UNITS)
        def _():
            for i, (p, step) in enumerate(early_hops + first_hops):
                kv_copy(u, p, i, step).wait_send()

        for i, (p, step) in enumerate(relay_hops):
            kv_copy(u, p, len(early_hops + first_hops) + i, step).wait_send()
        return carry

    lax.fori_loop(0, UNITS, drain_kv, 0)


def attend_kernel(*refs):
    me = lax.axis_index('cp')
    chip, core = me // 2, me % 2
    barrier = pltpu.get_barrier_semaphore()
    for c in range(4):
        @pl.when(chip == c)
        def _(c=c):
            chip_program(c, core, barrier, *refs)


def attend(q5, g5, keys, values, positions, freq):
    any_spec = pl.BlockSpec(memory_space=pl.ANY)
    hbm_spec = pl.BlockSpec(memory_space=pltpu.HBM)
    head_shape = pltpu.VMEM((2,) + q5.shape, jnp.bfloat16)
    half_shape = pltpu.HBM((BATCHES,) + q5.shape[1:], jnp.bfloat16)
    head_buf = pltpu.VMEM((2, 2, PAIR, GROUP, DIM), jnp.bfloat16)
    dma = pltpu.SemaphoreType.DMA
    return pl.pallas_call(
        attend_kernel, name='attend',
        in_specs=[any_spec] * 6,
        out_specs=[any_spec] + [hbm_spec] * 4,
        out_shape=[head_shape,
                   pltpu.HBM((2 * BATCHES, HEADS, 2, PAIR, DIM), jnp.bfloat16),
                   pltpu.HBM((BATCHES, HEADS, 2, N_PAIRS * PAIR, DIM), jnp.bfloat16),
                   half_shape, half_shape],
        scratch_shapes=[
            head_buf, head_buf, head_buf, head_buf,
            pltpu.VMEM((2, 2, N_PAIRS * PAIR, DIM), jnp.bfloat16),
            pltpu.VMEM((BATCHES, 2, 2, PAIR, DIM), jnp.float32),
            pltpu.VMEM((2, 2, PAIR, DIM), jnp.float32),
            pltpu.VMEM((2 * BATCHES, PAIR), jnp.int32),
            pltpu.VMEM((1, DIM), jnp.float32),
            pltpu.VMEM((2, 2, 2, HEADS * PAIR, DIM), jnp.bfloat16),
            pltpu.VMEM((2, 2, HEADS, 2, PAIR, DIM), jnp.bfloat16),
            pltpu.VMEM((PART_RING, 2, N_PAIRS * PAIR, DIM), jnp.float32),
            pltpu.VMEM((INBOX_RING, N_INBOX, 2, PAIR, DIM), jnp.float32),
            pltpu.VMEM((2, 2, 2, PAIR, DIM), jnp.bfloat16),
            pltpu.VMEM((PAIR, PAIR), jnp.bfloat16),
            pltpu.VMEM((DIM, N_PAIRS * PAIR), jnp.bfloat16),
            pltpu.VMEM((DIM, N_PAIRS * PAIR), jnp.bfloat16),
            pltpu.VMEM((N_PAIRS * PAIR, 32 * GROUP), jnp.float32),
            pltpu.VMEM((N_PAIRS * PAIR, 32 * GROUP), jnp.float32),
            pltpu.VMEM((4 * PAIR, PIECE * GROUP), jnp.float32),
            dma((2, 2, 2)), dma((BATCHES, 2)), dma((BATCHES, 2)), dma((BATCHES, 2)), dma((2,)), dma((BATCHES,)),
            dma((BATCHES,)), dma((BATCHES,)), dma((BATCHES,)), dma((BATCHES,)),
            dma((UNITS, 7)), dma((UNITS, 7)), dma((N_OUTBOX, PART_RING)), dma((INBOX_RING, N_INBOX)),
            dma((6, 2)), dma((4, 2)), dma((2, BATCHES)), dma((2, 2)), dma((BATCHES,)),
            pltpu.SemaphoreType.REGULAR((N_OUTBOX,)),
        ],
        compiler_params=pltpu.CompilerParams(
            collective_id=0, has_side_effects=True, vmem_limit_bytes=32512 * 1024),
    )(*(pltpu.with_memory_space_constraint(x, pltpu.HBM) for x in (q5, g5, keys, values, positions, freq)))


def place_kernel(odq, gkv, o_out, dq_out, gk_out, gv_out, in_v, out_v, perm, sems, in_s, out_s):
    n_batch = gkv.shape[0]

    def batch_in(b):
        return pltpu.make_async_copy(gkv.at[b], in_v.at[b], in_s.at[b])

    def batch_out(b):
        return [pltpu.make_async_copy(out_v.at[b, i], dst.at[b], out_s.at[b, i]) for i, dst in enumerate((gk_out, gv_out))]

    def start_in(b, carry):
        batch_in(b).start()
        return carry

    lax.fori_loop(0, n_batch, start_in, 0)
    part = n_batch // 4
    large = [pltpu.make_async_copy(odq.at[k, pl.ds(i * part, part)], dst.at[pl.ds(i * part, part)], sems.at[k, i])
             for i in range(4) for k, dst in enumerate((o_out, dq_out))]
    for copy in large:
        copy.start()
    row, col = iota(perm.shape, 0), iota(perm.shape, 1)
    perm[...] = (row == (col % PAIR) * HEADS + col // PAIR).astype(jnp.float32).astype(jnp.bfloat16)

    def regroup(b, carry):
        batch_in(b).wait()
        for i in range(2):
            rows = in_v[b, :, i].reshape(HEADS * PAIR, DIM)
            out_v[b, i] = dot_nn(perm[...], rows).astype(jnp.bfloat16)
        for copy in batch_out(b):
            copy.start()
        return carry

    lax.fori_loop(0, n_batch, regroup, 0)

    def finish_out(b, carry):
        for copy in batch_out(b):
            copy.wait()
        return carry

    lax.fori_loop(0, n_batch, finish_out, 0)
    for copy in large:
        copy.wait()


def place(odq, gkv):
    any_spec = pl.BlockSpec(memory_space=pl.ANY)
    n_batch = gkv.shape[0]
    head_shape = pltpu.HBM(odq.shape[1:], jnp.bfloat16)
    row_shape = pltpu.HBM((n_batch, HEADS * PAIR, DIM), jnp.bfloat16)
    dma = pltpu.SemaphoreType.DMA
    return pl.pallas_call(
        place_kernel, name='place', in_specs=[any_spec] * 2, out_specs=[any_spec] * 4,
        out_shape=[head_shape, head_shape, row_shape, row_shape],
        scratch_shapes=[pltpu.VMEM(gkv.shape, jnp.bfloat16), pltpu.VMEM((n_batch, 2, HEADS * PAIR, DIM), jnp.bfloat16),
                        pltpu.VMEM((HEADS * PAIR, HEADS * PAIR), jnp.bfloat16),
                        dma((2, 4)), dma((n_batch,)), dma((n_batch, 2))],
        compiler_params=pltpu.CompilerParams(vmem_limit_bytes=12 * 1024 * 1024),
    )(odq, pltpu.with_memory_space_constraint(gkv, pltpu.HBM))


def solution(mesh):
    head_spec = P(None, 'cp', 'tp', None)
    pos_spec = P(None, 'cp')

    def local_step(query, keys, values, positions, grad_out):
        batch, length, n_heads, dim = query.shape
        split_shape = (batch, length, HEADS, GROUP, dim)
        row_shape = (batch, length * HEADS, dim)
        outs = attend(query.reshape(split_shape), grad_out.reshape(split_shape), keys.reshape(row_shape),
                      values.reshape(row_shape), positions, jnp.asarray(lane_freq(dim)))
        return tuple(out.reshape(like.shape) for out, like in zip(place(*outs[:2]), (query, query, keys, values)))

    return jax.shard_map(local_step, mesh=mesh,
                         in_specs=(head_spec, head_spec, head_spec, pos_spec, head_spec),
                         out_specs=(head_spec, head_spec, head_spec, head_spec), check_vma=False)
```

```python
import functools

import jax
import jax.numpy as jnp
import numpy as np
from jax import lax
from jax.experimental import pallas as pl
from jax.experimental.pallas import tpu as pltpu
from jax.sharding import PartitionSpec as P

ROPE_THETA = 1000000.0
LOG2E = 1.4426950408889634
DIM = 128
GROUP = 8
HEADS = 4
PIECE = 64
PAIR = 128
N_PAIRS = 8
BATCHES = 8
UNITS = BATCHES * HEADS
KEY_BLOCK = 512
STEP_LAG = 2
MESH_ID = pl.DeviceIdType.MESH

X_STEP, Y_STEP = 1, 2
FIRST_HOP = [(0, 0, X_STEP), (0, 0, Y_STEP), (1, 1, X_STEP), (1, 1, Y_STEP), (2, 2, X_STEP), (2, 2, Y_STEP),
             (3, 3, X_STEP), (3, 3, Y_STEP), (4, 3, X_STEP), (4, 3, Y_STEP), (5, 2, Y_STEP), (5, 2, X_STEP),
             (6, 1, X_STEP)]
RELAY_HOP = [(0, 2, X_STEP), (1, 3, X_STEP), (2, 3, Y_STEP), (3, 2, Y_STEP), (4, 1, X_STEP), (5, 3, Y_STEP)]
SUM_LEAF = [(3, 0, Y_STEP), (4, 0, X_STEP), (2, 0, Y_STEP), (6, 0, X_STEP), (2, 1, Y_STEP), (5, 1, X_STEP),
            (0, 1, X_STEP), (3, 1, Y_STEP), (1, 2, Y_STEP), (4, 2, X_STEP), (0, 3, X_STEP), (1, 3, Y_STEP)]
SUM_RELAY = [(0, 2, Y_STEP), (1, 0, X_STEP), (2, 3, X_STEP), (3, 2, X_STEP), (4, 1, Y_STEP), (5, 0, Y_STEP)]

START_BATCHES = 6
START_UNITS = 8
START_RELAYS = 4
RELAY_LEAD = 6
START_EARLY = HEADS * START_BATCHES
FAST_UNITS = 2
EARLY_HOP = [(0, 0, X_STEP), (0, 0, Y_STEP), (1, 1, Y_STEP)]
SUM_LAG = 4
OWN_LAG = 8
PART_RING = OWN_LAG + 2
INBOX_RING = 9


def owner(pair):
    return pair if pair < 4 else 7 - pair


def inbox(chip):
    found = []
    for pair, src, step in SUM_LEAF + SUM_RELAY:
        if src ^ step == chip:
            found.append((pair, src))
    return found


def outbox(chip):
    return [(pair, step) for pair, src, step in SUM_LEAF + SUM_RELAY if src == chip]


N_INBOX = max(len(inbox(c)) for c in range(4))
N_OUTBOX = max(len(outbox(c)) for c in range(4))


def lane_freq(head_dim):
    exponent = np.arange(head_dim // 2, dtype=np.float64) * (2.0 / head_dim)
    return np.repeat(ROPE_THETA ** -exponent, 2).astype(np.float32)[None, :]


def dot_nn(a, b):
    return jnp.dot(a, b, preferred_element_type=jnp.float32)


def dot_nt(a, b):
    return lax.dot_general(a, b, (((1,), (1,)), ((), ())), preferred_element_type=jnp.float32)


def iota(shape, axis):
    return lax.broadcasted_iota(jnp.int32, shape, axis)


def identity():
    return (iota((DIM, DIM), 0) == iota((DIM, DIM), 1)).astype(jnp.float32).astype(jnp.bfloat16)


def swap_pairs(x):
    return jnp.where(iota(x.shape, 1) % 2 == 0, pltpu.roll(x, DIM - 1, axis=1), pltpu.roll(x, 1, axis=1))


def rows_steps(n_keys, tok, seg, q_v, g_v, tab, kv, kt, vt, part, o_v, dq_v, s_ref):
    core, start, place = seg
    rows = tok * GROUP
    scale = DIM ** -0.5
    c1 = scale * LOG2E
    toks = pl.ds(start, tok)

    def table(k):
        return jnp.broadcast_to(tab[k, core, toks, :][:, None, :], (tok, GROUP, DIM)).reshape(rows, DIM)

    x = q_v[core, toks].astype(jnp.float32).reshape(rows, DIM)
    qr = (x * table(0) + swap_pairs(x) * table(1)).astype(jnp.bfloat16)
    g = g_v[core, toks].astype(jnp.float32).reshape(rows, DIM).astype(jnp.bfloat16)
    blocks = [(a, min(KEY_BLOCK, n_keys - a)) for a in range(0, n_keys, KEY_BLOCK)]
    m8 = None
    for a, n in blocks:
        s = dot_nt(kv[0, a:a + n, :], qr) * c1
        if a + n == n_keys:
            last = s[n - PAIR:, :]
            q_tok = iota(last.shape, 1) // GROUP + place
            last = jnp.where(iota(last.shape, 0) <= q_tok, last, -jnp.inf)
            s = last if n == PAIR else jnp.concatenate([s[:n - PAIR, :], last], axis=0)
        s_ref[a:a + n, :] = s
        f = jnp.max(s.reshape(n // 8, 8, rows), axis=0)
        m8 = f if m8 is None else jnp.maximum(m8, f)
        yield
    row_max = jnp.max(m8, axis=0, keepdims=True)
    l8 = None
    o_t = None
    for a, n in blocks:
        p = jnp.exp2(s_ref[a:a + n, :] - row_max)
        s_ref[a:a + n, :] = p
        f = jnp.sum(p.reshape(n // 8, 8, rows), axis=0)
        l8 = f if l8 is None else l8 + f
        d = dot_nn(vt[:, a:a + n], p.astype(jnp.bfloat16))
        o_t = d if o_t is None else o_t + d
        yield
    inv = 1.0 / jnp.sum(l8, axis=0, keepdims=True)
    out_t = o_t * inv
    o_v[core, toks] = jnp.transpose(out_t).reshape(tok, GROUP, DIM).astype(jnp.bfloat16)
    delta = jnp.sum(dot_nt(identity(), g) * out_t, axis=0, keepdims=True)
    yield
    dq_t = None
    for a, n in blocks:
        p = s_ref[a:a + n, :] * inv
        ds = (p * (dot_nt(kv[1, a:a + n, :], g) - delta)).astype(jnp.bfloat16)
        part[1, a:a + n, :] += dot_nn(p.astype(jnp.bfloat16), g)
        part[0, a:a + n, :] += dot_nn(ds, qr)
        d = dot_nn(kt[:, a:a + n], ds)
        dq_t = d if dq_t is None else dq_t + d
        yield
    dq = jnp.transpose(dq_t) * scale
    dq = dq * table(0) - swap_pairs(dq) * table(1)
    dq_v[core, toks] = dq.reshape(tok, GROUP, DIM).astype(jnp.bfloat16)


def interleave(gens, lag):
    live, waiting, count = [], list(gens), 0
    while live or waiting:
        if waiting and (not live or count >= lag):
            live.append(waiting.pop(0))
            count = 0
        for gen in list(live):
            if next(gen, 'end') == 'end':
                live.remove(gen)
        count += 1


def unit_compute(c, q_v, g_v, tab, kv, o_v, dq_v, part, kt, vt, s_a, s_b, s_e):
    n_late, n_early = (N_PAIRS - c) * PAIR, (c + 1) * PAIR
    eye = identity()
    for a in range(0, n_late, 256):
        n = min(256, n_late - a)
        kt[:, a:a + n] = dot_nt(eye, kv[0, a:a + n, :]).astype(jnp.bfloat16)
        vt[:, a:a + n] = dot_nt(eye, kv[1, a:a + n, :]).astype(jnp.bfloat16)
    part[:, :n_late, :] = jnp.zeros((2, n_late, DIM), jnp.float32)
    refs = (q_v, g_v, tab, kv, kt, vt, part, o_v, dq_v)

    def step(i, carry):
        late = [rows_steps(n_late, 32, (1 - i, PIECE + 32 * k, i * PIECE + 32 * k), *refs, s)
                for k, s in ((0, s_a), (1, s_b))]
        early = rows_steps(n_early, PIECE, (i, 0, i * PIECE), *refs, s_e)
        interleave(late + [early], STEP_LAG)
        return carry

    lax.fori_loop(0, 2, step, 0)


def remote(src, dst, send_sem, recv_sem, device):
    return pltpu.make_async_remote_copy(src_ref=src, dst_ref=dst, send_sem=send_sem, recv_sem=recv_sem,
                                        device_id={'cp': device}, device_id_type=MESH_ID)


def chip_program(c, core, barrier, q_hbm, g_hbm, k_hbm, v_hbm, pos_hbm, freq_hbm, odq_hbm, gkv_hbm, kv_hbm, qs_hbm, gs_hbm,
                 q_v, g_v, o_v, dq_v, kv_v, tab_v, tab_x, pos_v, freq_v, raw_v, ready_v, part, recv, fin_v,
                 perm_in, kt, vt, s_a, s_b, s_e,
                 raw_s, kvl_s, kvx_s, kvx_r, tab_s, tab_r, qx_s, qx_r, gx_s, gx_r, ag_s, ag_r, sum_s, sum_r,
                 load_s, out_s, out_r, fin_s, fin_r, credit):
    o_hbm, dq_hbm = odq_hbm.at[0], odq_hbm.at[1]
    n_late = (N_PAIRS - c) * PAIR
    sib = 2 * c + 1 - core
    nbr = {step: 2 * (c ^ step) + core for step in (X_STEP, Y_STEP)}
    mine, other = BATCHES * core, BATCHES * (1 - core)
    early_hops = [(p, step) for p, src, step in EARLY_HOP if src == c]
    first_hops = [(p, step) for p, src, step in FIRST_HOP if src == c and (p, src, step) not in EARLY_HOP]
    relay_hops = [(p, step) for p, src, step in RELAY_HOP if src == c]
    leaves = [(p, step) for p, src, step in SUM_LEAF if src == c]
    relays = [(p, step) for p, src, step in SUM_RELAY if src == c]
    needed = [p for p in range(N_PAIRS - c) if owner(p) != c]
    sib_pieces = (2 * c + 1 - core, 15 - 2 * c - (1 - core))

    def split(u):
        return u // HEADS, u % HEADS

    def pair_rows(p):
        return pl.ds(p * PAIR, PAIR)

    own_pieces = (2 * c + core, 15 - 2 * c - core)

    def raw_in(b, side):
        src, slot = (mine, other)[side] + b, b % 2
        return [pltpu.make_async_copy(k_hbm.at[src], raw_v.at[slot, side, 0], raw_s.at[slot, side, 0]),
                pltpu.make_async_copy(v_hbm.at[src], raw_v.at[slot, side, 1], raw_s.at[slot, side, 1])]

    def start_raw(b):
        for side in (1, 0):
            for copy in raw_in(b, side):
                copy.start()

    def piece_rows(piece):
        return pl.ds(pl.multiple_of(piece * PIECE, PIECE), PIECE)

    def own_out(b, half):
        return pltpu.make_async_copy(ready_v.at[b % 2, 0, :, :, pl.ds(half * PIECE, PIECE), :],
                                     kv_hbm.at[b, :, :, piece_rows(own_pieces[half]), :], kvl_s.at[b, half])

    def kvx(b, half):
        return remote(ready_v.at[b % 2, 1, :, :, pl.ds(half * PIECE, PIECE), :],
                      kv_hbm.at[b, :, :, piece_rows(own_pieces[half]), :], kvx_s.at[b, half], kvx_r.at[b, half], sib)

    def kvx_in(b, half):
        dst = kv_hbm.at[b, :, :, piece_rows(sib_pieces[half]), :]
        return remote(dst, dst, kvx_s.at[b, half], kvx_r.at[b, half], sib)

    def make_table(tab, row):
        pos = pos_v[pl.ds(row, 1), :].astype(jnp.float32)
        angles = jnp.transpose(jnp.broadcast_to(pos, (PAIR, PAIR))) * freq_v[...]
        tab[0] = jnp.cos(angles)
        sine_val = jnp.sin(angles)
        tab[1] = jnp.where(iota(sine_val.shape, 1) % 2 == 0, -sine_val, sine_val)

    def make_ready(b):
        slot, part_rows = b % 2, PAIR // HEADS

        @pl.when(b >= 2)
        def _():
            for half in range(2):
                kvx(b - 2, half).wait_send()
            tab_out(b - 2).wait_send()

        @pl.when(b == 2)
        def _():
            for u in range(FAST_UNITS):
                for i, (p, step) in enumerate(early_hops + first_hops):
                    kv_copy(jnp.int32(u), p, i, step).wait_send()

        make_table(tab_x.at[slot], other + b)
        make_table(tab_v.at[b, :, core], mine + b)
        for side in (1, 0):
            for copy in raw_in(b, side):
                copy.wait()
            tab = tab_x.at[slot] if side else tab_v.at[b, :, core]
            for i in range(2):
                blocks = [dot_nn(perm_in[...], raw_v[slot, side, i, j * PAIR:(j + 1) * PAIR]) for j in range(HEADS)]
                for h in range(HEADS):
                    x = jnp.concatenate([block[h * part_rows:(h + 1) * part_rows] for block in blocks], axis=0)
                    if i == 0:
                        x = x * tab[0] + swap_pairs(x) * tab[1]
                    ready_v[slot, side, h, i] = x.astype(jnp.bfloat16)
        for half in range(2):
            own_out(b, half).start()

        @pl.when(b + 2 < BATCHES)
        def _():
            start_raw(b + 2)

    def send_ready(b):
        for half in range(2):
            kvx(b, half).start()
        tab_out(b).start()

    def qx(b):
        return remote(q_hbm.at[other + b], qs_hbm.at[b], qx_s.at[b], qx_r.at[b], sib)

    def gx(b):
        return remote(g_hbm.at[other + b], gs_hbm.at[b], gx_s.at[b], gx_r.at[b], sib)

    def tab_out(b):
        return remote(tab_x.at[b % 2], tab_v.at[b, :, core], tab_s.at[b % 2], tab_r.at[b], sib)

    def tab_arrive(b):
        dst = tab_v.at[b, :, 1 - core]
        return remote(dst, dst, tab_s.at[0], tab_r.at[b], sib)

    def small_in():
        return [pltpu.make_async_copy(pos_hbm, pos_v, load_s.at[5, 0]),
                pltpu.make_async_copy(freq_hbm, freq_v, load_s.at[5, 1])]

    def kv_copy(u, p, slot, step):
        b, h = split(u)
        ref = kv_hbm.at[b, h, :, pair_rows(p), :]
        return remote(ref, ref, ag_s.at[u, slot], ag_r.at[u, p], nbr[step])

    def send_kv(u, hops, base):
        for i, (p, step) in enumerate(hops):
            kv_copy(u, p, base + i, step).start()

    def have_own(b):
        for half in range(2):
            own_out(b, half).wait()
            kvx_in(b, half).wait_recv()

    def half_copy(u, p, slot, step, own):
        b, h = split(u)
        half = 0 if p == c else 1
        dst = kv_hbm.at[b, h, :, piece_rows((own_pieces if own else sib_pieces)[half]), :]
        src = ready_v.at[b % 2, 0, h, :, pl.ds(half * PIECE, PIECE), :] if own else dst
        return remote(src, dst, ag_s.at[u, slot], ag_r.at[u, p], nbr[step])

    def fast_hop(u, own):
        for i, (p, step) in enumerate(early_hops + first_hops):
            half_copy(u, p, i, step, own).start()

    def early_hop(u):
        send_kv(u, early_hops, 0)

    def first_hop(u):
        send_kv(u, first_hops, len(early_hops))

    def relay_hop(u):
        for p, _ in relay_hops:
            kv_copy(u, p, 0, X_STEP).wait_recv()
        send_kv(u, relay_hops, len(early_hops) + len(first_hops))

    def loads(u):
        b, h = split(u)
        slot = u % 2
        late = pl.ds(0, n_late)
        return [
            pltpu.make_async_copy(q_hbm.at[mine + b, :, h], q_v.at[slot, core], load_s.at[0, slot]),
            pltpu.make_async_copy(g_hbm.at[mine + b, :, h], g_v.at[slot, core], load_s.at[1, slot]),
            pltpu.make_async_copy(qs_hbm.at[b, :, h], q_v.at[slot, 1 - core], load_s.at[2, slot]),
            pltpu.make_async_copy(gs_hbm.at[b, :, h], g_v.at[slot, 1 - core], load_s.at[3, slot]),
            pltpu.make_async_copy(kv_hbm.at[b, h, :, late, :], kv_v.at[slot, :, late, :], load_s.at[4, slot]),
        ]

    def start_loads(u):
        @pl.when(u % HEADS == 0)
        def _():
            qx(u // HEADS).wait_recv()
            gx(u // HEADS).wait_recv()
            tab_arrive(u // HEADS).wait_recv()

        for p in needed:
            if p not in [r for r, _ in relay_hops]:
                kv_copy(u, p, 0, X_STEP).wait_recv()
        for copy in loads(u):
            copy.start()

    def out_local(u):
        b, h = split(u)
        slot = u % 2
        return [pltpu.make_async_copy(o_v.at[slot, core], o_hbm.at[mine + b, :, h], out_s.at[0, slot]),
                pltpu.make_async_copy(dq_v.at[slot, core], dq_hbm.at[mine + b, :, h], out_s.at[1, slot])]

    def out_remote(u):
        b, h = split(u)
        slot = u % 2
        return [remote(o_v.at[slot, 1 - core], o_hbm.at[mine + b, :, h], out_s.at[2, slot], out_r.at[0, b], sib),
                remote(dq_v.at[slot, 1 - core], dq_hbm.at[mine + b, :, h], out_s.at[3, slot], out_r.at[1, b], sib)]

    def out_arrive(b):
        return [remote(q_hbm.at[other + b], o_hbm.at[other + b], out_s.at[2, 0], out_r.at[0, b], sib),
                remote(q_hbm.at[other + b], dq_hbm.at[other + b], out_s.at[3, 0], out_r.at[1, b], sib)]

    def wait_outs(u):
        for copy in out_local(u):
            copy.wait()
        for copy in out_remote(u):
            copy.wait_send()

    def sum_copy(u, p, i, step):
        k, slot = inbox(c ^ step).index((p, c)), u % INBOX_RING
        return remote(part.at[u % PART_RING, :, pair_rows(p), :], recv.at[slot, k],
                      sum_s.at[i, u % PART_RING], sum_r.at[slot, k], nbr[step])

    def start_sum(u, p, i, step):
        k, slot = inbox(c ^ step).index((p, c)), u % INBOX_RING
        for j in range(2):
            remote(part.at[u % PART_RING, j, pair_rows(p), :], recv.at[slot, k, j],
                   sum_s.at[i, u % PART_RING], sum_r.at[slot, k], nbr[step]).start()

    def sum_arrive(u, k):
        dst = recv.at[u % INBOX_RING, k]
        return remote(dst, dst, sum_s.at[0, 0], sum_r.at[u % INBOX_RING, k], nbr[X_STEP])

    def give_credits(u, pairs):
        @pl.when(u + INBOX_RING < UNITS)
        def _():
            for k, (pair, src) in enumerate(inbox(c)):
                if pair in pairs:
                    pl.semaphore_signal(credit.at[outbox(src).index((pair, src ^ c))], inc=1,
                                        device_id={'cp': 2 * src + core}, device_id_type=MESH_ID)

    def take_credits(u, which):
        @pl.when(u >= INBOX_RING)
        def _():
            for i in which:
                pl.semaphore_wait(credit.at[i], 1)

    def messages(p):
        return [k for k, (pair, _) in enumerate(inbox(c)) if pair == p]

    def wait_sums(u):
        for i, (p, step) in enumerate(leaves + relays):
            sum_copy(u, p, i, step).wait_send()

    def send_leaves(u):
        take_credits(u, range(len(leaves)))
        for i, (p, step) in enumerate(leaves):
            start_sum(u, p, i, step)

    def add_relays(u):
        for p, _ in relays:
            for k in messages(p):
                sum_arrive(u, k).wait_recv()
                part[u % PART_RING, :, pair_rows(p), :] += recv[u % INBOX_RING, k]
        give_credits(u, [p for p, _ in relays])

    def send_relays(u):
        take_credits(u, range(len(leaves), len(leaves) + len(relays)))
        for i, (p, step) in enumerate(relays):
            start_sum(u, p, len(leaves) + i, step)

    def fin_local(u):
        b, h = split(u)
        return pltpu.make_async_copy(fin_v.at[u % 2, core], gkv_hbm.at[mine + b, h], fin_s.at[0, u % 2])

    def fin_remote(u):
        b, h = split(u)
        return remote(fin_v.at[u % 2, 1 - core], gkv_hbm.at[mine + b, h], fin_s.at[1, u % 2], fin_r.at[b], sib)

    def fin_arrive(b):
        dst = gkv_hbm.at[other + b]
        return remote(dst, dst, fin_s.at[1, 0], fin_r.at[b], sib)

    def wait_fin(u):
        fin_local(u).wait()
        fin_remote(u).wait_send()

    def finish(u):
        @pl.when(u >= 2)
        def _():
            wait_fin(u - 2)

        b, slot = u // HEADS, u % 2
        for late, p in ((0, c), (1, N_PAIRS - 1 - c)):
            total = part[u % PART_RING, :, pair_rows(p), :]
            for k in messages(p):
                sum_arrive(u, k).wait_recv()
                total = total + recv[u % INBOX_RING, k]
            for i in range(2):
                who = 1 - i if late else i
                toks = slice(late * PIECE, (late + 1) * PIECE)
                dk = total[0, i * PIECE:(i + 1) * PIECE] * (DIM ** -0.5)
                dk = dk * tab_v[b, 0, who, toks] - swap_pairs(dk) * tab_v[b, 1, who, toks]
                fin_v[slot, who, 0, toks] = dk.astype(jnp.bfloat16)
                fin_v[slot, who, 1, toks] = total[1, i * PIECE:(i + 1) * PIECE].astype(jnp.bfloat16)
        give_credits(u, [c, N_PAIRS - 1 - c])

    def send_fin(u):
        fin_local(u).start()
        fin_remote(u).start()

    def exchange_queries(b):
        qx(b).start()
        gx(b).start()

    for device in (sib, nbr[X_STEP], nbr[Y_STEP]):
        pl.semaphore_signal(barrier, inc=1, device_id={'cp': device}, device_id_type=MESH_ID)
    for copy in small_in():
        copy.start()
    start_raw(jnp.int32(0))
    start_raw(jnp.int32(1))
    row, col = iota(perm_in.shape, 0), iota(perm_in.shape, 1)
    part_rows = PAIR // HEADS
    perm_in[...] = (col == (row % part_rows) * HEADS + row // part_rows).astype(jnp.float32).astype(jnp.bfloat16)
    for copy in small_in():
        copy.wait()

    def up_to(op, first, last):
        def one(u, carry):
            op(u)
            return carry

        lax.fori_loop(first, last, one, 0)

    def start_step(j, carry):
        make_ready(j)

        @pl.when(j == 0)
        def _():
            pl.semaphore_wait(barrier, 3)

        send_ready(j)

        @pl.when(j == 0)
        def _():
            for u in range(FAST_UNITS):
                fast_hop(jnp.int32(u), True)
            have_own(j)
            for u in range(FAST_UNITS):
                fast_hop(jnp.int32(u), False)
            exchange_queries(j)

        up_to(relay_hop, jnp.where(j < START_RELAYS, jnp.maximum(j - 1, 0), START_RELAYS),
              jnp.minimum(j + j // 3, START_RELAYS))
        up_to(first_hop, jnp.clip(2 * j, FAST_UNITS, START_UNITS), jnp.clip(2 * j + 2, FAST_UNITS, START_UNITS))

        @pl.when(j >= 1)
        def _():
            have_own(j)

        up_to(early_hop, jnp.maximum(HEADS * j, FAST_UNITS), HEADS * j + HEADS)
        return carry

    lax.fori_loop(0, START_BATCHES, start_step, 0)
    start_loads(jnp.int32(0))

    def tick(t, carry):
        @pl.when((t % 2 == 0) & (t // 2 + START_BATCHES < BATCHES))
        def _():
            make_ready(t // 2 + START_BATCHES)
            send_ready(t // 2 + START_BATCHES)

        @pl.when((t % 2 == 1) & (t // 2 + START_BATCHES < BATCHES))
        def _():
            have_own(t // 2 + START_BATCHES)

        @pl.when((t % HEADS == 0) & (t // HEADS + 1 < BATCHES))
        def _():
            exchange_queries(t // HEADS + 1)

        @pl.when((t >= 1) & (2 * t - 2 + START_EARLY < UNITS))
        def _():
            early_hop(2 * t - 2 + START_EARLY)
            early_hop(2 * t - 1 + START_EARLY)

        @pl.when(t == 0)
        def _():
            for u in range(START_RELAYS, RELAY_LEAD - 1):
                relay_hop(jnp.int32(u))

        @pl.when(t + RELAY_LEAD - 1 < UNITS)
        def _():
            relay_hop(t + RELAY_LEAD - 1)

        @pl.when((t >= 1) & (t - 1 < UNITS))
        def _():
            send_leaves(t - 1)

        @pl.when((t >= 1 + SUM_LAG) & (t - 1 - SUM_LAG < UNITS))
        def _():
            add_relays(t - 1 - SUM_LAG)

        @pl.when((t >= 1 + OWN_LAG) & (t - 1 - OWN_LAG < UNITS))
        def _():
            finish(t - 1 - OWN_LAG)

        @pl.when((t >= 1 + SUM_LAG) & (t - 1 - SUM_LAG < UNITS))
        def _():
            send_relays(t - 1 - SUM_LAG)

        @pl.when((t >= 1 + OWN_LAG) & (t - 1 - OWN_LAG < UNITS))
        def _():
            send_fin(t - 1 - OWN_LAG)

        @pl.when(t + START_UNITS < UNITS)
        def _():
            first_hop(t + START_UNITS)

        @pl.when(t < UNITS)
        def _():
            for copy in loads(t):
                copy.wait()

            @pl.when(t + 1 < UNITS)
            def _():
                start_loads(t + 1)

            @pl.when(t >= 2)
            def _():
                wait_outs(t - 2)

            @pl.when(t >= PART_RING)
            def _():
                wait_sums(t - PART_RING)

            slot = t % 2
            unit_compute(c, q_v.at[slot], g_v.at[slot], tab_v.at[t // HEADS], kv_v.at[slot], o_v.at[slot],
                         dq_v.at[slot], part.at[t % PART_RING], kt, vt, s_a, s_b, s_e)
            for copy in out_local(t) + out_remote(t):
                copy.start()

        return carry

    lax.fori_loop(0, UNITS + 1 + OWN_LAG, tick, 0)

    for u in range(UNITS - 2, UNITS):
        wait_outs(jnp.int32(u))
        wait_fin(jnp.int32(u))

    def drain_batch(b, carry):
        @pl.when(b >= BATCHES - 2)
        def _():
            for half in range(2):
                kvx(b, half).wait_send()
            tab_out(b).wait_send()

        qx(b).wait_send()
        gx(b).wait_send()
        for copy in out_arrive(b):
            copy.wait_recv()
        fin_arrive(b).wait_recv()
        return carry

    lax.fori_loop(0, BATCHES, drain_batch, 0)

    def drain_sums(u, carry):
        wait_sums(u)
        return carry

    lax.fori_loop(UNITS - PART_RING, UNITS, drain_sums, 0)

    def drain_kv(u, carry):
        @pl.when(u >= FAST_UNITS)
        def _():
            for i, (p, step) in enumerate(early_hops + first_hops):
                kv_copy(u, p, i, step).wait_send()

        for i, (p, step) in enumerate(relay_hops):
            kv_copy(u, p, len(early_hops + first_hops) + i, step).wait_send()
        return carry

    lax.fori_loop(0, UNITS, drain_kv, 0)


def attend_kernel(*refs):
    me = lax.axis_index('cp')
    chip, core = me // 2, me % 2
    barrier = pltpu.get_barrier_semaphore()
    for c in range(4):
        @pl.when(chip == c)
        def _(c=c):
            chip_program(c, core, barrier, *refs)


def attend(q5, g5, keys, values, positions, freq):
    any_spec = pl.BlockSpec(memory_space=pl.ANY)
    hbm_spec = pl.BlockSpec(memory_space=pltpu.HBM)
    head_shape = pltpu.VMEM((2,) + q5.shape, jnp.bfloat16)
    half_shape = pltpu.HBM((BATCHES,) + q5.shape[1:], jnp.bfloat16)
    head_buf = pltpu.VMEM((2, 2, PAIR, GROUP, DIM), jnp.bfloat16)
    dma = pltpu.SemaphoreType.DMA
    return pl.pallas_call(
        attend_kernel, name='attend',
        in_specs=[any_spec] * 6,
        out_specs=[any_spec] + [hbm_spec] * 4,
        out_shape=[head_shape,
                   pltpu.HBM((2 * BATCHES, HEADS, 2, PAIR, DIM), jnp.bfloat16),
                   pltpu.HBM((BATCHES, HEADS, 2, N_PAIRS * PAIR, DIM), jnp.bfloat16),
                   half_shape, half_shape],
        scratch_shapes=[
            head_buf, head_buf, head_buf, head_buf,
            pltpu.VMEM((2, 2, N_PAIRS * PAIR, DIM), jnp.bfloat16),
            pltpu.VMEM((BATCHES, 2, 2, PAIR, DIM), jnp.float32),
            pltpu.VMEM((2, 2, PAIR, DIM), jnp.float32),
            pltpu.VMEM((2 * BATCHES, PAIR), jnp.int32),
            pltpu.VMEM((1, DIM), jnp.float32),
            pltpu.VMEM((2, 2, 2, HEADS * PAIR, DIM), jnp.bfloat16),
            pltpu.VMEM((2, 2, HEADS, 2, PAIR, DIM), jnp.bfloat16),
            pltpu.VMEM((PART_RING, 2, N_PAIRS * PAIR, DIM), jnp.float32),
            pltpu.VMEM((INBOX_RING, N_INBOX, 2, PAIR, DIM), jnp.float32),
            pltpu.VMEM((2, 2, 2, PAIR, DIM), jnp.bfloat16),
            pltpu.VMEM((PAIR, PAIR), jnp.bfloat16),
            pltpu.VMEM((DIM, N_PAIRS * PAIR), jnp.bfloat16),
            pltpu.VMEM((DIM, N_PAIRS * PAIR), jnp.bfloat16),
            pltpu.VMEM((N_PAIRS * PAIR, 32 * GROUP), jnp.float32),
            pltpu.VMEM((N_PAIRS * PAIR, 32 * GROUP), jnp.float32),
            pltpu.VMEM((4 * PAIR, PIECE * GROUP), jnp.float32),
            dma((2, 2, 2)), dma((BATCHES, 2)), dma((BATCHES, 2)), dma((BATCHES, 2)), dma((2,)), dma((BATCHES,)),
            dma((BATCHES,)), dma((BATCHES,)), dma((BATCHES,)), dma((BATCHES,)),
            dma((UNITS, 7)), dma((UNITS, 7)), dma((N_OUTBOX, PART_RING)), dma((INBOX_RING, N_INBOX)),
            dma((6, 2)), dma((4, 2)), dma((2, BATCHES)), dma((2, 2)), dma((BATCHES,)),
            pltpu.SemaphoreType.REGULAR((N_OUTBOX,)),
        ],
        compiler_params=pltpu.CompilerParams(
            collective_id=0, has_side_effects=True, vmem_limit_bytes=32512 * 1024),
    )(*(pltpu.with_memory_space_constraint(x, pltpu.HBM) for x in (q5, g5, keys, values, positions, freq)))


def place_kernel(odq, gkv, o_out, dq_out, gk_out, gv_out, in_v, out_v, perm, sems, in_s, out_s):
    n_batch = gkv.shape[0]

    def batch_in(b):
        return pltpu.make_async_copy(gkv.at[b], in_v.at[b], in_s.at[b])

    def batch_out(b):
        return [pltpu.make_async_copy(out_v.at[b, i], dst.at[b], out_s.at[b, i]) for i, dst in enumerate((gk_out, gv_out))]

    def start_in(b, carry):
        batch_in(b).start()
        return carry

    lax.fori_loop(0, n_batch, start_in, 0)
    part = n_batch // 4
    large = [pltpu.make_async_copy(odq.at[k, pl.ds(i * part, part)], dst.at[pl.ds(i * part, part)], sems.at[k, i])
             for i in range(4) for k, dst in enumerate((o_out, dq_out))]
    for copy in large:
        copy.start()
    row, col = iota(perm.shape, 0), iota(perm.shape, 1)
    perm[...] = (row == (col % PAIR) * HEADS + col // PAIR).astype(jnp.float32).astype(jnp.bfloat16)

    def regroup(b, carry):
        batch_in(b).wait()
        for i in range(2):
            rows = in_v[b, :, i].reshape(HEADS * PAIR, DIM)
            out_v[b, i] = dot_nn(perm[...], rows).astype(jnp.bfloat16)
        for copy in batch_out(b):
            copy.start()
        return carry

    lax.fori_loop(0, n_batch, regroup, 0)

    def finish_out(b, carry):
        for copy in batch_out(b):
            copy.wait()
        return carry

    lax.fori_loop(0, n_batch, finish_out, 0)
    for copy in large:
        copy.wait()


def place(odq, gkv):
    any_spec = pl.BlockSpec(memory_space=pl.ANY)
    n_batch = gkv.shape[0]
    head_shape = pltpu.HBM(odq.shape[1:], jnp.bfloat16)
    row_shape = pltpu.HBM((n_batch, HEADS * PAIR, DIM), jnp.bfloat16)
    dma = pltpu.SemaphoreType.DMA
    return pl.pallas_call(
        place_kernel, name='place', in_specs=[any_spec] * 2, out_specs=[any_spec] * 4,
        out_shape=[head_shape, head_shape, row_shape, row_shape],
        scratch_shapes=[pltpu.VMEM(gkv.shape, jnp.bfloat16), pltpu.VMEM((n_batch, 2, HEADS * PAIR, DIM), jnp.bfloat16),
                        pltpu.VMEM((HEADS * PAIR, HEADS * PAIR), jnp.bfloat16),
                        dma((2, 4)), dma((n_batch,)), dma((n_batch, 2))],
        compiler_params=pltpu.CompilerParams(vmem_limit_bytes=12 * 1024 * 1024),
    )(odq, pltpu.with_memory_space_constraint(gkv, pltpu.HBM))


def solution(mesh):
    head_spec = P(None, 'cp', 'tp', None)
    pos_spec = P(None, 'cp')

    def local_step(query, keys, values, positions, grad_out):
        batch, length, n_heads, dim = query.shape
        split_shape = (batch, length, HEADS, GROUP, dim)
        row_shape = (batch, length * HEADS, dim)
        outs = attend(query.reshape(split_shape), grad_out.reshape(split_shape), keys.reshape(row_shape),
                      values.reshape(row_shape), positions, jnp.asarray(lane_freq(dim)))
        return tuple(out.reshape(like.shape) for out, like in zip(place(*outs[:2]), (query, query, keys, values)))

    return jax.shard_map(local_step, mesh=mesh,
                         in_specs=(head_spec, head_spec, head_spec, pos_spec, head_spec),
                         out_specs=(head_spec, head_spec, head_spec, head_spec), check_vma=False)
```

```python
import functools

import jax
import jax.numpy as jnp
import numpy as np
from jax import lax
from jax.experimental import pallas as pl
from jax.experimental.pallas import tpu as pltpu
from jax.sharding import PartitionSpec as P

ROPE_THETA = 1000000.0
LOG2E = 1.4426950408889634
DIM = 128
GROUP = 8
HEADS = 4
PIECE = 64
PAIR = 128
N_PAIRS = 8
BATCHES = 8
UNITS = BATCHES * HEADS
KEY_BLOCK = 512
STEP_LAG = 2
MESH_ID = pl.DeviceIdType.MESH

X_STEP, Y_STEP = 1, 2
FIRST_HOP = [(0, 0, X_STEP), (0, 0, Y_STEP), (1, 1, X_STEP), (1, 1, Y_STEP), (2, 2, X_STEP), (2, 2, Y_STEP),
             (3, 3, X_STEP), (3, 3, Y_STEP), (4, 3, X_STEP), (4, 3, Y_STEP), (5, 2, Y_STEP), (5, 2, X_STEP),
             (6, 1, X_STEP)]
RELAY_HOP = [(0, 2, X_STEP), (1, 3, X_STEP), (2, 3, Y_STEP), (3, 2, Y_STEP), (4, 1, X_STEP), (5, 3, Y_STEP)]
SUM_LEAF = [(3, 0, Y_STEP), (4, 0, X_STEP), (2, 0, Y_STEP), (6, 0, X_STEP), (2, 1, Y_STEP), (5, 1, X_STEP),
            (0, 1, X_STEP), (3, 1, Y_STEP), (1, 2, Y_STEP), (4, 2, X_STEP), (0, 3, X_STEP), (1, 3, Y_STEP)]
SUM_RELAY = [(0, 2, Y_STEP), (1, 0, X_STEP), (2, 3, X_STEP), (3, 2, X_STEP), (4, 1, Y_STEP), (5, 0, Y_STEP)]

START_BATCHES = 6
START_UNITS = 8
START_RELAYS = 4
RELAY_LEAD = 6
HOP_LEADS = (8, 7, 8, 8)
START_EARLY = HEADS * START_BATCHES
FAST_UNITS = 2
EARLY_HOP = [(0, 0, X_STEP), (0, 0, Y_STEP), (1, 1, Y_STEP)]
SUM_LAG = 4
OWN_LAG = 8
PART_RING = OWN_LAG + 2
INBOX_RING = 9


def owner(pair):
    return pair if pair < 4 else 7 - pair


def inbox(chip):
    found = []
    for pair, src, step in SUM_LEAF + SUM_RELAY:
        if src ^ step == chip:
            found.append((pair, src))
    return found


def outbox(chip):
    return [(pair, step) for pair, src, step in SUM_LEAF + SUM_RELAY if src == chip]


N_INBOX = max(len(inbox(c)) for c in range(4))
N_OUTBOX = max(len(outbox(c)) for c in range(4))


def lane_freq(head_dim):
    exponent = np.arange(head_dim // 2, dtype=np.float64) * (2.0 / head_dim)
    return np.repeat(ROPE_THETA ** -exponent, 2).astype(np.float32)[None, :]


def dot_nn(a, b):
    return jnp.dot(a, b, preferred_element_type=jnp.float32)


def dot_nt(a, b):
    return lax.dot_general(a, b, (((1,), (1,)), ((), ())), preferred_element_type=jnp.float32)


def iota(shape, axis):
    return lax.broadcasted_iota(jnp.int32, shape, axis)


def identity():
    return (iota((DIM, DIM), 0) == iota((DIM, DIM), 1)).astype(jnp.float32).astype(jnp.bfloat16)


def swap_pairs(x):
    return jnp.where(iota(x.shape, 1) % 2 == 0, pltpu.roll(x, DIM - 1, axis=1), pltpu.roll(x, 1, axis=1))


def rows_steps(n_keys, tok, seg, q_v, g_v, tab, kv, kt, vt, part, o_v, dq_v, s_ref):
    core, start, place = seg
    rows = tok * GROUP
    scale = DIM ** -0.5
    c1 = scale * LOG2E
    toks = pl.ds(start, tok)

    def table(k):
        return jnp.broadcast_to(tab[k, core, toks, :][:, None, :], (tok, GROUP, DIM)).reshape(rows, DIM)

    x = q_v[core, toks].astype(jnp.float32).reshape(rows, DIM)
    qr = (x * table(0) + swap_pairs(x) * table(1)).astype(jnp.bfloat16)
    g = g_v[core, toks].astype(jnp.float32).reshape(rows, DIM).astype(jnp.bfloat16)
    blocks = [(a, min(KEY_BLOCK, n_keys - a)) for a in range(0, n_keys, KEY_BLOCK)]
    m8 = None
    for a, n in blocks:
        s = dot_nt(kv[0, a:a + n, :], qr) * c1
        if a + n == n_keys:
            last = s[n - PAIR:, :]
            q_tok = iota(last.shape, 1) // GROUP + place
            last = jnp.where(iota(last.shape, 0) <= q_tok, last, -jnp.inf)
            s = last if n == PAIR else jnp.concatenate([s[:n - PAIR, :], last], axis=0)
        s_ref[a:a + n, :] = s
        f = jnp.max(s.reshape(n // 8, 8, rows), axis=0)
        m8 = f if m8 is None else jnp.maximum(m8, f)
        yield
    row_max = jnp.max(m8, axis=0, keepdims=True)
    l8 = None
    o_t = None
    for a, n in blocks:
        p = jnp.exp2(s_ref[a:a + n, :] - row_max)
        s_ref[a:a + n, :] = p
        f = jnp.sum(p.reshape(n // 8, 8, rows), axis=0)
        l8 = f if l8 is None else l8 + f
        d = dot_nn(vt[:, a:a + n], p.astype(jnp.bfloat16))
        o_t = d if o_t is None else o_t + d
        yield
    inv = 1.0 / jnp.sum(l8, axis=0, keepdims=True)
    out_t = o_t * inv
    o_v[core, toks] = jnp.transpose(out_t).reshape(tok, GROUP, DIM).astype(jnp.bfloat16)
    delta = jnp.sum(dot_nt(identity(), g) * out_t, axis=0, keepdims=True)
    yield
    dq_t = None
    for a, n in blocks:
        p = s_ref[a:a + n, :] * inv
        ds = (p * (dot_nt(kv[1, a:a + n, :], g) - delta)).astype(jnp.bfloat16)
        part[1, a:a + n, :] += dot_nn(p.astype(jnp.bfloat16), g)
        part[0, a:a + n, :] += dot_nn(ds, qr)
        d = dot_nn(kt[:, a:a + n], ds)
        dq_t = d if dq_t is None else dq_t + d
        yield
    dq = jnp.transpose(dq_t) * scale
    dq = dq * table(0) - swap_pairs(dq) * table(1)
    dq_v[core, toks] = dq.reshape(tok, GROUP, DIM).astype(jnp.bfloat16)


def interleave(gens, lag):
    live, waiting, count = [], list(gens), 0
    while live or waiting:
        if waiting and (not live or count >= lag):
            live.append(waiting.pop(0))
            count = 0
        for gen in list(live):
            if next(gen, 'end') == 'end':
                live.remove(gen)
        count += 1


def unit_compute(c, q_v, g_v, tab, kv, o_v, dq_v, part, kt, vt, s_a, s_b, s_e):
    n_late, n_early = (N_PAIRS - c) * PAIR, (c + 1) * PAIR
    eye = identity()
    for a in range(0, n_late, 256):
        n = min(256, n_late - a)
        kt[:, a:a + n] = dot_nt(eye, kv[0, a:a + n, :]).astype(jnp.bfloat16)
        vt[:, a:a + n] = dot_nt(eye, kv[1, a:a + n, :]).astype(jnp.bfloat16)
    part[:, :n_late, :] = jnp.zeros((2, n_late, DIM), jnp.float32)
    refs = (q_v, g_v, tab, kv, kt, vt, part, o_v, dq_v)

    def step(i, carry):
        late = [rows_steps(n_late, 32, (1 - i, PIECE + 32 * k, i * PIECE + 32 * k), *refs, s)
                for k, s in ((0, s_a), (1, s_b))]
        early = rows_steps(n_early, PIECE, (i, 0, i * PIECE), *refs, s_e)
        interleave(late + [early], STEP_LAG)
        return carry

    lax.fori_loop(0, 2, step, 0)


def remote(src, dst, send_sem, recv_sem, device):
    return pltpu.make_async_remote_copy(src_ref=src, dst_ref=dst, send_sem=send_sem, recv_sem=recv_sem,
                                        device_id={'cp': device}, device_id_type=MESH_ID)


def chip_program(c, core, barrier, q_hbm, g_hbm, k_hbm, v_hbm, pos_hbm, freq_hbm, odq_hbm, gkv_hbm, kv_hbm, qs_hbm, gs_hbm,
                 q_v, g_v, o_v, dq_v, kv_v, tab_v, tab_x, pos_v, freq_v, raw_v, ready_v, part, recv, fin_v,
                 perm_in, kt, vt, s_a, s_b, s_e,
                 raw_s, kvl_s, kvx_s, kvx_r, tab_s, tab_r, qx_s, qx_r, gx_s, gx_r, ag_s, ag_r, sum_s, sum_r,
                 load_s, out_s, out_r, fin_s, fin_r, credit):
    o_hbm, dq_hbm = odq_hbm.at[0], odq_hbm.at[1]
    n_late = (N_PAIRS - c) * PAIR
    sib = 2 * c + 1 - core
    nbr = {step: 2 * (c ^ step) + core for step in (X_STEP, Y_STEP)}
    mine, other = BATCHES * core, BATCHES * (1 - core)
    early_hops = [(p, step) for p, src, step in EARLY_HOP if src == c]
    first_hops = [(p, step) for p, src, step in FIRST_HOP if src == c and (p, src, step) not in EARLY_HOP]
    relay_hops = [(p, step) for p, src, step in RELAY_HOP if src == c]
    leaves = [(p, step) for p, src, step in SUM_LEAF if src == c]
    relays = [(p, step) for p, src, step in SUM_RELAY if src == c]
    needed = [p for p in range(N_PAIRS - c) if owner(p) != c]
    sib_pieces = (2 * c + 1 - core, 15 - 2 * c - (1 - core))

    def split(u):
        return u // HEADS, u % HEADS

    def pair_rows(p):
        return pl.ds(p * PAIR, PAIR)

    own_pieces = (2 * c + core, 15 - 2 * c - core)

    def raw_in(b, side):
        src, slot = (mine, other)[side] + b, b % 2
        return [pltpu.make_async_copy(k_hbm.at[src], raw_v.at[slot, side, 0], raw_s.at[slot, side, 0]),
                pltpu.make_async_copy(v_hbm.at[src], raw_v.at[slot, side, 1], raw_s.at[slot, side, 1])]

    def start_raw(b):
        for side in (1, 0):
            for copy in raw_in(b, side):
                copy.start()

    def piece_rows(piece):
        return pl.ds(pl.multiple_of(piece * PIECE, PIECE), PIECE)

    def own_out(b, half):
        return pltpu.make_async_copy(ready_v.at[b % 2, 0, :, :, pl.ds(half * PIECE, PIECE), :],
                                     kv_hbm.at[b, :, :, piece_rows(own_pieces[half]), :], kvl_s.at[b, half])

    def kvx(b, half):
        return remote(ready_v.at[b % 2, 1, :, :, pl.ds(half * PIECE, PIECE), :],
                      kv_hbm.at[b, :, :, piece_rows(own_pieces[half]), :], kvx_s.at[b, half], kvx_r.at[b, half], sib)

    def kvx_in(b, half):
        dst = kv_hbm.at[b, :, :, piece_rows(sib_pieces[half]), :]
        return remote(dst, dst, kvx_s.at[b, half], kvx_r.at[b, half], sib)

    def make_table(tab, row):
        pos = pos_v[pl.ds(row, 1), :].astype(jnp.float32)
        angles = jnp.transpose(jnp.broadcast_to(pos, (PAIR, PAIR))) * freq_v[...]
        tab[0] = jnp.cos(angles)
        sine_val = jnp.sin(angles)
        tab[1] = jnp.where(iota(sine_val.shape, 1) % 2 == 0, -sine_val, sine_val)

    def make_ready(b):
        slot, part_rows = b % 2, PAIR // HEADS

        @pl.when(b >= 2)
        def _():
            for half in range(2):
                kvx(b - 2, half).wait_send()
            tab_out(b - 2).wait_send()

        @pl.when(b == 2)
        def _():
            for u in range(FAST_UNITS):
                for i, (p, step) in enumerate(early_hops + first_hops):
                    kv_copy(jnp.int32(u), p, i, step).wait_send()

        make_table(tab_x.at[slot], other + b)
        make_table(tab_v.at[b, :, core], mine + b)
        for side in (1, 0):
            for copy in raw_in(b, side):
                copy.wait()
            tab = tab_x.at[slot] if side else tab_v.at[b, :, core]
            for i in range(2):
                blocks = [dot_nn(perm_in[...], raw_v[slot, side, i, j * PAIR:(j + 1) * PAIR]) for j in range(HEADS)]
                for h in range(HEADS):
                    x = jnp.concatenate([block[h * part_rows:(h + 1) * part_rows] for block in blocks], axis=0)
                    if i == 0:
                        x = x * tab[0] + swap_pairs(x) * tab[1]
                    ready_v[slot, side, h, i] = x.astype(jnp.bfloat16)
        for half in range(2):
            own_out(b, half).start()

        @pl.when(b + 2 < BATCHES)
        def _():
            start_raw(b + 2)

    def send_ready(b):
        for half in range(2):
            kvx(b, half).start()
        tab_out(b).start()

    def qx(b):
        return remote(q_hbm.at[other + b], qs_hbm.at[b], qx_s.at[b], qx_r.at[b], sib)

    def gx(b):
        return remote(g_hbm.at[other + b], gs_hbm.at[b], gx_s.at[b], gx_r.at[b], sib)

    def tab_out(b):
        return remote(tab_x.at[b % 2], tab_v.at[b, :, core], tab_s.at[b % 2], tab_r.at[b], sib)

    def tab_arrive(b):
        dst = tab_v.at[b, :, 1 - core]
        return remote(dst, dst, tab_s.at[0], tab_r.at[b], sib)

    def small_in():
        return [pltpu.make_async_copy(pos_hbm, pos_v, load_s.at[5, 0]),
                pltpu.make_async_copy(freq_hbm, freq_v, load_s.at[5, 1])]

    def kv_copy(u, p, slot, step):
        b, h = split(u)
        ref = kv_hbm.at[b, h, :, pair_rows(p), :]
        return remote(ref, ref, ag_s.at[u, slot], ag_r.at[u, p], nbr[step])

    def send_kv(u, hops, base):
        for i, (p, step) in enumerate(hops):
            kv_copy(u, p, base + i, step).start()

    def have_own(b):
        for half in range(2):
            own_out(b, half).wait()
            kvx_in(b, half).wait_recv()

    def half_copy(u, p, slot, step, own):
        b, h = split(u)
        half = 0 if p == c else 1
        dst = kv_hbm.at[b, h, :, piece_rows((own_pieces if own else sib_pieces)[half]), :]
        src = ready_v.at[b % 2, 0, h, :, pl.ds(half * PIECE, PIECE), :] if own else dst
        return remote(src, dst, ag_s.at[u, slot], ag_r.at[u, p], nbr[step])

    def fast_hop(u, own):
        for i, (p, step) in enumerate(early_hops + first_hops):
            half_copy(u, p, i, step, own).start()

    def early_hop(u):
        send_kv(u, early_hops, 0)

    def first_hop(u):
        send_kv(u, first_hops, len(early_hops))

    def relay_hop(u):
        for p, _ in relay_hops:
            kv_copy(u, p, 0, X_STEP).wait_recv()
        send_kv(u, relay_hops, len(early_hops) + len(first_hops))

    def loads(u):
        b, h = split(u)
        slot = u % 2
        late = pl.ds(0, n_late)
        return [
            pltpu.make_async_copy(q_hbm.at[mine + b, :, h], q_v.at[slot, core], load_s.at[0, slot]),
            pltpu.make_async_copy(g_hbm.at[mine + b, :, h], g_v.at[slot, core], load_s.at[1, slot]),
            pltpu.make_async_copy(qs_hbm.at[b, :, h], q_v.at[slot, 1 - core], load_s.at[2, slot]),
            pltpu.make_async_copy(gs_hbm.at[b, :, h], g_v.at[slot, 1 - core], load_s.at[3, slot]),
            pltpu.make_async_copy(kv_hbm.at[b, h, :, late, :], kv_v.at[slot, :, late, :], load_s.at[4, slot]),
        ]

    def start_loads(u):
        @pl.when(u % HEADS == 0)
        def _():
            qx(u // HEADS).wait_recv()
            gx(u // HEADS).wait_recv()
            tab_arrive(u // HEADS).wait_recv()

        for p in needed:
            if p not in [r for r, _ in relay_hops]:
                kv_copy(u, p, 0, X_STEP).wait_recv()
        for copy in loads(u):
            copy.start()

    def out_local(u):
        b, h = split(u)
        slot = u % 2
        return [pltpu.make_async_copy(o_v.at[slot, core], o_hbm.at[mine + b, :, h], out_s.at[0, slot]),
                pltpu.make_async_copy(dq_v.at[slot, core], dq_hbm.at[mine + b, :, h], out_s.at[1, slot])]

    def out_remote(u):
        b, h = split(u)
        slot = u % 2
        return [remote(o_v.at[slot, 1 - core], o_hbm.at[mine + b, :, h], out_s.at[2, slot], out_r.at[0, b], sib),
                remote(dq_v.at[slot, 1 - core], dq_hbm.at[mine + b, :, h], out_s.at[3, slot], out_r.at[1, b], sib)]

    def out_arrive(b):
        return [remote(q_hbm.at[other + b], o_hbm.at[other + b], out_s.at[2, 0], out_r.at[0, b], sib),
                remote(q_hbm.at[other + b], dq_hbm.at[other + b], out_s.at[3, 0], out_r.at[1, b], sib)]

    def wait_outs(u):
        for copy in out_local(u):
            copy.wait()
        for copy in out_remote(u):
            copy.wait_send()

    def sum_copy(u, p, i, step):
        k, slot = inbox(c ^ step).index((p, c)), u % INBOX_RING
        return remote(part.at[u % PART_RING, :, pair_rows(p), :], recv.at[slot, k],
                      sum_s.at[i, u % PART_RING], sum_r.at[slot, k], nbr[step])

    def sum_arrive(u, k):
        dst = recv.at[u % INBOX_RING, k]
        return remote(dst, dst, sum_s.at[0, 0], sum_r.at[u % INBOX_RING, k], nbr[X_STEP])

    def give_credits(u, pairs):
        @pl.when(u + INBOX_RING < UNITS)
        def _():
            for k, (pair, src) in enumerate(inbox(c)):
                if pair in pairs:
                    pl.semaphore_signal(credit.at[outbox(src).index((pair, src ^ c))], inc=1,
                                        device_id={'cp': 2 * src + core}, device_id_type=MESH_ID)

    def take_credits(u, which):
        @pl.when(u >= INBOX_RING)
        def _():
            for i in which:
                pl.semaphore_wait(credit.at[i], 1)

    def messages(p):
        return [k for k, (pair, _) in enumerate(inbox(c)) if pair == p]

    def wait_sums(u):
        for i, (p, step) in enumerate(leaves + relays):
            sum_copy(u, p, i, step).wait_send()

    def send_leaves(u):
        take_credits(u, range(len(leaves)))
        for i, (p, step) in enumerate(leaves):
            sum_copy(u, p, i, step).start()

    def add_relays(u):
        for p, _ in relays:
            for k in messages(p):
                sum_arrive(u, k).wait_recv()
                part[u % PART_RING, :, pair_rows(p), :] += recv[u % INBOX_RING, k]
        give_credits(u, [p for p, _ in relays])

    def send_relays(u):
        take_credits(u, range(len(leaves), len(leaves) + len(relays)))
        for i, (p, step) in enumerate(relays):
            sum_copy(u, p, len(leaves) + i, step).start()

    def fin_local(u):
        b, h = split(u)
        return pltpu.make_async_copy(fin_v.at[u % 2, core], gkv_hbm.at[mine + b, h], fin_s.at[0, u % 2])

    def fin_remote(u):
        b, h = split(u)
        return remote(fin_v.at[u % 2, 1 - core], gkv_hbm.at[mine + b, h], fin_s.at[1, u % 2], fin_r.at[b], sib)

    def fin_arrive(b):
        dst = gkv_hbm.at[other + b]
        return remote(dst, dst, fin_s.at[1, 0], fin_r.at[b], sib)

    def wait_fin(u):
        fin_local(u).wait()
        fin_remote(u).wait_send()

    def finish(u):
        @pl.when(u >= 2)
        def _():
            wait_fin(u - 2)

        b, slot = u // HEADS, u % 2
        for late, p in ((0, c), (1, N_PAIRS - 1 - c)):
            total = part[u % PART_RING, :, pair_rows(p), :]
            for k in messages(p):
                sum_arrive(u, k).wait_recv()
                total = total + recv[u % INBOX_RING, k]
            for i in range(2):
                who = 1 - i if late else i
                toks = slice(late * PIECE, (late + 1) * PIECE)
                dk = total[0, i * PIECE:(i + 1) * PIECE] * (DIM ** -0.5)
                dk = dk * tab_v[b, 0, who, toks] - swap_pairs(dk) * tab_v[b, 1, who, toks]
                fin_v[slot, who, 0, toks] = dk.astype(jnp.bfloat16)
                fin_v[slot, who, 1, toks] = total[1, i * PIECE:(i + 1) * PIECE].astype(jnp.bfloat16)
        give_credits(u, [c, N_PAIRS - 1 - c])

    def send_fin(u):
        fin_local(u).start()
        fin_remote(u).start()

    def exchange_queries(b):
        qx(b).start()
        gx(b).start()

    for device in (sib, nbr[X_STEP], nbr[Y_STEP]):
        pl.semaphore_signal(barrier, inc=1, device_id={'cp': device}, device_id_type=MESH_ID)
    for copy in small_in():
        copy.start()
    start_raw(jnp.int32(0))
    start_raw(jnp.int32(1))
    row, col = iota(perm_in.shape, 0), iota(perm_in.shape, 1)
    part_rows = PAIR // HEADS
    perm_in[...] = (col == (row % part_rows) * HEADS + row // part_rows).astype(jnp.float32).astype(jnp.bfloat16)
    for copy in small_in():
        copy.wait()

    def up_to(op, first, last):
        def one(u, carry):
            op(u)
            return carry

        lax.fori_loop(first, last, one, 0)

    def start_step(j, carry):
        make_ready(j)

        @pl.when(j == 0)
        def _():
            pl.semaphore_wait(barrier, 3)

        send_ready(j)

        @pl.when(j == 0)
        def _():
            for u in range(FAST_UNITS):
                fast_hop(jnp.int32(u), True)
            have_own(j)
            for u in range(FAST_UNITS):
                fast_hop(jnp.int32(u), False)
            exchange_queries(j)

        up_to(relay_hop, jnp.where(j < START_RELAYS, jnp.maximum(j - 1, 0), START_RELAYS),
              jnp.minimum(j + j // 3, START_RELAYS))
        up_to(first_hop, jnp.clip(2 * j, FAST_UNITS, START_UNITS), jnp.clip(2 * j + 2, FAST_UNITS, START_UNITS))

        @pl.when(j >= 1)
        def _():
            have_own(j)

        up_to(early_hop, jnp.maximum(HEADS * j, FAST_UNITS), HEADS * j + HEADS)
        return carry

    lax.fori_loop(0, START_BATCHES, start_step, 0)
    start_loads(jnp.int32(0))

    def tick(t, carry):
        @pl.when((t % 2 == 0) & (t // 2 + START_BATCHES < BATCHES))
        def _():
            make_ready(t // 2 + START_BATCHES)
            send_ready(t // 2 + START_BATCHES)

        @pl.when((t % 2 == 1) & (t // 2 + START_BATCHES < BATCHES))
        def _():
            have_own(t // 2 + START_BATCHES)

        @pl.when((t % HEADS == 0) & (t // HEADS + 1 < BATCHES))
        def _():
            exchange_queries(t // HEADS + 1)

        @pl.when((t >= 1) & (2 * t - 2 + START_EARLY < UNITS))
        def _():
            early_hop(2 * t - 2 + START_EARLY)
            early_hop(2 * t - 1 + START_EARLY)

        @pl.when(t == 0)
        def _():
            for u in range(START_RELAYS, RELAY_LEAD - 1):
                relay_hop(jnp.int32(u))

        @pl.when(t + RELAY_LEAD - 1 < UNITS)
        def _():
            relay_hop(t + RELAY_LEAD - 1)

        @pl.when((t >= 1) & (t - 1 < UNITS))
        def _():
            send_leaves(t - 1)

        @pl.when((t >= 1 + OWN_LAG) & (t - 1 - OWN_LAG < UNITS))
        def _():
            finish(t - 1 - OWN_LAG)

        @pl.when((t >= 1 + SUM_LAG) & (t - 1 - SUM_LAG < UNITS))
        def _():
            add_relays(t - 1 - SUM_LAG)

        @pl.when((t >= 1 + OWN_LAG) & (t - 1 - OWN_LAG < UNITS))
        def _():
            send_fin(t - 1 - OWN_LAG)

        @pl.when((t >= 1 + SUM_LAG) & (t - 1 - SUM_LAG < UNITS))
        def _():
            send_relays(t - 1 - SUM_LAG)

        hop_lead = HOP_LEADS[c]

        @pl.when((t == 0) | ((t + hop_lead > START_UNITS) & (t + hop_lead < UNITS)))
        def _():
            first_hop(jnp.maximum(t + hop_lead, START_UNITS))

        @pl.when(t < UNITS)
        def _():
            for copy in loads(t):
                copy.wait()

            @pl.when(t + 1 < UNITS)
            def _():
                start_loads(t + 1)

            @pl.when(t >= 2)
            def _():
                wait_outs(t - 2)

            @pl.when(t >= PART_RING)
            def _():
                wait_sums(t - PART_RING)

            slot = t % 2
            unit_compute(c, q_v.at[slot], g_v.at[slot], tab_v.at[t // HEADS], kv_v.at[slot], o_v.at[slot],
                         dq_v.at[slot], part.at[t % PART_RING], kt, vt, s_a, s_b, s_e)
            for copy in out_local(t) + out_remote(t):
                copy.start()

        return carry

    lax.fori_loop(0, UNITS + 1 + OWN_LAG, tick, 0)

    for u in range(UNITS - 2, UNITS):
        wait_outs(jnp.int32(u))
        wait_fin(jnp.int32(u))

    def drain_batch(b, carry):
        @pl.when(b >= BATCHES - 2)
        def _():
            for half in range(2):
                kvx(b, half).wait_send()
            tab_out(b).wait_send()

        qx(b).wait_send()
        gx(b).wait_send()
        for copy in out_arrive(b):
            copy.wait_recv()
        fin_arrive(b).wait_recv()
        return carry

    lax.fori_loop(0, BATCHES, drain_batch, 0)

    def drain_sums(u, carry):
        wait_sums(u)
        return carry

    lax.fori_loop(UNITS - PART_RING, UNITS, drain_sums, 0)

    def drain_kv(u, carry):
        @pl.when(u >= FAST_UNITS)
        def _():
            for i, (p, step) in enumerate(early_hops + first_hops):
                kv_copy(u, p, i, step).wait_send()

        for i, (p, step) in enumerate(relay_hops):
            kv_copy(u, p, len(early_hops + first_hops) + i, step).wait_send()
        return carry

    lax.fori_loop(0, UNITS, drain_kv, 0)


def attend_kernel(*refs):
    me = lax.axis_index('cp')
    chip, core = me // 2, me % 2
    barrier = pltpu.get_barrier_semaphore()
    for c in range(4):
        @pl.when(chip == c)
        def _(c=c):
            chip_program(c, core, barrier, *refs)


def attend(q5, g5, keys, values, positions, freq):
    any_spec = pl.BlockSpec(memory_space=pl.ANY)
    hbm_spec = pl.BlockSpec(memory_space=pltpu.HBM)
    head_shape = pltpu.VMEM((2,) + q5.shape, jnp.bfloat16)
    half_shape = pltpu.HBM((BATCHES,) + q5.shape[1:], jnp.bfloat16)
    head_buf = pltpu.VMEM((2, 2, PAIR, GROUP, DIM), jnp.bfloat16)
    dma = pltpu.SemaphoreType.DMA
    return pl.pallas_call(
        attend_kernel, name='attend',
        in_specs=[any_spec] * 6,
        out_specs=[any_spec] + [hbm_spec] * 4,
        out_shape=[head_shape,
                   pltpu.HBM((2 * BATCHES, HEADS, 2, PAIR, DIM), jnp.bfloat16),
                   pltpu.HBM((BATCHES, HEADS, 2, N_PAIRS * PAIR, DIM), jnp.bfloat16),
                   half_shape, half_shape],
        scratch_shapes=[
            head_buf, head_buf, head_buf, head_buf,
            pltpu.VMEM((2, 2, N_PAIRS * PAIR, DIM), jnp.bfloat16),
            pltpu.VMEM((BATCHES, 2, 2, PAIR, DIM), jnp.float32),
            pltpu.VMEM((2, 2, PAIR, DIM), jnp.float32),
            pltpu.VMEM((2 * BATCHES, PAIR), jnp.int32),
            pltpu.VMEM((1, DIM), jnp.float32),
            pltpu.VMEM((2, 2, 2, HEADS * PAIR, DIM), jnp.bfloat16),
            pltpu.VMEM((2, 2, HEADS, 2, PAIR, DIM), jnp.bfloat16),
            pltpu.VMEM((PART_RING, 2, N_PAIRS * PAIR, DIM), jnp.float32),
            pltpu.VMEM((INBOX_RING, N_INBOX, 2, PAIR, DIM), jnp.float32),
            pltpu.VMEM((2, 2, 2, PAIR, DIM), jnp.bfloat16),
            pltpu.VMEM((PAIR, PAIR), jnp.bfloat16),
            pltpu.VMEM((DIM, N_PAIRS * PAIR), jnp.bfloat16),
            pltpu.VMEM((DIM, N_PAIRS * PAIR), jnp.bfloat16),
            pltpu.VMEM((N_PAIRS * PAIR, 32 * GROUP), jnp.float32),
            pltpu.VMEM((N_PAIRS * PAIR, 32 * GROUP), jnp.float32),
            pltpu.VMEM((4 * PAIR, PIECE * GROUP), jnp.float32),
            dma((2, 2, 2)), dma((BATCHES, 2)), dma((BATCHES, 2)), dma((BATCHES, 2)), dma((2,)), dma((BATCHES,)),
            dma((BATCHES,)), dma((BATCHES,)), dma((BATCHES,)), dma((BATCHES,)),
            dma((UNITS, 7)), dma((UNITS, 7)), dma((N_OUTBOX, PART_RING)), dma((INBOX_RING, N_INBOX)),
            dma((6, 2)), dma((4, 2)), dma((2, BATCHES)), dma((2, 2)), dma((BATCHES,)),
            pltpu.SemaphoreType.REGULAR((N_OUTBOX,)),
        ],
        compiler_params=pltpu.CompilerParams(
            collective_id=0, has_side_effects=True, vmem_limit_bytes=32512 * 1024),
    )(*(pltpu.with_memory_space_constraint(x, pltpu.HBM) for x in (q5, g5, keys, values, positions, freq)))


def place_kernel(odq, gkv, o_out, dq_out, gk_out, gv_out, in_v, out_v, perm, sems, in_s, out_s):
    n_batch = gkv.shape[0]

    def batch_in(b):
        return pltpu.make_async_copy(gkv.at[b], in_v.at[b], in_s.at[b])

    def batch_out(b):
        return [pltpu.make_async_copy(out_v.at[b, i], dst.at[b], out_s.at[b, i]) for i, dst in enumerate((gk_out, gv_out))]

    def start_in(b, carry):
        batch_in(b).start()
        return carry

    lax.fori_loop(0, n_batch, start_in, 0)
    part = n_batch // 4
    large = [pltpu.make_async_copy(odq.at[k, pl.ds(i * part, part)], dst.at[pl.ds(i * part, part)], sems.at[k, i])
             for i in range(4) for k, dst in enumerate((o_out, dq_out))]
    for copy in large:
        copy.start()
    row, col = iota(perm.shape, 0), iota(perm.shape, 1)
    perm[...] = (row == (col % PAIR) * HEADS + col // PAIR).astype(jnp.float32).astype(jnp.bfloat16)

    def regroup(b, carry):
        batch_in(b).wait()
        for i in range(2):
            rows = in_v[b, :, i].reshape(HEADS * PAIR, DIM)
            out_v[b, i] = dot_nn(perm[...], rows).astype(jnp.bfloat16)
        for copy in batch_out(b):
            copy.start()
        return carry

    lax.fori_loop(0, n_batch, regroup, 0)

    def finish_out(b, carry):
        for copy in batch_out(b):
            copy.wait()
        return carry

    lax.fori_loop(0, n_batch, finish_out, 0)
    for copy in large:
        copy.wait()


def place(odq, gkv):
    any_spec = pl.BlockSpec(memory_space=pl.ANY)
    n_batch = gkv.shape[0]
    head_shape = pltpu.HBM(odq.shape[1:], jnp.bfloat16)
    row_shape = pltpu.HBM((n_batch, HEADS * PAIR, DIM), jnp.bfloat16)
    dma = pltpu.SemaphoreType.DMA
    return pl.pallas_call(
        place_kernel, name='place', in_specs=[any_spec] * 2, out_specs=[any_spec] * 4,
        out_shape=[head_shape, head_shape, row_shape, row_shape],
        scratch_shapes=[pltpu.VMEM(gkv.shape, jnp.bfloat16), pltpu.VMEM((n_batch, 2, HEADS * PAIR, DIM), jnp.bfloat16),
                        pltpu.VMEM((HEADS * PAIR, HEADS * PAIR), jnp.bfloat16),
                        dma((2, 4)), dma((n_batch,)), dma((n_batch, 2))],
        compiler_params=pltpu.CompilerParams(vmem_limit_bytes=12 * 1024 * 1024),
    )(odq, pltpu.with_memory_space_constraint(gkv, pltpu.HBM))


def solution(mesh):
    head_spec = P(None, 'cp', 'tp', None)
    pos_spec = P(None, 'cp')

    def local_step(query, keys, values, positions, grad_out):
        batch, length, n_heads, dim = query.shape
        split_shape = (batch, length, HEADS, GROUP, dim)
        row_shape = (batch, length * HEADS, dim)
        outs = attend(query.reshape(split_shape), grad_out.reshape(split_shape), keys.reshape(row_shape),
                      values.reshape(row_shape), positions, jnp.asarray(lane_freq(dim)))
        return tuple(out.reshape(like.shape) for out, like in zip(place(*outs[:2]), (query, query, keys, values)))

    return jax.shard_map(local_step, mesh=mesh,
                         in_specs=(head_spec, head_spec, head_spec, pos_spec, head_spec),
                         out_specs=(head_spec, head_spec, head_spec, head_spec), check_vma=False)
```

```python
import functools

import jax
import jax.numpy as jnp
import numpy as np
from jax import lax
from jax.experimental import pallas as pl
from jax.experimental.pallas import tpu as pltpu
from jax.sharding import PartitionSpec as P

ROPE_THETA = 1000000.0
LOG2E = 1.4426950408889634
DIM = 128
GROUP = 8
HEADS = 4
PIECE = 64
PAIR = 128
N_PAIRS = 8
BATCHES = 8
UNITS = BATCHES * HEADS
KEY_BLOCK = 512
STEP_LAG = 2
MESH_ID = pl.DeviceIdType.MESH

X_STEP, Y_STEP = 1, 2
FIRST_HOP = [(0, 0, X_STEP), (0, 0, Y_STEP), (1, 1, X_STEP), (1, 1, Y_STEP), (2, 2, X_STEP), (2, 2, Y_STEP),
             (3, 3, X_STEP), (3, 3, Y_STEP), (4, 3, X_STEP), (4, 3, Y_STEP), (5, 2, Y_STEP), (5, 2, X_STEP),
             (6, 1, X_STEP)]
RELAY_HOP = [(0, 2, X_STEP), (1, 3, X_STEP), (2, 3, Y_STEP), (3, 2, Y_STEP), (4, 1, X_STEP), (5, 3, Y_STEP)]
SUM_LEAF = [(3, 0, Y_STEP), (4, 0, X_STEP), (2, 0, Y_STEP), (6, 0, X_STEP), (2, 1, Y_STEP), (5, 1, X_STEP),
            (0, 1, X_STEP), (3, 1, Y_STEP), (1, 2, Y_STEP), (4, 2, X_STEP), (0, 3, X_STEP), (1, 3, Y_STEP)]
SUM_RELAY = [(0, 2, Y_STEP), (1, 0, X_STEP), (2, 3, X_STEP), (3, 2, X_STEP), (4, 1, Y_STEP), (5, 0, Y_STEP)]

START_BATCHES = 6
START_UNITS = 8
START_RELAYS = 4
RELAY_LEAD = 6
HOP_LEADS = (8, 7, 8, 8)
START_EARLY = HEADS * START_BATCHES
FAST_UNITS = 2
EARLY_HOP = [(0, 0, X_STEP), (0, 0, Y_STEP), (1, 1, Y_STEP)]
SUM_LAG = 4
OWN_LAG = 8
PART_RING = OWN_LAG + 2
FIN_CLOSE = OWN_LAG + HEADS + 2
INBOX_RING = 9


def owner(pair):
    return pair if pair < 4 else 7 - pair


def inbox(chip):
    found = []
    for pair, src, step in SUM_LEAF + SUM_RELAY:
        if src ^ step == chip:
            found.append((pair, src))
    return found


def outbox(chip):
    return [(pair, step) for pair, src, step in SUM_LEAF + SUM_RELAY if src == chip]


N_INBOX = max(len(inbox(c)) for c in range(4))
N_OUTBOX = max(len(outbox(c)) for c in range(4))


def lane_freq(head_dim):
    exponent = np.arange(head_dim // 2, dtype=np.float64) * (2.0 / head_dim)
    return np.repeat(ROPE_THETA ** -exponent, 2).astype(np.float32)[None, :]


def dot_nn(a, b):
    return jnp.dot(a, b, preferred_element_type=jnp.float32)


def dot_nt(a, b):
    return lax.dot_general(a, b, (((1,), (1,)), ((), ())), preferred_element_type=jnp.float32)


def iota(shape, axis):
    return lax.broadcasted_iota(jnp.int32, shape, axis)


def identity():
    return (iota((DIM, DIM), 0) == iota((DIM, DIM), 1)).astype(jnp.float32).astype(jnp.bfloat16)


def swap_pairs(x):
    return jnp.where(iota(x.shape, 1) % 2 == 0, pltpu.roll(x, DIM - 1, axis=1), pltpu.roll(x, 1, axis=1))


def rows_steps(n_keys, tok, seg, q_v, g_v, tab, kv, kt, vt, part, o_v, dq_v, s_ref):
    core, start, place = seg
    rows = tok * GROUP
    scale = DIM ** -0.5
    c1 = scale * LOG2E
    toks = pl.ds(start, tok)

    def table(k):
        return jnp.broadcast_to(tab[k, core, toks, :][:, None, :], (tok, GROUP, DIM)).reshape(rows, DIM)

    x = q_v[core, toks].astype(jnp.float32).reshape(rows, DIM)
    qr = (x * table(0) + swap_pairs(x) * table(1)).astype(jnp.bfloat16)
    g = g_v[core, toks].astype(jnp.float32).reshape(rows, DIM).astype(jnp.bfloat16)
    blocks = [(a, min(KEY_BLOCK, n_keys - a)) for a in range(0, n_keys, KEY_BLOCK)]
    m8 = None
    for a, n in blocks:
        s = dot_nt(kv[0, a:a + n, :], qr) * c1
        if a + n == n_keys:
            last = s[n - PAIR:, :]
            q_tok = iota(last.shape, 1) // GROUP + place
            last = jnp.where(iota(last.shape, 0) <= q_tok, last, -jnp.inf)
            s = last if n == PAIR else jnp.concatenate([s[:n - PAIR, :], last], axis=0)
        s_ref[a:a + n, :] = s
        f = jnp.max(s.reshape(n // 8, 8, rows), axis=0)
        m8 = f if m8 is None else jnp.maximum(m8, f)
        yield
    row_max = jnp.max(m8, axis=0, keepdims=True)
    l8 = None
    o_t = None
    for a, n in blocks:
        p = jnp.exp2(s_ref[a:a + n, :] - row_max)
        s_ref[a:a + n, :] = p
        f = jnp.sum(p.reshape(n // 8, 8, rows), axis=0)
        l8 = f if l8 is None else l8 + f
        d = dot_nn(vt[:, a:a + n], p.astype(jnp.bfloat16))
        o_t = d if o_t is None else o_t + d
        yield
    inv = 1.0 / jnp.sum(l8, axis=0, keepdims=True)
    out_t = o_t * inv
    o_v[core, toks] = jnp.transpose(out_t).reshape(tok, GROUP, DIM).astype(jnp.bfloat16)
    delta = jnp.sum(dot_nt(identity(), g) * out_t, axis=0, keepdims=True)
    yield
    dq_t = None
    for a, n in blocks:
        p = s_ref[a:a + n, :] * inv
        ds = (p * (dot_nt(kv[1, a:a + n, :], g) - delta)).astype(jnp.bfloat16)
        part[1, a:a + n, :] += dot_nn(p.astype(jnp.bfloat16), g)
        part[0, a:a + n, :] += dot_nn(ds, qr)
        d = dot_nn(kt[:, a:a + n], ds)
        dq_t = d if dq_t is None else dq_t + d
        yield
    dq = jnp.transpose(dq_t) * scale
    dq = dq * table(0) - swap_pairs(dq) * table(1)
    dq_v[core, toks] = dq.reshape(tok, GROUP, DIM).astype(jnp.bfloat16)


def interleave(gens, lag):
    live, waiting, count = [], list(gens), 0
    while live or waiting:
        if waiting and (not live or count >= lag):
            live.append(waiting.pop(0))
            count = 0
        for gen in list(live):
            if next(gen, 'end') == 'end':
                live.remove(gen)
        count += 1


def unit_compute(c, q_v, g_v, tab, kv, o_v, dq_v, part, kt, vt, s_a, s_b, s_e):
    n_late, n_early = (N_PAIRS - c) * PAIR, (c + 1) * PAIR
    eye = identity()
    for a in range(0, n_late, 256):
        n = min(256, n_late - a)
        kt[:, a:a + n] = dot_nt(eye, kv[0, a:a + n, :]).astype(jnp.bfloat16)
        vt[:, a:a + n] = dot_nt(eye, kv[1, a:a + n, :]).astype(jnp.bfloat16)
    part[:, :n_late, :] = jnp.zeros((2, n_late, DIM), jnp.float32)
    refs = (q_v, g_v, tab, kv, kt, vt, part, o_v, dq_v)

    def step(i, carry):
        late = [rows_steps(n_late, 32, (1 - i, PIECE + 32 * k, i * PIECE + 32 * k), *refs, s)
                for k, s in ((0, s_a), (1, s_b))]
        early = rows_steps(n_early, PIECE, (i, 0, i * PIECE), *refs, s_e)
        interleave(late + [early], STEP_LAG)
        return carry

    lax.fori_loop(0, 2, step, 0)


def remote(src, dst, send_sem, recv_sem, device):
    return pltpu.make_async_remote_copy(src_ref=src, dst_ref=dst, send_sem=send_sem, recv_sem=recv_sem,
                                        device_id={'cp': device}, device_id_type=MESH_ID)


def chip_program(c, core, barrier, q_hbm, g_hbm, k_hbm, v_hbm, pos_hbm, freq_hbm, odq_hbm, gkv_hbm, kv_hbm, qs_hbm, gs_hbm,
                 q_v, g_v, o_v, dq_v, kv_v, tab_v, tab_x, pos_v, freq_v, raw_v, ready_v, part, recv, fin_v,
                 perm_in, kt, vt, s_a, s_b, s_e,
                 raw_s, kvl_s, kvx_s, kvx_r, tab_s, tab_r, qx_s, qx_r, gx_s, gx_r, ag_s, ag_r, sum_s, sum_r,
                 load_s, out_s, out_r, fin_s, fin_r, credit):
    o_hbm, dq_hbm = odq_hbm.at[0], odq_hbm.at[1]
    n_late = (N_PAIRS - c) * PAIR
    sib = 2 * c + 1 - core
    nbr = {step: 2 * (c ^ step) + core for step in (X_STEP, Y_STEP)}
    mine, other = BATCHES * core, BATCHES * (1 - core)
    early_hops = [(p, step) for p, src, step in EARLY_HOP if src == c]
    first_hops = [(p, step) for p, src, step in FIRST_HOP if src == c and (p, src, step) not in EARLY_HOP]
    relay_hops = [(p, step) for p, src, step in RELAY_HOP if src == c]
    leaves = [(p, step) for p, src, step in SUM_LEAF if src == c]
    relays = [(p, step) for p, src, step in SUM_RELAY if src == c]
    needed = [p for p in range(N_PAIRS - c) if owner(p) != c]
    sib_pieces = (2 * c + 1 - core, 15 - 2 * c - (1 - core))

    def split(u):
        return u // HEADS, u % HEADS

    def pair_rows(p):
        return pl.ds(p * PAIR, PAIR)

    own_pieces = (2 * c + core, 15 - 2 * c - core)

    def raw_in(b, side):
        src, slot = (mine, other)[side] + b, b % 2
        return [pltpu.make_async_copy(k_hbm.at[src], raw_v.at[slot, side, 0], raw_s.at[slot, side, 0]),
                pltpu.make_async_copy(v_hbm.at[src], raw_v.at[slot, side, 1], raw_s.at[slot, side, 1])]

    def start_raw(b):
        for side in (1, 0):
            for copy in raw_in(b, side):
                copy.start()

    def piece_rows(piece):
        return pl.ds(pl.multiple_of(piece * PIECE, PIECE), PIECE)

    def own_out(b, half):
        return pltpu.make_async_copy(ready_v.at[b % 2, 0, :, :, pl.ds(half * PIECE, PIECE), :],
                                     kv_hbm.at[b, :, :, piece_rows(own_pieces[half]), :], kvl_s.at[b, half])

    def kvx(b, half):
        return remote(ready_v.at[b % 2, 1, :, :, pl.ds(half * PIECE, PIECE), :],
                      kv_hbm.at[b, :, :, piece_rows(own_pieces[half]), :], kvx_s.at[b, half], kvx_r.at[b, half], sib)

    def kvx_in(b, half):
        dst = kv_hbm.at[b, :, :, piece_rows(sib_pieces[half]), :]
        return remote(dst, dst, kvx_s.at[b, half], kvx_r.at[b, half], sib)

    def make_table(tab, row):
        pos = pos_v[pl.ds(row, 1), :].astype(jnp.float32)
        angles = jnp.transpose(jnp.broadcast_to(pos, (PAIR, PAIR))) * freq_v[...]
        tab[0] = jnp.cos(angles)
        sine_val = jnp.sin(angles)
        tab[1] = jnp.where(iota(sine_val.shape, 1) % 2 == 0, -sine_val, sine_val)

    def make_ready(b):
        slot, part_rows = b % 2, PAIR // HEADS

        @pl.when(b >= 2)
        def _():
            for half in range(2):
                kvx(b - 2, half).wait_send()
            tab_out(b - 2).wait_send()

        @pl.when(b == 2)
        def _():
            for u in range(FAST_UNITS):
                for i, (p, step) in enumerate(early_hops + first_hops):
                    kv_copy(jnp.int32(u), p, i, step).wait_send()

        make_table(tab_x.at[slot], other + b)
        make_table(tab_v.at[b, :, core], mine + b)
        for side in (1, 0):
            for copy in raw_in(b, side):
                copy.wait()
            tab = tab_x.at[slot] if side else tab_v.at[b, :, core]
            for i in range(2):
                blocks = [dot_nn(perm_in[...], raw_v[slot, side, i, j * PAIR:(j + 1) * PAIR]) for j in range(HEADS)]
                for h in range(HEADS):
                    x = jnp.concatenate([block[h * part_rows:(h + 1) * part_rows] for block in blocks], axis=0)
                    if i == 0:
                        x = x * tab[0] + swap_pairs(x) * tab[1]
                    ready_v[slot, side, h, i] = x.astype(jnp.bfloat16)
        for half in range(2):
            own_out(b, half).start()

        @pl.when(b + 2 < BATCHES)
        def _():
            start_raw(b + 2)

    def send_ready(b):
        for half in range(2):
            kvx(b, half).start()
        tab_out(b).start()

    def qx(b):
        return remote(q_hbm.at[other + b], qs_hbm.at[b], qx_s.at[b], qx_r.at[b], sib)

    def gx(b):
        return remote(g_hbm.at[other + b], gs_hbm.at[b], gx_s.at[b], gx_r.at[b], sib)

    def tab_out(b):
        return remote(tab_x.at[b % 2], tab_v.at[b, :, core], tab_s.at[b % 2], tab_r.at[b], sib)

    def tab_arrive(b):
        dst = tab_v.at[b, :, 1 - core]
        return remote(dst, dst, tab_s.at[0], tab_r.at[b], sib)

    def small_in():
        return [pltpu.make_async_copy(pos_hbm, pos_v, load_s.at[5, 0]),
                pltpu.make_async_copy(freq_hbm, freq_v, load_s.at[5, 1])]

    def kv_copy(u, p, slot, step):
        b, h = split(u)
        ref = kv_hbm.at[b, h, :, pair_rows(p), :]
        return remote(ref, ref, ag_s.at[u, slot], ag_r.at[u, p], nbr[step])

    def send_kv(u, hops, base):
        for i, (p, step) in enumerate(hops):
            kv_copy(u, p, base + i, step).start()

    def have_own(b):
        for half in range(2):
            own_out(b, half).wait()
            kvx_in(b, half).wait_recv()

    def half_copy(u, p, slot, step, own):
        b, h = split(u)
        half = 0 if p == c else 1
        dst = kv_hbm.at[b, h, :, piece_rows((own_pieces if own else sib_pieces)[half]), :]
        src = ready_v.at[b % 2, 0, h, :, pl.ds(half * PIECE, PIECE), :] if own else dst
        return remote(src, dst, ag_s.at[u, slot], ag_r.at[u, p], nbr[step])

    def fast_hop(u, own):
        for i, (p, step) in enumerate(early_hops + first_hops):
            half_copy(u, p, i, step, own).start()

    def early_hop(u):
        send_kv(u, early_hops, 0)

    def first_hop(u):
        send_kv(u, first_hops, len(early_hops))

    def relay_hop(u):
        for p, _ in relay_hops:
            kv_copy(u, p, 0, X_STEP).wait_recv()
        send_kv(u, relay_hops, len(early_hops) + len(first_hops))

    def loads(u):
        b, h = split(u)
        slot = u % 2
        late = pl.ds(0, n_late)
        return [
            pltpu.make_async_copy(q_hbm.at[mine + b, :, h], q_v.at[slot, core], load_s.at[0, slot]),
            pltpu.make_async_copy(g_hbm.at[mine + b, :, h], g_v.at[slot, core], load_s.at[1, slot]),
            pltpu.make_async_copy(qs_hbm.at[b, :, h], q_v.at[slot, 1 - core], load_s.at[2, slot]),
            pltpu.make_async_copy(gs_hbm.at[b, :, h], g_v.at[slot, 1 - core], load_s.at[3, slot]),
            pltpu.make_async_copy(kv_hbm.at[b, h, :, late, :], kv_v.at[slot, :, late, :], load_s.at[4, slot]),
        ]

    def start_loads(u):
        @pl.when(u % HEADS == 0)
        def _():
            qx(u // HEADS).wait_recv()
            gx(u // HEADS).wait_recv()
            tab_arrive(u // HEADS).wait_recv()

        for p in needed:
            if p not in [r for r, _ in relay_hops]:
                kv_copy(u, p, 0, X_STEP).wait_recv()
        for copy in loads(u):
            copy.start()

    def out_local(u):
        b, h = split(u)
        slot = u % 2
        return [pltpu.make_async_copy(o_v.at[slot, core], o_hbm.at[mine + b, :, h], out_s.at[0, slot]),
                pltpu.make_async_copy(dq_v.at[slot, core], dq_hbm.at[mine + b, :, h], out_s.at[1, slot])]

    def out_remote(u):
        b, h = split(u)
        slot = u % 2
        return [remote(o_v.at[slot, 1 - core], o_hbm.at[mine + b, :, h], out_s.at[2, slot], out_r.at[0, b], sib),
                remote(dq_v.at[slot, 1 - core], dq_hbm.at[mine + b, :, h], out_s.at[3, slot], out_r.at[1, b], sib)]

    def out_arrive(b):
        return [remote(q_hbm.at[other + b], o_hbm.at[other + b], out_s.at[2, 0], out_r.at[0, b], sib),
                remote(q_hbm.at[other + b], dq_hbm.at[other + b], out_s.at[3, 0], out_r.at[1, b], sib)]

    def wait_outs(u):
        for copy in out_local(u):
            copy.wait()
        for copy in out_remote(u):
            copy.wait_send()

    def sum_copy(u, p, i, step):
        k, slot = inbox(c ^ step).index((p, c)), u % INBOX_RING
        return remote(part.at[u % PART_RING, :, pair_rows(p), :], recv.at[slot, k],
                      sum_s.at[i, u % PART_RING], sum_r.at[slot, k], nbr[step])

    def sum_arrive(u, k):
        dst = recv.at[u % INBOX_RING, k]
        return remote(dst, dst, sum_s.at[0, 0], sum_r.at[u % INBOX_RING, k], nbr[X_STEP])

    def give_credits(u, pairs):
        @pl.when(u + INBOX_RING < UNITS)
        def _():
            for k, (pair, src) in enumerate(inbox(c)):
                if pair in pairs:
                    pl.semaphore_signal(credit.at[outbox(src).index((pair, src ^ c))], inc=1,
                                        device_id={'cp': 2 * src + core}, device_id_type=MESH_ID)

    def take_credits(u, which):
        @pl.when(u >= INBOX_RING)
        def _():
            for i in which:
                pl.semaphore_wait(credit.at[i], 1)

    def messages(p):
        return [k for k, (pair, _) in enumerate(inbox(c)) if pair == p]

    def wait_sums(u):
        for i, (p, step) in enumerate(leaves + relays):
            sum_copy(u, p, i, step).wait_send()

    def send_leaves(u):
        take_credits(u, range(len(leaves)))
        for i, (p, step) in enumerate(leaves):
            sum_copy(u, p, i, step).start()

    def add_relays(u):
        for p, _ in relays:
            for k in messages(p):
                sum_arrive(u, k).wait_recv()
                part[u % PART_RING, :, pair_rows(p), :] += recv[u % INBOX_RING, k]
        give_credits(u, [p for p, _ in relays])

    def send_relays(u):
        take_credits(u, range(len(leaves), len(leaves) + len(relays)))
        for i, (p, step) in enumerate(relays):
            sum_copy(u, p, len(leaves) + i, step).start()

    def fin_local(u):
        b, h = split(u)
        return pltpu.make_async_copy(fin_v.at[u % 2, core], gkv_hbm.at[mine + b, h], fin_s.at[0, u % 2])

    def fin_remote(u):
        b, h = split(u)
        return remote(fin_v.at[u % 2, 1 - core], gkv_hbm.at[mine + b, h], fin_s.at[1, u % 2], fin_r.at[b], sib)

    def fin_arrive(b):
        dst = gkv_hbm.at[other + b]
        return remote(dst, dst, fin_s.at[1, 0], fin_r.at[b], sib)

    def wait_fin(u):
        fin_local(u).wait()
        fin_remote(u).wait_send()

    def finish(u):
        @pl.when(u >= 2)
        def _():
            wait_fin(u - 2)

        b, slot = u // HEADS, u % 2
        for late, p in ((0, c), (1, N_PAIRS - 1 - c)):
            total = part[u % PART_RING, :, pair_rows(p), :]
            for k in messages(p):
                sum_arrive(u, k).wait_recv()
                total = total + recv[u % INBOX_RING, k]
            for i in range(2):
                who = 1 - i if late else i
                toks = slice(late * PIECE, (late + 1) * PIECE)
                dk = total[0, i * PIECE:(i + 1) * PIECE] * (DIM ** -0.5)
                dk = dk * tab_v[b, 0, who, toks] - swap_pairs(dk) * tab_v[b, 1, who, toks]
                fin_v[slot, who, 0, toks] = dk.astype(jnp.bfloat16)
                fin_v[slot, who, 1, toks] = total[1, i * PIECE:(i + 1) * PIECE].astype(jnp.bfloat16)
        give_credits(u, [c, N_PAIRS - 1 - c])

    def send_fin(u):
        fin_local(u).start()
        fin_remote(u).start()

    last_step = UNITS + OWN_LAG

    def close_copies(t):
        batch = t // HEADS

        @pl.when((t >= FAST_UNITS) & (t < UNITS))
        def _():
            for i, (p, step) in enumerate(early_hops + first_hops):
                kv_copy(t, p, i, step).wait_send()

        @pl.when(t < UNITS)
        def _():
            for i, (p, step) in enumerate(relay_hops):
                kv_copy(t, p, len(early_hops + first_hops) + i, step).wait_send()

        @pl.when((t % HEADS == HEADS - 1) & (t < UNITS))
        def _():
            qx(batch).wait_send()
            gx(batch).wait_send()

        @pl.when((t % HEADS == 0) & (t >= 2 * HEADS) & (batch - 2 < BATCHES))
        def _():
            for copy in out_arrive(batch - 2):
                copy.wait_recv()

        @pl.when((t % HEADS == FIN_CLOSE % HEADS) & (t >= FIN_CLOSE))
        def _():
            fin_arrive((t - FIN_CLOSE) // HEADS).wait_recv()

        @pl.when(t >= UNITS)
        def _():
            wait_sums(t - PART_RING)

        @pl.when((t >= UNITS) & (t < UNITS + 2))
        def _():
            wait_outs(t - 2)

        @pl.when(t == 3 * HEADS)
        def _():
            for b in range(BATCHES - 2, BATCHES):
                for half in range(2):
                    kvx(jnp.int32(b), half).wait_send()
                tab_out(jnp.int32(b)).wait_send()

    def exchange_queries(b):
        qx(b).start()
        gx(b).start()

    for device in (sib, nbr[X_STEP], nbr[Y_STEP]):
        pl.semaphore_signal(barrier, inc=1, device_id={'cp': device}, device_id_type=MESH_ID)
    for copy in small_in():
        copy.start()
    start_raw(jnp.int32(0))
    start_raw(jnp.int32(1))
    row, col = iota(perm_in.shape, 0), iota(perm_in.shape, 1)
    part_rows = PAIR // HEADS
    perm_in[...] = (col == (row % part_rows) * HEADS + row // part_rows).astype(jnp.float32).astype(jnp.bfloat16)
    for copy in small_in():
        copy.wait()

    def up_to(op, first, last):
        def one(u, carry):
            op(u)
            return carry

        lax.fori_loop(first, last, one, 0)

    def start_step(j, carry):
        make_ready(j)

        @pl.when(j == 0)
        def _():
            pl.semaphore_wait(barrier, 3)

        send_ready(j)

        @pl.when(j == 0)
        def _():
            for u in range(FAST_UNITS):
                fast_hop(jnp.int32(u), True)
            have_own(j)
            for u in range(FAST_UNITS):
                fast_hop(jnp.int32(u), False)
            exchange_queries(j)

        up_to(relay_hop, jnp.where(j < START_RELAYS, jnp.maximum(j - 1, 0), START_RELAYS),
              jnp.minimum(j + j // 3, START_RELAYS))
        up_to(first_hop, jnp.clip(2 * j, FAST_UNITS, START_UNITS), jnp.clip(2 * j + 2, FAST_UNITS, START_UNITS))

        @pl.when(j >= 1)
        def _():
            have_own(j)

        up_to(early_hop, jnp.maximum(HEADS * j, FAST_UNITS), HEADS * j + HEADS)
        return carry

    lax.fori_loop(0, START_BATCHES, start_step, 0)
    start_loads(jnp.int32(0))

    def tick(t, carry):
        @pl.when((t % 2 == 0) & (t // 2 + START_BATCHES < BATCHES))
        def _():
            make_ready(t // 2 + START_BATCHES)
            send_ready(t // 2 + START_BATCHES)

        @pl.when((t % 2 == 1) & (t // 2 + START_BATCHES < BATCHES))
        def _():
            have_own(t // 2 + START_BATCHES)

        @pl.when((t % HEADS == 0) & (t // HEADS + 1 < BATCHES))
        def _():
            exchange_queries(t // HEADS + 1)

        @pl.when((t >= 1) & (2 * t - 2 + START_EARLY < UNITS))
        def _():
            early_hop(2 * t - 2 + START_EARLY)
            early_hop(2 * t - 1 + START_EARLY)

        @pl.when(t == 0)
        def _():
            for u in range(START_RELAYS, RELAY_LEAD - 1):
                relay_hop(jnp.int32(u))

        @pl.when(t + RELAY_LEAD - 1 < UNITS)
        def _():
            relay_hop(t + RELAY_LEAD - 1)

        @pl.when((t >= 1) & (t - 1 < UNITS))
        def _():
            send_leaves(t - 1)

        @pl.when((t >= 1 + OWN_LAG) & (t - 1 - OWN_LAG < UNITS))
        def _():
            finish(t - 1 - OWN_LAG)

        @pl.when((t >= 1 + SUM_LAG) & (t - 1 - SUM_LAG < UNITS))
        def _():
            add_relays(t - 1 - SUM_LAG)

        @pl.when((t >= 1 + OWN_LAG) & (t - 1 - OWN_LAG < UNITS))
        def _():
            send_fin(t - 1 - OWN_LAG)

        @pl.when((t >= 1 + SUM_LAG) & (t - 1 - SUM_LAG < UNITS))
        def _():
            send_relays(t - 1 - SUM_LAG)

        hop_lead = HOP_LEADS[c]

        @pl.when((t == 0) | ((t + hop_lead > START_UNITS) & (t + hop_lead < UNITS)))
        def _():
            first_hop(jnp.maximum(t + hop_lead, START_UNITS))

        @pl.when(t < UNITS)
        def _():
            for copy in loads(t):
                copy.wait()

            @pl.when(t + 1 < UNITS)
            def _():
                start_loads(t + 1)

            @pl.when(t >= 2)
            def _():
                wait_outs(t - 2)

            @pl.when(t >= PART_RING)
            def _():
                wait_sums(t - PART_RING)

            slot = t % 2
            unit_compute(c, q_v.at[slot], g_v.at[slot], tab_v.at[t // HEADS], kv_v.at[slot], o_v.at[slot],
                         dq_v.at[slot], part.at[t % PART_RING], kt, vt, s_a, s_b, s_e)
            for copy in out_local(t) + out_remote(t):
                copy.start()

        close_copies(t)
        return carry

    lax.fori_loop(0, last_step + 1, tick, 0)

    for u in range(UNITS - 2, UNITS):
        wait_fin(jnp.int32(u))
    for u in range(last_step + 1 - PART_RING, UNITS):
        wait_sums(jnp.int32(u))
    for b in range((last_step - FIN_CLOSE) // HEADS + 1, BATCHES):
        fin_arrive(jnp.int32(b)).wait_recv()


def attend_kernel(*refs):
    me = lax.axis_index('cp')
    chip, core = me // 2, me % 2
    barrier = pltpu.get_barrier_semaphore()
    for c in range(4):
        @pl.when(chip == c)
        def _(c=c):
            chip_program(c, core, barrier, *refs)


def attend(q5, g5, keys, values, positions, freq):
    any_spec = pl.BlockSpec(memory_space=pl.ANY)
    hbm_spec = pl.BlockSpec(memory_space=pltpu.HBM)
    head_shape = pltpu.VMEM((2,) + q5.shape, jnp.bfloat16)
    half_shape = pltpu.HBM((BATCHES,) + q5.shape[1:], jnp.bfloat16)
    head_buf = pltpu.VMEM((2, 2, PAIR, GROUP, DIM), jnp.bfloat16)
    dma = pltpu.SemaphoreType.DMA
    return pl.pallas_call(
        attend_kernel, name='attend',
        in_specs=[any_spec] * 6,
        out_specs=[any_spec] + [hbm_spec] * 4,
        out_shape=[head_shape,
                   pltpu.HBM((2 * BATCHES, HEADS, 2, PAIR, DIM), jnp.bfloat16),
                   pltpu.HBM((BATCHES, HEADS, 2, N_PAIRS * PAIR, DIM), jnp.bfloat16),
                   half_shape, half_shape],
        scratch_shapes=[
            head_buf, head_buf, head_buf, head_buf,
            pltpu.VMEM((2, 2, N_PAIRS * PAIR, DIM), jnp.bfloat16),
            pltpu.VMEM((BATCHES, 2, 2, PAIR, DIM), jnp.float32),
            pltpu.VMEM((2, 2, PAIR, DIM), jnp.float32),
            pltpu.VMEM((2 * BATCHES, PAIR), jnp.int32),
            pltpu.VMEM((1, DIM), jnp.float32),
            pltpu.VMEM((2, 2, 2, HEADS * PAIR, DIM), jnp.bfloat16),
            pltpu.VMEM((2, 2, HEADS, 2, PAIR, DIM), jnp.bfloat16),
            pltpu.VMEM((PART_RING, 2, N_PAIRS * PAIR, DIM), jnp.float32),
            pltpu.VMEM((INBOX_RING, N_INBOX, 2, PAIR, DIM), jnp.float32),
            pltpu.VMEM((2, 2, 2, PAIR, DIM), jnp.bfloat16),
            pltpu.VMEM((PAIR, PAIR), jnp.bfloat16),
            pltpu.VMEM((DIM, N_PAIRS * PAIR), jnp.bfloat16),
            pltpu.VMEM((DIM, N_PAIRS * PAIR), jnp.bfloat16),
            pltpu.VMEM((N_PAIRS * PAIR, 32 * GROUP), jnp.float32),
            pltpu.VMEM((N_PAIRS * PAIR, 32 * GROUP), jnp.float32),
            pltpu.VMEM((4 * PAIR, PIECE * GROUP), jnp.float32),
            dma((2, 2, 2)), dma((BATCHES, 2)), dma((BATCHES, 2)), dma((BATCHES, 2)), dma((2,)), dma((BATCHES,)),
            dma((BATCHES,)), dma((BATCHES,)), dma((BATCHES,)), dma((BATCHES,)),
            dma((UNITS, 7)), dma((UNITS, 7)), dma((N_OUTBOX, PART_RING)), dma((INBOX_RING, N_INBOX)),
            dma((6, 2)), dma((4, 2)), dma((2, BATCHES)), dma((2, 2)), dma((BATCHES,)),
            pltpu.SemaphoreType.REGULAR((N_OUTBOX,)),
        ],
        compiler_params=pltpu.CompilerParams(
            collective_id=0, has_side_effects=True, vmem_limit_bytes=32512 * 1024),
    )(*(pltpu.with_memory_space_constraint(x, pltpu.HBM) for x in (q5, g5, keys, values, positions, freq)))


def place_kernel(odq, gkv, o_out, dq_out, gk_out, gv_out, in_v, out_v, perm, sems, in_s, out_s):
    n_batch = gkv.shape[0]

    def batch_in(b):
        return pltpu.make_async_copy(gkv.at[b], in_v.at[b], in_s.at[b])

    def batch_out(b):
        return [pltpu.make_async_copy(out_v.at[b, i], dst.at[b], out_s.at[b, i]) for i, dst in enumerate((gk_out, gv_out))]

    def start_in(b, carry):
        batch_in(b).start()
        return carry

    lax.fori_loop(0, n_batch, start_in, 0)
    part = n_batch // 4
    large = [pltpu.make_async_copy(odq.at[k, pl.ds(i * part, part)], dst.at[pl.ds(i * part, part)], sems.at[k, i])
             for i in range(4) for k, dst in enumerate((o_out, dq_out))]
    for copy in large:
        copy.start()
    row, col = iota(perm.shape, 0), iota(perm.shape, 1)
    perm[...] = (row == (col % PAIR) * HEADS + col // PAIR).astype(jnp.float32).astype(jnp.bfloat16)

    def regroup(b, carry):
        batch_in(b).wait()
        for i in range(2):
            rows = in_v[b, :, i].reshape(HEADS * PAIR, DIM)
            out_v[b, i] = dot_nn(perm[...], rows).astype(jnp.bfloat16)
        for copy in batch_out(b):
            copy.start()
        return carry

    lax.fori_loop(0, n_batch, regroup, 0)

    def finish_out(b, carry):
        for copy in batch_out(b):
            copy.wait()
        return carry

    lax.fori_loop(0, n_batch, finish_out, 0)
    for copy in large:
        copy.wait()


def place(odq, gkv):
    any_spec = pl.BlockSpec(memory_space=pl.ANY)
    n_batch = gkv.shape[0]
    head_shape = pltpu.HBM(odq.shape[1:], jnp.bfloat16)
    row_shape = pltpu.HBM((n_batch, HEADS * PAIR, DIM), jnp.bfloat16)
    dma = pltpu.SemaphoreType.DMA
    return pl.pallas_call(
        place_kernel, name='place', in_specs=[any_spec] * 2, out_specs=[any_spec] * 4,
        out_shape=[head_shape, head_shape, row_shape, row_shape],
        scratch_shapes=[pltpu.VMEM(gkv.shape, jnp.bfloat16), pltpu.VMEM((n_batch, 2, HEADS * PAIR, DIM), jnp.bfloat16),
                        pltpu.VMEM((HEADS * PAIR, HEADS * PAIR), jnp.bfloat16),
                        dma((2, 4)), dma((n_batch,)), dma((n_batch, 2))],
        compiler_params=pltpu.CompilerParams(vmem_limit_bytes=12 * 1024 * 1024),
    )(odq, pltpu.with_memory_space_constraint(gkv, pltpu.HBM))


def solution(mesh):
    head_spec = P(None, 'cp', 'tp', None)
    pos_spec = P(None, 'cp')

    def local_step(query, keys, values, positions, grad_out):
        batch, length, n_heads, dim = query.shape
        split_shape = (batch, length, HEADS, GROUP, dim)
        row_shape = (batch, length * HEADS, dim)
        outs = attend(query.reshape(split_shape), grad_out.reshape(split_shape), keys.reshape(row_shape),
                      values.reshape(row_shape), positions, jnp.asarray(lane_freq(dim)))
        return tuple(out.reshape(like.shape) for out, like in zip(place(*outs[:2]), (query, query, keys, values)))

    return jax.shard_map(local_step, mesh=mesh,
                         in_specs=(head_spec, head_spec, head_spec, pos_spec, head_spec),
                         out_specs=(head_spec, head_spec, head_spec, head_spec), check_vma=False)
```

```python
import functools

import jax
import jax.numpy as jnp
import numpy as np
from jax import lax
from jax.experimental import pallas as pl
from jax.experimental.pallas import tpu as pltpu
from jax.sharding import PartitionSpec as P

ROPE_THETA = 1000000.0
LOG2E = 1.4426950408889634
DIM = 128
GROUP = 8
HEADS = 4
PIECE = 64
PAIR = 128
N_PAIRS = 8
BATCHES = 8
UNITS = BATCHES * HEADS
KEY_BLOCK = 512
STEP_LAG = 2
MESH_ID = pl.DeviceIdType.MESH

X_STEP, Y_STEP = 1, 2
FIRST_HOP = [(0, 0, X_STEP), (0, 0, Y_STEP), (1, 1, X_STEP), (1, 1, Y_STEP), (2, 2, X_STEP), (2, 2, Y_STEP),
             (3, 3, X_STEP), (3, 3, Y_STEP), (4, 3, X_STEP), (4, 3, Y_STEP), (5, 2, Y_STEP), (5, 2, X_STEP),
             (6, 1, X_STEP)]
RELAY_HOP = [(0, 2, X_STEP), (1, 3, X_STEP), (2, 3, Y_STEP), (3, 2, Y_STEP), (4, 1, X_STEP), (5, 3, Y_STEP)]
SUM_LEAF = [(3, 0, Y_STEP), (4, 0, X_STEP), (2, 0, Y_STEP), (6, 0, X_STEP), (2, 1, Y_STEP), (5, 1, X_STEP),
            (0, 1, X_STEP), (3, 1, Y_STEP), (1, 2, Y_STEP), (4, 2, X_STEP), (0, 3, X_STEP), (1, 3, Y_STEP)]
SUM_RELAY = [(0, 2, Y_STEP), (1, 0, X_STEP), (2, 3, X_STEP), (3, 2, X_STEP), (4, 1, Y_STEP), (5, 0, Y_STEP)]

START_BATCHES = 6
START_UNITS = 8
START_RELAYS = 4
RELAY_LEAD = 6
HOP_LEADS = (8, 7, 8, 8)
START_EARLY = HEADS * START_BATCHES
FAST_UNITS = 2
EARLY_HOP = [(0, 0, X_STEP), (0, 0, Y_STEP), (1, 1, Y_STEP)]
SUM_LAG = 4
OWN_LAG = 8
PART_RING = OWN_LAG + 2
FIN_CLOSE = OWN_LAG + HEADS + 2
INBOX_RING = 9


def owner(pair):
    return pair if pair < 4 else 7 - pair


def inbox(chip):
    found = []
    for pair, src, step in SUM_LEAF + SUM_RELAY:
        if src ^ step == chip:
            found.append((pair, src))
    return found


def outbox(chip):
    return [(pair, step) for pair, src, step in SUM_LEAF + SUM_RELAY if src == chip]


N_INBOX = max(len(inbox(c)) for c in range(4))
N_OUTBOX = max(len(outbox(c)) for c in range(4))


def lane_freq(head_dim):
    exponent = np.arange(head_dim // 2, dtype=np.float64) * (2.0 / head_dim)
    return np.repeat(ROPE_THETA ** -exponent, 2).astype(np.float32)[None, :]


def dot_nn(a, b):
    return jnp.dot(a, b, preferred_element_type=jnp.float32)


def dot_nt(a, b):
    return lax.dot_general(a, b, (((1,), (1,)), ((), ())), preferred_element_type=jnp.float32)


def iota(shape, axis):
    return lax.broadcasted_iota(jnp.int32, shape, axis)


def identity():
    return (iota((DIM, DIM), 0) == iota((DIM, DIM), 1)).astype(jnp.float32).astype(jnp.bfloat16)


def swap_pairs(x):
    return jnp.where(iota(x.shape, 1) % 2 == 0, pltpu.roll(x, DIM - 1, axis=1), pltpu.roll(x, 1, axis=1))


def rows_steps(n_keys, tok, seg, q_v, g_v, tab, kv, kt, vt, part, o_v, dq_v, s_ref):
    core, start, place = seg
    rows = tok * GROUP
    scale = DIM ** -0.5
    c1 = scale * LOG2E
    toks = pl.ds(start, tok)

    def table(k):
        return jnp.broadcast_to(tab[k, core, toks, :][:, None, :], (tok, GROUP, DIM)).reshape(rows, DIM)

    x = q_v[core, toks].astype(jnp.float32).reshape(rows, DIM)
    qr = (x * table(0) + swap_pairs(x) * table(1)).astype(jnp.bfloat16)
    g = g_v[core, toks].astype(jnp.float32).reshape(rows, DIM).astype(jnp.bfloat16)
    blocks = [(a, min(KEY_BLOCK, n_keys - a)) for a in range(0, n_keys, KEY_BLOCK)]
    m8 = None
    for a, n in blocks:
        s = dot_nt(kv[0, a:a + n, :], qr) * c1
        if a + n == n_keys:
            last = s[n - PAIR:, :]
            q_tok = iota(last.shape, 1) // GROUP + place
            last = jnp.where(iota(last.shape, 0) <= q_tok, last, -jnp.inf)
            s = last if n == PAIR else jnp.concatenate([s[:n - PAIR, :], last], axis=0)
        s_ref[a:a + n, :] = s
        f = jnp.max(s.reshape(n // 8, 8, rows), axis=0)
        m8 = f if m8 is None else jnp.maximum(m8, f)
        yield
    row_max = jnp.max(m8, axis=0, keepdims=True)
    l8 = None
    o_t = None
    for a, n in blocks:
        p = jnp.exp2(s_ref[a:a + n, :] - row_max)
        s_ref[a:a + n, :] = p
        f = jnp.sum(p.reshape(n // 8, 8, rows), axis=0)
        l8 = f if l8 is None else l8 + f
        d = dot_nn(vt[:, a:a + n], p.astype(jnp.bfloat16))
        o_t = d if o_t is None else o_t + d
        yield
    inv = 1.0 / jnp.sum(l8, axis=0, keepdims=True)
    out_t = o_t * inv
    o_v[core, toks] = jnp.transpose(out_t).reshape(tok, GROUP, DIM).astype(jnp.bfloat16)
    delta = jnp.sum(dot_nt(identity(), g) * out_t, axis=0, keepdims=True)
    yield
    dq_t = None
    for a, n in blocks:
        p = s_ref[a:a + n, :] * inv
        ds = (p * (dot_nt(kv[1, a:a + n, :], g) - delta)).astype(jnp.bfloat16)
        part[1, a:a + n, :] += dot_nn(p.astype(jnp.bfloat16), g)
        part[0, a:a + n, :] += dot_nn(ds, qr)
        d = dot_nn(kt[:, a:a + n], ds)
        dq_t = d if dq_t is None else dq_t + d
        yield
    dq = jnp.transpose(dq_t) * scale
    dq = dq * table(0) - swap_pairs(dq) * table(1)
    dq_v[core, toks] = dq.reshape(tok, GROUP, DIM).astype(jnp.bfloat16)


def interleave(gens, lag):
    live, waiting, count = [], list(gens), 0
    while live or waiting:
        if waiting and (not live or count >= lag):
            live.append(waiting.pop(0))
            count = 0
        for gen in list(live):
            if next(gen, 'end') == 'end':
                live.remove(gen)
        count += 1


def unit_compute(c, q_v, g_v, tab, kv, o_v, dq_v, part, kt, vt, s_a, s_b, s_e):
    n_late, n_early = (N_PAIRS - c) * PAIR, (c + 1) * PAIR
    eye = identity()
    for a in range(0, n_late, 256):
        n = min(256, n_late - a)
        kt[:, a:a + n] = dot_nt(eye, kv[0, a:a + n, :]).astype(jnp.bfloat16)
        vt[:, a:a + n] = dot_nt(eye, kv[1, a:a + n, :]).astype(jnp.bfloat16)
    part[:, :n_late, :] = jnp.zeros((2, n_late, DIM), jnp.float32)
    refs = (q_v, g_v, tab, kv, kt, vt, part, o_v, dq_v)

    def step(i, carry):
        late = [rows_steps(n_late, 32, (1 - i, PIECE + 32 * k, i * PIECE + 32 * k), *refs, s)
                for k, s in ((0, s_a), (1, s_b))]
        early = rows_steps(n_early, PIECE, (i, 0, i * PIECE), *refs, s_e)
        interleave(late + [early], STEP_LAG)
        return carry

    lax.fori_loop(0, 2, step, 0)


def remote(src, dst, send_sem, recv_sem, device):
    return pltpu.make_async_remote_copy(src_ref=src, dst_ref=dst, send_sem=send_sem, recv_sem=recv_sem,
                                        device_id={'cp': device}, device_id_type=MESH_ID)


def chip_program(c, core, barrier, q_hbm, g_hbm, k_hbm, v_hbm, pos_hbm, freq_hbm, odq_hbm, gkv_hbm, kv_hbm, qs_hbm, gs_hbm,
                 q_v, g_v, o_v, dq_v, kv_v, tab_v, tab_x, pos_v, freq_v, raw_v, ready_v, part, recv, fin_v,
                 perm_in, kt, vt, s_a, s_b, s_e,
                 raw_s, kvl_s, kvx_s, kvx_r, tab_s, tab_r, qx_s, qx_r, gx_s, gx_r, ag_s, ag_r, sum_s, sum_r,
                 load_s, out_s, out_r, fin_s, fin_r, credit):
    o_hbm, dq_hbm = odq_hbm.at[0], odq_hbm.at[1]
    n_late = (N_PAIRS - c) * PAIR
    sib = 2 * c + 1 - core
    nbr = {step: 2 * (c ^ step) + core for step in (X_STEP, Y_STEP)}
    mine, other = BATCHES * core, BATCHES * (1 - core)
    early_hops = [(p, step) for p, src, step in EARLY_HOP if src == c]
    first_hops = [(p, step) for p, src, step in FIRST_HOP if src == c and (p, src, step) not in EARLY_HOP]
    relay_hops = [(p, step) for p, src, step in RELAY_HOP if src == c]
    leaves = [(p, step) for p, src, step in SUM_LEAF if src == c]
    relays = [(p, step) for p, src, step in SUM_RELAY if src == c]
    needed = [p for p in range(N_PAIRS - c) if owner(p) != c]
    sib_pieces = (2 * c + 1 - core, 15 - 2 * c - (1 - core))

    def split(u):
        return u // HEADS, u % HEADS

    def pair_rows(p):
        return pl.ds(p * PAIR, PAIR)

    own_pieces = (2 * c + core, 15 - 2 * c - core)

    def raw_in(b, side):
        src, slot = (mine, other)[side] + b, b % 2
        return [pltpu.make_async_copy(k_hbm.at[src], raw_v.at[slot, side, 0], raw_s.at[slot, side, 0]),
                pltpu.make_async_copy(v_hbm.at[src], raw_v.at[slot, side, 1], raw_s.at[slot, side, 1])]

    def start_raw(b):
        for side in (0, 1):
            for copy in raw_in(b, side):
                copy.start()

    def piece_rows(piece):
        return pl.ds(pl.multiple_of(piece * PIECE, PIECE), PIECE)

    def own_out(b, half):
        return pltpu.make_async_copy(ready_v.at[b % 2, 0, :, :, pl.ds(half * PIECE, PIECE), :],
                                     kv_hbm.at[b, :, :, piece_rows(own_pieces[half]), :], kvl_s.at[b, half])

    def kvx(b, half):
        return remote(ready_v.at[b % 2, 1, :, :, pl.ds(half * PIECE, PIECE), :],
                      kv_hbm.at[b, :, :, piece_rows(own_pieces[half]), :], kvx_s.at[b, half], kvx_r.at[b, half], sib)

    def kvx_in(b, half):
        dst = kv_hbm.at[b, :, :, piece_rows(sib_pieces[half]), :]
        return remote(dst, dst, kvx_s.at[b, half], kvx_r.at[b, half], sib)

    def make_table(tab, row):
        pos = pos_v[pl.ds(row, 1), :].astype(jnp.float32)
        angles = jnp.transpose(jnp.broadcast_to(pos, (PAIR, PAIR))) * freq_v[...]
        tab[0] = jnp.cos(angles)
        sine_val = jnp.sin(angles)
        tab[1] = jnp.where(iota(sine_val.shape, 1) % 2 == 0, -sine_val, sine_val)

    def make_ready(b, at_start=False):
        slot, part_rows = b % 2, PAIR // HEADS

        @pl.when(b >= 2)
        def _():
            for half in range(2):
                kvx(b - 2, half).wait_send()
            tab_out(b - 2).wait_send()

        @pl.when(b == 2)
        def _():
            for u in range(FAST_UNITS):
                for i, (p, step) in enumerate(early_hops + first_hops):
                    kv_copy(jnp.int32(u), p, i, step).wait_send()

        for side in (0, 1):
            tab = tab_x.at[slot] if side else tab_v.at[b, :, core]
            make_table(tab, (mine, other)[side] + b)
            for copy in raw_in(b, side):
                copy.wait()
            for i in range(2):
                blocks = [dot_nn(perm_in[...], raw_v[slot, side, i, j * PAIR:(j + 1) * PAIR]) for j in range(HEADS)]
                for h in range(HEADS):
                    x = jnp.concatenate([block[h * part_rows:(h + 1) * part_rows] for block in blocks], axis=0)
                    if i == 0:
                        x = x * tab[0] + swap_pairs(x) * tab[1]
                    ready_v[slot, side, h, i] = x.astype(jnp.bfloat16)
            if side == 0:
                for half in range(2):
                    own_out(b, half).start()
                if at_start:
                    @pl.when(b == 0)
                    def _():
                        pl.semaphore_wait(barrier, 3)
                        for u in range(FAST_UNITS):
                            fast_hop(jnp.int32(u), True)

        @pl.when(b + 2 < BATCHES)
        def _():
            start_raw(b + 2)

    def send_ready(b):
        for half in range(2):
            kvx(b, half).start()
        tab_out(b).start()

    def qx(b):
        return remote(q_hbm.at[other + b], qs_hbm.at[b], qx_s.at[b], qx_r.at[b], sib)

    def gx(b):
        return remote(g_hbm.at[other + b], gs_hbm.at[b], gx_s.at[b], gx_r.at[b], sib)

    def tab_out(b):
        return remote(tab_x.at[b % 2], tab_v.at[b, :, core], tab_s.at[b % 2], tab_r.at[b], sib)

    def tab_arrive(b):
        dst = tab_v.at[b, :, 1 - core]
        return remote(dst, dst, tab_s.at[0], tab_r.at[b], sib)

    def small_in():
        return [pltpu.make_async_copy(pos_hbm, pos_v, load_s.at[5, 0]),
                pltpu.make_async_copy(freq_hbm, freq_v, load_s.at[5, 1])]

    def kv_copy(u, p, slot, step):
        b, h = split(u)
        ref = kv_hbm.at[b, h, :, pair_rows(p), :]
        return remote(ref, ref, ag_s.at[u, slot], ag_r.at[u, p], nbr[step])

    def send_kv(u, hops, base):
        for i, (p, step) in enumerate(hops):
            kv_copy(u, p, base + i, step).start()

    def have_own(b):
        for half in range(2):
            own_out(b, half).wait()
            kvx_in(b, half).wait_recv()

    def half_copy(u, p, slot, step, own):
        b, h = split(u)
        half = 0 if p == c else 1
        dst = kv_hbm.at[b, h, :, piece_rows((own_pieces if own else sib_pieces)[half]), :]
        src = ready_v.at[b % 2, 0, h, :, pl.ds(half * PIECE, PIECE), :] if own else dst
        return remote(src, dst, ag_s.at[u, slot], ag_r.at[u, p], nbr[step])

    def fast_hop(u, own):
        for i, (p, step) in enumerate(early_hops + first_hops):
            half_copy(u, p, i, step, own).start()

    def early_hop(u):
        send_kv(u, early_hops, 0)

    def first_hop(u):
        send_kv(u, first_hops, len(early_hops))

    def relay_hop(u):
        for p, _ in relay_hops:
            kv_copy(u, p, 0, X_STEP).wait_recv()
        send_kv(u, relay_hops, len(early_hops) + len(first_hops))

    def loads(u):
        b, h = split(u)
        slot = u % 2
        late = pl.ds(0, n_late)
        return [
            pltpu.make_async_copy(q_hbm.at[mine + b, :, h], q_v.at[slot, core], load_s.at[0, slot]),
            pltpu.make_async_copy(g_hbm.at[mine + b, :, h], g_v.at[slot, core], load_s.at[1, slot]),
            pltpu.make_async_copy(qs_hbm.at[b, :, h], q_v.at[slot, 1 - core], load_s.at[2, slot]),
            pltpu.make_async_copy(gs_hbm.at[b, :, h], g_v.at[slot, 1 - core], load_s.at[3, slot]),
            pltpu.make_async_copy(kv_hbm.at[b, h, :, late, :], kv_v.at[slot, :, late, :], load_s.at[4, slot]),
        ]

    def start_loads(u):
        @pl.when(u % HEADS == 0)
        def _():
            qx(u // HEADS).wait_recv()
            gx(u // HEADS).wait_recv()
            tab_arrive(u // HEADS).wait_recv()

        for p in needed:
            if p not in [r for r, _ in relay_hops]:
                kv_copy(u, p, 0, X_STEP).wait_recv()
        for copy in loads(u):
            copy.start()

    def out_local(u):
        b, h = split(u)
        slot = u % 2
        return [pltpu.make_async_copy(o_v.at[slot, core], o_hbm.at[mine + b, :, h], out_s.at[0, slot]),
                pltpu.make_async_copy(dq_v.at[slot, core], dq_hbm.at[mine + b, :, h], out_s.at[1, slot])]

    def out_remote(u):
        b, h = split(u)
        slot = u % 2
        return [remote(o_v.at[slot, 1 - core], o_hbm.at[mine + b, :, h], out_s.at[2, slot], out_r.at[0, b], sib),
                remote(dq_v.at[slot, 1 - core], dq_hbm.at[mine + b, :, h], out_s.at[3, slot], out_r.at[1, b], sib)]

    def out_arrive(b):
        return [remote(q_hbm.at[other + b], o_hbm.at[other + b], out_s.at[2, 0], out_r.at[0, b], sib),
                remote(q_hbm.at[other + b], dq_hbm.at[other + b], out_s.at[3, 0], out_r.at[1, b], sib)]

    def wait_outs(u):
        for copy in out_local(u):
            copy.wait()
        for copy in out_remote(u):
            copy.wait_send()

    def sum_copy(u, p, i, step):
        k, slot = inbox(c ^ step).index((p, c)), u % INBOX_RING
        return remote(part.at[u % PART_RING, :, pair_rows(p), :], recv.at[slot, k],
                      sum_s.at[i, u % PART_RING], sum_r.at[slot, k], nbr[step])

    def sum_arrive(u, k):
        dst = recv.at[u % INBOX_RING, k]
        return remote(dst, dst, sum_s.at[0, 0], sum_r.at[u % INBOX_RING, k], nbr[X_STEP])

    def give_credits(u, pairs):
        @pl.when(u + INBOX_RING < UNITS)
        def _():
            for k, (pair, src) in enumerate(inbox(c)):
                if pair in pairs:
                    pl.semaphore_signal(credit.at[outbox(src).index((pair, src ^ c))], inc=1,
                                        device_id={'cp': 2 * src + core}, device_id_type=MESH_ID)

    def take_credits(u, which):
        @pl.when(u >= INBOX_RING)
        def _():
            for i in which:
                pl.semaphore_wait(credit.at[i], 1)

    def messages(p):
        return [k for k, (pair, _) in enumerate(inbox(c)) if pair == p]

    def wait_sums(u):
        for i, (p, step) in enumerate(leaves + relays):
            sum_copy(u, p, i, step).wait_send()

    def send_leaves(u):
        take_credits(u, range(len(leaves)))
        for i, (p, step) in enumerate(leaves):
            sum_copy(u, p, i, step).start()

    def add_relays(u):
        for p, _ in relays:
            for k in messages(p):
                sum_arrive(u, k).wait_recv()
                part[u % PART_RING, :, pair_rows(p), :] += recv[u % INBOX_RING, k]
        give_credits(u, [p for p, _ in relays])

    def send_relays(u):
        take_credits(u, range(len(leaves), len(leaves) + len(relays)))
        for i, (p, step) in enumerate(relays):
            sum_copy(u, p, len(leaves) + i, step).start()

    def fin_local(u):
        b, h = split(u)
        return pltpu.make_async_copy(fin_v.at[u % 2, core], gkv_hbm.at[mine + b, h], fin_s.at[0, u % 2])

    def fin_remote(u):
        b, h = split(u)
        return remote(fin_v.at[u % 2, 1 - core], gkv_hbm.at[mine + b, h], fin_s.at[1, u % 2], fin_r.at[b], sib)

    def fin_arrive(b):
        dst = gkv_hbm.at[other + b]
        return remote(dst, dst, fin_s.at[1, 0], fin_r.at[b], sib)

    def wait_fin(u):
        fin_local(u).wait()
        fin_remote(u).wait_send()

    def finish(u):
        @pl.when(u >= 2)
        def _():
            wait_fin(u - 2)

        b, slot = u // HEADS, u % 2
        for late, p in ((0, c), (1, N_PAIRS - 1 - c)):
            total = part[u % PART_RING, :, pair_rows(p), :]
            for k in messages(p):
                sum_arrive(u, k).wait_recv()
                total = total + recv[u % INBOX_RING, k]
            for i in range(2):
                who = 1 - i if late else i
                toks = slice(late * PIECE, (late + 1) * PIECE)
                dk = total[0, i * PIECE:(i + 1) * PIECE] * (DIM ** -0.5)
                dk = dk * tab_v[b, 0, who, toks] - swap_pairs(dk) * tab_v[b, 1, who, toks]
                fin_v[slot, who, 0, toks] = dk.astype(jnp.bfloat16)
                fin_v[slot, who, 1, toks] = total[1, i * PIECE:(i + 1) * PIECE].astype(jnp.bfloat16)
        give_credits(u, [c, N_PAIRS - 1 - c])

    def send_fin(u):
        fin_local(u).start()
        fin_remote(u).start()

    last_step = UNITS + OWN_LAG

    def close_copies(t):
        batch = t // HEADS

        @pl.when((t >= FAST_UNITS) & (t < UNITS))
        def _():
            for i, (p, step) in enumerate(early_hops + first_hops):
                kv_copy(t, p, i, step).wait_send()

        @pl.when(t < UNITS)
        def _():
            for i, (p, step) in enumerate(relay_hops):
                kv_copy(t, p, len(early_hops + first_hops) + i, step).wait_send()

        @pl.when((t % HEADS == HEADS - 1) & (t < UNITS))
        def _():
            qx(batch).wait_send()
            gx(batch).wait_send()

        @pl.when((t % HEADS == 0) & (t >= 2 * HEADS) & (batch - 2 < BATCHES))
        def _():
            for copy in out_arrive(batch - 2):
                copy.wait_recv()

        @pl.when((t % HEADS == FIN_CLOSE % HEADS) & (t >= FIN_CLOSE))
        def _():
            fin_arrive((t - FIN_CLOSE) // HEADS).wait_recv()

        @pl.when(t >= UNITS)
        def _():
            wait_sums(t - PART_RING)

        @pl.when((t >= UNITS) & (t < UNITS + 2))
        def _():
            wait_outs(t - 2)

        @pl.when(t == 3 * HEADS)
        def _():
            for b in range(BATCHES - 2, BATCHES):
                for half in range(2):
                    kvx(jnp.int32(b), half).wait_send()
                tab_out(jnp.int32(b)).wait_send()

    def exchange_queries(b):
        qx(b).start()
        gx(b).start()

    for copy in small_in():
        copy.start()
    start_raw(jnp.int32(0))
    for device in (sib, nbr[X_STEP], nbr[Y_STEP]):
        pl.semaphore_signal(barrier, inc=1, device_id={'cp': device}, device_id_type=MESH_ID)
    start_raw(jnp.int32(1))
    row, col = iota(perm_in.shape, 0), iota(perm_in.shape, 1)
    part_rows = PAIR // HEADS
    perm_in[...] = (col == (row % part_rows) * HEADS + row // part_rows).astype(jnp.float32).astype(jnp.bfloat16)
    for copy in small_in():
        copy.wait()

    def up_to(op, first, last):
        def one(u, carry):
            op(u)
            return carry

        lax.fori_loop(first, last, one, 0)

    def start_step(j, carry):
        make_ready(j, at_start=True)
        send_ready(j)

        @pl.when(j == 0)
        def _():
            have_own(j)
            for u in range(FAST_UNITS):
                fast_hop(jnp.int32(u), False)
            exchange_queries(j)

        up_to(relay_hop, jnp.where(j < START_RELAYS, jnp.maximum(j - 1, 0), START_RELAYS),
              jnp.minimum(j + j // 3, START_RELAYS))
        up_to(first_hop, jnp.clip(2 * j, FAST_UNITS, START_UNITS), jnp.clip(2 * j + 2, FAST_UNITS, START_UNITS))

        @pl.when(j >= 1)
        def _():
            have_own(j)

        up_to(early_hop, jnp.maximum(HEADS * j, FAST_UNITS), HEADS * j + HEADS)
        return carry

    lax.fori_loop(0, START_BATCHES, start_step, 0)
    start_loads(jnp.int32(0))

    def tick(t, carry):
        @pl.when((t % 2 == 0) & (t // 2 + START_BATCHES < BATCHES))
        def _():
            make_ready(t // 2 + START_BATCHES)
            send_ready(t // 2 + START_BATCHES)

        @pl.when((t % 2 == 1) & (t // 2 + START_BATCHES < BATCHES))
        def _():
            have_own(t // 2 + START_BATCHES)

        @pl.when((t % HEADS == 0) & (t // HEADS + 1 < BATCHES))
        def _():
            exchange_queries(t // HEADS + 1)

        @pl.when((t >= 1) & (2 * t - 2 + START_EARLY < UNITS))
        def _():
            early_hop(2 * t - 2 + START_EARLY)
            early_hop(2 * t - 1 + START_EARLY)

        @pl.when(t == 0)
        def _():
            for u in range(START_RELAYS, RELAY_LEAD - 1):
                relay_hop(jnp.int32(u))

        @pl.when(t + RELAY_LEAD - 1 < UNITS)
        def _():
            relay_hop(t + RELAY_LEAD - 1)

        @pl.when((t >= 1) & (t - 1 < UNITS))
        def _():
            send_leaves(t - 1)

        @pl.when((t >= 1 + OWN_LAG) & (t - 1 - OWN_LAG < UNITS))
        def _():
            finish(t - 1 - OWN_LAG)

        @pl.when((t >= 1 + SUM_LAG) & (t - 1 - SUM_LAG < UNITS))
        def _():
            add_relays(t - 1 - SUM_LAG)

        @pl.when((t >= 1 + OWN_LAG) & (t - 1 - OWN_LAG < UNITS))
        def _():
            send_fin(t - 1 - OWN_LAG)

        @pl.when((t >= 1 + SUM_LAG) & (t - 1 - SUM_LAG < UNITS))
        def _():
            send_relays(t - 1 - SUM_LAG)

        hop_lead = HOP_LEADS[c]

        @pl.when((t == 0) | ((t + hop_lead > START_UNITS) & (t + hop_lead < UNITS)))
        def _():
            first_hop(jnp.maximum(t + hop_lead, START_UNITS))

        @pl.when(t < UNITS)
        def _():
            for copy in loads(t):
                copy.wait()

            @pl.when(t + 1 < UNITS)
            def _():
                start_loads(t + 1)

            @pl.when(t >= 2)
            def _():
                wait_outs(t - 2)

            @pl.when(t >= PART_RING)
            def _():
                wait_sums(t - PART_RING)

            slot = t % 2
            unit_compute(c, q_v.at[slot], g_v.at[slot], tab_v.at[t // HEADS], kv_v.at[slot], o_v.at[slot],
                         dq_v.at[slot], part.at[t % PART_RING], kt, vt, s_a, s_b, s_e)
            for copy in out_local(t) + out_remote(t):
                copy.start()

        close_copies(t)
        return carry

    lax.fori_loop(0, last_step + 1, tick, 0)

    for u in range(UNITS - 2, UNITS):
        wait_fin(jnp.int32(u))
    for u in range(last_step + 1 - PART_RING, UNITS):
        wait_sums(jnp.int32(u))
    for b in range((last_step - FIN_CLOSE) // HEADS + 1, BATCHES):
        fin_arrive(jnp.int32(b)).wait_recv()


def attend_kernel(*refs):
    me = lax.axis_index('cp')
    chip, core = me // 2, me % 2
    barrier = pltpu.get_barrier_semaphore()
    for c in range(4):
        @pl.when(chip == c)
        def _(c=c):
            chip_program(c, core, barrier, *refs)


def attend(q5, g5, keys, values, positions, freq):
    any_spec = pl.BlockSpec(memory_space=pl.ANY)
    hbm_spec = pl.BlockSpec(memory_space=pltpu.HBM)
    head_shape = pltpu.VMEM((2,) + q5.shape, jnp.bfloat16)
    half_shape = pltpu.HBM((BATCHES,) + q5.shape[1:], jnp.bfloat16)
    head_buf = pltpu.VMEM((2, 2, PAIR, GROUP, DIM), jnp.bfloat16)
    dma = pltpu.SemaphoreType.DMA
    return pl.pallas_call(
        attend_kernel, name='attend',
        in_specs=[any_spec] * 6,
        out_specs=[any_spec] + [hbm_spec] * 4,
        out_shape=[head_shape,
                   pltpu.HBM((2 * BATCHES, HEADS, 2, PAIR, DIM), jnp.bfloat16),
                   pltpu.HBM((BATCHES, HEADS, 2, N_PAIRS * PAIR, DIM), jnp.bfloat16),
                   half_shape, half_shape],
        scratch_shapes=[
            head_buf, head_buf, head_buf, head_buf,
            pltpu.VMEM((2, 2, N_PAIRS * PAIR, DIM), jnp.bfloat16),
            pltpu.VMEM((BATCHES, 2, 2, PAIR, DIM), jnp.float32),
            pltpu.VMEM((2, 2, PAIR, DIM), jnp.float32),
            pltpu.VMEM((2 * BATCHES, PAIR), jnp.int32),
            pltpu.VMEM((1, DIM), jnp.float32),
            pltpu.VMEM((2, 2, 2, HEADS * PAIR, DIM), jnp.bfloat16),
            pltpu.VMEM((2, 2, HEADS, 2, PAIR, DIM), jnp.bfloat16),
            pltpu.VMEM((PART_RING, 2, N_PAIRS * PAIR, DIM), jnp.float32),
            pltpu.VMEM((INBOX_RING, N_INBOX, 2, PAIR, DIM), jnp.float32),
            pltpu.VMEM((2, 2, 2, PAIR, DIM), jnp.bfloat16),
            pltpu.VMEM((PAIR, PAIR), jnp.bfloat16),
            pltpu.VMEM((DIM, N_PAIRS * PAIR), jnp.bfloat16),
            pltpu.VMEM((DIM, N_PAIRS * PAIR), jnp.bfloat16),
            pltpu.VMEM((N_PAIRS * PAIR, 32 * GROUP), jnp.float32),
            pltpu.VMEM((N_PAIRS * PAIR, 32 * GROUP), jnp.float32),
            pltpu.VMEM((4 * PAIR, PIECE * GROUP), jnp.float32),
            dma((2, 2, 2)), dma((BATCHES, 2)), dma((BATCHES, 2)), dma((BATCHES, 2)), dma((2,)), dma((BATCHES,)),
            dma((BATCHES,)), dma((BATCHES,)), dma((BATCHES,)), dma((BATCHES,)),
            dma((UNITS, 7)), dma((UNITS, 7)), dma((N_OUTBOX, PART_RING)), dma((INBOX_RING, N_INBOX)),
            dma((6, 2)), dma((4, 2)), dma((2, BATCHES)), dma((2, 2)), dma((BATCHES,)),
            pltpu.SemaphoreType.REGULAR((N_OUTBOX,)),
        ],
        compiler_params=pltpu.CompilerParams(
            collective_id=0, has_side_effects=True, vmem_limit_bytes=32512 * 1024),
    )(*(pltpu.with_memory_space_constraint(x, pltpu.HBM) for x in (q5, g5, keys, values, positions, freq)))


def place_kernel(odq, gkv, o_out, dq_out, gk_out, gv_out, in_v, out_v, perm, sems, in_s, out_s):
    n_batch = gkv.shape[0]

    def batch_in(b):
        return pltpu.make_async_copy(gkv.at[b], in_v.at[b], in_s.at[b])

    def batch_out(b):
        return [pltpu.make_async_copy(out_v.at[b, i], dst.at[b], out_s.at[b, i]) for i, dst in enumerate((gk_out, gv_out))]

    def start_in(b, carry):
        batch_in(b).start()
        return carry

    lax.fori_loop(0, n_batch, start_in, 0)
    part = n_batch // 4
    large = [pltpu.make_async_copy(odq.at[k, pl.ds(i * part, part)], dst.at[pl.ds(i * part, part)], sems.at[k, i])
             for i in range(4) for k, dst in enumerate((o_out, dq_out))]
    for copy in large:
        copy.start()
    row, col = iota(perm.shape, 0), iota(perm.shape, 1)
    perm[...] = (row == (col % PAIR) * HEADS + col // PAIR).astype(jnp.float32).astype(jnp.bfloat16)

    def regroup(b, carry):
        batch_in(b).wait()
        for i in range(2):
            rows = in_v[b, :, i].reshape(HEADS * PAIR, DIM)
            out_v[b, i] = dot_nn(perm[...], rows).astype(jnp.bfloat16)
        for copy in batch_out(b):
            copy.start()
        return carry

    lax.fori_loop(0, n_batch, regroup, 0)

    def finish_out(b, carry):
        for copy in batch_out(b):
            copy.wait()
        return carry

    lax.fori_loop(0, n_batch, finish_out, 0)
    for copy in large:
        copy.wait()


def place(odq, gkv):
    any_spec = pl.BlockSpec(memory_space=pl.ANY)
    n_batch = gkv.shape[0]
    head_shape = pltpu.HBM(odq.shape[1:], jnp.bfloat16)
    row_shape = pltpu.HBM((n_batch, HEADS * PAIR, DIM), jnp.bfloat16)
    dma = pltpu.SemaphoreType.DMA
    return pl.pallas_call(
        place_kernel, name='place', in_specs=[any_spec] * 2, out_specs=[any_spec] * 4,
        out_shape=[head_shape, head_shape, row_shape, row_shape],
        scratch_shapes=[pltpu.VMEM(gkv.shape, jnp.bfloat16), pltpu.VMEM((n_batch, 2, HEADS * PAIR, DIM), jnp.bfloat16),
                        pltpu.VMEM((HEADS * PAIR, HEADS * PAIR), jnp.bfloat16),
                        dma((2, 4)), dma((n_batch,)), dma((n_batch, 2))],
        compiler_params=pltpu.CompilerParams(vmem_limit_bytes=12 * 1024 * 1024),
    )(odq, pltpu.with_memory_space_constraint(gkv, pltpu.HBM))


def solution(mesh):
    head_spec = P(None, 'cp', 'tp', None)
    pos_spec = P(None, 'cp')

    def local_step(query, keys, values, positions, grad_out):
        batch, length, n_heads, dim = query.shape
        split_shape = (batch, length, HEADS, GROUP, dim)
        row_shape = (batch, length * HEADS, dim)
        outs = attend(query.reshape(split_shape), grad_out.reshape(split_shape), keys.reshape(row_shape),
                      values.reshape(row_shape), positions, jnp.asarray(lane_freq(dim)))
        return tuple(out.reshape(like.shape) for out, like in zip(place(*outs[:2]), (query, query, keys, values)))

    return jax.shard_map(local_step, mesh=mesh,
                         in_specs=(head_spec, head_spec, head_spec, pos_spec, head_spec),
                         out_specs=(head_spec, head_spec, head_spec, head_spec), check_vma=False)
```

```python
import functools

import jax
import jax.numpy as jnp
import numpy as np
from jax import lax
from jax.experimental import pallas as pl
from jax.experimental.pallas import tpu as pltpu
from jax.sharding import PartitionSpec as P

ROPE_THETA = 1000000.0
LOG2E = 1.4426950408889634
DIM = 128
GROUP = 8
HEADS = 4
PIECE = 64
PAIR = 128
N_PAIRS = 8
BATCHES = 8
UNITS = BATCHES * HEADS
KEY_BLOCK = 512
STEP_LAG = 2
MESH_ID = pl.DeviceIdType.MESH

X_STEP, Y_STEP = 1, 2
FIRST_HOP = [(0, 0, X_STEP), (0, 0, Y_STEP), (1, 1, X_STEP), (1, 1, Y_STEP), (2, 2, X_STEP), (2, 2, Y_STEP),
             (3, 3, X_STEP), (3, 3, Y_STEP), (4, 3, X_STEP), (4, 3, Y_STEP), (5, 2, Y_STEP), (5, 2, X_STEP),
             (6, 1, X_STEP)]
RELAY_HOP = [(0, 2, X_STEP), (1, 3, X_STEP), (2, 3, Y_STEP), (3, 2, Y_STEP), (4, 1, X_STEP), (5, 3, Y_STEP)]
SUM_LEAF = [(3, 0, Y_STEP), (4, 0, X_STEP), (2, 0, Y_STEP), (6, 0, X_STEP), (2, 1, Y_STEP), (5, 1, X_STEP),
            (0, 1, X_STEP), (3, 1, Y_STEP), (1, 2, Y_STEP), (4, 2, X_STEP), (0, 3, X_STEP), (1, 3, Y_STEP)]
SUM_RELAY = [(0, 2, Y_STEP), (1, 0, X_STEP), (2, 3, X_STEP), (3, 2, X_STEP), (4, 1, Y_STEP), (5, 0, Y_STEP)]

START_BATCHES = 6
START_UNITS = 8
START_RELAYS = 4
RELAY_LEAD = 6
HOP_LEADS = (8, 7, 8, 8)
START_EARLY = HEADS * START_BATCHES
FAST_UNITS = HEADS
EARLY_HOP = [(0, 0, X_STEP), (0, 0, Y_STEP), (1, 1, Y_STEP)]
SUM_LAG = 4
OWN_LAG = 8
PART_RING = OWN_LAG + 2
FIN_CLOSE = OWN_LAG + HEADS + 2
INBOX_RING = 9


def owner(pair):
    return pair if pair < 4 else 7 - pair


def inbox(chip):
    found = []
    for pair, src, step in SUM_LEAF + SUM_RELAY:
        if src ^ step == chip:
            found.append((pair, src))
    return found


def outbox(chip):
    return [(pair, step) for pair, src, step in SUM_LEAF + SUM_RELAY if src == chip]


N_INBOX = max(len(inbox(c)) for c in range(4))
N_OUTBOX = max(len(outbox(c)) for c in range(4))


def lane_freq(head_dim):
    exponent = np.arange(head_dim // 2, dtype=np.float64) * (2.0 / head_dim)
    return np.repeat(ROPE_THETA ** -exponent, 2).astype(np.float32)[None, :]


def dot_nn(a, b):
    return jnp.dot(a, b, preferred_element_type=jnp.float32)


def dot_nt(a, b):
    return lax.dot_general(a, b, (((1,), (1,)), ((), ())), preferred_element_type=jnp.float32)


def iota(shape, axis):
    return lax.broadcasted_iota(jnp.int32, shape, axis)


def identity():
    return (iota((DIM, DIM), 0) == iota((DIM, DIM), 1)).astype(jnp.float32).astype(jnp.bfloat16)


def swap_pairs(x):
    return jnp.where(iota(x.shape, 1) % 2 == 0, pltpu.roll(x, DIM - 1, axis=1), pltpu.roll(x, 1, axis=1))


def rows_steps(n_keys, tok, seg, q_v, g_v, tab, kv, kt, vt, part, o_v, dq_v, s_ref):
    core, start, place = seg
    rows = tok * GROUP
    scale = DIM ** -0.5
    c1 = scale * LOG2E
    toks = pl.ds(start, tok)

    def table(k):
        return jnp.broadcast_to(tab[k, core, toks, :][:, None, :], (tok, GROUP, DIM)).reshape(rows, DIM)

    x = q_v[core, toks].astype(jnp.float32).reshape(rows, DIM)
    qr = (x * table(0) + swap_pairs(x) * table(1)).astype(jnp.bfloat16)
    g = g_v[core, toks].astype(jnp.float32).reshape(rows, DIM).astype(jnp.bfloat16)
    blocks = [(a, min(KEY_BLOCK, n_keys - a)) for a in range(0, n_keys, KEY_BLOCK)]
    m8 = None
    for a, n in blocks:
        s = dot_nt(kv[0, a:a + n, :], qr) * c1
        if a + n == n_keys:
            last = s[n - PAIR:, :]
            q_tok = iota(last.shape, 1) // GROUP + place
            last = jnp.where(iota(last.shape, 0) <= q_tok, last, -jnp.inf)
            s = last if n == PAIR else jnp.concatenate([s[:n - PAIR, :], last], axis=0)
        s_ref[a:a + n, :] = s
        f = jnp.max(s.reshape(n // 8, 8, rows), axis=0)
        m8 = f if m8 is None else jnp.maximum(m8, f)
        yield
    row_max = jnp.max(m8, axis=0, keepdims=True)
    l8 = None
    o_t = None
    for a, n in blocks:
        p = jnp.exp2(s_ref[a:a + n, :] - row_max)
        s_ref[a:a + n, :] = p
        f = jnp.sum(p.reshape(n // 8, 8, rows), axis=0)
        l8 = f if l8 is None else l8 + f
        d = dot_nn(vt[:, a:a + n], p.astype(jnp.bfloat16))
        o_t = d if o_t is None else o_t + d
        yield
    inv = 1.0 / jnp.sum(l8, axis=0, keepdims=True)
    out_t = o_t * inv
    o_v[core, toks] = jnp.transpose(out_t).reshape(tok, GROUP, DIM).astype(jnp.bfloat16)
    delta = jnp.sum(dot_nt(identity(), g) * out_t, axis=0, keepdims=True)
    yield
    dq_t = None
    for a, n in blocks:
        p = s_ref[a:a + n, :] * inv
        ds = (p * (dot_nt(kv[1, a:a + n, :], g) - delta)).astype(jnp.bfloat16)
        part[1, a:a + n, :] += dot_nn(p.astype(jnp.bfloat16), g)
        part[0, a:a + n, :] += dot_nn(ds, qr)
        d = dot_nn(kt[:, a:a + n], ds)
        dq_t = d if dq_t is None else dq_t + d
        yield
    dq = jnp.transpose(dq_t) * scale
    dq = dq * table(0) - swap_pairs(dq) * table(1)
    dq_v[core, toks] = dq.reshape(tok, GROUP, DIM).astype(jnp.bfloat16)


def interleave(gens, lag):
    live, waiting, count = [], list(gens), 0
    while live or waiting:
        if waiting and (not live or count >= lag):
            live.append(waiting.pop(0))
            count = 0
        for gen in list(live):
            if next(gen, 'end') == 'end':
                live.remove(gen)
        count += 1


def unit_compute(c, q_v, g_v, tab, kv, o_v, dq_v, part, kt, vt, s_a, s_b, s_e):
    n_late, n_early = (N_PAIRS - c) * PAIR, (c + 1) * PAIR
    eye = identity()
    for a in range(0, n_late, 256):
        n = min(256, n_late - a)
        kt[:, a:a + n] = dot_nt(eye, kv[0, a:a + n, :]).astype(jnp.bfloat16)
        vt[:, a:a + n] = dot_nt(eye, kv[1, a:a + n, :]).astype(jnp.bfloat16)
    part[:, :n_late, :] = jnp.zeros((2, n_late, DIM), jnp.float32)
    refs = (q_v, g_v, tab, kv, kt, vt, part, o_v, dq_v)

    def step(i, carry):
        late = [rows_steps(n_late, 32, (1 - i, PIECE + 32 * k, i * PIECE + 32 * k), *refs, s)
                for k, s in ((0, s_a), (1, s_b))]
        early = rows_steps(n_early, PIECE, (i, 0, i * PIECE), *refs, s_e)
        interleave(late + [early], STEP_LAG)
        return carry

    lax.fori_loop(0, 2, step, 0)


def remote(src, dst, send_sem, recv_sem, device):
    return pltpu.make_async_remote_copy(src_ref=src, dst_ref=dst, send_sem=send_sem, recv_sem=recv_sem,
                                        device_id={'cp': device}, device_id_type=MESH_ID)


def chip_program(c, core, barrier, q_hbm, g_hbm, k_hbm, v_hbm, pos_hbm, freq_hbm, odq_hbm, gkv_hbm, kv_hbm, qs_hbm, gs_hbm,
                 q_v, g_v, o_v, dq_v, kv_v, tab_v, tab_x, pos_v, freq_v, raw_v, ready_v, part, recv, fin_v,
                 perm_in, kt, vt, s_a, s_b, s_e,
                 raw_s, kvl_s, kvx_s, kvx_r, tab_s, tab_r, qx_s, qx_r, gx_s, gx_r, fast_s, ag_s, ag_r, sum_s, sum_r,
                 load_s, out_s, out_r, fin_s, fin_r, credit):
    o_hbm, dq_hbm = odq_hbm.at[0], odq_hbm.at[1]
    n_late = (N_PAIRS - c) * PAIR
    sib = 2 * c + 1 - core
    nbr = {step: 2 * (c ^ step) + core for step in (X_STEP, Y_STEP)}
    mine, other = BATCHES * core, BATCHES * (1 - core)
    early_hops = [(p, step) for p, src, step in EARLY_HOP if src == c]
    first_hops = [(p, step) for p, src, step in FIRST_HOP if src == c and (p, src, step) not in EARLY_HOP]
    relay_hops = [(p, step) for p, src, step in RELAY_HOP if src == c]
    leaves = [(p, step) for p, src, step in SUM_LEAF if src == c]
    relays = [(p, step) for p, src, step in SUM_RELAY if src == c]
    needed = [p for p in range(N_PAIRS - c) if owner(p) != c]
    sib_pieces = (2 * c + 1 - core, 15 - 2 * c - (1 - core))

    def split(u):
        return u // HEADS, u % HEADS

    def pair_rows(p):
        return pl.ds(p * PAIR, PAIR)

    own_pieces = (2 * c + core, 15 - 2 * c - core)

    def raw_in(b, side):
        src, slot = (mine, other)[side] + b, b % 2
        return [pltpu.make_async_copy(k_hbm.at[src], raw_v.at[slot, side, 0], raw_s.at[slot, side, 0]),
                pltpu.make_async_copy(v_hbm.at[src], raw_v.at[slot, side, 1], raw_s.at[slot, side, 1])]

    def start_raw(b):
        for side in (0, 1):
            for copy in raw_in(b, side):
                copy.start()

    def piece_rows(piece):
        return pl.ds(pl.multiple_of(piece * PIECE, PIECE), PIECE)

    def own_out(b, half):
        return pltpu.make_async_copy(ready_v.at[b % 2, 0, :, :, pl.ds(half * PIECE, PIECE), :],
                                     kv_hbm.at[b, :, :, piece_rows(own_pieces[half]), :], kvl_s.at[b, half])

    def kvx(b, half):
        return remote(ready_v.at[b % 2, 1, :, :, pl.ds(half * PIECE, PIECE), :],
                      kv_hbm.at[b, :, :, piece_rows(own_pieces[half]), :], kvx_s.at[b, half], kvx_r.at[b, half], sib)

    def kvx_in(b, half):
        dst = kv_hbm.at[b, :, :, piece_rows(sib_pieces[half]), :]
        return remote(dst, dst, kvx_s.at[b, half], kvx_r.at[b, half], sib)

    def make_table(tab, row):
        pos = pos_v[pl.ds(row, 1), :].astype(jnp.float32)
        angles = jnp.transpose(jnp.broadcast_to(pos, (PAIR, PAIR))) * freq_v[...]
        tab[0] = jnp.cos(angles)
        sine_val = jnp.sin(angles)
        tab[1] = jnp.where(iota(sine_val.shape, 1) % 2 == 0, -sine_val, sine_val)

    def make_ready(b, at_start=False):
        slot, part_rows = b % 2, PAIR // HEADS

        @pl.when(b >= 2)
        def _():
            for half in range(2):
                kvx(b - 2, half).wait_send()
            tab_out(b - 2).wait_send()

        if at_start:
            @pl.when(b == 2)
            def _():
                up_to(lambda u: close_fast(u, True), 0, FAST_UNITS)

            @pl.when(b == 5)
            def _():
                up_to(lambda u: close_fast(u, False), 0, FAST_UNITS)

        for side in (0, 1):
            tab = tab_x.at[slot] if side else tab_v.at[b, :, core]
            make_table(tab, (mine, other)[side] + b)
            for copy in raw_in(b, side):
                copy.wait()
            for i in range(2):
                blocks = [dot_nn(perm_in[...], raw_v[slot, side, i, j * PAIR:(j + 1) * PAIR]) for j in range(HEADS)]
                for h in range(HEADS):
                    x = jnp.concatenate([block[h * part_rows:(h + 1) * part_rows] for block in blocks], axis=0)
                    if i == 0:
                        x = x * tab[0] + swap_pairs(x) * tab[1]
                    ready_v[slot, side, h, i] = x.astype(jnp.bfloat16)
            if side == 0:
                for half in range(2):
                    own_out(b, half).start()
                if at_start:
                    @pl.when(b == 0)
                    def _():
                        pl.semaphore_wait(barrier, 3)
                        up_to(lambda u: fast_hop(u, True), 0, FAST_UNITS)

        @pl.when(b + 2 < BATCHES)
        def _():
            start_raw(b + 2)

    def send_ready(b):
        for half in range(2):
            kvx(b, half).start()
        tab_out(b).start()

    def qx(b):
        return remote(q_hbm.at[other + b], qs_hbm.at[b], qx_s.at[b], qx_r.at[b], sib)

    def gx(b):
        return remote(g_hbm.at[other + b], gs_hbm.at[b], gx_s.at[b], gx_r.at[b], sib)

    def tab_out(b):
        return remote(tab_x.at[b % 2], tab_v.at[b, :, core], tab_s.at[b % 2], tab_r.at[b], sib)

    def tab_arrive(b):
        dst = tab_v.at[b, :, 1 - core]
        return remote(dst, dst, tab_s.at[0], tab_r.at[b], sib)

    def small_in():
        return [pltpu.make_async_copy(pos_hbm, pos_v, load_s.at[5, 0]),
                pltpu.make_async_copy(freq_hbm, freq_v, load_s.at[5, 1])]

    def kv_copy(u, p, slot, step):
        b, h = split(u)
        ref = kv_hbm.at[b, h, :, pair_rows(p), :]
        return remote(ref, ref, ag_s.at[u, slot], ag_r.at[u, p], nbr[step])

    def send_kv(u, hops, base):
        for i, (p, step) in enumerate(hops):
            kv_copy(u, p, base + i, step).start()

    def have_own(b):
        for half in range(2):
            own_out(b, half).wait()
            kvx_in(b, half).wait_recv()

    def half_copy(u, p, slot, step, own):
        b, h = split(u)
        half = 0 if p == c else 1
        dst = kv_hbm.at[b, h, :, piece_rows((own_pieces if own else sib_pieces)[half]), :]
        src = ready_v.at[b % 2, 0, h, :, pl.ds(half * PIECE, PIECE), :] if own else dst
        return remote(src, dst, (fast_s if own else ag_s).at[u, slot], ag_r.at[u, p], nbr[step])

    def fast_hop(u, own):
        for i, (p, step) in enumerate(early_hops + first_hops):
            half_copy(u, p, i, step, own).start()

    def close_fast(u, own):
        for i, (p, step) in enumerate(early_hops + first_hops):
            half_copy(u, p, i, step, own).wait_send()

    def early_hop(u):
        send_kv(u, early_hops, 0)

    def first_hop(u):
        send_kv(u, first_hops, len(early_hops))

    def relay_hop(u):
        for p, _ in relay_hops:
            kv_copy(u, p, 0, X_STEP).wait_recv()
        send_kv(u, relay_hops, len(early_hops) + len(first_hops))

    def loads(u):
        b, h = split(u)
        slot = u % 2
        late = pl.ds(0, n_late)
        return [
            pltpu.make_async_copy(q_hbm.at[mine + b, :, h], q_v.at[slot, core], load_s.at[0, slot]),
            pltpu.make_async_copy(g_hbm.at[mine + b, :, h], g_v.at[slot, core], load_s.at[1, slot]),
            pltpu.make_async_copy(qs_hbm.at[b, :, h], q_v.at[slot, 1 - core], load_s.at[2, slot]),
            pltpu.make_async_copy(gs_hbm.at[b, :, h], g_v.at[slot, 1 - core], load_s.at[3, slot]),
            pltpu.make_async_copy(kv_hbm.at[b, h, :, late, :], kv_v.at[slot, :, late, :], load_s.at[4, slot]),
        ]

    def start_loads(u):
        @pl.when(u % HEADS == 0)
        def _():
            qx(u // HEADS).wait_recv()
            gx(u // HEADS).wait_recv()
            tab_arrive(u // HEADS).wait_recv()

        for p in needed:
            if p not in [r for r, _ in relay_hops]:
                kv_copy(u, p, 0, X_STEP).wait_recv()
        for copy in loads(u):
            copy.start()

    def out_local(u):
        b, h = split(u)
        slot = u % 2
        return [pltpu.make_async_copy(o_v.at[slot, core], o_hbm.at[mine + b, :, h], out_s.at[0, slot]),
                pltpu.make_async_copy(dq_v.at[slot, core], dq_hbm.at[mine + b, :, h], out_s.at[1, slot])]

    def out_remote(u):
        b, h = split(u)
        slot = u % 2
        return [remote(o_v.at[slot, 1 - core], o_hbm.at[mine + b, :, h], out_s.at[2, slot], out_r.at[0, b], sib),
                remote(dq_v.at[slot, 1 - core], dq_hbm.at[mine + b, :, h], out_s.at[3, slot], out_r.at[1, b], sib)]

    def out_arrive(b):
        return [remote(q_hbm.at[other + b], o_hbm.at[other + b], out_s.at[2, 0], out_r.at[0, b], sib),
                remote(q_hbm.at[other + b], dq_hbm.at[other + b], out_s.at[3, 0], out_r.at[1, b], sib)]

    def wait_outs(u):
        for copy in out_local(u):
            copy.wait()
        for copy in out_remote(u):
            copy.wait_send()

    def sum_copy(u, p, i, step):
        k, slot = inbox(c ^ step).index((p, c)), u % INBOX_RING
        return remote(part.at[u % PART_RING, :, pair_rows(p), :], recv.at[slot, k],
                      sum_s.at[i, u % PART_RING], sum_r.at[slot, k], nbr[step])

    def sum_arrive(u, k):
        dst = recv.at[u % INBOX_RING, k]
        return remote(dst, dst, sum_s.at[0, 0], sum_r.at[u % INBOX_RING, k], nbr[X_STEP])

    def give_credits(u, pairs):
        @pl.when(u + INBOX_RING < UNITS)
        def _():
            for k, (pair, src) in enumerate(inbox(c)):
                if pair in pairs:
                    pl.semaphore_signal(credit.at[outbox(src).index((pair, src ^ c))], inc=1,
                                        device_id={'cp': 2 * src + core}, device_id_type=MESH_ID)

    def take_credits(u, which):
        @pl.when(u >= INBOX_RING)
        def _():
            for i in which:
                pl.semaphore_wait(credit.at[i], 1)

    def messages(p):
        return [k for k, (pair, _) in enumerate(inbox(c)) if pair == p]

    def wait_sums(u):
        for i, (p, step) in enumerate(leaves + relays):
            sum_copy(u, p, i, step).wait_send()

    def send_leaves(u):
        take_credits(u, range(len(leaves)))
        for i, (p, step) in enumerate(leaves):
            sum_copy(u, p, i, step).start()

    def add_relays(u):
        for p, _ in relays:
            for k in messages(p):
                sum_arrive(u, k).wait_recv()
                part[u % PART_RING, :, pair_rows(p), :] += recv[u % INBOX_RING, k]
        give_credits(u, [p for p, _ in relays])

    def send_relays(u):
        take_credits(u, range(len(leaves), len(leaves) + len(relays)))
        for i, (p, step) in enumerate(relays):
            sum_copy(u, p, len(leaves) + i, step).start()

    def fin_local(u):
        b, h = split(u)
        return pltpu.make_async_copy(fin_v.at[u % 2, core], gkv_hbm.at[mine + b, h], fin_s.at[0, u % 2])

    def fin_remote(u):
        b, h = split(u)
        return remote(fin_v.at[u % 2, 1 - core], gkv_hbm.at[mine + b, h], fin_s.at[1, u % 2], fin_r.at[b], sib)

    def fin_arrive(b):
        dst = gkv_hbm.at[other + b]
        return remote(dst, dst, fin_s.at[1, 0], fin_r.at[b], sib)

    def wait_fin(u):
        fin_local(u).wait()
        fin_remote(u).wait_send()

    def finish(u):
        @pl.when(u >= 2)
        def _():
            wait_fin(u - 2)

        b, slot = u // HEADS, u % 2
        for late, p in ((0, c), (1, N_PAIRS - 1 - c)):
            total = part[u % PART_RING, :, pair_rows(p), :]
            for k in messages(p):
                sum_arrive(u, k).wait_recv()
                total = total + recv[u % INBOX_RING, k]
            for i in range(2):
                who = 1 - i if late else i
                toks = slice(late * PIECE, (late + 1) * PIECE)
                dk = total[0, i * PIECE:(i + 1) * PIECE] * (DIM ** -0.5)
                dk = dk * tab_v[b, 0, who, toks] - swap_pairs(dk) * tab_v[b, 1, who, toks]
                fin_v[slot, who, 0, toks] = dk.astype(jnp.bfloat16)
                fin_v[slot, who, 1, toks] = total[1, i * PIECE:(i + 1) * PIECE].astype(jnp.bfloat16)
        give_credits(u, [c, N_PAIRS - 1 - c])

    def send_fin(u):
        fin_local(u).start()
        fin_remote(u).start()

    last_step = UNITS + OWN_LAG

    def close_copies(t):
        batch = t // HEADS

        @pl.when((t >= FAST_UNITS) & (t < UNITS))
        def _():
            for i, (p, step) in enumerate(early_hops + first_hops):
                kv_copy(t, p, i, step).wait_send()

        @pl.when(t < UNITS)
        def _():
            for i, (p, step) in enumerate(relay_hops):
                kv_copy(t, p, len(early_hops + first_hops) + i, step).wait_send()

        @pl.when((t % HEADS == HEADS - 1) & (t < UNITS))
        def _():
            qx(batch).wait_send()
            gx(batch).wait_send()

        @pl.when((t % HEADS == 0) & (t >= 2 * HEADS) & (batch - 2 < BATCHES))
        def _():
            for copy in out_arrive(batch - 2):
                copy.wait_recv()

        @pl.when((t % HEADS == FIN_CLOSE % HEADS) & (t >= FIN_CLOSE))
        def _():
            fin_arrive((t - FIN_CLOSE) // HEADS).wait_recv()

        @pl.when(t >= UNITS)
        def _():
            wait_sums(t - PART_RING)

        @pl.when((t >= UNITS) & (t < UNITS + 2))
        def _():
            wait_outs(t - 2)

        @pl.when(t == 3 * HEADS)
        def _():
            for b in range(BATCHES - 2, BATCHES):
                for half in range(2):
                    kvx(jnp.int32(b), half).wait_send()
                tab_out(jnp.int32(b)).wait_send()

    def exchange_queries(b):
        qx(b).start()
        gx(b).start()

    for copy in small_in():
        copy.start()
    start_raw(jnp.int32(0))
    for device in (sib, nbr[X_STEP], nbr[Y_STEP]):
        pl.semaphore_signal(barrier, inc=1, device_id={'cp': device}, device_id_type=MESH_ID)
    start_raw(jnp.int32(1))
    row, col = iota(perm_in.shape, 0), iota(perm_in.shape, 1)
    part_rows = PAIR // HEADS
    perm_in[...] = (col == (row % part_rows) * HEADS + row // part_rows).astype(jnp.float32).astype(jnp.bfloat16)
    for copy in small_in():
        copy.wait()

    def up_to(op, first, last):
        def one(u, carry):
            op(u)
            return carry

        lax.fori_loop(first, last, one, 0)

    def start_step(j, carry):
        make_ready(j, at_start=True)
        send_ready(j)

        @pl.when(j == 0)
        def _():
            have_own(j)
            up_to(lambda u: fast_hop(u, False), 0, FAST_UNITS)
            exchange_queries(j)

        up_to(relay_hop, jnp.where(j < START_RELAYS, jnp.maximum(j - 1, 0), START_RELAYS),
              jnp.minimum(j + j // 3, START_RELAYS))
        up_to(first_hop, jnp.clip(2 * j, FAST_UNITS, START_UNITS), jnp.clip(2 * j + 2, FAST_UNITS, START_UNITS))

        @pl.when(j >= 1)
        def _():
            have_own(j)

        up_to(early_hop, jnp.maximum(HEADS * j, FAST_UNITS), HEADS * j + HEADS)
        return carry

    lax.fori_loop(0, START_BATCHES, start_step, 0)
    start_loads(jnp.int32(0))

    def tick(t, carry):
        @pl.when((t % 2 == 0) & (t // 2 + START_BATCHES < BATCHES))
        def _():
            make_ready(t // 2 + START_BATCHES)
            send_ready(t // 2 + START_BATCHES)

        @pl.when((t % 2 == 1) & (t // 2 + START_BATCHES < BATCHES))
        def _():
            have_own(t // 2 + START_BATCHES)

        @pl.when((t % HEADS == 0) & (t // HEADS + 1 < BATCHES))
        def _():
            exchange_queries(t // HEADS + 1)

        @pl.when((t >= 1) & (2 * t - 2 + START_EARLY < UNITS))
        def _():
            early_hop(2 * t - 2 + START_EARLY)
            early_hop(2 * t - 1 + START_EARLY)

        @pl.when(t == 0)
        def _():
            for u in range(START_RELAYS, RELAY_LEAD - 1):
                relay_hop(jnp.int32(u))

        @pl.when(t + RELAY_LEAD - 1 < UNITS)
        def _():
            relay_hop(t + RELAY_LEAD - 1)

        @pl.when((t >= 1) & (t - 1 < UNITS))
        def _():
            send_leaves(t - 1)

        @pl.when((t >= 1 + OWN_LAG) & (t - 1 - OWN_LAG < UNITS))
        def _():
            finish(t - 1 - OWN_LAG)

        @pl.when((t >= 1 + SUM_LAG) & (t - 1 - SUM_LAG < UNITS))
        def _():
            add_relays(t - 1 - SUM_LAG)

        @pl.when((t >= 1 + OWN_LAG) & (t - 1 - OWN_LAG < UNITS))
        def _():
            send_fin(t - 1 - OWN_LAG)

        @pl.when((t >= 1 + SUM_LAG) & (t - 1 - SUM_LAG < UNITS))
        def _():
            send_relays(t - 1 - SUM_LAG)

        hop_lead = HOP_LEADS[c]

        @pl.when((t == 0) | ((t + hop_lead > START_UNITS) & (t + hop_lead < UNITS)))
        def _():
            first_hop(jnp.maximum(t + hop_lead, START_UNITS))

        @pl.when(t < UNITS)
        def _():
            for copy in loads(t):
                copy.wait()

            @pl.when(t + 1 < UNITS)
            def _():
                start_loads(t + 1)

            @pl.when(t >= 2)
            def _():
                wait_outs(t - 2)

            @pl.when(t >= PART_RING)
            def _():
                wait_sums(t - PART_RING)

            slot = t % 2
            unit_compute(c, q_v.at[slot], g_v.at[slot], tab_v.at[t // HEADS], kv_v.at[slot], o_v.at[slot],
                         dq_v.at[slot], part.at[t % PART_RING], kt, vt, s_a, s_b, s_e)
            for copy in out_local(t) + out_remote(t):
                copy.start()

        close_copies(t)
        return carry

    lax.fori_loop(0, last_step + 1, tick, 0)

    for u in range(UNITS - 2, UNITS):
        wait_fin(jnp.int32(u))
    for u in range(last_step + 1 - PART_RING, UNITS):
        wait_sums(jnp.int32(u))
    for b in range((last_step - FIN_CLOSE) // HEADS + 1, BATCHES):
        fin_arrive(jnp.int32(b)).wait_recv()


def attend_kernel(*refs):
    me = lax.axis_index('cp')
    chip, core = me // 2, me % 2
    barrier = pltpu.get_barrier_semaphore()
    for c in range(4):
        @pl.when(chip == c)
        def _(c=c):
            chip_program(c, core, barrier, *refs)


def attend(q5, g5, keys, values, positions, freq):
    any_spec = pl.BlockSpec(memory_space=pl.ANY)
    hbm_spec = pl.BlockSpec(memory_space=pltpu.HBM)
    head_shape = pltpu.VMEM((2,) + q5.shape, jnp.bfloat16)
    half_shape = pltpu.HBM((BATCHES,) + q5.shape[1:], jnp.bfloat16)
    head_buf = pltpu.VMEM((2, 2, PAIR, GROUP, DIM), jnp.bfloat16)
    dma = pltpu.SemaphoreType.DMA
    return pl.pallas_call(
        attend_kernel, name='attend',
        in_specs=[any_spec] * 6,
        out_specs=[any_spec] + [hbm_spec] * 4,
        out_shape=[head_shape,
                   pltpu.HBM((2 * BATCHES, HEADS, 2, PAIR, DIM), jnp.bfloat16),
                   pltpu.HBM((BATCHES, HEADS, 2, N_PAIRS * PAIR, DIM), jnp.bfloat16),
                   half_shape, half_shape],
        scratch_shapes=[
            head_buf, head_buf, head_buf, head_buf,
            pltpu.VMEM((2, 2, N_PAIRS * PAIR, DIM), jnp.bfloat16),
            pltpu.VMEM((BATCHES, 2, 2, PAIR, DIM), jnp.float32),
            pltpu.VMEM((2, 2, PAIR, DIM), jnp.float32),
            pltpu.VMEM((2 * BATCHES, PAIR), jnp.int32),
            pltpu.VMEM((1, DIM), jnp.float32),
            pltpu.VMEM((2, 2, 2, HEADS * PAIR, DIM), jnp.bfloat16),
            pltpu.VMEM((2, 2, HEADS, 2, PAIR, DIM), jnp.bfloat16),
            pltpu.VMEM((PART_RING, 2, N_PAIRS * PAIR, DIM), jnp.float32),
            pltpu.VMEM((INBOX_RING, N_INBOX, 2, PAIR, DIM), jnp.float32),
            pltpu.VMEM((2, 2, 2, PAIR, DIM), jnp.bfloat16),
            pltpu.VMEM((PAIR, PAIR), jnp.bfloat16),
            pltpu.VMEM((DIM, N_PAIRS * PAIR), jnp.bfloat16),
            pltpu.VMEM((DIM, N_PAIRS * PAIR), jnp.bfloat16),
            pltpu.VMEM((N_PAIRS * PAIR, 32 * GROUP), jnp.float32),
            pltpu.VMEM((N_PAIRS * PAIR, 32 * GROUP), jnp.float32),
            pltpu.VMEM((4 * PAIR, PIECE * GROUP), jnp.float32),
            dma((2, 2, 2)), dma((BATCHES, 2)), dma((BATCHES, 2)), dma((BATCHES, 2)), dma((2,)), dma((BATCHES,)),
            dma((BATCHES,)), dma((BATCHES,)), dma((BATCHES,)), dma((BATCHES,)),
            dma((FAST_UNITS, 4)), dma((UNITS, 7)), dma((UNITS, 7)), dma((N_OUTBOX, PART_RING)), dma((INBOX_RING, N_INBOX)),
            dma((6, 2)), dma((4, 2)), dma((2, BATCHES)), dma((2, 2)), dma((BATCHES,)),
            pltpu.SemaphoreType.REGULAR((N_OUTBOX,)),
        ],
        compiler_params=pltpu.CompilerParams(
            collective_id=0, has_side_effects=True, vmem_limit_bytes=32512 * 1024),
    )(*(pltpu.with_memory_space_constraint(x, pltpu.HBM) for x in (q5, g5, keys, values, positions, freq)))


def place_kernel(odq, gkv, o_out, dq_out, gk_out, gv_out, in_v, out_v, perm, sems, in_s, out_s):
    n_batch = gkv.shape[0]

    def batch_in(b):
        return pltpu.make_async_copy(gkv.at[b], in_v.at[b], in_s.at[b])

    def batch_out(b):
        return [pltpu.make_async_copy(out_v.at[b, i], dst.at[b], out_s.at[b, i]) for i, dst in enumerate((gk_out, gv_out))]

    def start_in(b, carry):
        batch_in(b).start()
        return carry

    lax.fori_loop(0, n_batch, start_in, 0)
    part = n_batch // 4
    large = [pltpu.make_async_copy(odq.at[k, pl.ds(i * part, part)], dst.at[pl.ds(i * part, part)], sems.at[k, i])
             for i in range(4) for k, dst in enumerate((o_out, dq_out))]
    for copy in large:
        copy.start()
    row, col = iota(perm.shape, 0), iota(perm.shape, 1)
    perm[...] = (row == (col % PAIR) * HEADS + col // PAIR).astype(jnp.float32).astype(jnp.bfloat16)

    def regroup(b, carry):
        batch_in(b).wait()
        for i in range(2):
            rows = in_v[b, :, i].reshape(HEADS * PAIR, DIM)
            out_v[b, i] = dot_nn(perm[...], rows).astype(jnp.bfloat16)
        for copy in batch_out(b):
            copy.start()
        return carry

    lax.fori_loop(0, n_batch, regroup, 0)

    def finish_out(b, carry):
        for copy in batch_out(b):
            copy.wait()
        return carry

    lax.fori_loop(0, n_batch, finish_out, 0)
    for copy in large:
        copy.wait()


def place(odq, gkv):
    any_spec = pl.BlockSpec(memory_space=pl.ANY)
    n_batch = gkv.shape[0]
    head_shape = pltpu.HBM(odq.shape[1:], jnp.bfloat16)
    row_shape = pltpu.HBM((n_batch, HEADS * PAIR, DIM), jnp.bfloat16)
    dma = pltpu.SemaphoreType.DMA
    return pl.pallas_call(
        place_kernel, name='place', in_specs=[any_spec] * 2, out_specs=[any_spec] * 4,
        out_shape=[head_shape, head_shape, row_shape, row_shape],
        scratch_shapes=[pltpu.VMEM(gkv.shape, jnp.bfloat16), pltpu.VMEM((n_batch, 2, HEADS * PAIR, DIM), jnp.bfloat16),
                        pltpu.VMEM((HEADS * PAIR, HEADS * PAIR), jnp.bfloat16),
                        dma((2, 4)), dma((n_batch,)), dma((n_batch, 2))],
        compiler_params=pltpu.CompilerParams(vmem_limit_bytes=12 * 1024 * 1024),
    )(odq, pltpu.with_memory_space_constraint(gkv, pltpu.HBM))


def solution(mesh):
    head_spec = P(None, 'cp', 'tp', None)
    pos_spec = P(None, 'cp')

    def local_step(query, keys, values, positions, grad_out):
        batch, length, n_heads, dim = query.shape
        split_shape = (batch, length, HEADS, GROUP, dim)
        row_shape = (batch, length * HEADS, dim)
        outs = attend(query.reshape(split_shape), grad_out.reshape(split_shape), keys.reshape(row_shape),
                      values.reshape(row_shape), positions, jnp.asarray(lane_freq(dim)))
        return tuple(out.reshape(like.shape) for out, like in zip(place(*outs[:2]), (query, query, keys, values)))

    return jax.shard_map(local_step, mesh=mesh,
                         in_specs=(head_spec, head_spec, head_spec, pos_spec, head_spec),
                         out_specs=(head_spec, head_spec, head_spec, head_spec), check_vma=False)
```

```python
import functools

import jax
import jax.numpy as jnp
import numpy as np
from jax import lax
from jax.experimental import pallas as pl
from jax.experimental.pallas import tpu as pltpu
from jax.sharding import PartitionSpec as P

ROPE_THETA = 1000000.0
LOG2E = 1.4426950408889634
DIM = 128
GROUP = 8
HEADS = 4
PIECE = 64
PAIR = 128
N_PAIRS = 8
BATCHES = 8
UNITS = BATCHES * HEADS
KEY_BLOCK = 512
STEP_LAGS = (1, 2, 2, 2)
MESH_ID = pl.DeviceIdType.MESH

X_STEP, Y_STEP = 1, 2
FIRST_HOP = [(0, 0, X_STEP), (0, 0, Y_STEP), (1, 1, X_STEP), (1, 1, Y_STEP), (2, 2, X_STEP), (2, 2, Y_STEP),
             (3, 3, X_STEP), (3, 3, Y_STEP), (4, 3, X_STEP), (4, 3, Y_STEP), (5, 2, Y_STEP), (5, 2, X_STEP),
             (6, 1, X_STEP)]
RELAY_HOP = [(0, 2, X_STEP), (1, 3, X_STEP), (2, 3, Y_STEP), (3, 2, Y_STEP), (4, 1, X_STEP), (5, 3, Y_STEP)]
SUM_LEAF = [(3, 0, Y_STEP), (4, 0, X_STEP), (2, 0, Y_STEP), (6, 0, X_STEP), (2, 1, Y_STEP), (5, 1, X_STEP),
            (0, 1, X_STEP), (3, 1, Y_STEP), (1, 2, Y_STEP), (4, 2, X_STEP), (0, 3, X_STEP), (1, 3, Y_STEP)]
SUM_RELAY = [(0, 2, Y_STEP), (1, 0, X_STEP), (2, 3, X_STEP), (3, 2, X_STEP), (4, 1, Y_STEP), (5, 0, Y_STEP)]

START_BATCHES = 6
START_UNITS = 8
START_RELAYS = 4
RELAY_LEAD = 6
HOP_LEADS = (8, 7, 8, 8)
START_EARLY = HEADS * START_BATCHES
FAST_UNITS = HEADS
EARLY_HOP = [(0, 0, X_STEP), (0, 0, Y_STEP), (1, 1, Y_STEP)]
SUM_LAG = 4
OWN_LAG = 8
PART_RING = OWN_LAG + 2
FIN_CLOSE = OWN_LAG + HEADS + 2
INBOX_RING = 9


def owner(pair):
    return pair if pair < 4 else 7 - pair


def inbox(chip):
    found = []
    for pair, src, step in SUM_LEAF + SUM_RELAY:
        if src ^ step == chip:
            found.append((pair, src))
    return found


def outbox(chip):
    return [(pair, step) for pair, src, step in SUM_LEAF + SUM_RELAY if src == chip]


N_INBOX = max(len(inbox(c)) for c in range(4))
N_OUTBOX = max(len(outbox(c)) for c in range(4))


def lane_freq(head_dim):
    exponent = np.arange(head_dim // 2, dtype=np.float64) * (2.0 / head_dim)
    return np.repeat(ROPE_THETA ** -exponent, 2).astype(np.float32)[None, :]


def dot_nn(a, b):
    return jnp.dot(a, b, preferred_element_type=jnp.float32)


def dot_nt(a, b):
    return lax.dot_general(a, b, (((1,), (1,)), ((), ())), preferred_element_type=jnp.float32)


def iota(shape, axis):
    return lax.broadcasted_iota(jnp.int32, shape, axis)


def identity():
    return (iota((DIM, DIM), 0) == iota((DIM, DIM), 1)).astype(jnp.float32).astype(jnp.bfloat16)


def swap_pairs(x):
    return jnp.where(iota(x.shape, 1) % 2 == 0, pltpu.roll(x, DIM - 1, axis=1), pltpu.roll(x, 1, axis=1))


def rows_steps(n_keys, tok, seg, q_v, g_v, tab, kv, kt, vt, part, o_v, dq_v, s_ref):
    core, start, place = seg
    rows = tok * GROUP
    scale = DIM ** -0.5
    c1 = scale * LOG2E
    toks = pl.ds(start, tok)

    def table(k):
        return jnp.broadcast_to(tab[k, core, toks, :][:, None, :], (tok, GROUP, DIM)).reshape(rows, DIM)

    x = q_v[core, toks].astype(jnp.float32).reshape(rows, DIM)
    qr = (x * table(0) + swap_pairs(x) * table(1)).astype(jnp.bfloat16)
    g = g_v[core, toks].astype(jnp.float32).reshape(rows, DIM).astype(jnp.bfloat16)
    blocks = [(a, min(KEY_BLOCK, n_keys - a)) for a in range(0, n_keys, KEY_BLOCK)]
    m8 = None
    for a, n in blocks:
        s = dot_nt(kv[0, a:a + n, :], qr) * c1
        if a + n == n_keys:
            last = s[n - PAIR:, :]
            q_tok = iota(last.shape, 1) // GROUP + place
            last = jnp.where(iota(last.shape, 0) <= q_tok, last, -jnp.inf)
            s = last if n == PAIR else jnp.concatenate([s[:n - PAIR, :], last], axis=0)
        s_ref[a:a + n, :] = s
        f = jnp.max(s.reshape(n // 8, 8, rows), axis=0)
        m8 = f if m8 is None else jnp.maximum(m8, f)
        yield
    row_max = jnp.max(m8, axis=0, keepdims=True)
    l8 = None
    o_t = None
    for a, n in blocks:
        p = jnp.exp2(s_ref[a:a + n, :] - row_max)
        s_ref[a:a + n, :] = p
        f = jnp.sum(p.reshape(n // 8, 8, rows), axis=0)
        l8 = f if l8 is None else l8 + f
        d = dot_nn(vt[:, a:a + n], p.astype(jnp.bfloat16))
        o_t = d if o_t is None else o_t + d
        yield
    inv = 1.0 / jnp.sum(l8, axis=0, keepdims=True)
    out_t = o_t * inv
    o_v[core, toks] = jnp.transpose(out_t).reshape(tok, GROUP, DIM).astype(jnp.bfloat16)
    delta = jnp.sum(dot_nt(identity(), g) * out_t, axis=0, keepdims=True)
    yield
    dq_t = None
    for a, n in blocks:
        p = s_ref[a:a + n, :] * inv
        ds = (p * (dot_nt(kv[1, a:a + n, :], g) - delta)).astype(jnp.bfloat16)
        part[1, a:a + n, :] += dot_nn(p.astype(jnp.bfloat16), g)
        part[0, a:a + n, :] += dot_nn(ds, qr)
        d = dot_nn(kt[:, a:a + n], ds)
        dq_t = d if dq_t is None else dq_t + d
        yield
    dq = jnp.transpose(dq_t) * scale
    dq = dq * table(0) - swap_pairs(dq) * table(1)
    dq_v[core, toks] = dq.reshape(tok, GROUP, DIM).astype(jnp.bfloat16)


def interleave(gens, lag):
    live, waiting, count = [], list(gens), 0
    while live or waiting:
        if waiting and (not live or count >= lag):
            live.append(waiting.pop(0))
            count = 0
        for gen in list(live):
            if next(gen, 'end') == 'end':
                live.remove(gen)
        count += 1


def unit_compute(c, q_v, g_v, tab, kv, o_v, dq_v, part, kt, vt, s_a, s_b, s_e):
    n_late, n_early = (N_PAIRS - c) * PAIR, (c + 1) * PAIR
    eye = identity()
    for a in range(0, n_late, 256):
        n = min(256, n_late - a)
        kt[:, a:a + n] = dot_nt(eye, kv[0, a:a + n, :]).astype(jnp.bfloat16)
        vt[:, a:a + n] = dot_nt(eye, kv[1, a:a + n, :]).astype(jnp.bfloat16)
    part[:, :n_late, :] = jnp.zeros((2, n_late, DIM), jnp.float32)
    refs = (q_v, g_v, tab, kv, kt, vt, part, o_v, dq_v)

    def step(i, carry):
        late = [rows_steps(n_late, 32, (1 - i, PIECE + 32 * k, i * PIECE + 32 * k), *refs, s)
                for k, s in ((0, s_a), (1, s_b))]
        early = rows_steps(n_early, PIECE, (i, 0, i * PIECE), *refs, s_e)
        interleave(late + [early], STEP_LAGS[c])
        return carry

    lax.fori_loop(0, 2, step, 0)


def remote(src, dst, send_sem, recv_sem, device):
    return pltpu.make_async_remote_copy(src_ref=src, dst_ref=dst, send_sem=send_sem, recv_sem=recv_sem,
                                        device_id={'cp': device}, device_id_type=MESH_ID)


def chip_program(c, core, barrier, q_hbm, g_hbm, k_hbm, v_hbm, pos_hbm, freq_hbm, odq_hbm, gkv_hbm, kv_hbm, qs_hbm, gs_hbm,
                 q_v, g_v, o_v, dq_v, kv_v, tab_v, tab_x, pos_v, freq_v, raw_v, ready_v, part, recv, fin_v,
                 perm_in, kt, vt, s_a, s_b, s_e,
                 raw_s, kvl_s, kvx_s, kvx_r, tab_s, tab_r, qx_s, qx_r, gx_s, gx_r, fast_s, ag_s, ag_r, sum_s, sum_r,
                 load_s, out_s, out_r, fin_s, fin_r, credit):
    o_hbm, dq_hbm = odq_hbm.at[0], odq_hbm.at[1]
    n_late = (N_PAIRS - c) * PAIR
    sib = 2 * c + 1 - core
    nbr = {step: 2 * (c ^ step) + core for step in (X_STEP, Y_STEP)}
    mine, other = BATCHES * core, BATCHES * (1 - core)
    early_hops = [(p, step) for p, src, step in EARLY_HOP if src == c]
    first_hops = [(p, step) for p, src, step in FIRST_HOP if src == c and (p, src, step) not in EARLY_HOP]
    relay_hops = [(p, step) for p, src, step in RELAY_HOP if src == c]
    leaves = [(p, step) for p, src, step in SUM_LEAF if src == c]
    relays = [(p, step) for p, src, step in SUM_RELAY if src == c]
    needed = [p for p in range(N_PAIRS - c) if owner(p) != c]
    sib_pieces = (2 * c + 1 - core, 15 - 2 * c - (1 - core))

    def split(u):
        return u // HEADS, u % HEADS

    def pair_rows(p):
        return pl.ds(p * PAIR, PAIR)

    own_pieces = (2 * c + core, 15 - 2 * c - core)

    def raw_in(b, side):
        src, slot = (mine, other)[side] + b, b % 2
        return [pltpu.make_async_copy(k_hbm.at[src], raw_v.at[slot, side, 0], raw_s.at[slot, side, 0]),
                pltpu.make_async_copy(v_hbm.at[src], raw_v.at[slot, side, 1], raw_s.at[slot, side, 1])]

    def start_raw(b):
        for side in (0, 1):
            for copy in raw_in(b, side):
                copy.start()

    def piece_rows(piece):
        return pl.ds(pl.multiple_of(piece * PIECE, PIECE), PIECE)

    def own_out(b, half):
        return pltpu.make_async_copy(ready_v.at[b % 2, 0, :, :, pl.ds(half * PIECE, PIECE), :],
                                     kv_hbm.at[b, :, :, piece_rows(own_pieces[half]), :], kvl_s.at[b, half])

    def kvx(b, half):
        return remote(ready_v.at[b % 2, 1, :, :, pl.ds(half * PIECE, PIECE), :],
                      kv_hbm.at[b, :, :, piece_rows(own_pieces[half]), :], kvx_s.at[b, half], kvx_r.at[b, half], sib)

    def kvx_in(b, half):
        dst = kv_hbm.at[b, :, :, piece_rows(sib_pieces[half]), :]
        return remote(dst, dst, kvx_s.at[b, half], kvx_r.at[b, half], sib)

    def make_table(tab, row):
        pos = pos_v[pl.ds(row, 1), :].astype(jnp.float32)
        angles = jnp.transpose(jnp.broadcast_to(pos, (PAIR, PAIR))) * freq_v[...]
        tab[0] = jnp.cos(angles)
        sine_val = jnp.sin(angles)
        tab[1] = jnp.where(iota(sine_val.shape, 1) % 2 == 0, -sine_val, sine_val)

    def make_ready(b, at_start=False):
        slot, part_rows = b % 2, PAIR // HEADS

        @pl.when(b >= 2)
        def _():
            for half in range(2):
                kvx(b - 2, half).wait_send()
            tab_out(b - 2).wait_send()

        if at_start:
            @pl.when(b == 2)
            def _():
                up_to(lambda u: close_fast(u, True), 0, FAST_UNITS)

            @pl.when(b == 5)
            def _():
                up_to(lambda u: close_fast(u, False), 0, FAST_UNITS)

        for side in (0, 1):
            tab = tab_x.at[slot] if side else tab_v.at[b, :, core]
            make_table(tab, (mine, other)[side] + b)
            for copy in raw_in(b, side):
                copy.wait()
            for i in range(2):
                blocks = [dot_nn(perm_in[...], raw_v[slot, side, i, j * PAIR:(j + 1) * PAIR]) for j in range(HEADS)]
                for h in range(HEADS):
                    x = jnp.concatenate([block[h * part_rows:(h + 1) * part_rows] for block in blocks], axis=0)
                    if i == 0:
                        x = x * tab[0] + swap_pairs(x) * tab[1]
                    ready_v[slot, side, h, i] = x.astype(jnp.bfloat16)
            if side == 0:
                for half in range(2):
                    own_out(b, half).start()
                if at_start:
                    @pl.when(b == 0)
                    def _():
                        pl.semaphore_wait(barrier, 3)
                        up_to(lambda u: fast_hop(u, True), 0, FAST_UNITS)

        @pl.when(b + 2 < BATCHES)
        def _():
            start_raw(b + 2)

    def send_ready(b):
        for half in range(2):
            kvx(b, half).start()
        tab_out(b).start()

    def qx(b):
        return remote(q_hbm.at[other + b], qs_hbm.at[b], qx_s.at[b], qx_r.at[b], sib)

    def gx(b):
        return remote(g_hbm.at[other + b], gs_hbm.at[b], gx_s.at[b], gx_r.at[b], sib)

    def tab_out(b):
        return remote(tab_x.at[b % 2], tab_v.at[b, :, core], tab_s.at[b % 2], tab_r.at[b], sib)

    def tab_arrive(b):
        dst = tab_v.at[b, :, 1 - core]
        return remote(dst, dst, tab_s.at[0], tab_r.at[b], sib)

    def small_in():
        return [pltpu.make_async_copy(pos_hbm, pos_v, load_s.at[5, 0]),
                pltpu.make_async_copy(freq_hbm, freq_v, load_s.at[5, 1])]

    def kv_copy(u, p, slot, step):
        b, h = split(u)
        ref = kv_hbm.at[b, h, :, pair_rows(p), :]
        return remote(ref, ref, ag_s.at[u, slot], ag_r.at[u, p], nbr[step])

    def send_kv(u, hops, base):
        for i, (p, step) in enumerate(hops):
            kv_copy(u, p, base + i, step).start()

    def have_own(b):
        for half in range(2):
            own_out(b, half).wait()
            kvx_in(b, half).wait_recv()

    def half_copy(u, p, slot, step, own):
        b, h = split(u)
        half = 0 if p == c else 1
        dst = kv_hbm.at[b, h, :, piece_rows((own_pieces if own else sib_pieces)[half]), :]
        src = ready_v.at[b % 2, 0, h, :, pl.ds(half * PIECE, PIECE), :] if own else dst
        return remote(src, dst, (fast_s if own else ag_s).at[u, slot], ag_r.at[u, p], nbr[step])

    def fast_hop(u, own):
        for i, (p, step) in enumerate(early_hops + first_hops):
            half_copy(u, p, i, step, own).start()

    def close_fast(u, own):
        for i, (p, step) in enumerate(early_hops + first_hops):
            half_copy(u, p, i, step, own).wait_send()

    def early_hop(u):
        send_kv(u, early_hops, 0)

    def first_hop(u):
        send_kv(u, first_hops, len(early_hops))

    def relay_hop(u):
        for p, _ in relay_hops:
            kv_copy(u, p, 0, X_STEP).wait_recv()
        send_kv(u, relay_hops, len(early_hops) + len(first_hops))

    def loads(u):
        b, h = split(u)
        slot = u % 2
        late = pl.ds(0, n_late)
        return [
            pltpu.make_async_copy(q_hbm.at[mine + b, :, h], q_v.at[slot, core], load_s.at[0, slot]),
            pltpu.make_async_copy(g_hbm.at[mine + b, :, h], g_v.at[slot, core], load_s.at[1, slot]),
            pltpu.make_async_copy(qs_hbm.at[b, :, h], q_v.at[slot, 1 - core], load_s.at[2, slot]),
            pltpu.make_async_copy(gs_hbm.at[b, :, h], g_v.at[slot, 1 - core], load_s.at[3, slot]),
            pltpu.make_async_copy(kv_hbm.at[b, h, :, late, :], kv_v.at[slot, :, late, :], load_s.at[4, slot]),
        ]

    def start_loads(u):
        @pl.when(u % HEADS == 0)
        def _():
            qx(u // HEADS).wait_recv()
            gx(u // HEADS).wait_recv()
            tab_arrive(u // HEADS).wait_recv()

        for p in needed:
            if p not in [r for r, _ in relay_hops]:
                kv_copy(u, p, 0, X_STEP).wait_recv()
        for copy in loads(u):
            copy.start()

    def out_local(u):
        b, h = split(u)
        slot = u % 2
        return [pltpu.make_async_copy(o_v.at[slot, core], o_hbm.at[mine + b, :, h], out_s.at[0, slot]),
                pltpu.make_async_copy(dq_v.at[slot, core], dq_hbm.at[mine + b, :, h], out_s.at[1, slot])]

    def out_remote(u):
        b, h = split(u)
        slot = u % 2
        return [remote(o_v.at[slot, 1 - core], o_hbm.at[mine + b, :, h], out_s.at[2, slot], out_r.at[0, b], sib),
                remote(dq_v.at[slot, 1 - core], dq_hbm.at[mine + b, :, h], out_s.at[3, slot], out_r.at[1, b], sib)]

    def out_arrive(b):
        return [remote(q_hbm.at[other + b], o_hbm.at[other + b], out_s.at[2, 0], out_r.at[0, b], sib),
                remote(q_hbm.at[other + b], dq_hbm.at[other + b], out_s.at[3, 0], out_r.at[1, b], sib)]

    def wait_outs(u):
        for copy in out_local(u):
            copy.wait()
        for copy in out_remote(u):
            copy.wait_send()

    def sum_copy(u, p, i, step):
        k, slot = inbox(c ^ step).index((p, c)), u % INBOX_RING
        return remote(part.at[u % PART_RING, :, pair_rows(p), :], recv.at[slot, k],
                      sum_s.at[i, u % PART_RING], sum_r.at[slot, k], nbr[step])

    def sum_arrive(u, k):
        dst = recv.at[u % INBOX_RING, k]
        return remote(dst, dst, sum_s.at[0, 0], sum_r.at[u % INBOX_RING, k], nbr[X_STEP])

    def give_credits(u, pairs):
        @pl.when(u + INBOX_RING < UNITS)
        def _():
            for k, (pair, src) in enumerate(inbox(c)):
                if pair in pairs:
                    pl.semaphore_signal(credit.at[outbox(src).index((pair, src ^ c))], inc=1,
                                        device_id={'cp': 2 * src + core}, device_id_type=MESH_ID)

    def take_credits(u, which):
        @pl.when(u >= INBOX_RING)
        def _():
            for i in which:
                pl.semaphore_wait(credit.at[i], 1)

    def messages(p):
        return [k for k, (pair, _) in enumerate(inbox(c)) if pair == p]

    def wait_sums(u):
        for i, (p, step) in enumerate(leaves + relays):
            sum_copy(u, p, i, step).wait_send()

    def send_leaves(u):
        take_credits(u, range(len(leaves)))
        for i, (p, step) in enumerate(leaves):
            sum_copy(u, p, i, step).start()

    def add_relays(u):
        for p, _ in relays:
            for k in messages(p):
                sum_arrive(u, k).wait_recv()
                part[u % PART_RING, :, pair_rows(p), :] += recv[u % INBOX_RING, k]
        give_credits(u, [p for p, _ in relays])

    def send_relays(u):
        take_credits(u, range(len(leaves), len(leaves) + len(relays)))
        for i, (p, step) in enumerate(relays):
            sum_copy(u, p, len(leaves) + i, step).start()

    def fin_local(u):
        b, h = split(u)
        return pltpu.make_async_copy(fin_v.at[u % 2, core], gkv_hbm.at[mine + b, h], fin_s.at[0, u % 2])

    def fin_remote(u):
        b, h = split(u)
        return remote(fin_v.at[u % 2, 1 - core], gkv_hbm.at[mine + b, h], fin_s.at[1, u % 2], fin_r.at[b], sib)

    def fin_arrive(b):
        dst = gkv_hbm.at[other + b]
        return remote(dst, dst, fin_s.at[1, 0], fin_r.at[b], sib)

    def wait_fin(u):
        fin_local(u).wait()
        fin_remote(u).wait_send()

    def finish(u):
        @pl.when(u >= 2)
        def _():
            wait_fin(u - 2)

        b, slot = u // HEADS, u % 2
        for late, p in ((0, c), (1, N_PAIRS - 1 - c)):
            total = part[u % PART_RING, :, pair_rows(p), :]
            for k in messages(p):
                sum_arrive(u, k).wait_recv()
                total = total + recv[u % INBOX_RING, k]
            for i in range(2):
                who = 1 - i if late else i
                toks = slice(late * PIECE, (late + 1) * PIECE)
                dk = total[0, i * PIECE:(i + 1) * PIECE] * (DIM ** -0.5)
                dk = dk * tab_v[b, 0, who, toks] - swap_pairs(dk) * tab_v[b, 1, who, toks]
                fin_v[slot, who, 0, toks] = dk.astype(jnp.bfloat16)
                fin_v[slot, who, 1, toks] = total[1, i * PIECE:(i + 1) * PIECE].astype(jnp.bfloat16)
        give_credits(u, [c, N_PAIRS - 1 - c])

    def send_fin(u):
        fin_local(u).start()
        fin_remote(u).start()

    last_step = UNITS + OWN_LAG

    def close_copies(t):
        batch = t // HEADS

        @pl.when((t >= FAST_UNITS) & (t < UNITS))
        def _():
            for i, (p, step) in enumerate(early_hops + first_hops):
                kv_copy(t, p, i, step).wait_send()

        @pl.when(t < UNITS)
        def _():
            for i, (p, step) in enumerate(relay_hops):
                kv_copy(t, p, len(early_hops + first_hops) + i, step).wait_send()

        @pl.when((t % HEADS == HEADS - 1) & (t < UNITS))
        def _():
            qx(batch).wait_send()
            gx(batch).wait_send()

        @pl.when((t % HEADS == 0) & (t >= 2 * HEADS) & (batch - 2 < BATCHES))
        def _():
            for copy in out_arrive(batch - 2):
                copy.wait_recv()

        @pl.when((t % HEADS == FIN_CLOSE % HEADS) & (t >= FIN_CLOSE))
        def _():
            fin_arrive((t - FIN_CLOSE) // HEADS).wait_recv()

        @pl.when(t >= UNITS)
        def _():
            wait_sums(t - PART_RING)

        @pl.when((t >= UNITS) & (t < UNITS + 2))
        def _():
            wait_outs(t - 2)

        @pl.when(t == 3 * HEADS)
        def _():
            for b in range(BATCHES - 2, BATCHES):
                for half in range(2):
                    kvx(jnp.int32(b), half).wait_send()
                tab_out(jnp.int32(b)).wait_send()

    def exchange_queries(b):
        qx(b).start()
        gx(b).start()

    for copy in small_in():
        copy.start()
    start_raw(jnp.int32(0))
    for device in (sib, nbr[X_STEP], nbr[Y_STEP]):
        pl.semaphore_signal(barrier, inc=1, device_id={'cp': device}, device_id_type=MESH_ID)
    start_raw(jnp.int32(1))
    row, col = iota(perm_in.shape, 0), iota(perm_in.shape, 1)
    part_rows = PAIR // HEADS
    perm_in[...] = (col == (row % part_rows) * HEADS + row // part_rows).astype(jnp.float32).astype(jnp.bfloat16)
    for copy in small_in():
        copy.wait()

    def up_to(op, first, last):
        def one(u, carry):
            op(u)
            return carry

        lax.fori_loop(first, last, one, 0)

    def start_step(j, carry):
        make_ready(j, at_start=True)
        send_ready(j)

        @pl.when(j == 0)
        def _():
            have_own(j)
            up_to(lambda u: fast_hop(u, False), 0, FAST_UNITS)
            exchange_queries(j)

        up_to(relay_hop, jnp.where(j < START_RELAYS, jnp.maximum(j - 1, 0), START_RELAYS),
              jnp.minimum(j + j // 3, START_RELAYS))
        up_to(first_hop, jnp.clip(2 * j, FAST_UNITS, START_UNITS), jnp.clip(2 * j + 2, FAST_UNITS, START_UNITS))

        @pl.when(j >= 1)
        def _():
            have_own(j)

        up_to(early_hop, jnp.maximum(HEADS * j, FAST_UNITS), HEADS * j + HEADS)
        return carry

    lax.fori_loop(0, START_BATCHES, start_step, 0)
    start_loads(jnp.int32(0))

    def tick(t, carry):
        @pl.when((t % 2 == 0) & (t // 2 + START_BATCHES < BATCHES))
        def _():
            make_ready(t // 2 + START_BATCHES)
            send_ready(t // 2 + START_BATCHES)

        @pl.when((t % 2 == 1) & (t // 2 + START_BATCHES < BATCHES))
        def _():
            have_own(t // 2 + START_BATCHES)

        @pl.when((t % HEADS == 0) & (t // HEADS + 1 < BATCHES))
        def _():
            exchange_queries(t // HEADS + 1)

        @pl.when((t >= 1) & (2 * t - 2 + START_EARLY < UNITS))
        def _():
            early_hop(2 * t - 2 + START_EARLY)
            early_hop(2 * t - 1 + START_EARLY)

        @pl.when(t == 0)
        def _():
            for u in range(START_RELAYS, RELAY_LEAD - 1):
                relay_hop(jnp.int32(u))

        @pl.when(t + RELAY_LEAD - 1 < UNITS)
        def _():
            relay_hop(t + RELAY_LEAD - 1)

        @pl.when((t >= 1) & (t - 1 < UNITS))
        def _():
            send_leaves(t - 1)

        @pl.when((t >= 1 + OWN_LAG) & (t - 1 - OWN_LAG < UNITS))
        def _():
            finish(t - 1 - OWN_LAG)

        @pl.when((t >= 1 + SUM_LAG) & (t - 1 - SUM_LAG < UNITS))
        def _():
            add_relays(t - 1 - SUM_LAG)

        @pl.when((t >= 1 + OWN_LAG) & (t - 1 - OWN_LAG < UNITS))
        def _():
            send_fin(t - 1 - OWN_LAG)

        @pl.when((t >= 1 + SUM_LAG) & (t - 1 - SUM_LAG < UNITS))
        def _():
            send_relays(t - 1 - SUM_LAG)

        hop_lead = HOP_LEADS[c]

        @pl.when((t == 0) | ((t + hop_lead > START_UNITS) & (t + hop_lead < UNITS)))
        def _():
            first_hop(jnp.maximum(t + hop_lead, START_UNITS))

        @pl.when(t < UNITS)
        def _():
            for copy in loads(t):
                copy.wait()

            @pl.when(t + 1 < UNITS)
            def _():
                start_loads(t + 1)

            @pl.when(t >= 2)
            def _():
                wait_outs(t - 2)

            @pl.when(t >= PART_RING)
            def _():
                wait_sums(t - PART_RING)

            slot = t % 2
            unit_compute(c, q_v.at[slot], g_v.at[slot], tab_v.at[t // HEADS], kv_v.at[slot], o_v.at[slot],
                         dq_v.at[slot], part.at[t % PART_RING], kt, vt, s_a, s_b, s_e)
            for copy in out_local(t) + out_remote(t):
                copy.start()

        close_copies(t)
        return carry

    lax.fori_loop(0, last_step + 1, tick, 0)

    for u in range(UNITS - 2, UNITS):
        wait_fin(jnp.int32(u))
    for u in range(last_step + 1 - PART_RING, UNITS):
        wait_sums(jnp.int32(u))
    for b in range((last_step - FIN_CLOSE) // HEADS + 1, BATCHES):
        fin_arrive(jnp.int32(b)).wait_recv()


def attend_kernel(*refs):
    me = lax.axis_index('cp')
    chip, core = me // 2, me % 2
    barrier = pltpu.get_barrier_semaphore()
    for c in range(4):
        @pl.when(chip == c)
        def _(c=c):
            chip_program(c, core, barrier, *refs)


def attend(q5, g5, keys, values, positions, freq):
    any_spec = pl.BlockSpec(memory_space=pl.ANY)
    hbm_spec = pl.BlockSpec(memory_space=pltpu.HBM)
    head_shape = pltpu.VMEM((2,) + q5.shape, jnp.bfloat16)
    half_shape = pltpu.HBM((BATCHES,) + q5.shape[1:], jnp.bfloat16)
    head_buf = pltpu.VMEM((2, 2, PAIR, GROUP, DIM), jnp.bfloat16)
    dma = pltpu.SemaphoreType.DMA
    return pl.pallas_call(
        attend_kernel, name='attend',
        in_specs=[any_spec] * 6,
        out_specs=[any_spec] + [hbm_spec] * 4,
        out_shape=[head_shape,
                   pltpu.HBM((2 * BATCHES, HEADS, 2, PAIR, DIM), jnp.bfloat16),
                   pltpu.HBM((BATCHES, HEADS, 2, N_PAIRS * PAIR, DIM), jnp.bfloat16),
                   half_shape, half_shape],
        scratch_shapes=[
            head_buf, head_buf, head_buf, head_buf,
            pltpu.VMEM((2, 2, N_PAIRS * PAIR, DIM), jnp.bfloat16),
            pltpu.VMEM((BATCHES, 2, 2, PAIR, DIM), jnp.float32),
            pltpu.VMEM((2, 2, PAIR, DIM), jnp.float32),
            pltpu.VMEM((2 * BATCHES, PAIR), jnp.int32),
            pltpu.VMEM((1, DIM), jnp.float32),
            pltpu.VMEM((2, 2, 2, HEADS * PAIR, DIM), jnp.bfloat16),
            pltpu.VMEM((2, 2, HEADS, 2, PAIR, DIM), jnp.bfloat16),
            pltpu.VMEM((PART_RING, 2, N_PAIRS * PAIR, DIM), jnp.float32),
            pltpu.VMEM((INBOX_RING, N_INBOX, 2, PAIR, DIM), jnp.float32),
            pltpu.VMEM((2, 2, 2, PAIR, DIM), jnp.bfloat16),
            pltpu.VMEM((PAIR, PAIR), jnp.bfloat16),
            pltpu.VMEM((DIM, N_PAIRS * PAIR), jnp.bfloat16),
            pltpu.VMEM((DIM, N_PAIRS * PAIR), jnp.bfloat16),
            pltpu.VMEM((N_PAIRS * PAIR, 32 * GROUP), jnp.float32),
            pltpu.VMEM((N_PAIRS * PAIR, 32 * GROUP), jnp.float32),
            pltpu.VMEM((4 * PAIR, PIECE * GROUP), jnp.float32),
            dma((2, 2, 2)), dma((BATCHES, 2)), dma((BATCHES, 2)), dma((BATCHES, 2)), dma((2,)), dma((BATCHES,)),
            dma((BATCHES,)), dma((BATCHES,)), dma((BATCHES,)), dma((BATCHES,)),
            dma((FAST_UNITS, 4)), dma((UNITS, 7)), dma((UNITS, 7)), dma((N_OUTBOX, PART_RING)), dma((INBOX_RING, N_INBOX)),
            dma((6, 2)), dma((4, 2)), dma((2, BATCHES)), dma((2, 2)), dma((BATCHES,)),
            pltpu.SemaphoreType.REGULAR((N_OUTBOX,)),
        ],
        compiler_params=pltpu.CompilerParams(
            collective_id=0, has_side_effects=True, vmem_limit_bytes=32512 * 1024),
    )(*(pltpu.with_memory_space_constraint(x, pltpu.HBM) for x in (q5, g5, keys, values, positions, freq)))


def place_kernel(odq, gkv, o_out, dq_out, gk_out, gv_out, in_v, out_v, perm, sems, in_s, out_s):
    n_batch = gkv.shape[0]

    def batch_in(b):
        return pltpu.make_async_copy(gkv.at[b], in_v.at[b], in_s.at[b])

    def batch_out(b):
        return [pltpu.make_async_copy(out_v.at[b, i], dst.at[b], out_s.at[b, i]) for i, dst in enumerate((gk_out, gv_out))]

    def start_in(b, carry):
        batch_in(b).start()
        return carry

    lax.fori_loop(0, n_batch, start_in, 0)
    part = n_batch // 4
    large = [pltpu.make_async_copy(odq.at[k, pl.ds(i * part, part)], dst.at[pl.ds(i * part, part)], sems.at[k, i])
             for i in range(4) for k, dst in enumerate((o_out, dq_out))]
    for copy in large:
        copy.start()
    row, col = iota(perm.shape, 0), iota(perm.shape, 1)
    size = PAIR // HEADS
    perm[...] = (row == (col % size) * HEADS + col // size).astype(jnp.float32).astype(jnp.bfloat16)

    def regroup(b, carry):
        batch_in(b).wait()
        for i in range(2):
            for j in range(HEADS):
                rows = jnp.concatenate([in_v[b, h, i, j * size:(j + 1) * size] for h in range(HEADS)], axis=0)
                out_v[b, i, j * PAIR:(j + 1) * PAIR] = dot_nn(perm[...], rows).astype(jnp.bfloat16)
        for copy in batch_out(b):
            copy.start()
        return carry

    lax.fori_loop(0, n_batch, regroup, 0)

    def finish_out(b, carry):
        for copy in batch_out(b):
            copy.wait()
        return carry

    lax.fori_loop(0, n_batch, finish_out, 0)
    for copy in large:
        copy.wait()


def place(odq, gkv):
    any_spec = pl.BlockSpec(memory_space=pl.ANY)
    n_batch = gkv.shape[0]
    head_shape = pltpu.HBM(odq.shape[1:], jnp.bfloat16)
    row_shape = pltpu.HBM((n_batch, HEADS * PAIR, DIM), jnp.bfloat16)
    dma = pltpu.SemaphoreType.DMA
    return pl.pallas_call(
        place_kernel, name='place', in_specs=[any_spec] * 2, out_specs=[any_spec] * 4,
        out_shape=[head_shape, head_shape, row_shape, row_shape],
        scratch_shapes=[pltpu.VMEM(gkv.shape, jnp.bfloat16), pltpu.VMEM((n_batch, 2, HEADS * PAIR, DIM), jnp.bfloat16),
                        pltpu.VMEM((PAIR, PAIR), jnp.bfloat16),
                        dma((2, 4)), dma((n_batch,)), dma((n_batch, 2))],
        compiler_params=pltpu.CompilerParams(vmem_limit_bytes=12 * 1024 * 1024),
    )(odq, pltpu.with_memory_space_constraint(gkv, pltpu.HBM))


def solution(mesh):
    head_spec = P(None, 'cp', 'tp', None)
    pos_spec = P(None, 'cp')

    def local_step(query, keys, values, positions, grad_out):
        batch, length, n_heads, dim = query.shape
        split_shape = (batch, length, HEADS, GROUP, dim)
        row_shape = (batch, length * HEADS, dim)
        outs = attend(query.reshape(split_shape), grad_out.reshape(split_shape), keys.reshape(row_shape),
                      values.reshape(row_shape), positions, jnp.asarray(lane_freq(dim)))
        return tuple(out.reshape(like.shape) for out, like in zip(place(*outs[:2]), (query, query, keys, values)))

    return jax.shard_map(local_step, mesh=mesh,
                         in_specs=(head_spec, head_spec, head_spec, pos_spec, head_spec),
                         out_specs=(head_spec, head_spec, head_spec, head_spec), check_vma=False)
```

```python
import functools

import jax
import jax.numpy as jnp
import numpy as np
from jax import lax
from jax.experimental import pallas as pl
from jax.experimental.pallas import tpu as pltpu
from jax.sharding import PartitionSpec as P

ROPE_THETA = 1000000.0
LOG2E = 1.4426950408889634
DIM = 128
GROUP = 8
HEADS = 4
PIECE = 64
PAIR = 128
N_PAIRS = 8
BATCHES = 8
UNITS = BATCHES * HEADS
KEY_BLOCK = 512
STEP_LAG = 2
MESH_ID = pl.DeviceIdType.MESH

X_STEP, Y_STEP = 1, 2
FIRST_HOP = [(0, 0, X_STEP), (0, 0, Y_STEP), (1, 1, X_STEP), (1, 1, Y_STEP), (2, 2, X_STEP), (2, 2, Y_STEP),
             (3, 3, X_STEP), (3, 3, Y_STEP), (4, 3, X_STEP), (4, 3, Y_STEP), (5, 2, Y_STEP), (5, 2, X_STEP),
             (6, 1, X_STEP)]
RELAY_HOP = [(0, 2, X_STEP), (1, 3, X_STEP), (2, 3, Y_STEP), (3, 2, Y_STEP), (4, 1, X_STEP), (5, 3, Y_STEP)]
SUM_LEAF = [(3, 0, Y_STEP), (4, 0, X_STEP), (2, 0, Y_STEP), (6, 0, X_STEP), (2, 1, Y_STEP), (5, 1, X_STEP),
            (0, 1, X_STEP), (3, 1, Y_STEP), (1, 2, Y_STEP), (4, 2, X_STEP), (0, 3, X_STEP), (1, 3, Y_STEP)]
SUM_RELAY = [(0, 2, Y_STEP), (1, 0, X_STEP), (2, 3, X_STEP), (3, 2, X_STEP), (4, 1, Y_STEP), (5, 0, Y_STEP)]

START_BATCHES = 6
START_UNITS = 8
START_RELAYS = 4
RELAY_LEAD = 6
HOP_LEADS = (8, 7, 8, 8)
START_EARLY = HEADS * START_BATCHES
FAST_UNITS = HEADS
EARLY_HOP = [(0, 0, X_STEP), (0, 0, Y_STEP), (1, 1, Y_STEP)]
SUM_LAG = 4
OWN_LAG = 8
PART_RING = OWN_LAG + 2
FIN_CLOSE = OWN_LAG + HEADS + 2
INBOX_RING = 9


def owner(pair):
    return pair if pair < 4 else 7 - pair


def inbox(chip):
    found = []
    for pair, src, step in SUM_LEAF + SUM_RELAY:
        if src ^ step == chip:
            found.append((pair, src))
    return found


def outbox(chip):
    return [(pair, step) for pair, src, step in SUM_LEAF + SUM_RELAY if src == chip]


N_INBOX = max(len(inbox(c)) for c in range(4))
N_OUTBOX = max(len(outbox(c)) for c in range(4))


def lane_freq(head_dim):
    exponent = np.arange(head_dim // 2, dtype=np.float64) * (2.0 / head_dim)
    return np.repeat(ROPE_THETA ** -exponent, 2).astype(np.float32)[None, :]


def dot_nn(a, b):
    return jnp.dot(a, b, preferred_element_type=jnp.float32)


def dot_nt(a, b):
    return lax.dot_general(a, b, (((1,), (1,)), ((), ())), preferred_element_type=jnp.float32)


def iota(shape, axis):
    return lax.broadcasted_iota(jnp.int32, shape, axis)


def identity():
    return (iota((DIM, DIM), 0) == iota((DIM, DIM), 1)).astype(jnp.float32).astype(jnp.bfloat16)


def swap_pairs(x):
    return jnp.where(iota(x.shape, 1) % 2 == 0, pltpu.roll(x, DIM - 1, axis=1), pltpu.roll(x, 1, axis=1))


def rows_steps(n_keys, tok, seg, q_v, g_v, tab, kv, kt, vt, part, o_v, dq_v, s_ref):
    core, start, place = seg
    rows = tok * GROUP
    scale = DIM ** -0.5
    c1 = scale * LOG2E
    toks = pl.ds(start, tok)

    def table(k):
        return jnp.broadcast_to(tab[k, core, toks, :][:, None, :], (tok, GROUP, DIM)).reshape(rows, DIM)

    x = q_v[core, toks].astype(jnp.float32).reshape(rows, DIM)
    qr = (x * table(0) + swap_pairs(x) * table(1)).astype(jnp.bfloat16)
    g = g_v[core, toks].astype(jnp.float32).reshape(rows, DIM).astype(jnp.bfloat16)
    blocks = [(a, min(KEY_BLOCK, n_keys - a)) for a in range(0, n_keys, KEY_BLOCK)]
    m8 = None
    for a, n in blocks:
        s = dot_nt(kv[0, a:a + n, :], qr) * c1
        if a + n == n_keys:
            last = s[n - PAIR:, :]
            q_tok = iota(last.shape, 1) // GROUP + place
            last = jnp.where(iota(last.shape, 0) <= q_tok, last, -jnp.inf)
            s = last if n == PAIR else jnp.concatenate([s[:n - PAIR, :], last], axis=0)
        s_ref[a:a + n, :] = s
        f = jnp.max(s.reshape(n // 8, 8, rows), axis=0)
        m8 = f if m8 is None else jnp.maximum(m8, f)
        yield
    row_max = jnp.max(m8, axis=0, keepdims=True)
    l8 = None
    o_t = None
    for a, n in blocks:
        p = jnp.exp2(s_ref[a:a + n, :] - row_max)
        s_ref[a:a + n, :] = p
        f = jnp.sum(p.reshape(n // 8, 8, rows), axis=0)
        l8 = f if l8 is None else l8 + f
        d = dot_nn(vt[:, a:a + n], p.astype(jnp.bfloat16))
        o_t = d if o_t is None else o_t + d
        yield
    inv = 1.0 / jnp.sum(l8, axis=0, keepdims=True)
    out_t = o_t * inv
    o_v[core, toks] = jnp.transpose(out_t).reshape(tok, GROUP, DIM).astype(jnp.bfloat16)
    delta = jnp.sum(dot_nt(identity(), g) * out_t, axis=0, keepdims=True)
    yield
    dq_t = None
    for a, n in blocks:
        p = s_ref[a:a + n, :] * inv
        ds = (p * (dot_nt(kv[1, a:a + n, :], g) - delta)).astype(jnp.bfloat16)
        part[1, a:a + n, :] += dot_nn(p.astype(jnp.bfloat16), g)
        part[0, a:a + n, :] += dot_nn(ds, qr)
        d = dot_nn(kt[:, a:a + n], ds)
        dq_t = d if dq_t is None else dq_t + d
        yield
    dq = jnp.transpose(dq_t) * scale
    dq = dq * table(0) - swap_pairs(dq) * table(1)
    dq_v[core, toks] = dq.reshape(tok, GROUP, DIM).astype(jnp.bfloat16)


def interleave(gens, lag):
    live, waiting, count = [], list(gens), 0
    while live or waiting:
        if waiting and (not live or count >= lag):
            live.append(waiting.pop(0))
            count = 0
        for gen in list(live):
            if next(gen, 'end') == 'end':
                live.remove(gen)
        count += 1


def unit_compute(c, q_v, g_v, tab, kv, o_v, dq_v, part, kt, vt, s_a, s_b, s_e):
    n_late, n_early = (N_PAIRS - c) * PAIR, (c + 1) * PAIR
    eye = identity()
    for a in range(0, n_late, 256):
        n = min(256, n_late - a)
        kt[:, a:a + n] = dot_nt(eye, kv[0, a:a + n, :]).astype(jnp.bfloat16)
        vt[:, a:a + n] = dot_nt(eye, kv[1, a:a + n, :]).astype(jnp.bfloat16)
    part[:, :n_late, :] = jnp.zeros((2, n_late, DIM), jnp.float32)
    refs = (q_v, g_v, tab, kv, kt, vt, part, o_v, dq_v)

    def step(i, carry):
        late = [rows_steps(n_late, 32, (1 - i, PIECE + 32 * k, i * PIECE + 32 * k), *refs, s)
                for k, s in ((0, s_a), (1, s_b))]
        early = rows_steps(n_early, PIECE, (i, 0, i * PIECE), *refs, s_e)
        interleave(late + [early], STEP_LAG)
        return carry

    lax.fori_loop(0, 2, step, 0)


def remote(src, dst, send_sem, recv_sem, device):
    return pltpu.make_async_remote_copy(src_ref=src, dst_ref=dst, send_sem=send_sem, recv_sem=recv_sem,
                                        device_id={'cp': device}, device_id_type=MESH_ID)


def chip_program(c, core, barrier, q_hbm, g_hbm, k_hbm, v_hbm, pos_hbm, freq_hbm, odq_hbm, gkv_hbm, kv_hbm, qs_hbm, gs_hbm,
                 q_v, g_v, o_v, dq_v, kv_v, tab_v, tab_x, pos_v, freq_v, raw_v, ready_v, part, recv, fin_v,
                 perm_in, kt, vt, s_a, s_b, s_e,
                 raw_s, kvl_s, kvx_s, kvx_r, tab_s, tab_r, qx_s, qx_r, gx_s, gx_r, fast_s, ag_s, ag_r, sum_s, sum_r,
                 load_s, out_s, out_r, fin_s, fin_r, credit):
    o_hbm, dq_hbm = odq_hbm.at[0], odq_hbm.at[1]
    n_late = (N_PAIRS - c) * PAIR
    sib = 2 * c + 1 - core
    nbr = {step: 2 * (c ^ step) + core for step in (X_STEP, Y_STEP)}
    mine, other = BATCHES * core, BATCHES * (1 - core)
    early_hops = [(p, step) for p, src, step in EARLY_HOP if src == c]
    first_hops = [(p, step) for p, src, step in FIRST_HOP if src == c and (p, src, step) not in EARLY_HOP]
    relay_hops = [(p, step) for p, src, step in RELAY_HOP if src == c]
    leaves = [(p, step) for p, src, step in SUM_LEAF if src == c]
    relays = [(p, step) for p, src, step in SUM_RELAY if src == c]
    needed = [p for p in range(N_PAIRS - c) if owner(p) != c]
    sib_pieces = (2 * c + 1 - core, 15 - 2 * c - (1 - core))

    def split(u):
        return u // HEADS, u % HEADS

    def pair_rows(p):
        return pl.ds(p * PAIR, PAIR)

    own_pieces = (2 * c + core, 15 - 2 * c - core)

    def raw_in(b, side):
        src, slot = (mine, other)[side] + b, b % 2
        return [pltpu.make_async_copy(k_hbm.at[src], raw_v.at[slot, side, 0], raw_s.at[slot, side, 0]),
                pltpu.make_async_copy(v_hbm.at[src], raw_v.at[slot, side, 1], raw_s.at[slot, side, 1])]

    def start_raw(b):
        for side in (0, 1):
            for copy in raw_in(b, side):
                copy.start()

    def piece_rows(piece):
        return pl.ds(pl.multiple_of(piece * PIECE, PIECE), PIECE)

    def own_out(b, half):
        return pltpu.make_async_copy(ready_v.at[b % 2, 0, :, :, pl.ds(half * PIECE, PIECE), :],
                                     kv_hbm.at[b, :, :, piece_rows(own_pieces[half]), :], kvl_s.at[b, half])

    def kvx(b, half):
        return remote(ready_v.at[b % 2, 1, :, :, pl.ds(half * PIECE, PIECE), :],
                      kv_hbm.at[b, :, :, piece_rows(own_pieces[half]), :], kvx_s.at[b, half], kvx_r.at[b, half], sib)

    def kvx_in(b, half):
        dst = kv_hbm.at[b, :, :, piece_rows(sib_pieces[half]), :]
        return remote(dst, dst, kvx_s.at[b, half], kvx_r.at[b, half], sib)

    def make_table(tab, row):
        pos = pos_v[pl.ds(row, 1), :].astype(jnp.float32)
        angles = jnp.transpose(jnp.broadcast_to(pos, (PAIR, PAIR))) * freq_v[...]
        tab[0] = jnp.cos(angles)
        sine_val = jnp.sin(angles)
        tab[1] = jnp.where(iota(sine_val.shape, 1) % 2 == 0, -sine_val, sine_val)

    def make_ready(b, at_start=False):
        slot, part_rows = b % 2, PAIR // HEADS

        @pl.when(b >= 2)
        def _():
            for half in range(2):
                kvx(b - 2, half).wait_send()
            tab_out(b - 2).wait_send()

        if at_start:
            @pl.when(b == 2)
            def _():
                up_to(lambda u: close_fast(u, True), 0, FAST_UNITS)

            @pl.when(b == 5)
            def _():
                up_to(lambda u: close_fast(u, False), 0, FAST_UNITS)

        for side in (0, 1):
            tab = tab_x.at[slot] if side else tab_v.at[b, :, core]
            for i in (1, 0):
                if i == 0:
                    make_table(tab, (mine, other)[side] + b)
                raw_in(b, side)[i].wait()
                blocks = [dot_nn(perm_in[...], raw_v[slot, side, i, j * PAIR:(j + 1) * PAIR]) for j in range(HEADS)]
                for h in range(HEADS):
                    x = jnp.concatenate([block[h * part_rows:(h + 1) * part_rows] for block in blocks], axis=0)
                    if i == 0:
                        x = x * tab[0] + swap_pairs(x) * tab[1]
                    ready_v[slot, side, h, i] = x.astype(jnp.bfloat16)
                if at_start and side == 0:
                    @pl.when(b == 0)
                    def _(i=i):
                        if i == 1:
                            for copy in small_in():
                                copy.wait()
                            pl.semaphore_wait(barrier, 3)
                        up_to(lambda u: fast_own(u, i), 0, FAST_UNITS)
            if side == 0:
                for half in range(2):
                    own_out(b, half).start()

        @pl.when(b + 2 < BATCHES)
        def _():
            start_raw(b + 2)

    def send_ready(b):
        for half in range(2):
            kvx(b, half).start()
        tab_out(b).start()

    def qx(b):
        return remote(q_hbm.at[other + b], qs_hbm.at[b], qx_s.at[b], qx_r.at[b], sib)

    def gx(b):
        return remote(g_hbm.at[other + b], gs_hbm.at[b], gx_s.at[b], gx_r.at[b], sib)

    def tab_out(b):
        return remote(tab_x.at[b % 2], tab_v.at[b, :, core], tab_s.at[b % 2], tab_r.at[b], sib)

    def tab_arrive(b):
        dst = tab_v.at[b, :, 1 - core]
        return remote(dst, dst, tab_s.at[0], tab_r.at[b], sib)

    def small_in():
        return [pltpu.make_async_copy(pos_hbm, pos_v, load_s.at[5, 0]),
                pltpu.make_async_copy(freq_hbm, freq_v, load_s.at[5, 1])]

    def kv_copy(u, p, slot, step):
        b, h = split(u)
        ref = kv_hbm.at[b, h, :, pair_rows(p), :]
        return remote(ref, ref, ag_s.at[u, slot], ag_r.at[u, p], nbr[step])

    def send_kv(u, hops, base):
        for i, (p, step) in enumerate(hops):
            kv_copy(u, p, base + i, step).start()

    def have_own(b):
        for half in range(2):
            own_out(b, half).wait()
            kvx_in(b, half).wait_recv()

    def half_copy(u, p, slot, step, own):
        b, h = split(u)
        half = 0 if p == c else 1
        dst = kv_hbm.at[b, h, :, piece_rows((own_pieces if own else sib_pieces)[half]), :]
        src = ready_v.at[b % 2, 0, h, :, pl.ds(half * PIECE, PIECE), :] if own else dst
        return remote(src, dst, (fast_s if own else ag_s).at[u, slot], ag_r.at[u, p], nbr[step])

    def fast_hop(u, own):
        for i, (p, step) in enumerate(early_hops + first_hops):
            half_copy(u, p, i, step, own).start()

    def fast_own(u, j):
        b, h = split(u)
        for i, (p, step) in enumerate(early_hops + first_hops):
            half = 0 if p == c else 1
            remote(ready_v.at[b % 2, 0, h, j, pl.ds(half * PIECE, PIECE), :],
                   kv_hbm.at[b, h, j, piece_rows(own_pieces[half]), :],
                   fast_s.at[u, i], ag_r.at[u, p], nbr[step]).start()

    def close_fast(u, own):
        for i, (p, step) in enumerate(early_hops + first_hops):
            half_copy(u, p, i, step, own).wait_send()

    def early_hop(u):
        send_kv(u, early_hops, 0)

    def first_hop(u):
        send_kv(u, first_hops, len(early_hops))

    def relay_hop(u):
        for p, _ in relay_hops:
            kv_copy(u, p, 0, X_STEP).wait_recv()
        send_kv(u, relay_hops, len(early_hops) + len(first_hops))

    def loads(u):
        b, h = split(u)
        slot = u % 2
        late = pl.ds(0, n_late)
        return [
            pltpu.make_async_copy(q_hbm.at[mine + b, :, h], q_v.at[slot, core], load_s.at[0, slot]),
            pltpu.make_async_copy(g_hbm.at[mine + b, :, h], g_v.at[slot, core], load_s.at[1, slot]),
            pltpu.make_async_copy(qs_hbm.at[b, :, h], q_v.at[slot, 1 - core], load_s.at[2, slot]),
            pltpu.make_async_copy(gs_hbm.at[b, :, h], g_v.at[slot, 1 - core], load_s.at[3, slot]),
            pltpu.make_async_copy(kv_hbm.at[b, h, :, late, :], kv_v.at[slot, :, late, :], load_s.at[4, slot]),
        ]

    def start_loads(u):
        @pl.when(u % HEADS == 0)
        def _():
            qx(u // HEADS).wait_recv()
            gx(u // HEADS).wait_recv()
            tab_arrive(u // HEADS).wait_recv()

        for p in needed:
            if p not in [r for r, _ in relay_hops]:
                kv_copy(u, p, 0, X_STEP).wait_recv()
        for copy in loads(u):
            copy.start()

    def out_local(u):
        b, h = split(u)
        slot = u % 2
        return [pltpu.make_async_copy(o_v.at[slot, core], o_hbm.at[mine + b, :, h], out_s.at[0, slot]),
                pltpu.make_async_copy(dq_v.at[slot, core], dq_hbm.at[mine + b, :, h], out_s.at[1, slot])]

    def out_remote(u):
        b, h = split(u)
        slot = u % 2
        return [remote(o_v.at[slot, 1 - core], o_hbm.at[mine + b, :, h], out_s.at[2, slot], out_r.at[0, b], sib),
                remote(dq_v.at[slot, 1 - core], dq_hbm.at[mine + b, :, h], out_s.at[3, slot], out_r.at[1, b], sib)]

    def out_arrive(b):
        return [remote(q_hbm.at[other + b], o_hbm.at[other + b], out_s.at[2, 0], out_r.at[0, b], sib),
                remote(q_hbm.at[other + b], dq_hbm.at[other + b], out_s.at[3, 0], out_r.at[1, b], sib)]

    def wait_outs(u):
        for copy in out_local(u):
            copy.wait()
        for copy in out_remote(u):
            copy.wait_send()

    def sum_copy(u, p, i, step):
        k, slot = inbox(c ^ step).index((p, c)), u % INBOX_RING
        return remote(part.at[u % PART_RING, :, pair_rows(p), :], recv.at[slot, k],
                      sum_s.at[i, u % PART_RING], sum_r.at[slot, k], nbr[step])

    def sum_arrive(u, k):
        dst = recv.at[u % INBOX_RING, k]
        return remote(dst, dst, sum_s.at[0, 0], sum_r.at[u % INBOX_RING, k], nbr[X_STEP])

    def give_credits(u, pairs):
        @pl.when(u + INBOX_RING < UNITS)
        def _():
            for k, (pair, src) in enumerate(inbox(c)):
                if pair in pairs:
                    pl.semaphore_signal(credit.at[outbox(src).index((pair, src ^ c))], inc=1,
                                        device_id={'cp': 2 * src + core}, device_id_type=MESH_ID)

    def take_credits(u, which):
        @pl.when(u >= INBOX_RING)
        def _():
            for i in which:
                pl.semaphore_wait(credit.at[i], 1)

    def messages(p):
        return [k for k, (pair, _) in enumerate(inbox(c)) if pair == p]

    def wait_sums(u):
        for i, (p, step) in enumerate(leaves + relays):
            sum_copy(u, p, i, step).wait_send()

    def send_leaves(u):
        take_credits(u, range(len(leaves)))
        for i, (p, step) in enumerate(leaves):
            sum_copy(u, p, i, step).start()

    def add_relays(u):
        for p, _ in relays:
            for k in messages(p):
                sum_arrive(u, k).wait_recv()
                part[u % PART_RING, :, pair_rows(p), :] += recv[u % INBOX_RING, k]
        give_credits(u, [p for p, _ in relays])

    def send_relays(u):
        take_credits(u, range(len(leaves), len(leaves) + len(relays)))
        for i, (p, step) in enumerate(relays):
            sum_copy(u, p, len(leaves) + i, step).start()

    def fin_local(u):
        b, h = split(u)
        return pltpu.make_async_copy(fin_v.at[u % 2, core], gkv_hbm.at[mine + b, h], fin_s.at[0, u % 2])

    def fin_remote(u):
        b, h = split(u)
        return remote(fin_v.at[u % 2, 1 - core], gkv_hbm.at[mine + b, h], fin_s.at[1, u % 2], fin_r.at[b], sib)

    def fin_arrive(b):
        dst = gkv_hbm.at[other + b]
        return remote(dst, dst, fin_s.at[1, 0], fin_r.at[b], sib)

    def wait_fin(u):
        fin_local(u).wait()
        fin_remote(u).wait_send()

    def finish(u):
        @pl.when(u >= 2)
        def _():
            wait_fin(u - 2)

        b, slot = u // HEADS, u % 2
        for late, p in ((0, c), (1, N_PAIRS - 1 - c)):
            total = part[u % PART_RING, :, pair_rows(p), :]
            for k in messages(p):
                sum_arrive(u, k).wait_recv()
                total = total + recv[u % INBOX_RING, k]
            for i in range(2):
                who = 1 - i if late else i
                toks = slice(late * PIECE, (late + 1) * PIECE)
                dk = total[0, i * PIECE:(i + 1) * PIECE] * (DIM ** -0.5)
                dk = dk * tab_v[b, 0, who, toks] - swap_pairs(dk) * tab_v[b, 1, who, toks]
                fin_v[slot, who, 0, toks] = dk.astype(jnp.bfloat16)
                fin_v[slot, who, 1, toks] = total[1, i * PIECE:(i + 1) * PIECE].astype(jnp.bfloat16)
        give_credits(u, [c, N_PAIRS - 1 - c])

    def send_fin(u):
        fin_local(u).start()
        fin_remote(u).start()

    last_step = UNITS + OWN_LAG

    def close_copies(t):
        batch = t // HEADS

        @pl.when((t >= FAST_UNITS) & (t < UNITS))
        def _():
            for i, (p, step) in enumerate(early_hops + first_hops):
                kv_copy(t, p, i, step).wait_send()

        @pl.when(t < UNITS)
        def _():
            for i, (p, step) in enumerate(relay_hops):
                kv_copy(t, p, len(early_hops + first_hops) + i, step).wait_send()

        @pl.when((t % HEADS == HEADS - 1) & (t < UNITS))
        def _():
            qx(batch).wait_send()
            gx(batch).wait_send()

        @pl.when((t % HEADS == 0) & (t >= 2 * HEADS) & (batch - 2 < BATCHES))
        def _():
            for copy in out_arrive(batch - 2):
                copy.wait_recv()

        @pl.when((t % HEADS == FIN_CLOSE % HEADS) & (t >= FIN_CLOSE))
        def _():
            fin_arrive((t - FIN_CLOSE) // HEADS).wait_recv()

        @pl.when(t >= UNITS)
        def _():
            wait_sums(t - PART_RING)

        @pl.when((t >= UNITS) & (t < UNITS + 2))
        def _():
            wait_outs(t - 2)

        @pl.when(t == 3 * HEADS)
        def _():
            for b in range(BATCHES - 2, BATCHES):
                for half in range(2):
                    kvx(jnp.int32(b), half).wait_send()
                tab_out(jnp.int32(b)).wait_send()

    def exchange_queries(b):
        qx(b).start()
        gx(b).start()

    for copy in small_in():
        copy.start()
    start_raw(jnp.int32(0))
    for device in (sib, nbr[X_STEP], nbr[Y_STEP]):
        pl.semaphore_signal(barrier, inc=1, device_id={'cp': device}, device_id_type=MESH_ID)
    start_raw(jnp.int32(1))
    row, col = iota(perm_in.shape, 0), iota(perm_in.shape, 1)
    part_rows = PAIR // HEADS
    perm_in[...] = (col == (row % part_rows) * HEADS + row // part_rows).astype(jnp.float32).astype(jnp.bfloat16)

    def up_to(op, first, last):
        def one(u, carry):
            op(u)
            return carry

        lax.fori_loop(first, last, one, 0)

    def start_step(j, carry):
        make_ready(j, at_start=True)
        send_ready(j)

        @pl.when(j == 0)
        def _():
            have_own(j)
            up_to(lambda u: fast_hop(u, False), 0, FAST_UNITS)
            exchange_queries(j)

        up_to(relay_hop, jnp.where(j < START_RELAYS, jnp.maximum(j - 1, 0), START_RELAYS),
              jnp.minimum(j + j // 3, START_RELAYS))
        up_to(first_hop, jnp.clip(2 * j, FAST_UNITS, START_UNITS), jnp.clip(2 * j + 2, FAST_UNITS, START_UNITS))

        @pl.when(j >= 1)
        def _():
            have_own(j)

        up_to(early_hop, jnp.maximum(HEADS * j, FAST_UNITS), HEADS * j + HEADS)
        return carry

    lax.fori_loop(0, START_BATCHES, start_step, 0)
    start_loads(jnp.int32(0))

    def tick(t, carry):
        @pl.when((t % 2 == 0) & (t // 2 + START_BATCHES < BATCHES))
        def _():
            make_ready(t // 2 + START_BATCHES)
            send_ready(t // 2 + START_BATCHES)

        @pl.when((t % 2 == 1) & (t // 2 + START_BATCHES < BATCHES))
        def _():
            have_own(t // 2 + START_BATCHES)

        @pl.when((t % HEADS == 0) & (t // HEADS + 1 < BATCHES))
        def _():
            exchange_queries(t // HEADS + 1)

        @pl.when((t >= 1) & (2 * t - 2 + START_EARLY < UNITS))
        def _():
            early_hop(2 * t - 2 + START_EARLY)
            early_hop(2 * t - 1 + START_EARLY)

        @pl.when(t == 0)
        def _():
            for u in range(START_RELAYS, RELAY_LEAD - 1):
                relay_hop(jnp.int32(u))

        @pl.when(t + RELAY_LEAD - 1 < UNITS)
        def _():
            relay_hop(t + RELAY_LEAD - 1)

        @pl.when((t >= 1) & (t - 1 < UNITS))
        def _():
            send_leaves(t - 1)

        @pl.when((t >= 1 + OWN_LAG) & (t - 1 - OWN_LAG < UNITS))
        def _():
            finish(t - 1 - OWN_LAG)

        @pl.when((t >= 1 + SUM_LAG) & (t - 1 - SUM_LAG < UNITS))
        def _():
            add_relays(t - 1 - SUM_LAG)

        @pl.when((t >= 1 + OWN_LAG) & (t - 1 - OWN_LAG < UNITS))
        def _():
            send_fin(t - 1 - OWN_LAG)

        @pl.when((t >= 1 + SUM_LAG) & (t - 1 - SUM_LAG < UNITS))
        def _():
            send_relays(t - 1 - SUM_LAG)

        hop_lead = HOP_LEADS[c]

        @pl.when((t == 0) | ((t + hop_lead > START_UNITS) & (t + hop_lead < UNITS)))
        def _():
            first_hop(jnp.maximum(t + hop_lead, START_UNITS))

        @pl.when(t < UNITS)
        def _():
            for copy in loads(t):
                copy.wait()

            @pl.when(t + 1 < UNITS)
            def _():
                start_loads(t + 1)

            @pl.when(t >= 2)
            def _():
                wait_outs(t - 2)

            @pl.when(t >= PART_RING)
            def _():
                wait_sums(t - PART_RING)

            slot = t % 2
            unit_compute(c, q_v.at[slot], g_v.at[slot], tab_v.at[t // HEADS], kv_v.at[slot], o_v.at[slot],
                         dq_v.at[slot], part.at[t % PART_RING], kt, vt, s_a, s_b, s_e)
            for copy in out_local(t) + out_remote(t):
                copy.start()

        close_copies(t)
        return carry

    lax.fori_loop(0, last_step + 1, tick, 0)

    for u in range(UNITS - 2, UNITS):
        wait_fin(jnp.int32(u))
    for u in range(last_step + 1 - PART_RING, UNITS):
        wait_sums(jnp.int32(u))
    for b in range((last_step - FIN_CLOSE) // HEADS + 1, BATCHES):
        fin_arrive(jnp.int32(b)).wait_recv()


def attend_kernel(*refs):
    me = lax.axis_index('cp')
    chip, core = me // 2, me % 2
    barrier = pltpu.get_barrier_semaphore()
    for c in range(4):
        @pl.when(chip == c)
        def _(c=c):
            chip_program(c, core, barrier, *refs)


def attend(q5, g5, keys, values, positions, freq):
    any_spec = pl.BlockSpec(memory_space=pl.ANY)
    hbm_spec = pl.BlockSpec(memory_space=pltpu.HBM)
    head_shape = pltpu.VMEM((2,) + q5.shape, jnp.bfloat16)
    half_shape = pltpu.HBM((BATCHES,) + q5.shape[1:], jnp.bfloat16)
    head_buf = pltpu.VMEM((2, 2, PAIR, GROUP, DIM), jnp.bfloat16)
    dma = pltpu.SemaphoreType.DMA
    return pl.pallas_call(
        attend_kernel, name='attend',
        in_specs=[any_spec] * 6,
        out_specs=[any_spec] + [hbm_spec] * 4,
        out_shape=[head_shape,
                   pltpu.HBM((2 * BATCHES, HEADS, 2, PAIR, DIM), jnp.bfloat16),
                   pltpu.HBM((BATCHES, HEADS, 2, N_PAIRS * PAIR, DIM), jnp.bfloat16),
                   half_shape, half_shape],
        scratch_shapes=[
            head_buf, head_buf, head_buf, head_buf,
            pltpu.VMEM((2, 2, N_PAIRS * PAIR, DIM), jnp.bfloat16),
            pltpu.VMEM((BATCHES, 2, 2, PAIR, DIM), jnp.float32),
            pltpu.VMEM((2, 2, PAIR, DIM), jnp.float32),
            pltpu.VMEM((2 * BATCHES, PAIR), jnp.int32),
            pltpu.VMEM((1, DIM), jnp.float32),
            pltpu.VMEM((2, 2, 2, HEADS * PAIR, DIM), jnp.bfloat16),
            pltpu.VMEM((2, 2, HEADS, 2, PAIR, DIM), jnp.bfloat16),
            pltpu.VMEM((PART_RING, 2, N_PAIRS * PAIR, DIM), jnp.float32),
            pltpu.VMEM((INBOX_RING, N_INBOX, 2, PAIR, DIM), jnp.float32),
            pltpu.VMEM((2, 2, 2, PAIR, DIM), jnp.bfloat16),
            pltpu.VMEM((PAIR, PAIR), jnp.bfloat16),
            pltpu.VMEM((DIM, N_PAIRS * PAIR), jnp.bfloat16),
            pltpu.VMEM((DIM, N_PAIRS * PAIR), jnp.bfloat16),
            pltpu.VMEM((N_PAIRS * PAIR, 32 * GROUP), jnp.float32),
            pltpu.VMEM((N_PAIRS * PAIR, 32 * GROUP), jnp.float32),
            pltpu.VMEM((4 * PAIR, PIECE * GROUP), jnp.float32),
            dma((2, 2, 2)), dma((BATCHES, 2)), dma((BATCHES, 2)), dma((BATCHES, 2)), dma((2,)), dma((BATCHES,)),
            dma((BATCHES,)), dma((BATCHES,)), dma((BATCHES,)), dma((BATCHES,)),
            dma((FAST_UNITS, 4)), dma((UNITS, 7)), dma((UNITS, 7)), dma((N_OUTBOX, PART_RING)), dma((INBOX_RING, N_INBOX)),
            dma((6, 2)), dma((4, 2)), dma((2, BATCHES)), dma((2, 2)), dma((BATCHES,)),
            pltpu.SemaphoreType.REGULAR((N_OUTBOX,)),
        ],
        compiler_params=pltpu.CompilerParams(
            collective_id=0, has_side_effects=True, vmem_limit_bytes=32512 * 1024),
    )(*(pltpu.with_memory_space_constraint(x, pltpu.HBM) for x in (q5, g5, keys, values, positions, freq)))


def place_kernel(odq, gkv, o_out, dq_out, gk_out, gv_out, in_v, out_v, perm, sems, in_s, out_s):
    n_batch = gkv.shape[0]

    def batch_in(b):
        return pltpu.make_async_copy(gkv.at[b], in_v.at[b], in_s.at[b])

    def batch_out(b):
        return [pltpu.make_async_copy(out_v.at[b, i], dst.at[b], out_s.at[b, i]) for i, dst in enumerate((gk_out, gv_out))]

    def start_in(b, carry):
        batch_in(b).start()
        return carry

    lax.fori_loop(0, n_batch, start_in, 0)
    part = n_batch // 4
    large = [pltpu.make_async_copy(odq.at[k, pl.ds(i * part, part)], dst.at[pl.ds(i * part, part)], sems.at[k, i])
             for i in range(4) for k, dst in enumerate((o_out, dq_out))]
    for copy in large:
        copy.start()
    row, col = iota(perm.shape, 0), iota(perm.shape, 1)
    perm[...] = (row == (col % PAIR) * HEADS + col // PAIR).astype(jnp.float32).astype(jnp.bfloat16)

    def regroup(b, carry):
        batch_in(b).wait()
        for i in range(2):
            rows = in_v[b, :, i].reshape(HEADS * PAIR, DIM)
            out_v[b, i] = dot_nn(perm[...], rows).astype(jnp.bfloat16)
        for copy in batch_out(b):
            copy.start()
        return carry

    lax.fori_loop(0, n_batch, regroup, 0)

    def finish_out(b, carry):
        for copy in batch_out(b):
            copy.wait()
        return carry

    lax.fori_loop(0, n_batch, finish_out, 0)
    for copy in large:
        copy.wait()


def place(odq, gkv):
    any_spec = pl.BlockSpec(memory_space=pl.ANY)
    n_batch = gkv.shape[0]
    head_shape = pltpu.HBM(odq.shape[1:], jnp.bfloat16)
    row_shape = pltpu.HBM((n_batch, HEADS * PAIR, DIM), jnp.bfloat16)
    dma = pltpu.SemaphoreType.DMA
    return pl.pallas_call(
        place_kernel, name='place', in_specs=[any_spec] * 2, out_specs=[any_spec] * 4,
        out_shape=[head_shape, head_shape, row_shape, row_shape],
        scratch_shapes=[pltpu.VMEM(gkv.shape, jnp.bfloat16), pltpu.VMEM((n_batch, 2, HEADS * PAIR, DIM), jnp.bfloat16),
                        pltpu.VMEM((HEADS * PAIR, HEADS * PAIR), jnp.bfloat16),
                        dma((2, 4)), dma((n_batch,)), dma((n_batch, 2))],
        compiler_params=pltpu.CompilerParams(vmem_limit_bytes=12 * 1024 * 1024),
    )(odq, pltpu.with_memory_space_constraint(gkv, pltpu.HBM))


def solution(mesh):
    head_spec = P(None, 'cp', 'tp', None)
    pos_spec = P(None, 'cp')

    def local_step(query, keys, values, positions, grad_out):
        batch, length, n_heads, dim = query.shape
        split_shape = (batch, length, HEADS, GROUP, dim)
        row_shape = (batch, length * HEADS, dim)
        outs = attend(query.reshape(split_shape), grad_out.reshape(split_shape), keys.reshape(row_shape),
                      values.reshape(row_shape), positions, jnp.asarray(lane_freq(dim)))
        return tuple(out.reshape(like.shape) for out, like in zip(place(*outs[:2]), (query, query, keys, values)))

    return jax.shard_map(local_step, mesh=mesh,
                         in_specs=(head_spec, head_spec, head_spec, pos_spec, head_spec),
                         out_specs=(head_spec, head_spec, head_spec, head_spec), check_vma=False)
```
